32 devices in a mesh: dp: 8 (over z, y), tensor: 4 (over x, core).
Axes of the slice: x: 2, y: 2, z: 4, core: 2. Of those that a mesh axis runs over, the one named last changes fastest.
Arguments:
- inputs: bfloat16 [8192, 1152], P(('dp', 'tensor')), may hold values from -6 to 6
- segments: int32 [8192], P('dp'), may hold values from 0 to 16, as said below
- w_query: bfloat16 [1152, 1024], P('dp', 'tensor'), may hold values from -0.1875 to 0.1875
- w_key: bfloat16 [1152, 256], P('dp'), may hold values from -0.1875 to 0.1875
- w_value: bfloat16 [1152, 256], P('dp'), may hold values from -0.1875 to 0.1875
- w_out: bfloat16 [1024, 1152], P('tensor', 'dp'), may hold values from -0.375 to 0.375
- g_in: bfloat16 [1152], P('dp'), may hold values from 0.25 to 1.75
- g_attn: bfloat16 [1152], P('dp'), may hold values from 0.25 to 1.75
- g_query: bfloat16 [256], replicated, may hold values from 0.25 to 1.75
- g_key: bfloat16 [256], replicated, may hold values from 0.25 to 1.75
- w_gate: bfloat16 [1152, 6912], P('dp', 'tensor'), may hold values from -0.1875 to 0.1875
- w_up: bfloat16 [1152, 6912], P('dp', 'tensor'), may hold values from -0.1875 to 0.1875
- w_down: bfloat16 [6912, 1152], P('tensor', 'dp'), may hold values from -0.078125 to 0.078125
- g_pre: bfloat16 [1152], P('dp'), may hold values from 0.25 to 1.75
- g_post: bfloat16 [1152], P('dp'), may hold values from 0.25 to 1.75
- cotangent: bfloat16 [8192, 1152], P(('dp', 'tensor')), may hold values from -6 to 6
Outputs:
- output: bfloat16 [8192, 1152], P(('dp', 'tensor'))
- d_inputs: bfloat16 [8192, 1152], P(('dp', 'tensor'))
- grad_query: float32 [1152, 1024], P('dp', 'tensor')
- grad_key: float32 [1152, 256], P(('dp', 'tensor'))
- grad_value: float32 [1152, 256], P(('dp', 'tensor'))
- grad_out: float32 [1024, 1152], P('tensor', 'dp')
- grad_g_in: float32 [1152], P(('dp', 'tensor'))
- grad_g_attn: float32 [1152], P(('dp', 'tensor'))
- grad_g_query: float32 [256], P(('dp', 'tensor'))
- grad_g_key: float32 [256], P(('dp', 'tensor'))
- grad_gate: float32 [1152, 6912], P('dp', 'tensor')
- grad_up: float32 [1152, 6912], P('dp', 'tensor')
- grad_down: float32 [6912, 1152], P('tensor', 'dp')
- grad_g_pre: float32 [1152], P(('dp', 'tensor'))
- grad_g_post: float32 [1152], P(('dp', 'tensor'))
The draws below stay inside these ranges and needn't reach their ends.
Inputs may be any that keep to these rules, and one draw needn't show every extreme that they name: `segments`: within each block of 1024 rows segment numbers start at 0 and rise by one at the first row of each packed sequence; a sequence starts at every multiple of 512 rows, so none is longer than 512. Every block holds one sequence of exactly 512 rows, and each of its other spans of 512 rows starting at a multiple of 512 holds exactly 16 sequences of uneven lengths.
All inputs are finite; a program needn't handle non-finite values.
Results may differ from the reference program's by a relative error of at most 0.02.
Values may be sent and summed in bfloat16 or wider, within the bound.
A program may use at most 192 MiB of HBM per device.

```python
from functools import partial
import jax
import jax.numpy as jnp
from jax import lax

D = 1152
HQ = 4
HD = 256
FF = 6912
TOK_DEV = 1024
SEGMAX = 512
TOKENS = 8192
HPD = 1
N_DP = 8
N_TENSOR = 4


def draw_segments(key, part):
    tile_count = TOKENS // SEGMAX
    block_count = TOKENS // TOK_DEV
    per_block = TOK_DEV // SEGMAX
    cut_count = min(SEGMAX, 16)
    key_rows, key_whole = jax.random.split(key, 2)
    offsets = jnp.arange(SEGMAX, dtype=jnp.int32)
    raw_scores = jax.random.randint(key_rows, (tile_count, SEGMAX), 0, 1048576) * SEGMAX + offsets[None, :]
    raw_scores = jnp.where(offsets[None, :] == 0, jnp.full_like(raw_scores, -1), raw_scores)
    order = jnp.argsort(raw_scores, axis=1, stable=True)
    ranks = jnp.argsort(order, axis=1, stable=True)
    first = (offsets == 0)[None, :]
    cuts = ranks < cut_count
    whole = jax.random.randint(key_whole, (block_count, 1), 0, per_block)
    tile_place = jnp.broadcast_to(jnp.arange(per_block, dtype=jnp.int32)[None, :], (block_count, per_block))
    single = (tile_place == whole).reshape(tile_count, 1)
    cuts = jnp.where(single, first, cuts)
    flags = cuts.reshape(block_count, TOK_DEV).astype(jnp.int32)
    numbers = jnp.cumsum(flags, axis=1) - 1
    return numbers.reshape(TOKENS).astype(jnp.int32)


def shard_levels(key, dims, shards, smallest, top_value):
    def one(dim, shards_of):
        heights = jax.random.uniform(jax.random.fold_in(jax.random.fold_in(key, 6), dim), (shards_of,), jnp.float32, smallest / len(shards), top_value / len(shards))
        return jnp.repeat(jnp.exp(heights), dims[dim] // shards_of).reshape((-1,) + (1,) * (len(dims) - dim - 1))

    level = one(*shards[0])
    for cut in shards[1:]:
        level = level * one(*cut)
    return level


def normal_values(rng, extent, width, most, cuts=(), held_as=jnp.bfloat16):
    drawn = width * jax.random.normal(rng, extent, jnp.float32)
    if cuts:
        drawn = drawn * shard_levels(rng, extent, cuts, -0.22, 0.18)
    return jnp.clip(drawn, -most, most).astype(held_as)


def setup_inputs(seed: int = 0) -> dict:
    key_list = jax.random.split(jax.random.key(seed), 17)
    inputs = normal_values(key_list[0], (TOKENS, D), 1.0, 6.0, ((0, 32),))
    segments = draw_segments(jax.random.fold_in(key_list[16], 71), 0)
    w_query = normal_values(key_list[2], (D, HQ * HD), D ** -0.5, 0.1875, ((0, 8), (1, 4)))
    w_key = normal_values(key_list[3], (D, HD), D ** -0.5, 0.1875, ((0, 8),))
    w_value = normal_values(key_list[4], (D, HD), D ** -0.5, 0.1875, ((0, 8),))
    w_out = normal_values(key_list[5], (HQ * HD, D), HD ** -0.5, 0.375, ((0, 4), (1, 8)))
    g_in = jnp.clip(1.0 + 0.15 * jax.random.normal(key_list[6], (D,), jnp.float32), 0.25, 1.75).astype(jnp.bfloat16)
    g_attn = jnp.clip(1.0 + 0.15 * jax.random.normal(key_list[7], (D,), jnp.float32), 0.25, 1.75).astype(jnp.bfloat16)
    g_query = jnp.clip(1.0 + 0.15 * jax.random.normal(key_list[8], (HD,), jnp.float32), 0.25, 1.75).astype(jnp.bfloat16)
    g_key = jnp.clip(1.0 + 0.15 * jax.random.normal(key_list[9], (HD,), jnp.float32), 0.25, 1.75).astype(jnp.bfloat16)
    w_gate = normal_values(key_list[10], (D, FF), D ** -0.5, 0.1875, ((0, 8), (1, 4)))
    w_up = normal_values(key_list[11], (D, FF), D ** -0.5, 0.1875, ((0, 8), (1, 4)))
    w_down = normal_values(key_list[12], (FF, D), FF ** -0.5, 0.078125, ((0, 4), (1, 8)))
    g_pre = jnp.clip(1.0 + 0.15 * jax.random.normal(key_list[13], (D,), jnp.float32), 0.25, 1.75).astype(jnp.bfloat16)
    g_post = jnp.clip(1.0 + 0.15 * jax.random.normal(key_list[14], (D,), jnp.float32), 0.25, 1.75).astype(jnp.bfloat16)
    cotangent = normal_values(key_list[15], (TOKENS, D), 1.0, 6.0, ((0, 32),))
    return dict(inputs=inputs, segments=segments, w_query=w_query, w_key=w_key, w_value=w_value, w_out=w_out, g_in=g_in, g_attn=g_attn, g_query=g_query, g_key=g_key, w_gate=w_gate, w_up=w_up, w_down=w_down, g_pre=g_pre, g_post=g_post, cotangent=cotangent)


EPSILON = 1e-06
THETA = 1000000.0
NEG_LARGE = -1e+30

def rms_scale(values, gain_vec):
    inverse = lax.rsqrt(lax.optimization_barrier(jnp.mean(values * values, axis=-1, keepdims=True)) + EPSILON)
    return values * inverse * gain_vec

def gelu_product(gate_proj, up_proj):
    return jax.nn.gelu(gate_proj, approximate=True) * up_proj

def rotary_tables(segments):
    count = segments.shape[0]
    row_index = jnp.arange(count, dtype=jnp.int32)
    previous = jnp.concatenate([jnp.full((1,), -1, jnp.int32), segments[:-1]])
    starts = jnp.where(segments != previous, row_index, jnp.zeros_like(row_index))
    seq_start = lax.cummax(starts, axis=0)
    position = (row_index - seq_start).astype(jnp.float32)
    half_width = HD // 2
    exponent = -2.0 * jnp.arange(half_width, dtype=jnp.float32) / HD
    inverse = jnp.power(jnp.float32(THETA), exponent)
    angles = position[:, None] * inverse[None, :]
    cosine = jnp.concatenate([jnp.cos(angles), jnp.cos(angles)], axis=1)
    sine_tab = jnp.concatenate([jnp.sin(angles), jnp.sin(angles)], axis=1)
    return (cosine, sine_tab)

def prepare(projection, gain_vec, cosine, sine_tab):
    normed = rms_scale(projection, gain_vec)
    half_width = HD // 2
    turned = jnp.concatenate([-normed[..., half_width:], normed[..., :half_width]], axis=-1)
    return normed * cosine[:, None, :] + turned * sine_tab[:, None, :]

def visible(segments):
    tile_count = segments.shape[0] // SEGMAX
    seg_tiles = segments.reshape(tile_count, SEGMAX)
    offsets = jnp.arange(SEGMAX, dtype=jnp.int32)
    same = seg_tiles[:, :, None] == seg_tiles[:, None, :]
    return same & (offsets[:, None] >= offsets[None, :])

def tile_scores(query_ready, key_ready, segments):
    row_count, head_count, head_width = query_ready.shape
    tile_count = row_count // SEGMAX
    query_tiles = query_ready.reshape(tile_count, SEGMAX, head_count, head_width).astype(jnp.float32)
    key_tiles = key_ready.reshape(tile_count, SEGMAX, head_width).astype(jnp.float32)
    scores = jnp.einsum('tqhd,tkd->thqk', query_tiles, key_tiles) * head_width ** (-0.5)
    return jnp.where(visible(segments)[:, None], scores, NEG_LARGE)

def attend(query_ready, key_ready, value_b, segments):
    row_count, head_count, head_width = query_ready.shape
    tile_count = row_count // SEGMAX
    scores = tile_scores(query_ready, key_ready, segments)
    row_max = lax.optimization_barrier(jnp.max(scores, axis=-1, keepdims=True))
    row_total = lax.optimization_barrier(jnp.sum(jnp.exp(scores - row_max), axis=-1, keepdims=True))
    log_total = row_max + jnp.log(row_total)
    probs = jnp.exp(scores - log_total).astype(jnp.bfloat16)
    value_tiles = value_b.reshape(tile_count, SEGMAX, head_width).astype(jnp.float32)
    attended = jnp.einsum('thqk,tkd->tqhd', probs.astype(jnp.float32), value_tiles)
    return (attended.reshape(row_count, head_count * head_width).astype(jnp.bfloat16), log_total)

def attend_back(query_ready, key_ready, value_b, segments, log_total, d_attended):
    row_count, head_count, head_width = query_ready.shape
    tile_count = row_count // SEGMAX
    scores = tile_scores(query_ready, key_ready, segments)
    prob_vals = jnp.exp(scores - log_total)
    prob_b = prob_vals.astype(jnp.bfloat16).astype(jnp.float32)
    grad_tiles = d_attended.reshape(tile_count, SEGMAX, head_count, head_width).astype(jnp.float32)
    value_tiles = value_b.reshape(tile_count, SEGMAX, head_width).astype(jnp.float32)
    query_tiles = query_ready.reshape(tile_count, SEGMAX, head_count, head_width).astype(jnp.float32)
    key_tiles = key_ready.reshape(tile_count, SEGMAX, head_width).astype(jnp.float32)
    d_value = jnp.einsum('thqk,tqhd->tkd', prob_b, grad_tiles).reshape(row_count, head_width)
    d_probs = jnp.einsum('tqhd,tkd->thqk', grad_tiles, value_tiles)
    row_delta = lax.optimization_barrier(jnp.sum(prob_vals * d_probs, axis=-1, keepdims=True))
    d_scores = (prob_vals * (d_probs - row_delta) * head_width ** (-0.5)).astype(jnp.bfloat16).astype(jnp.float32)
    d_query = jnp.einsum('thqk,tkd->tqhd', d_scores, key_tiles).reshape(row_count, head_count, head_width)
    d_key = jnp.einsum('thqk,tqhd->tkd', d_scores, query_tiles).reshape(row_count, head_width)
    return (d_query, d_key, d_value)

def layer_block(inputs, segments, cotangent, weights, gains):
    w_query, w_key, w_value, w_out, w_gate, w_up, w_down = weights
    gain_in, gain_attn, gain_query, gain_key, gain_pre, gain_post = gains
    cosine, sine_tab = rotary_tables(segments)
    row_count = inputs.shape[0]
    group_width = HPD * HD
    inputs_f = inputs.astype(jnp.float32)
    normed_in = rms_scale(inputs_f, gain_in).astype(jnp.bfloat16)
    key_proj = jnp.dot(normed_in, w_key, preferred_element_type=jnp.float32)
    value_b = jnp.dot(normed_in, w_value, preferred_element_type=jnp.float32).astype(jnp.bfloat16)
    key_ready = prepare(key_proj[:, None, :], gain_key, cosine, sine_tab)[:, 0, :].astype(jnp.bfloat16)
    query_list = []
    ready_list = []
    attended_list = []
    total_list = []
    for group_idx in range(N_TENSOR):
        w_group = w_query[:, group_idx * group_width:(group_idx + 1) * group_width]
        query_proj = jnp.dot(normed_in, w_group, preferred_element_type=jnp.float32).reshape(row_count, HPD, HD)
        query_ready = prepare(query_proj, gain_query, cosine, sine_tab).astype(jnp.bfloat16)
        attended_part, log_total = attend(query_ready, key_ready, value_b, segments)
        query_list.append(query_proj)
        ready_list.append(query_ready)
        attended_list.append(attended_part)
        total_list.append(log_total)
    attended = jnp.concatenate(attended_list, axis=1)
    projected = jnp.dot(attended, w_out, preferred_element_type=jnp.float32)
    residual_mid = inputs_f + rms_scale(projected, gain_attn)
    normed_mid = rms_scale(residual_mid, gain_pre).astype(jnp.bfloat16)
    gate_proj = jnp.dot(normed_mid, w_gate, preferred_element_type=jnp.float32)
    up_proj = jnp.dot(normed_mid, w_up, preferred_element_type=jnp.float32)
    hidden = gelu_product(gate_proj, up_proj).astype(jnp.bfloat16)
    feed = jnp.dot(hidden, w_down, preferred_element_type=jnp.float32)
    output = (residual_mid + rms_scale(feed, gain_post)).astype(jnp.bfloat16)
    grad_output = cotangent.astype(jnp.float32)
    d_feed_f, grad_g_post = jax.vjp(rms_scale, feed, gain_post)[1](grad_output)
    d_feed = d_feed_f.astype(jnp.bfloat16)
    grad_down = jnp.dot(hidden.T, d_feed, preferred_element_type=jnp.float32)
    d_hidden = jnp.dot(d_feed, w_down.T, preferred_element_type=jnp.float32)
    d_gate_f, d_up_f = jax.vjp(gelu_product, gate_proj, up_proj)[1](d_hidden)
    d_gate = d_gate_f.astype(jnp.bfloat16)
    d_up = d_up_f.astype(jnp.bfloat16)
    grad_gate = jnp.dot(normed_mid.T, d_gate, preferred_element_type=jnp.float32)
    grad_up = jnp.dot(normed_mid.T, d_up, preferred_element_type=jnp.float32)
    d_normed_mid = jnp.dot(d_gate, w_gate.T, preferred_element_type=jnp.float32) + jnp.dot(d_up, w_up.T, preferred_element_type=jnp.float32)
    d_mid_n, grad_g_pre = jax.vjp(rms_scale, residual_mid, gain_pre)[1](d_normed_mid)
    d_mid = grad_output + d_mid_n
    d_proj_f, grad_g_attn = jax.vjp(rms_scale, projected, gain_attn)[1](d_mid)
    d_proj = d_proj_f.astype(jnp.bfloat16)
    grad_out = jnp.dot(attended.T, d_proj, preferred_element_type=jnp.float32)
    d_attended = jnp.dot(d_proj, w_out.T, preferred_element_type=jnp.float32).astype(jnp.bfloat16)
    rotate_fn = partial(prepare, cosine=cosine, sine_tab=sine_tab)
    pull_key = jax.vjp(rotate_fn, key_proj[:, None, :], gain_key)[1]
    grad_query_parts = []
    grad_key = jnp.zeros((D, HD), jnp.float32)
    grad_value = jnp.zeros((D, HD), jnp.float32)
    grad_g_query = jnp.zeros((HD,), jnp.float32)
    grad_g_key = jnp.zeros((HD,), jnp.float32)
    d_normed_in = jnp.zeros((row_count, D), jnp.float32)
    for group_idx in range(N_TENSOR):
        col_lo = group_idx * group_width
        w_group = w_query[:, col_lo:col_lo + group_width]
        d_query_ready, d_key_ready, d_value_f = attend_back(ready_list[group_idx], key_ready, value_b, segments, total_list[group_idx], d_attended[:, col_lo:col_lo + group_width])
        d_query_f, gain_q_part = jax.vjp(rotate_fn, query_list[group_idx], gain_query)[1](d_query_ready)
        d_key_f, gain_k_part = pull_key(d_key_ready[:, None, :])
        d_query = d_query_f.reshape(row_count, group_width).astype(jnp.bfloat16)
        d_key = d_key_f[:, 0, :].astype(jnp.bfloat16)
        d_value = d_value_f.astype(jnp.bfloat16)
        grad_query_parts.append(jnp.dot(normed_in.T, d_query, preferred_element_type=jnp.float32))
        grad_key = grad_key + jnp.dot(normed_in.T, d_key, preferred_element_type=jnp.float32)
        grad_value = grad_value + jnp.dot(normed_in.T, d_value, preferred_element_type=jnp.float32)
        d_normed_in = d_normed_in + jnp.dot(d_query, w_group.T, preferred_element_type=jnp.float32)
        d_normed_in = d_normed_in + jnp.dot(d_key, w_key.T, preferred_element_type=jnp.float32)
        d_normed_in = d_normed_in + jnp.dot(d_value, w_value.T, preferred_element_type=jnp.float32)
        grad_g_query = grad_g_query + gain_q_part
        grad_g_key = grad_g_key + gain_k_part
    grad_query = jnp.concatenate(grad_query_parts, axis=1)
    d_in_n, grad_g_in = jax.vjp(rms_scale, inputs_f, gain_in)[1](d_normed_in)
    d_inputs = (d_mid + d_in_n).astype(jnp.bfloat16)
    grads = (grad_query, grad_key, grad_value, grad_out, grad_g_in, grad_g_attn, grad_g_query, grad_g_key, grad_gate, grad_up, grad_down, grad_g_pre, grad_g_post)
    return ((output, d_inputs), grads)

def reference(inputs, segments, w_query, w_key, w_value, w_out, g_in, g_attn, g_query, g_key, w_gate, w_up, w_down, g_pre, g_post, cotangent):
    weights = (w_query, w_key, w_value, w_out, w_gate, w_up, w_down)
    gains = (g_in.astype(jnp.float32), g_attn.astype(jnp.float32), g_query.astype(jnp.float32), g_key.astype(jnp.float32), g_pre.astype(jnp.float32), g_post.astype(jnp.float32))
    blocks = (inputs.reshape(N_DP, TOK_DEV, D), segments.reshape(N_DP, TOK_DEV), cotangent.reshape(N_DP, TOK_DEV, D))
    zeros = (jnp.zeros((D, HQ * HD), jnp.float32), jnp.zeros((D, HD), jnp.float32), jnp.zeros((D, HD), jnp.float32), jnp.zeros((HQ * HD, D), jnp.float32), jnp.zeros((D,), jnp.float32), jnp.zeros((D,), jnp.float32), jnp.zeros((HD,), jnp.float32), jnp.zeros((HD,), jnp.float32), jnp.zeros((D, FF), jnp.float32), jnp.zeros((D, FF), jnp.float32), jnp.zeros((FF, D), jnp.float32), jnp.zeros((D,), jnp.float32), jnp.zeros((D,), jnp.float32))

    def one_block(carry, block):
        results, grads = layer_block(block[0], block[1], block[2], weights, gains)
        return (jax.tree.map(jnp.add, carry, grads), results)
    totals, stacked = lax.scan(one_block, zeros, blocks)
    output = stacked[0].reshape(TOKENS, D)
    d_inputs = stacked[1].reshape(TOKENS, D)
    return (output, d_inputs, totals[0], totals[1], totals[2], totals[3], totals[4], totals[5], totals[6], totals[7], totals[8], totals[9], totals[10], totals[11], totals[12])
```

```python
import functools
from functools import partial

import jax
import jax.numpy as jnp
from jax import lax
from jax.experimental import pallas as pl
from jax.experimental.pallas import tpu as pltpu
from jax.sharding import PartitionSpec as P

HD = 256
SEGMAX = 512
MESH = pl.DeviceIdType.MESH
BF = jnp.bfloat16
F32 = jnp.float32


def ring_pos(dev, n):
    return (1 - dev % 2) * (dev // 2) + (dev % 2) * (n - 1 - dev // 2)


def ring_dev(pos, n):
    high = pos // (n // 2)
    return (1 - high) * (2 * pos) + high * (2 * (n - 1 - pos) + 1)


def barrier(peers):
    sem = pltpu.get_barrier_semaphore()
    for peer in peers:
        pl.semaphore_signal(sem, inc=1, device_id=peer, device_id_type=MESH)
    pl.semaphore_wait(sem, len(peers))


def reach(bias, way, n):
    return n // 2 if bias == way else n // 2 - 1


class Ring:
    def __init__(self, n, parts, send_sem, recv_sem, land=None):
        self.n, self.parts, self.land = n, parts, land
        self.send_sem, self.recv_sem = send_sem, recv_sem
        self.me = lax.axis_index("dp")
        self.pos = ring_pos(self.me, n)
        self.peer = [{"dp": self.dev(1)}, {"dp": self.dev(-1)}]

    def dev(self, offset):
        return ring_dev((self.pos + (offset + self.n) % self.n) % self.n, self.n)

    def reach(self, part, way):
        return reach(part % 2, way, self.n)

    def gather(self, part, way, hop, ahead):
        away = hop - 1 if ahead else hop
        block = self.parts[part](self.dev(-away if way == 0 else away))
        return pltpu.make_async_remote_copy(
            block,
            block,
            self.send_sem.at[part, way, hop - 1],
            self.recv_sem.at[part, way, hop - 1],
            device_id=self.peer[way],
            device_id_type=MESH,
        )

    def gather_step(self, part, way, hop):
        if hop > 1:
            self.gather(part, way, hop - 1, False).wait_recv()
        if hop <= self.reach(part, way):
            self.gather(part, way, hop, True).start()

    def gather_sends_done(self, part):
        for way in range(2):
            for hop in range(1, self.reach(part, way) + 1):
                self.gather(part, way, hop, True).wait_send()

    def target(self, part, way, hop):
        away = self.reach(part, way) - hop + 1
        return self.dev(away if way == 0 else -away)

    def slot(self, part, way, hop):
        return self.land(part, hop - 1 + (self.reach(part, 0) if way else 0))

    def reduce(self, part, way, hop):
        return pltpu.make_async_remote_copy(
            self.parts[part](self.target(part, way, hop)),
            self.slot(part, way, hop),
            self.send_sem.at[part, way, hop - 1],
            self.recv_sem.at[part, way, hop - 1],
            device_id=self.peer[way],
            device_id_type=MESH,
        )

    def reduce_step(self, part, way, hop):
        if hop > self.reach(part, way):
            return
        if hop > 1:
            self.reduce(part, way, hop - 1).wait_recv()
            own = self.parts[part](self.target(part, way, hop))
            came = self.slot(part, way, hop - 1)
            own[...] = (own[...].astype(F32) + came[...].astype(F32)).astype(BF)
        self.reduce(part, way, hop).start()

    def reduce_end(self, part):
        total = self.parts[part](self.me)[...].astype(F32)
        for way in range(2):
            last = self.reach(part, way)
            self.reduce(part, way, last).wait_recv()
            total = total + self.slot(part, way, last)[...].astype(F32)
        return total

    def reduce_sends_done(self, part):
        for way in range(2):
            for hop in range(1, self.reach(part, way) + 1):
                self.reduce(part, way, hop).wait_send()


def part_views(attn, ffn, attn_cut, ffn_cut):
    views = []
    for low, high in attn_cut:
        views.append(lambda b, low=low, high=high: attn.at[b, :, pl.ds(low, high - low)])
    for chunk in range(ffn.shape[0]):
        for low, high in ffn_cut:
            views.append(
                lambda b, c=chunk, low=low, high=high: ffn.at[c, b, :, pl.ds(low, high - low)]
            )
    return views


def halves(cols, step=128):
    mid = cols // 2 // step * step
    return ((0, mid), (mid, cols))


def gather_kernel(n, attn_ref, ffn_ref, attn_out, ffn_out, local_sem, send_sem, recv_sem):
    parts = part_views(attn_out, ffn_out, halves(attn_ref.shape[-1]), halves(ffn_ref.shape[-1]))
    ring = Ring(n, parts, send_sem, recv_sem)
    mine = [
        pltpu.make_async_copy(attn_ref, attn_out.at[ring.me], local_sem.at[0]),
        pltpu.make_async_copy(ffn_ref, ffn_out.at[:, ring.me], local_sem.at[1]),
    ]
    for copy in mine:
        copy.start()
    barrier(ring.peer)
    for copy in mine:
        copy.wait()
    width = 4
    for low in range(0, len(parts), width):
        for hop in range(1, n // 2 + 2):
            for part in range(low, min(low + width, len(parts))):
                for way in range(2):
                    if hop <= ring.reach(part, way) + 1:
                        ring.gather_step(part, way, hop)
    for part in range(len(parts)):
        ring.gather_sends_done(part)


def reduce_kernel(n, attn_ref, ffn_ref, attn_out, ffn_out, attn_buf, ffn_buf, attn_land, ffn_land, local_sem, send_sem, recv_sem):
    acut, fcut = halves(attn_ref.shape[-1]), halves(ffn_ref.shape[-1])
    parts = part_views(attn_buf, ffn_buf, acut, fcut)
    landing = part_views(attn_land, ffn_land, acut, fcut)
    ring = Ring(n, parts, send_sem, recv_sem, lambda part, slot: landing[part](slot))
    load = [
        pltpu.make_async_copy(attn_ref, attn_buf, local_sem.at[0]),
        pltpu.make_async_copy(ffn_ref, ffn_buf, local_sem.at[1]),
    ]
    for copy in load:
        copy.start()
    barrier(ring.peer)
    for copy in load:
        copy.wait()
    width = 4
    for low in range(0, len(parts), width):
        for hop in range(1, n // 2 + 1):
            for part in range(low, min(low + width, len(parts))):
                for way in range(2):
                    ring.reduce_step(part, way, hop)
        for part in range(low, min(low + width, len(parts))):
            total = ring.reduce_end(part)
            if part < 2:
                attn_out[:, acut[part][0] : acut[part][1]] = total
            else:
                cut = fcut[part % 2]
                ffn_out[part // 2 - 1, :, cut[0] : cut[1]] = total
    for part in range(len(parts)):
        ring.reduce_sends_done(part)


VMEM_LIMIT = 60 * 2**20


def vmem_specs(count):
    return [pl.BlockSpec(memory_space=pltpu.VMEM)] * count


def any_specs(count):
    return [pl.BlockSpec(memory_space=pl.ANY)] * count


def ring_gather(n, attn, ffn):
    chunks = ffn.shape[0]
    sems = pltpu.SemaphoreType.DMA((2 * (chunks + 1), 2, n // 2))
    return pl.pallas_call(
        partial(gather_kernel, n),
        out_shape=(
            jax.ShapeDtypeStruct((n,) + attn.shape, BF),
            jax.ShapeDtypeStruct((chunks, n) + ffn.shape[1:], BF),
        ),
        in_specs=any_specs(2),
        out_specs=vmem_specs(2),
        scratch_shapes=[pltpu.SemaphoreType.DMA((2,)), sems, sems],
        compiler_params=pltpu.CompilerParams(
            collective_id=0, has_side_effects=True, vmem_limit_bytes=VMEM_LIMIT
        ),
    )(attn, ffn)


def ring_reduce(n, attn, ffn):
    chunks, _, rows, cols = ffn.shape
    sems = pltpu.SemaphoreType.DMA((2 * (chunks + 1), 2, n // 2))
    return pl.pallas_call(
        partial(reduce_kernel, n),
        out_shape=(
            jax.ShapeDtypeStruct(attn.shape[1:], F32),
            jax.ShapeDtypeStruct((chunks, rows, cols), F32),
        ),
        in_specs=any_specs(2),
        out_specs=vmem_specs(2),
        scratch_shapes=[
            pltpu.VMEM(attn.shape, BF),
            pltpu.VMEM(ffn.shape, BF),
            pltpu.VMEM((n - 1,) + attn.shape[1:], BF),
            pltpu.VMEM((chunks, n - 1, rows, cols), BF),
            pltpu.SemaphoreType.DMA((2,)),
            sems,
            sems,
        ],
        compiler_params=pltpu.CompilerParams(
            collective_id=1, has_side_effects=True, vmem_limit_bytes=VMEM_LIMIT
        ),
    )(attn, ffn)


CHUNK = 256


def pack_rows(array, rows):
    return jnp.pad(array, ((0, rows - array.shape[0]), (0, 0)))


def pack_ffn(gate, up, down_t, rows):
    width = gate.shape[1]
    chunks = -(-width // CHUNK)

    def cut(array):
        array = jnp.pad(array, ((0, rows - array.shape[0]), (0, chunks * CHUNK - width)))
        return array.reshape(rows, chunks, CHUNK).transpose(1, 0, 2)

    return jnp.concatenate([cut(gate), cut(up), cut(down_t)], axis=2)


def unpack_ffn(packed, width):
    chunks, rows = packed.shape[:2]
    out = []
    for k in range(3):
        piece = packed[:, :, k * CHUNK : (k + 1) * CHUNK]
        out.append(piece.transpose(1, 0, 2).reshape(rows, chunks * CHUNK)[:, :width])
    return out


def pack_blocks(array, n, rows):
    depth = array.shape[0] // n
    return jnp.pad(array.reshape(n, depth, -1), ((0, 0), (0, rows - depth), (0, 0)))


EPSILON = 1e-06
THETA = 1000000.0
NEG_LARGE = -1e30


def rms_scale(values, gain_vec):
    inverse = lax.rsqrt(jnp.mean(values * values, axis=-1, keepdims=True) + EPSILON)
    return values * inverse * gain_vec


def gelu_product(gate_proj, up_proj):
    return jax.nn.gelu(gate_proj, approximate=True) * up_proj


def rows_product(left, right):
    return lax.dot_general(
        left, right, (((0,), (0,)), ((), ())), preferred_element_type=jnp.float32
    )


def cols_product(left, right):
    return lax.dot_general(
        left, right, (((1,), (1,)), ((), ())), preferred_element_type=jnp.float32
    )


def plain_product(left, right):
    return jnp.dot(left, right, preferred_element_type=jnp.float32)


def rotary_tables(segments):
    count = segments.shape[0]
    row_index = jnp.arange(count, dtype=jnp.int32)
    previous = jnp.concatenate([jnp.full((1,), -1, jnp.int32), segments[:-1]])
    starts = jnp.where(segments != previous, row_index, jnp.zeros_like(row_index))
    seq_start = lax.cummax(starts, axis=0)
    position = (row_index - seq_start).astype(jnp.float32)
    half_width = HD // 2
    exponent = -2.0 * jnp.arange(half_width, dtype=jnp.float32) / HD
    inverse = jnp.power(jnp.float32(THETA), exponent)
    angles = position[:, None] * inverse[None, :]
    cosine = jnp.concatenate([jnp.cos(angles), jnp.cos(angles)], axis=1)
    sine_tab = jnp.concatenate([jnp.sin(angles), jnp.sin(angles)], axis=1)
    return (cosine, sine_tab)


def prepare(projection, gain_vec, cosine, sine_tab):
    normed = rms_scale(projection, gain_vec)
    half_width = HD // 2
    turned = jnp.concatenate([-normed[..., half_width:], normed[..., :half_width]], axis=-1)
    return normed * cosine[:, None, :] + turned * sine_tab[:, None, :]


def visible(segments):
    tile_count = segments.shape[0] // SEGMAX
    seg_tiles = segments.reshape(tile_count, SEGMAX)
    offsets = jnp.arange(SEGMAX, dtype=jnp.int32)
    same = seg_tiles[:, :, None] == seg_tiles[:, None, :]
    return same & (offsets[:, None] >= offsets[None, :])


def tile_scores(query_tiles, key_tiles, segments):
    head_width = key_tiles.shape[-1]
    scores = jnp.einsum(
        "tqhd,tkd->thqk", query_tiles, key_tiles, preferred_element_type=jnp.float32
    ) * head_width ** (-0.5)
    return jnp.where(visible(segments)[:, None], scores, NEG_LARGE)


def attend(query_ready, key_ready, value_b, segments):
    row_count, head_count, head_width = query_ready.shape
    tile_count = row_count // SEGMAX
    query_tiles = query_ready.reshape(tile_count, SEGMAX, head_count, head_width)
    key_tiles = key_ready.reshape(tile_count, SEGMAX, head_width)
    value_tiles = value_b.reshape(tile_count, SEGMAX, head_width)
    scores = tile_scores(query_tiles, key_tiles, segments)
    row_max = jnp.max(scores, axis=-1, keepdims=True)
    row_total = jnp.sum(jnp.exp(scores - row_max), axis=-1, keepdims=True)
    log_total = row_max + jnp.log(row_total)
    probs = jnp.exp(scores - log_total).astype(jnp.bfloat16)
    attended = jnp.einsum("thqk,tkd->tqhd", probs, value_tiles, preferred_element_type=jnp.float32)
    return (attended.reshape(row_count, head_count * head_width).astype(jnp.bfloat16), log_total)


def attend_back(query_ready, key_ready, value_b, segments, log_total, d_attended):
    row_count, head_count, head_width = query_ready.shape
    tile_count = row_count // SEGMAX
    query_tiles = query_ready.reshape(tile_count, SEGMAX, head_count, head_width)
    key_tiles = key_ready.reshape(tile_count, SEGMAX, head_width)
    value_tiles = value_b.reshape(tile_count, SEGMAX, head_width)
    grad_tiles = d_attended.reshape(tile_count, SEGMAX, head_count, head_width)
    scores = tile_scores(query_tiles, key_tiles, segments)
    prob_vals = jnp.exp(scores - log_total)
    prob_b = prob_vals.astype(jnp.bfloat16)
    d_value = jnp.einsum(
        "thqk,tqhd->tkd", prob_b, grad_tiles, preferred_element_type=jnp.float32
    ).reshape(row_count, head_width)
    d_probs = jnp.einsum(
        "tqhd,tkd->thqk", grad_tiles, value_tiles, preferred_element_type=jnp.float32
    )
    row_delta = jnp.sum(prob_vals * d_probs, axis=-1, keepdims=True)
    d_scores = (prob_vals * (d_probs - row_delta) * head_width ** (-0.5)).astype(jnp.bfloat16)
    d_query = jnp.einsum(
        "thqk,tkd->tqhd", d_scores, key_tiles, preferred_element_type=jnp.float32
    ).reshape(row_count, head_count, head_width)
    d_key = jnp.einsum(
        "thqk,tqhd->tkd", d_scores, query_tiles, preferred_element_type=jnp.float32
    ).reshape(row_count, head_width)
    return (d_query, d_key, d_value)


def local(
    inputs,
    segments,
    w_query,
    w_key,
    w_value,
    w_out,
    g_in,
    g_attn,
    g_query,
    g_key,
    w_gate,
    w_up,
    w_down,
    g_pre,
    g_post,
    cotangent,
):
    n = lax.axis_size("dp")
    depth = w_query.shape[0]
    rows = -(-depth // 16) * 16
    width = w_gate.shape[1]
    gains = jnp.stack([g_in, g_attn, g_pre, g_post], axis=1)
    attn_pack = jnp.concatenate(
        [w_query, w_key, w_value, w_out.T, jnp.pad(gains, ((0, 0), (0, 124)))], axis=1
    )
    attn_all, ffn_all = ring_gather(
        n, pack_rows(attn_pack, rows), pack_ffn(w_gate, w_up, w_down.T, rows)
    )
    attn_all = attn_all[:, :depth].reshape(n * depth, -1)
    ffn_all = ffn_all[:, :, :depth].reshape(ffn_all.shape[0], n * depth, -1)
    wq_full, wk_full, wv_full, wo_t = (attn_all[:, k * HD : (k + 1) * HD] for k in range(4))
    wo_full = wo_t.T
    gin_full, gattn_full, gpre_full, gpost_full = (attn_all[:, 4 * HD + k] for k in range(4))
    wg_full, wu_full, wd_t = unpack_ffn(ffn_all, width)
    wd_full = wd_t.T
    gain_in = gin_full.astype(jnp.float32)
    gain_attn = gattn_full.astype(jnp.float32)
    gain_query = g_query.astype(jnp.float32)
    gain_key = g_key.astype(jnp.float32)
    cosine, sine_tab = rotary_tables(segments)
    inputs_f = inputs.astype(jnp.float32)
    normed_shard = rms_scale(inputs_f, gain_in).astype(jnp.bfloat16)
    normed_in = lax.all_gather(normed_shard, "tensor", axis=0, tiled=True)
    row_count = normed_in.shape[0]
    head_count = wq_full.shape[1] // HD
    key_proj = plain_product(normed_in, wk_full)
    value_b = plain_product(normed_in, wv_full).astype(jnp.bfloat16)
    key_ready = prepare(key_proj[:, None, :], gain_key, cosine, sine_tab)[:, 0, :].astype(
        jnp.bfloat16
    )
    query_proj = plain_product(normed_in, wq_full).reshape(row_count, head_count, HD)
    query_ready = prepare(query_proj, gain_query, cosine, sine_tab).astype(jnp.bfloat16)
    attended, log_total = attend(query_ready, key_ready, value_b, segments)
    projected = lax.psum_scatter(
        plain_product(attended, wo_full), "tensor", scatter_dimension=0, tiled=True
    )
    residual_mid = inputs_f + rms_scale(projected, gain_attn)
    gain_pre = gpre_full.astype(jnp.float32)
    gain_post = gpost_full.astype(jnp.float32)
    normed_mid = lax.all_gather(
        rms_scale(residual_mid, gain_pre).astype(jnp.bfloat16), "tensor", axis=0, tiled=True
    )
    gate_proj = plain_product(normed_mid, wg_full)
    up_proj = plain_product(normed_mid, wu_full)
    hidden = gelu_product(gate_proj, up_proj).astype(jnp.bfloat16)
    feed = lax.psum_scatter(
        plain_product(hidden, wd_full), "tensor", scatter_dimension=0, tiled=True
    )
    output = (residual_mid + rms_scale(feed, gain_post)).astype(jnp.bfloat16)
    wg_back, wu_back, wd_back = wg_full, wu_full, wd_full
    grad_output = cotangent.astype(jnp.float32)
    d_feed_f, grad_g_post = jax.vjp(rms_scale, feed, gain_post)[1](grad_output)
    d_feed = lax.all_gather(d_feed_f.astype(jnp.bfloat16), "tensor", axis=0, tiled=True)
    d_hidden = cols_product(d_feed, wd_back)
    d_gate_f, d_up_f = jax.vjp(gelu_product, gate_proj, up_proj)[1](d_hidden)
    d_gate = d_gate_f.astype(jnp.bfloat16)
    d_up = d_up_f.astype(jnp.bfloat16)
    grad_gate = rows_product(normed_mid, d_gate)
    grad_up = rows_product(normed_mid, d_up)
    d_normed_mid = lax.psum_scatter(
        cols_product(d_gate, wg_back) + cols_product(d_up, wu_back),
        "tensor",
        scatter_dimension=0,
        tiled=True,
    )
    d_mid_n, grad_g_pre = jax.vjp(rms_scale, residual_mid, gain_pre)[1](d_normed_mid)
    d_mid = grad_output + d_mid_n
    d_proj_f, grad_g_attn = jax.vjp(rms_scale, projected, gain_attn)[1](d_mid)
    wq_back, wk_back, wv_back, wo_back = wq_full, wk_full, wv_full, wo_full
    d_proj = lax.all_gather(d_proj_f.astype(jnp.bfloat16), "tensor", axis=0, tiled=True)
    d_attended = cols_product(d_proj, wo_back).astype(jnp.bfloat16)
    d_query_ready, d_key_ready, d_value_f = attend_back(
        query_ready, key_ready, value_b, segments, log_total, d_attended
    )
    rotate_fn = partial(prepare, cosine=cosine, sine_tab=sine_tab)
    d_query_f, grad_g_query = jax.vjp(rotate_fn, query_proj, gain_query)[1](d_query_ready)
    d_key_f, grad_g_key = jax.vjp(rotate_fn, key_proj[:, None, :], gain_key)[1](
        d_key_ready[:, None, :]
    )
    d_query = d_query_f.reshape(row_count, head_count * HD).astype(jnp.bfloat16)
    d_key = d_key_f[:, 0, :].astype(jnp.bfloat16)
    d_value = d_value_f.astype(jnp.bfloat16)
    grad_query = rows_product(normed_in, d_query)
    grad_key = rows_product(normed_in, d_key)
    grad_value = rows_product(normed_in, d_value)
    d_normed_terms = (
        cols_product(d_query, wq_back)
        + cols_product(d_key, wk_back)
        + cols_product(d_value, wv_back)
    )
    d_normed_in = lax.psum_scatter(
        d_normed_terms.astype(jnp.bfloat16), "tensor", scatter_dimension=0, tiled=True
    ).astype(jnp.float32)
    d_in_n, grad_g_in = jax.vjp(rms_scale, inputs_f, gain_in)[1](d_normed_in)
    d_inputs = (d_mid + d_in_n).astype(jnp.bfloat16)
    attn_part = jnp.concatenate(
        [grad_query, grad_key, grad_value, rows_product(d_proj, attended)], axis=1
    ).astype(BF)
    attn_part = pack_blocks(attn_part, n, rows)
    ffn_part = pack_ffn(
        grad_gate.astype(BF), grad_up.astype(BF), rows_product(d_feed, hidden).astype(BF), n * depth
    )
    ffn_part = jax.vmap(lambda a: pack_blocks(a, n, rows))(ffn_part)
    attn_sum, ffn_sum = ring_reduce(n, attn_part, ffn_part)
    attn_sum, ffn_sum = attn_sum[:depth], ffn_sum[:, :depth]
    sum_gate, sum_up, sum_down_t = unpack_ffn(ffn_sum, width)
    split_grads = (
        attn_sum[:, :HD],
        attn_sum[:, 3 * HD : 4 * HD].T,
        sum_gate,
        sum_up,
        sum_down_t.T,
    )
    sum_key, sum_value = attn_sum[:, HD : 2 * HD], attn_sum[:, 2 * HD : 3 * HD]
    shared = (
        lax.psum_scatter(sum_key, "tensor", scatter_dimension=0, tiled=True),
        lax.psum_scatter(sum_value, "tensor", scatter_dimension=0, tiled=True),
        lax.psum_scatter(grad_g_in, ("dp", "tensor"), scatter_dimension=0, tiled=True),
        lax.psum_scatter(grad_g_attn, ("dp", "tensor"), scatter_dimension=0, tiled=True),
        lax.psum_scatter(grad_g_pre, ("dp", "tensor"), scatter_dimension=0, tiled=True),
        lax.psum_scatter(grad_g_post, ("dp", "tensor"), scatter_dimension=0, tiled=True),
        lax.psum_scatter(grad_g_query, ("dp", "tensor"), scatter_dimension=0, tiled=True),
        lax.psum_scatter(grad_g_key, ("dp", "tensor"), scatter_dimension=0, tiled=True),
    )
    return (
        output,
        d_inputs,
        split_grads[0],
        shared[0],
        shared[1],
        split_grads[1],
        shared[2],
        shared[3],
        shared[6],
        shared[7],
        split_grads[2],
        split_grads[3],
        split_grads[4],
        shared[4],
        shared[5],
    )


def solution(mesh):
    return jax.shard_map(
        local,
        mesh=mesh,
        in_specs=(
            P(("dp", "tensor"), None),
            P("dp"),
            P("dp", "tensor"),
            P("dp", None),
            P("dp", None),
            P("tensor", "dp"),
            P("dp"),
            P("dp"),
            P(),
            P(),
            P("dp", "tensor"),
            P("dp", "tensor"),
            P("tensor", "dp"),
            P("dp"),
            P("dp"),
            P(("dp", "tensor"), None),
        ),
        out_specs=(
            P(("dp", "tensor"), None),
            P(("dp", "tensor"), None),
            P("dp", "tensor"),
            P(("dp", "tensor"), None),
            P(("dp", "tensor"), None),
            P("tensor", "dp"),
            P(("dp", "tensor")),
            P(("dp", "tensor")),
            P(("dp", "tensor")),
            P(("dp", "tensor")),
            P("dp", "tensor"),
            P("dp", "tensor"),
            P("tensor", "dp"),
            P(("dp", "tensor")),
            P(("dp", "tensor")),
        ),
        check_vma=False,
    )
```

```python
from functools import partial

import jax
import jax.numpy as jnp
from jax import lax
from jax.experimental import pallas as pl
from jax.experimental.pallas import tpu as pltpu
from jax.sharding import PartitionSpec as P

HD = 256
SEGMAX = 512
MESH = pl.DeviceIdType.MESH
BF = jnp.bfloat16
F32 = jnp.float32


def ring_pos(dev, n):
    return (1 - dev % 2) * (dev // 2) + (dev % 2) * (n - 1 - dev // 2)


def ring_dev(pos, n):
    high = pos // (n // 2)
    return (1 - high) * (2 * pos) + high * (2 * (n - 1 - pos) + 1)


def barrier(peers):
    sem = pltpu.get_barrier_semaphore()
    for peer in peers:
        pl.semaphore_signal(sem, inc=1, device_id=peer, device_id_type=MESH)
    pl.semaphore_wait(sem, len(peers))


def reach(bias, way, n):
    return n // 2 if bias == way else n // 2 - 1


class Ring:
    def __init__(self, n, parts, send_sem, recv_sem, land=None):
        self.n, self.parts, self.land = n, parts, land
        self.send_sem, self.recv_sem = send_sem, recv_sem
        self.me = lax.axis_index("dp")
        self.pos = ring_pos(self.me, n)
        self.peer = [{"dp": self.dev(1)}, {"dp": self.dev(-1)}]

    def dev(self, offset):
        return ring_dev((self.pos + (offset + self.n) % self.n) % self.n, self.n)

    def reach(self, part, way):
        return reach(part % 2, way, self.n)

    def gather(self, part, way, hop, ahead):
        away = hop - 1 if ahead else hop
        block = self.parts[part](self.dev(-away if way == 0 else away))
        return pltpu.make_async_remote_copy(
            block,
            block,
            self.send_sem.at[part, way, hop - 1],
            self.recv_sem.at[part, way, hop - 1],
            device_id=self.peer[way],
            device_id_type=MESH,
        )

    def gather_step(self, part, way, hop):
        if hop > 1:
            self.gather(part, way, hop - 1, False).wait_recv()
        if hop <= self.reach(part, way):
            self.gather(part, way, hop, True).start()

    def gather_sends_done(self, part):
        for way in range(2):
            for hop in range(1, self.reach(part, way) + 1):
                self.gather(part, way, hop, True).wait_send()

    def target(self, part, way, hop):
        away = self.reach(part, way) - hop + 1
        return self.dev(away if way == 0 else -away)

    def slot(self, part, way, hop):
        return self.land(part, hop - 1 + (self.reach(part, 0) if way else 0))

    def reduce(self, part, way, hop):
        return pltpu.make_async_remote_copy(
            self.parts[part](self.target(part, way, hop)),
            self.slot(part, way, hop),
            self.send_sem.at[part, way, hop - 1],
            self.recv_sem.at[part, way, hop - 1],
            device_id=self.peer[way],
            device_id_type=MESH,
        )

    def reduce_step(self, part, way, hop):
        if hop > self.reach(part, way):
            return
        if hop > 1:
            self.reduce(part, way, hop - 1).wait_recv()
            own = self.parts[part](self.target(part, way, hop))
            came = self.slot(part, way, hop - 1)
            own[...] = (own[...].astype(F32) + came[...].astype(F32)).astype(BF)
        self.reduce(part, way, hop).start()

    def reduce_end(self, part):
        total = self.parts[part](self.me)[...].astype(F32)
        for way in range(2):
            last = self.reach(part, way)
            self.reduce(part, way, last).wait_recv()
            total = total + self.slot(part, way, last)[...].astype(F32)
        return total

    def reduce_sends_done(self, part):
        for way in range(2):
            for hop in range(1, self.reach(part, way) + 1):
                self.reduce(part, way, hop).wait_send()


def part_views(attn, ffn, attn_cut, ffn_cut):
    views = []
    for low, high in attn_cut:
        views.append(lambda b, low=low, high=high: attn.at[b, :, pl.ds(low, high - low)])
    for chunk in range(ffn.shape[0]):
        for low, high in ffn_cut:
            views.append(
                lambda b, c=chunk, low=low, high=high: ffn.at[c, b, :, pl.ds(low, high - low)]
            )
    return views


def halves(cols, step=128):
    mid = cols // 2 // step * step
    return ((0, mid), (mid, cols))


def gather_kernel(n, attn_ref, ffn_ref, attn_out, ffn_out, local_sem, send_sem, recv_sem):
    parts = part_views(attn_out, ffn_out, halves(attn_ref.shape[-1]), halves(ffn_ref.shape[-1]))
    ring = Ring(n, parts, send_sem, recv_sem)
    mine = [
        pltpu.make_async_copy(attn_ref, attn_out.at[ring.me], local_sem.at[0]),
        pltpu.make_async_copy(ffn_ref, ffn_out.at[:, ring.me], local_sem.at[1]),
    ]
    for copy in mine:
        copy.start()
    barrier(ring.peer)
    for copy in mine:
        copy.wait()
    width = 4
    for low in range(0, len(parts), width):
        for hop in range(1, n // 2 + 2):
            for part in range(low, min(low + width, len(parts))):
                for way in range(2):
                    if hop <= ring.reach(part, way) + 1:
                        ring.gather_step(part, way, hop)
    for part in range(len(parts)):
        ring.gather_sends_done(part)


def reduce_kernel(n, attn_ref, ffn_ref, attn_out, ffn_out, attn_buf, ffn_buf, attn_land, ffn_land, local_sem, send_sem, recv_sem):
    acut, fcut = halves(attn_ref.shape[-1]), halves(ffn_ref.shape[-1])
    parts = part_views(attn_buf, ffn_buf, acut, fcut)
    landing = part_views(attn_land, ffn_land, acut, fcut)
    ring = Ring(n, parts, send_sem, recv_sem, lambda part, slot: landing[part](slot))
    load = [
        pltpu.make_async_copy(attn_ref, attn_buf, local_sem.at[0]),
        pltpu.make_async_copy(ffn_ref, ffn_buf, local_sem.at[1]),
    ]
    for copy in load:
        copy.start()
    barrier(ring.peer)
    for copy in load:
        copy.wait()
    width = 4
    for low in range(0, len(parts), width):
        for hop in range(1, n // 2 + 1):
            for part in range(low, min(low + width, len(parts))):
                for way in range(2):
                    ring.reduce_step(part, way, hop)
        for part in range(low, min(low + width, len(parts))):
            total = ring.reduce_end(part)
            if part < 2:
                attn_out[:, acut[part][0] : acut[part][1]] = total
            else:
                cut = fcut[part % 2]
                ffn_out[part // 2 - 1, :, cut[0] : cut[1]] = total
    for part in range(len(parts)):
        ring.reduce_sends_done(part)


VMEM_LIMIT = 60 * 2**20


def vmem_specs(count):
    return [pl.BlockSpec(memory_space=pltpu.VMEM)] * count


def any_specs(count):
    return [pl.BlockSpec(memory_space=pl.ANY)] * count


def ring_gather(n, attn, ffn):
    chunks = ffn.shape[0]
    sems = pltpu.SemaphoreType.DMA((2 * (chunks + 1), 2, n // 2))
    return pl.pallas_call(
        partial(gather_kernel, n),
        out_shape=(
            jax.ShapeDtypeStruct((n,) + attn.shape, BF),
            jax.ShapeDtypeStruct((chunks, n) + ffn.shape[1:], BF),
        ),
        in_specs=any_specs(2),
        out_specs=vmem_specs(2),
        scratch_shapes=[pltpu.SemaphoreType.DMA((2,)), sems, sems],
        compiler_params=pltpu.CompilerParams(
            collective_id=0, has_side_effects=True, vmem_limit_bytes=VMEM_LIMIT
        ),
    )(attn, ffn)


def ring_reduce(n, attn, ffn):
    chunks, _, rows, cols = ffn.shape
    sems = pltpu.SemaphoreType.DMA((2 * (chunks + 1), 2, n // 2))
    return pl.pallas_call(
        partial(reduce_kernel, n),
        out_shape=(
            jax.ShapeDtypeStruct(attn.shape[1:], F32),
            jax.ShapeDtypeStruct((chunks, rows, cols), F32),
        ),
        in_specs=any_specs(2),
        out_specs=vmem_specs(2),
        scratch_shapes=[
            pltpu.VMEM(attn.shape, BF),
            pltpu.VMEM(ffn.shape, BF),
            pltpu.VMEM((n - 1,) + attn.shape[1:], BF),
            pltpu.VMEM((chunks, n - 1, rows, cols), BF),
            pltpu.SemaphoreType.DMA((2,)),
            sems,
            sems,
        ],
        compiler_params=pltpu.CompilerParams(
            collective_id=1, has_side_effects=True, vmem_limit_bytes=VMEM_LIMIT
        ),
    )(attn, ffn)


CHUNK = 256


def pack_rows(array, rows):
    return jnp.pad(array, ((0, rows - array.shape[0]), (0, 0)))


def pack_ffn(gate, up, down_t, rows):
    width = gate.shape[1]
    chunks = -(-width // CHUNK)

    def cut(array):
        array = jnp.pad(array, ((0, rows - array.shape[0]), (0, chunks * CHUNK - width)))
        return array.reshape(rows, chunks, CHUNK).transpose(1, 0, 2)

    return jnp.concatenate([cut(gate), cut(up), cut(down_t)], axis=2)


def unpack_ffn(packed, width):
    chunks, rows = packed.shape[:2]
    out = []
    for k in range(3):
        piece = packed[:, :, k * CHUNK : (k + 1) * CHUNK]
        out.append(piece.transpose(1, 0, 2).reshape(rows, chunks * CHUNK)[:, :width])
    return out


def pack_blocks(array, n, rows):
    depth = array.shape[0] // n
    return jnp.pad(array.reshape(n, depth, -1), ((0, 0), (0, rows - depth), (0, 0)))


EPSILON = 1e-06
THETA = 1000000.0
NEG_LARGE = -1e30


def rms_scale(values, gain_vec):
    inverse = lax.rsqrt(jnp.mean(values * values, axis=-1, keepdims=True) + EPSILON)
    return values * inverse * gain_vec


def gelu_product(gate_proj, up_proj):
    return jax.nn.gelu(gate_proj, approximate=True) * up_proj


def rows_product(left, right):
    return lax.dot_general(
        left, right, (((0,), (0,)), ((), ())), preferred_element_type=jnp.float32
    )


def cols_product(left, right):
    return lax.dot_general(
        left, right, (((1,), (1,)), ((), ())), preferred_element_type=jnp.float32
    )


def plain_product(left, right):
    return jnp.dot(left, right, preferred_element_type=jnp.float32)


def rotary_tables(segments):
    count = segments.shape[0]
    row_index = jnp.arange(count, dtype=jnp.int32)
    previous = jnp.concatenate([jnp.full((1,), -1, jnp.int32), segments[:-1]])
    starts = jnp.where(segments != previous, row_index, jnp.zeros_like(row_index))
    seq_start = lax.cummax(starts, axis=0)
    position = (row_index - seq_start).astype(jnp.float32)
    half_width = HD // 2
    exponent = -2.0 * jnp.arange(half_width, dtype=jnp.float32) / HD
    inverse = jnp.power(jnp.float32(THETA), exponent)
    angles = position[:, None] * inverse[None, :]
    cosine = jnp.concatenate([jnp.cos(angles), jnp.cos(angles)], axis=1)
    sine_tab = jnp.concatenate([jnp.sin(angles), jnp.sin(angles)], axis=1)
    return (cosine, sine_tab)


def prepare(projection, gain_vec, cosine, sine_tab):
    normed = rms_scale(projection, gain_vec)
    half_width = HD // 2
    turned = jnp.concatenate([-normed[..., half_width:], normed[..., :half_width]], axis=-1)
    return normed * cosine[:, None, :] + turned * sine_tab[:, None, :]


def visible(segments):
    tile_count = segments.shape[0] // SEGMAX
    seg_tiles = segments.reshape(tile_count, SEGMAX)
    offsets = jnp.arange(SEGMAX, dtype=jnp.int32)
    same = seg_tiles[:, :, None] == seg_tiles[:, None, :]
    return same & (offsets[:, None] >= offsets[None, :])


def tile_scores(query_tiles, key_tiles, segments):
    head_width = key_tiles.shape[-1]
    scores = jnp.einsum(
        "tqhd,tkd->thqk", query_tiles, key_tiles, preferred_element_type=jnp.float32
    ) * head_width ** (-0.5)
    return jnp.where(visible(segments)[:, None], scores, NEG_LARGE)


def attend(query_ready, key_ready, value_b, segments):
    row_count, head_count, head_width = query_ready.shape
    tile_count = row_count // SEGMAX
    query_tiles = query_ready.reshape(tile_count, SEGMAX, head_count, head_width)
    key_tiles = key_ready.reshape(tile_count, SEGMAX, head_width)
    value_tiles = value_b.reshape(tile_count, SEGMAX, head_width)
    scores = tile_scores(query_tiles, key_tiles, segments)
    row_max = jnp.max(scores, axis=-1, keepdims=True)
    row_total = jnp.sum(jnp.exp(scores - row_max), axis=-1, keepdims=True)
    log_total = row_max + jnp.log(row_total)
    probs = jnp.exp(scores - log_total).astype(jnp.bfloat16)
    attended = jnp.einsum("thqk,tkd->tqhd", probs, value_tiles, preferred_element_type=jnp.float32)
    return (attended.reshape(row_count, head_count * head_width).astype(jnp.bfloat16), log_total)


def attend_back(query_ready, key_ready, value_b, segments, log_total, d_attended):
    row_count, head_count, head_width = query_ready.shape
    tile_count = row_count // SEGMAX
    query_tiles = query_ready.reshape(tile_count, SEGMAX, head_count, head_width)
    key_tiles = key_ready.reshape(tile_count, SEGMAX, head_width)
    value_tiles = value_b.reshape(tile_count, SEGMAX, head_width)
    grad_tiles = d_attended.reshape(tile_count, SEGMAX, head_count, head_width)
    scores = tile_scores(query_tiles, key_tiles, segments)
    prob_vals = jnp.exp(scores - log_total)
    prob_b = prob_vals.astype(jnp.bfloat16)
    d_value = jnp.einsum(
        "thqk,tqhd->tkd", prob_b, grad_tiles, preferred_element_type=jnp.float32
    ).reshape(row_count, head_width)
    d_probs = jnp.einsum(
        "tqhd,tkd->thqk", grad_tiles, value_tiles, preferred_element_type=jnp.float32
    )
    row_delta = jnp.sum(prob_vals * d_probs, axis=-1, keepdims=True)
    d_scores = (prob_vals * (d_probs - row_delta) * head_width ** (-0.5)).astype(jnp.bfloat16)
    d_query = jnp.einsum(
        "thqk,tkd->tqhd", d_scores, key_tiles, preferred_element_type=jnp.float32
    ).reshape(row_count, head_count, head_width)
    d_key = jnp.einsum(
        "thqk,tqhd->tkd", d_scores, query_tiles, preferred_element_type=jnp.float32
    ).reshape(row_count, head_width)
    return (d_query, d_key, d_value)


def local(
    inputs,
    segments,
    w_query,
    w_key,
    w_value,
    w_out,
    g_in,
    g_attn,
    g_query,
    g_key,
    w_gate,
    w_up,
    w_down,
    g_pre,
    g_post,
    cotangent,
):
    n = lax.axis_size("dp")
    depth = w_query.shape[0]
    rows = -(-depth // 16) * 16
    width = w_gate.shape[1]
    gains = jnp.stack([g_in, g_attn, g_pre, g_post], axis=1)
    attn_pack = jnp.concatenate(
        [w_query, w_key, w_value, w_out.T, jnp.pad(gains, ((0, 0), (0, 124)))], axis=1
    )
    attn_all, ffn_all = ring_gather(
        n, pack_rows(attn_pack, rows), pack_ffn(w_gate, w_up, w_down.T, rows)
    )
    attn_all = attn_all[:, :depth].reshape(n * depth, -1)
    ffn_all = ffn_all[:, :, :depth].reshape(ffn_all.shape[0], n * depth, -1)
    wq_full, wk_full, wv_full, wo_t = (attn_all[:, k * HD : (k + 1) * HD] for k in range(4))
    wo_full = wo_t.T
    gin_full, gattn_full, gpre_full, gpost_full = (attn_all[:, 4 * HD + k] for k in range(4))
    wg_full, wu_full, wd_t = unpack_ffn(ffn_all, width)
    wd_full = wd_t.T
    gain_in = gin_full.astype(jnp.float32)
    gain_attn = gattn_full.astype(jnp.float32)
    gain_query = g_query.astype(jnp.float32)
    gain_key = g_key.astype(jnp.float32)
    cosine, sine_tab = rotary_tables(segments)
    inputs_f = inputs.astype(jnp.float32)
    normed_shard = rms_scale(inputs_f, gain_in).astype(jnp.bfloat16)
    normed_in = lax.all_gather(normed_shard, "tensor", axis=0, tiled=True)
    row_count = normed_in.shape[0]
    head_count = wq_full.shape[1] // HD
    key_proj = plain_product(normed_in, wk_full)
    value_b = plain_product(normed_in, wv_full).astype(jnp.bfloat16)
    key_ready = prepare(key_proj[:, None, :], gain_key, cosine, sine_tab)[:, 0, :].astype(
        jnp.bfloat16
    )
    query_proj = plain_product(normed_in, wq_full).reshape(row_count, head_count, HD)
    query_ready = prepare(query_proj, gain_query, cosine, sine_tab).astype(jnp.bfloat16)
    attended, log_total = attend(query_ready, key_ready, value_b, segments)
    projected = lax.psum_scatter(
        plain_product(attended, wo_full), "tensor", scatter_dimension=0, tiled=True
    )
    residual_mid = inputs_f + rms_scale(projected, gain_attn)
    gain_pre = gpre_full.astype(jnp.float32)
    gain_post = gpost_full.astype(jnp.float32)
    normed_mid = lax.all_gather(
        rms_scale(residual_mid, gain_pre).astype(jnp.bfloat16), "tensor", axis=0, tiled=True
    )
    gate_proj = plain_product(normed_mid, wg_full)
    up_proj = plain_product(normed_mid, wu_full)
    hidden = gelu_product(gate_proj, up_proj).astype(jnp.bfloat16)
    feed = lax.psum_scatter(
        plain_product(hidden, wd_full), "tensor", scatter_dimension=0, tiled=True
    )
    output = (residual_mid + rms_scale(feed, gain_post)).astype(jnp.bfloat16)
    wg_back, wu_back, wd_back = wg_full, wu_full, wd_full
    grad_output = cotangent.astype(jnp.float32)
    d_feed_f, grad_g_post = jax.vjp(rms_scale, feed, gain_post)[1](grad_output)
    d_feed = lax.all_gather(d_feed_f.astype(jnp.bfloat16), "tensor", axis=0, tiled=True)
    d_hidden = cols_product(d_feed, wd_back)
    d_gate_f, d_up_f = jax.vjp(gelu_product, gate_proj, up_proj)[1](d_hidden)
    d_gate = d_gate_f.astype(jnp.bfloat16)
    d_up = d_up_f.astype(jnp.bfloat16)
    grad_gate = rows_product(normed_mid, d_gate)
    grad_up = rows_product(normed_mid, d_up)
    d_normed_mid = lax.psum_scatter(
        cols_product(d_gate, wg_back) + cols_product(d_up, wu_back),
        "tensor",
        scatter_dimension=0,
        tiled=True,
    )
    d_mid_n, grad_g_pre = jax.vjp(rms_scale, residual_mid, gain_pre)[1](d_normed_mid)
    d_mid = grad_output + d_mid_n
    d_proj_f, grad_g_attn = jax.vjp(rms_scale, projected, gain_attn)[1](d_mid)
    wq_back, wk_back, wv_back, wo_back = wq_full, wk_full, wv_full, wo_full
    d_proj = lax.all_gather(d_proj_f.astype(jnp.bfloat16), "tensor", axis=0, tiled=True)
    d_attended = cols_product(d_proj, wo_back).astype(jnp.bfloat16)
    d_query_ready, d_key_ready, d_value_f = attend_back(
        query_ready, key_ready, value_b, segments, log_total, d_attended
    )
    rotate_fn = partial(prepare, cosine=cosine, sine_tab=sine_tab)
    d_query_f, grad_g_query = jax.vjp(rotate_fn, query_proj, gain_query)[1](d_query_ready)
    d_key_f, grad_g_key = jax.vjp(rotate_fn, key_proj[:, None, :], gain_key)[1](
        d_key_ready[:, None, :]
    )
    d_query = d_query_f.reshape(row_count, head_count * HD).astype(jnp.bfloat16)
    d_key = d_key_f[:, 0, :].astype(jnp.bfloat16)
    d_value = d_value_f.astype(jnp.bfloat16)
    grad_query = rows_product(normed_in, d_query)
    grad_key = rows_product(normed_in, d_key)
    grad_value = rows_product(normed_in, d_value)
    d_normed_terms = (
        cols_product(d_query, wq_back)
        + cols_product(d_key, wk_back)
        + cols_product(d_value, wv_back)
    )
    d_normed_in = lax.psum_scatter(
        d_normed_terms.astype(jnp.bfloat16), "tensor", scatter_dimension=0, tiled=True
    ).astype(jnp.float32)
    d_in_n, grad_g_in = jax.vjp(rms_scale, inputs_f, gain_in)[1](d_normed_in)
    d_inputs = (d_mid + d_in_n).astype(jnp.bfloat16)
    attn_part = jnp.concatenate(
        [grad_query, grad_key, grad_value, rows_product(d_proj, attended)], axis=1
    ).astype(BF)
    attn_part = pack_blocks(attn_part, n, rows)
    ffn_part = pack_ffn(
        grad_gate.astype(BF), grad_up.astype(BF), rows_product(d_feed, hidden).astype(BF), n * depth
    )
    ffn_part = jax.vmap(lambda a: pack_blocks(a, n, rows))(ffn_part)
    attn_sum, ffn_sum = ring_reduce(n, attn_part, ffn_part)
    attn_sum, ffn_sum = attn_sum[:depth], ffn_sum[:, :depth]
    sum_gate, sum_up, sum_down_t = unpack_ffn(ffn_sum, width)
    split_grads = (
        attn_sum[:, :HD],
        attn_sum[:, 3 * HD : 4 * HD].T,
        sum_gate,
        sum_up,
        sum_down_t.T,
    )
    sum_key, sum_value = attn_sum[:, HD : 2 * HD], attn_sum[:, 2 * HD : 3 * HD]
    shared = (
        lax.psum_scatter(sum_key, "tensor", scatter_dimension=0, tiled=True),
        lax.psum_scatter(sum_value, "tensor", scatter_dimension=0, tiled=True),
        lax.psum_scatter(grad_g_in, ("dp", "tensor"), scatter_dimension=0, tiled=True),
        lax.psum_scatter(grad_g_attn, ("dp", "tensor"), scatter_dimension=0, tiled=True),
        lax.psum_scatter(grad_g_pre, ("dp", "tensor"), scatter_dimension=0, tiled=True),
        lax.psum_scatter(grad_g_post, ("dp", "tensor"), scatter_dimension=0, tiled=True),
        lax.psum_scatter(grad_g_query, ("dp", "tensor"), scatter_dimension=0, tiled=True),
        lax.psum_scatter(grad_g_key, ("dp", "tensor"), scatter_dimension=0, tiled=True),
    )
    return (
        output,
        d_inputs,
        split_grads[0],
        shared[0],
        shared[1],
        split_grads[1],
        shared[2],
        shared[3],
        shared[6],
        shared[7],
        split_grads[2],
        split_grads[3],
        split_grads[4],
        shared[4],
        shared[5],
    )


SCALE = HD**-0.5
ROOT = 0.7978845608028654
CUBIC = 0.044715


def dot_nn(a, b):
    return jnp.dot(a, b, preferred_element_type=F32)


def dot_nt(a, b):
    return lax.dot_general(a, b, (((1,), (1,)), ((), ())), preferred_element_type=F32)


def dot_tn(a, b):
    return lax.dot_general(a, b, (((0,), (0,)), ((), ())), preferred_element_type=F32)


def inverse_rms(values):
    return lax.rsqrt(jnp.mean(values * values, axis=-1, keepdims=True) + EPSILON)


def rms_back(values, gain_vec, grad):
    inverse = inverse_rms(values)
    unit = values * inverse
    scaled = grad * gain_vec
    back = inverse * (scaled - unit * jnp.mean(scaled * unit, axis=-1, keepdims=True))
    return back, grad * unit


def gelu_parts(gate):
    bent = jnp.tanh(ROOT * (gate + CUBIC * gate * gate * gate))
    return 0.5 * gate * (1.0 + bent), bent


class Quad:
    def __init__(self, part, near, far, gather_sems, reduce_sems):
        self.me = lax.axis_index("tensor")
        self.twin = self.me + 1 - 2 * (self.me % 2)
        self.across = (self.me + 2) % 4
        self.corner = (self.twin + 2) % 4
        self.part, self.near, self.far = part, near, far
        self.gather_sems, self.reduce_sems = gather_sems, reduce_sems

    def copy(self, src, dst, sems, use, k, peer):
        return pltpu.make_async_remote_copy(
            src,
            dst,
            sems[0].at[use, k],
            sems[1].at[use, k],
            device_id={"tensor": peer},
            device_id_type=MESH,
        )

    def gather(self, use, k, buf):
        block = buf.at[self.across if k == 2 else self.me]
        peer = self.across if k == 1 else self.twin
        return self.copy(block, block, self.gather_sems, use, k, peer)

    def gather_start(self, use, buf):
        self.gather(use, 1, buf).start()
        self.gather(use, 0, buf).start()

    def gather_relay(self, use, buf):
        self.gather(use, 1, buf).wait_recv()
        self.gather(use, 2, buf).start()

    def gather_end(self, use, buf):
        self.gather(use, 0, buf).wait_recv()
        self.gather(use, 2, buf).wait_recv()
        for k in range(3):
            self.gather(use, k, buf).wait_send()

    def reduce(self, use, k):
        block = self.part.at[(self.twin, self.corner, self.across)[k]]
        land = self.far if k == 2 else self.near.at[k]
        peer = self.across if k == 2 else self.twin
        return self.copy(block, land, self.reduce_sems, use, k, peer)

    def reduce_start(self, use):
        self.reduce(use, 1).start()
        self.reduce(use, 0).start()

    def reduce_relay(self, use):
        self.reduce(use, 1).wait_recv()
        for low in range(0, self.part.shape[1], 64):
            rows = pl.ds(low, 64)
            total = self.part[self.across, rows].astype(F32) + self.near[1, rows].astype(F32)
            self.part[self.across, rows] = total.astype(BF)
        self.reduce(use, 2).start()

    def reduce_end(self, use):
        self.reduce(use, 0).wait_recv()
        self.reduce(use, 2).wait_recv()
        for k in range(3):
            self.reduce(use, k).wait_send()


class Queue:
    def __init__(self):
        self.steps = []

    def add(self, tag, fn):
        self.steps.append((tag, fn))

    def run(self, count, ready=None):
        while count > 0 and self.steps:
            tag, fn = self.steps[0]
            if ready is not None and tag not in ready:
                return
            self.steps.pop(0)
            fn()
            count -= 1

    def until(self, tag):
        while any(t == tag for t, _ in self.steps):
            self.run(1)


def layer_kernel(
    n,
    x_ref,
    cot_ref,
    seg_row,
    freq_ref,
    gq_ref,
    gk_ref,
    attn_in,
    ffn_in,
    out_ref,
    dx_ref,
    sums_ref,
    ggate_hbm,
    gup_hbm,
    gdown_hbm,
    attn,
    ffn,
    attn_land,
    ffn_land,
    gate_buf,
    up_buf,
    hid_buf,
    acc,
    part,
    near,
    far,
    xa,
    nm,
    df,
    proj_s,
    res_s,
    gains,
    gsum,
    gqk,
    q_proj,
    k_proj,
    qr,
    kr,
    vb,
    att,
    probs,
    cos_s,
    sin_s,
    stage,
    kvg,
    kvg_land,
    local_sem,
    stage_sem,
    ag_send,
    ag_recv,
    rs_send,
    rs_recv,
    qg_send,
    qg_recv,
    qr_send,
    qr_recv,
    kv_send,
    kv_recv,
):
    chunks = ffn.shape[0]
    rows, width = x_ref.shape
    attn_cut = ((0, 2 * HD), (2 * HD, 4 * HD), (4 * HD, attn.shape[-1]))
    ffn_cut = halves(ffn.shape[-1])
    parts = part_views(attn, ffn, attn_cut, ffn_cut)
    landing = part_views(attn_land, ffn_land, attn_cut, ffn_cut)
    first = len(attn_cut)
    ring = Ring(n, parts, ag_send, ag_recv)
    back = Ring(n, parts, rs_send, rs_recv, lambda p, slot: landing[p](slot))
    quad = Quad(part, near, far, (qg_send, qg_recv), (qr_send, qr_recv))
    me = quad.me

    def of_chunk(c):
        return range(first + 2 * c, first + 2 * c + 2)

    def piece(c, k):
        return ffn[c, :, :, k * HD : (k + 1) * HD].reshape(width, HD)

    def attn_cols(low, high):
        return attn[:, :, low:high].reshape(width, high - low)

    mine = [
        pltpu.make_async_copy(attn_in, attn.at[ring.me], local_sem.at[0]),
        pltpu.make_async_copy(ffn_in, ffn.at[:, ring.me], local_sem.at[1]),
        pltpu.make_async_copy(x_ref, xa.at[me], local_sem.at[2]),
    ]
    for copy in mine:
        copy.start()
    barrier(ring.peer + [{"tensor": quad.twin}, {"tensor": quad.across}])
    for copy in mine:
        copy.wait()
    quad.gather_start(0, xa)

    queue = Queue()
    slots = [[] for _ in range(2 * chunks + n + 4)]
    for p in range(first):
        for hop in range(1, n // 2 + 2):
            slots[hop - 1].append((-1, p, hop))
    for c in range(chunks):
        for hop in range(1, n // 2 + 2):
            for p in of_chunk(c):
                slots[2 * (c + 1) + hop - 1].append((c, p, hop))
    for slot in slots:
        for c, p, hop in slot:
            for way in range(2):
                if hop <= ring.reach(p, way) + 1:
                    queue.add(c, partial(ring.gather_step, p, way, hop))

    queue.run(2 * first)
    quarter = SEGMAX // 2

    def seg_column(seg_j, half):
        cut = seg_j[:, half * quarter : (half + 1) * quarter].astype(F32)
        return jnp.transpose(jnp.broadcast_to(cut, (128, quarter)))[:, :1]

    def tables(tile, _):
        seg_j = seg_row[pl.ds(tile, 1), :]
        for half in range(2):
            r = 2 * tile + half
            same = seg_column(seg_j, half) == seg_j.astype(F32)
            j = lax.broadcasted_iota(jnp.int32, (quarter, SEGMAX), 1)
            start = jnp.min(jnp.where(same, j, SEGMAX).astype(F32), axis=1, keepdims=True)
            i = lax.broadcasted_iota(jnp.int32, (quarter, 1), 0).astype(F32) + half * quarter
            angle = (i - start) * freq_ref[...]
            cos_s[r] = jnp.cos(angle)
            sin_s[r] = jnp.sin(angle)
        return 0

    lax.fori_loop(0, N_TILES, tables, 0)
    quad.gather_relay(0, xa)
    queue.until(-1)
    flipped = jnp.transpose(attn_cols(4 * HD, 4 * HD + 128).astype(F32))
    gains[...] = flipped[:8]
    quad.gather_end(0, xa)
    gain_in, gain_attn = gains[0:1, :], gains[1:2, :]
    gain_pre, gain_post = gains[2:3, :], gains[3:4, :]
    gain_q, gain_k = gq_ref[...], gk_ref[...]
    queue.run(4)

    sub = 32
    per = rows // sub

    def normalize(i, _):
        b, at = i // per, pl.ds(pl.multiple_of(i % per * sub, sub), sub)
        values = xa[b, at].astype(F32)
        xa[b, at] = (values * inverse_rms(values) * gains[0:1, :]).astype(BF)
        return 0

    lax.fori_loop(0, 4 * per, normalize, 0)

    def rope(values, gain_vec, r):
        normed = values * inverse_rms(values) * gain_vec
        low, high = normed[:, : HD // 2], normed[:, HD // 2 :]
        cosine, sine = cos_s[r], sin_s[r]
        return jnp.concatenate([low * cosine - high * sine, high * cosine + low * sine], axis=1)

    queue.run(2)

    def project(r, _):
        block = xa[r]
        query = dot_nn(block, attn_cols(HD, 2 * HD))
        q_proj[r] = query.astype(BF)
        qr[r] = rope(query, gq_ref[...], r).astype(BF)
        key = dot_nn(block, attn_cols(2 * HD, 3 * HD))
        k_proj[r] = key.astype(BF)
        kr[r] = rope(key, gk_ref[...], r).astype(BF)
        vb[r] = dot_nn(block, attn_cols(3 * HD, 4 * HD)).astype(BF)
        return 0

    lax.fori_loop(0, 4, project, 0)
    queue.run(4)

    def attend_tile(tile, _):
        two = pl.ds(2 * tile, 2)
        keys = kr[two].reshape(SEGMAX, HD)
        values = vb[two].reshape(SEGMAX, HD)
        seg_j = seg_row[pl.ds(tile, 1), :]
        for half in range(2):
            r = 2 * tile + half
            scores = dot_nt(qr[r], keys) * SCALE
            j = lax.broadcasted_iota(jnp.int32, (quarter, SEGMAX), 1)
            i = lax.broadcasted_iota(jnp.int32, (quarter, SEGMAX), 0) + half * quarter
            seen = (seg_column(seg_j, half) == seg_j.astype(F32)) & (i >= j)
            scores = jnp.where(seen, scores, NEG_LARGE)
            powers = jnp.exp(scores - jnp.max(scores, axis=1, keepdims=True))
            weights = (powers / jnp.sum(powers, axis=1, keepdims=True)).astype(BF)
            probs[r] = weights
            att[r] = dot_nn(weights, values).astype(BF)
        return 0

    lax.fori_loop(0, N_TILES, attend_tile, 0)
    queue.run(2)

    def out_block(r, _):
        acc[r] = dot_nt(att[r], attn_cols(0, HD))
        part[r] = acc[r].astype(BF)
        return 0

    lax.fori_loop(0, 4, out_block, 0)
    quad.reduce_start(0)
    queue.run(2)
    quad.reduce_relay(0)
    queue.run(10)
    quad.reduce_end(0)

    def total(at):
        return acc[me, at] + near[0, at].astype(F32) + far[at].astype(F32)

    def at_rows(i):
        return pl.ds(pl.multiple_of(i * sub, sub), sub)

    def middle(i, _):
        at = at_rows(i)
        projected = total(at)
        proj_s[at] = projected.astype(BF)
        mid = x_ref[at].astype(F32) + projected * inverse_rms(projected) * gains[1:2, :]
        res_s[at] = mid
        nm[me, at] = (mid * inverse_rms(mid) * gains[2:3, :]).astype(BF)
        return 0

    lax.fori_loop(0, per, middle, 0)
    quad.gather_start(1, nm)
    queue.run(6)
    quad.gather_relay(1, nm)
    queue.run(4)
    quad.gather_end(1, nm)

    for c in range(chunks):
        queue.until(c)

        def ffn_block(r, _):
            block = nm[r]
            gate = dot_nn(block, piece(c, 0))
            up = dot_nn(block, piece(c, 1))
            gate_buf[c, r] = gate.astype(BF)
            up_buf[c, r] = up.astype(BF)
            hidden = (gelu_parts(gate)[0] * up).astype(BF)
            grown = dot_nt(hidden, piece(c, 2))
            if c > 0:
                grown = grown + acc[r]
            acc[r] = grown
            if c == chunks - 1:
                part[r] = grown.astype(BF)
            return 0

        lax.fori_loop(0, 4, ffn_block, 0)
    queue.run(10**6)
    quad.reduce_start(1)
    for p in range(len(parts)):
        ring.gather_sends_done(p)
    quad.reduce_relay(1)
    quad.reduce_end(1)
    eight = (8, width)

    def fold(values):
        return jnp.sum(values.reshape(sub // 8, 8, values.shape[-1]), axis=0)

    def after_feed(i, carry):
        at = at_rows(i)
        feed = total(at)
        out_ref[at] = (res_s[at] + feed * inverse_rms(feed) * gains[3:4, :]).astype(BF)
        grad, gain_part = rms_back(feed, gains[3:4, :], cot_ref[at].astype(F32))
        df[me, at] = grad.astype(BF)
        return carry + fold(gain_part)

    gain_sum = lax.fori_loop(0, per, after_feed, jnp.zeros(eight, F32))
    gsum[3:4, :] = jnp.sum(gain_sum, axis=0, keepdims=True)
    quad.gather_start(2, df)
    quad.gather_relay(2, df)
    quad.gather_end(2, df)

    queue = Queue()
    slots = [[] for _ in range(2 * (chunks + 3) + n)]
    for c in range(chunks):
        for hop in range(1, n // 2 + 1):
            for p in of_chunk(c):
                slots[2 * c + hop].append((c, p, hop))
    stage_count = [0]

    def finish(c, p):
        low = ffn_cut[(p - first) % 2]
        k = stage_count[0]
        stage_count[0] += 1
        copies = []
        for which, hbm in ((0, ggate_hbm), (1, gup_hbm), (2, gdown_hbm)):
            left = max(low[0], which * HD)
            right = min(low[1], (which + 1) * HD)
            if left < right:
                copies.append(
                    pltpu.make_async_copy(
                        stage.at[k % 2, :, pl.ds(left - low[0], right - left)],
                        hbm.at[:, pl.ds(c * HD + left - which * HD, right - left)],
                        stage_sem.at[k % 2, len(copies)],
                    )
                )
        if k >= 2:
            for copy in pending[k - 2]:
                copy.wait()
        stage[k % 2] = back.reduce_end(p)
        for copy in copies:
            copy.start()
        pending.append(copies)

    pending = []
    for s, slot in enumerate(slots):
        for c, p, hop in slot:
            for way in range(2):
                if hop <= back.reach(p, way):
                    queue.add(c, partial(back.reduce_step, p, way, hop))
        c = (s - n // 2 - 1) // 2
        if s >= n // 2 + 1 and (s - n // 2 - 1) % 2 == 0 and c < chunks:
            for p in of_chunk(c):
                queue.add(c, partial(finish, c, p))
    ready = set()

    for c in range(chunks):

        def back_block(r, _):
            grad = dot_nn(df[r], piece(c, 2))
            gate, up = gate_buf[c, r].astype(F32), up_buf[c, r].astype(F32)
            act, bent = gelu_parts(gate)
            slope = 0.5 * (1.0 + bent) + 0.5 * gate * (1.0 - bent * bent) * ROOT * (
                1.0 + 3.0 * CUBIC * gate * gate
            )
            d_gate = (grad * up * slope).astype(BF)
            d_up = (grad * act).astype(BF)
            hid_buf[r] = (act * up).astype(BF)
            gate_buf[c, r] = d_gate
            up_buf[c, r] = d_up
            grown = dot_nt(d_gate, piece(c, 0)) + dot_nt(d_up, piece(c, 1))
            if c > 0:
                grown = grown + acc[r]
            acc[r] = grown
            if c == chunks - 1:
                part[r] = grown.astype(BF)
            return 0

        lax.fori_loop(0, 4, back_block, 0)
        queue.run(PACE[0], ready)

        def grad_piece(k, left, right):
            value = dot_tn(left.reshape(4 * rows, width), right.reshape(4 * rows, HD))
            ffn[c, :, :, k * HD : (k + 1) * HD] = value.astype(BF).reshape(n, width // n, HD)

        grad_piece(2, df[...], hid_buf[...])
        if c == chunks - 1:
            quad.reduce_start(2)
        queue.run(PACE[1], ready)
        grad_piece(0, nm[...], gate_buf[c])
        queue.run(PACE[1], ready)
        if c == chunks - 1:
            quad.reduce_relay(2)
        grad_piece(1, nm[...], up_buf[c])
        ready.add(c)
        queue.run(PACE[1], ready)

    queue.run(PACE[2], ready)
    quad.reduce_end(2)

    def after_ffn(i, carry):
        at = at_rows(i)
        grad, pre_part = rms_back(res_s[at], gains[2:3, :], total(at))
        grad = cot_ref[at].astype(F32) + grad
        res_s[at] = grad
        grad, attn_part = rms_back(proj_s[at].astype(F32), gains[1:2, :], grad)
        df[me, at] = grad.astype(BF)
        return carry[0] + fold(pre_part), carry[1] + fold(attn_part)

    zero = jnp.zeros(eight, F32)
    pre_sum, attn_sum = lax.fori_loop(0, per, after_ffn, (zero, zero))
    gsum[2:3, :] = jnp.sum(pre_sum, axis=0, keepdims=True)
    gsum[1:2, :] = jnp.sum(attn_sum, axis=0, keepdims=True)
    quad.gather_start(3, df)
    queue.run(PACE[3], ready)
    quad.gather_relay(3, df)
    queue.run(PACE[4], ready)
    quad.gather_end(3, df)

    d_q, d_k, d_v, datt = (gate_buf.at[k] for k in range(4))
    def back_out(r, _):
        datt[r] = dot_nn(df[r], attn_cols(0, HD)).astype(BF)
        return 0

    lax.fori_loop(0, 4, back_out, 0)
    queue.run(PACE[5], ready)
    gqk[...] = jnp.zeros_like(gqk)

    def unrope(grad, projection, gain_vec, r, row):
        low, high = grad[:, : HD // 2], grad[:, HD // 2 :]
        cosine, sine = cos_s[r], sin_s[r]
        grad = jnp.concatenate([low * cosine + high * sine, high * cosine - low * sine], axis=1)
        grad, gain_part = rms_back(projection, gain_vec, grad)
        gqk[row : row + 1, :] += jnp.sum(gain_part, axis=0, keepdims=True)
        return grad.astype(BF)

    def back_tile(tile, _):
        two = pl.ds(2 * tile, 2)
        keys = kr[two].reshape(SEGMAX, HD)
        values = vb[two].reshape(SEGMAX, HD)
        d_key = jnp.zeros((SEGMAX, HD), F32)
        d_value = jnp.zeros((SEGMAX, HD), F32)
        for half in range(2):
            r = 2 * tile + half
            d_att = datt[r]
            weights = probs[r]
            d_value = d_value + dot_tn(weights, d_att)
            d_probs = dot_nt(d_att, values)
            weights = weights.astype(F32)
            delta = jnp.sum(weights * d_probs, axis=1, keepdims=True)
            d_scores = (weights * (d_probs - delta) * SCALE).astype(BF)
            d_key = d_key + dot_tn(d_scores, qr[r])
            d_query = dot_nn(d_scores, keys)
            d_q[r] = unrope(d_query, q_proj[r].astype(F32), gq_ref[...], r, 4)
        for half in range(2):
            r = 2 * tile + half
            cut = slice(half * quarter, (half + 1) * quarter)
            d_k[r] = unrope(d_key[cut], k_proj[r].astype(F32), gk_ref[...], r, 5)
            d_v[r] = d_value[cut].astype(BF)
        return 0

    lax.fori_loop(0, N_TILES, back_tile, 0)
    queue.run(PACE[5], ready)

    def back_in(r, _):
        grown = dot_nt(d_q[r], attn_cols(HD, 2 * HD))
        grown = grown + dot_nt(d_k[r], attn_cols(2 * HD, 3 * HD))
        grown = grown + dot_nt(d_v[r], attn_cols(3 * HD, 4 * HD))
        acc[r] = grown
        part[r] = grown.astype(BF)
        return 0

    lax.fori_loop(0, 4, back_in, 0)
    quad.reduce_start(3)
    queue.run(PACE[5], ready)

    def attn_grad(low, left, right):
        value = dot_tn(left.reshape(4 * rows, width), right.reshape(4 * rows, HD))
        attn[:, :, low : low + HD] = value.astype(BF).reshape(n, width // n, HD)

    attn_grad(0, df[...], att[...])
    quad.reduce_relay(3)
    for k, grad in enumerate((d_q, d_k, d_v)):
        attn_grad((k + 1) * HD, xa[...], grad[...])
        queue.run(PACE[5], ready)
    queue.run(PACE[6], ready)
    quad.reduce_end(3)

    def after_attn(i, carry):
        at = at_rows(i)
        grad, gain_part = rms_back(x_ref[at].astype(F32), gains[0:1, :], total(at))
        dx_ref[at] = (res_s[at] + grad).astype(BF)
        return carry + fold(gain_part)

    gain_sum = lax.fori_loop(0, per, after_attn, zero)
    gsum[0:1, :] = jnp.sum(gain_sum, axis=0, keepdims=True)
    gsum[4:8, :] = jnp.zeros((4, width), F32)
    tall = jnp.concatenate([gsum[...], jnp.zeros((120, width), F32)], axis=0)
    tall = jnp.transpose(tall).reshape(n, width // n, 128)
    short = jnp.concatenate([gqk[...], jnp.zeros((120, HD), F32)], axis=0)
    short = jnp.transpose(short).reshape(n, HD // n, 128)
    attn[:, :, 4 * HD : 4 * HD + 128] = tall.astype(BF)
    attn[:, : HD // n, 4 * HD : 4 * HD + 128] = (tall[:, : HD // n] + short).astype(BF)

    for hop in range(1, n // 2 + 1):
        for p in range(first):
            for way in range(2):
                if hop <= back.reach(p, way):
                    queue.add(-1, partial(back.reduce_step, p, way, hop))
    queue.run(10**6)
    sums_ref[:, : 2 * HD] = back.reduce_end(0)
    kvg[0, :, : 2 * HD] = back.reduce_end(1).astype(BF)
    kvg[0, :, 2 * HD :] = back.reduce_end(2).astype(BF)
    for k, peer in enumerate((quad.twin, quad.across)):
        copy = pltpu.make_async_remote_copy(
            kvg.at[k],
            kvg_land.at[k],
            kv_send.at[k],
            kv_recv.at[k],
            device_id={"tensor": peer},
            device_id_type=MESH,
        )
        copy.start()
        copy.wait()
        grown = kvg[k].astype(F32) + kvg_land[k].astype(F32)
        if k == 0:
            kvg[1] = grown.astype(BF)
        else:
            sums_ref[:, 2 * HD :] = grown
    for p in range(len(parts)):
        back.reduce_sends_done(p)
    for copies in pending[-2:]:
        for copy in copies:
            copy.wait()


PACE = (1, 1, 2, 6, 4, 1, 4)
N_TILES = 2


def run_layer(n, x, cot, segments, g_query, g_key, attn_pack, ffn_pack):
    rows, width = x.shape
    chunks, depth, cols = ffn_pack.shape
    tokens = segments.shape[0]
    wide = attn_pack.shape[1]
    parts = 3 + 2 * chunks
    exponent = -2.0 * jnp.arange(HD // 2, dtype=F32) / HD
    freq = jnp.power(jnp.float32(THETA), exponent)[None, :]
    vmem, dma = pltpu.VMEM, pltpu.SemaphoreType.DMA
    grown = chunks * HD
    return pl.pallas_call(
        partial(layer_kernel, n),
        out_shape=(
            jax.ShapeDtypeStruct((rows, width), BF),
            jax.ShapeDtypeStruct((rows, width), BF),
            jax.ShapeDtypeStruct((depth, wide), F32),
            jax.ShapeDtypeStruct((depth, grown), F32),
            jax.ShapeDtypeStruct((depth, grown), F32),
            jax.ShapeDtypeStruct((depth, grown), F32),
        ),
        in_specs=vmem_specs(6) + any_specs(2),
        out_specs=vmem_specs(3) + any_specs(3),
        scratch_shapes=[
            vmem((n, depth, wide), BF),
            vmem((chunks, n, depth, cols), BF),
            vmem((n - 1, depth, wide), BF),
            vmem((chunks, n - 1, depth, cols), BF),
            vmem((chunks, 4, rows, HD), BF),
            vmem((chunks, 4, rows, HD), BF),
            vmem((4, rows, HD), BF),
            vmem((4, rows, width), F32),
            vmem((4, rows, width), BF),
            vmem((2, rows, width), BF),
            vmem((rows, width), BF),
            vmem((4, rows, width), BF),
            vmem((4, rows, width), BF),
            vmem((4, rows, width), BF),
            vmem((rows, width), BF),
            vmem((rows, width), F32),
            vmem((8, width), F32),
            vmem((8, width), F32),
            vmem((8, HD), F32),
            vmem((4, rows, HD), BF),
            vmem((4, rows, HD), BF),
            vmem((4, rows, HD), BF),
            vmem((4, rows, HD), BF),
            vmem((4, rows, HD), BF),
            vmem((4, rows, HD), BF),
            vmem((4, rows, SEGMAX), BF),
            vmem((4, rows, HD // 2), F32),
            vmem((4, rows, HD // 2), F32),
            vmem((2, depth, cols // 2), F32),
            vmem((2, depth, wide - 2 * HD), BF),
            vmem((2, depth, wide - 2 * HD), BF),
            dma((3,)),
            dma((2, 2)),
            dma((parts, 2, n // 2)),
            dma((parts, 2, n // 2)),
            dma((parts, 2, n // 2)),
            dma((parts, 2, n // 2)),
            dma((4, 3)),
            dma((4, 3)),
            dma((4, 3)),
            dma((4, 3)),
            dma((2,)),
            dma((2,)),
        ],
        compiler_params=pltpu.CompilerParams(
            collective_id=2, has_side_effects=True, vmem_limit_bytes=67043328
        ),
    )(
        x,
        cot,
        segments.reshape(N_TILES, SEGMAX),
        freq,
        g_query.astype(F32)[None, :],
        g_key.astype(F32)[None, :],
        attn_pack,
        ffn_pack,
    )


def fused_local(
    inputs, segments, w_query, w_key, w_value, w_out, g_in, g_attn, g_query, g_key,
    w_gate, w_up, w_down, g_pre, g_post, cotangent,
):
    n = lax.axis_size("dp")
    depth = w_query.shape[0]
    width = w_gate.shape[1]
    gains = jnp.stack([g_in, g_attn, g_pre, g_post], axis=1)
    attn_pack = jnp.concatenate(
        [w_out.T, w_query, w_key, w_value, jnp.pad(gains, ((0, 0), (0, 124)))], axis=1
    )
    ffn_pack = pack_ffn(w_gate, w_up, w_down.T, depth)
    output, d_inputs, sums, g_gate, g_up, g_down = run_layer(
        n, inputs, cotangent, segments, g_query, g_key, attn_pack, ffn_pack
    )
    spot = lax.axis_index("tensor")
    part = depth // 4
    mine = lax.dynamic_slice_in_dim(sums[:, 2 * HD :], spot * part, part, 0)
    small = HD // n // 4
    few = lax.dynamic_slice_in_dim(sums[:, 4 * HD :], spot * small, small, 0)
    return (
        output,
        d_inputs,
        sums[:, HD : 2 * HD],
        mine[:, :HD],
        mine[:, HD : 2 * HD],
        sums[:, :HD].T,
        mine[:, 2 * HD],
        mine[:, 2 * HD + 1],
        few[:, 4],
        few[:, 5],
        g_gate[:, :width],
        g_up[:, :width],
        g_down[:, :width].T,
        mine[:, 2 * HD + 2],
        mine[:, 2 * HD + 3],
    )


def fits(mesh, depth, tokens, rows):
    return depth % 16 == 0 and mesh.shape["tensor"] == 4 and tokens == 2 * SEGMAX


def layer(mesh):
    def body(*args):
        inputs, segments, w_query = args[0], args[1], args[2]
        if fits(mesh, w_query.shape[0], segments.shape[0], inputs.shape[0]):
            return fused_local(*args)
        return local(*args)

    return body


def solution(mesh):
    return jax.shard_map(
        layer(mesh),
        mesh=mesh,
        in_specs=(
            P(("dp", "tensor"), None),
            P("dp"),
            P("dp", "tensor"),
            P("dp", None),
            P("dp", None),
            P("tensor", "dp"),
            P("dp"),
            P("dp"),
            P(),
            P(),
            P("dp", "tensor"),
            P("dp", "tensor"),
            P("tensor", "dp"),
            P("dp"),
            P("dp"),
            P(("dp", "tensor"), None),
        ),
        out_specs=(
            P(("dp", "tensor"), None),
            P(("dp", "tensor"), None),
            P("dp", "tensor"),
            P(("dp", "tensor"), None),
            P(("dp", "tensor"), None),
            P("tensor", "dp"),
            P(("dp", "tensor")),
            P(("dp", "tensor")),
            P(("dp", "tensor")),
            P(("dp", "tensor")),
            P("dp", "tensor"),
            P("dp", "tensor"),
            P("tensor", "dp"),
            P(("dp", "tensor")),
            P(("dp", "tensor")),
        ),
        check_vma=False,
    )
```

```python
from functools import partial

import jax
import jax.numpy as jnp
from jax import lax
from jax.experimental import pallas as pl
from jax.experimental.pallas import tpu as pltpu
from jax.sharding import PartitionSpec as P

HD = 256
SEGMAX = 512
MESH = pl.DeviceIdType.MESH
BF = jnp.bfloat16
F32 = jnp.float32


def ring_pos(dev, n):
    return (1 - dev % 2) * (dev // 2) + (dev % 2) * (n - 1 - dev // 2)


def ring_dev(pos, n):
    high = pos // (n // 2)
    return (1 - high) * (2 * pos) + high * (2 * (n - 1 - pos) + 1)


def barrier(peers):
    sem = pltpu.get_barrier_semaphore()
    for peer in peers:
        pl.semaphore_signal(sem, inc=1, device_id=peer, device_id_type=MESH)
    pl.semaphore_wait(sem, len(peers))


def reach(bias, way, n):
    return n // 2 if bias == way else n // 2 - 1


class Ring:
    def __init__(self, n, parts, send_sem, recv_sem, land=None):
        self.n, self.parts, self.land = n, parts, land
        self.send_sem, self.recv_sem = send_sem, recv_sem
        self.me = lax.axis_index("dp")
        self.pos = ring_pos(self.me, n)
        self.peer = [{"dp": self.dev(1)}, {"dp": self.dev(-1)}]

    def dev(self, offset):
        return ring_dev((self.pos + (offset + self.n) % self.n) % self.n, self.n)

    def reach(self, part, way):
        return reach(part % 2, way, self.n)

    def gather(self, part, way, hop, ahead):
        away = hop - 1 if ahead else hop
        block = self.parts[part](self.dev(-away if way == 0 else away))
        return pltpu.make_async_remote_copy(
            block,
            block,
            self.send_sem.at[part, way, hop - 1],
            self.recv_sem.at[part, way, hop - 1],
            device_id=self.peer[way],
            device_id_type=MESH,
        )

    def gather_step(self, part, way, hop):
        if hop > 1:
            self.gather(part, way, hop - 1, False).wait_recv()
        if hop <= self.reach(part, way):
            self.gather(part, way, hop, True).start()

    def gather_sends_done(self, part):
        for way in range(2):
            for hop in range(1, self.reach(part, way) + 1):
                self.gather(part, way, hop, True).wait_send()

    def target(self, part, way, hop):
        away = self.reach(part, way) - hop + 1
        return self.dev(away if way == 0 else -away)

    def slot(self, part, way, hop):
        return self.land(part, hop - 1 + (self.reach(part, 0) if way else 0))

    def reduce(self, part, way, hop):
        return pltpu.make_async_remote_copy(
            self.parts[part](self.target(part, way, hop)),
            self.slot(part, way, hop),
            self.send_sem.at[part, way, hop - 1],
            self.recv_sem.at[part, way, hop - 1],
            device_id=self.peer[way],
            device_id_type=MESH,
        )

    def reduce_step(self, part, way, hop):
        if hop > self.reach(part, way):
            return
        if hop > 1:
            self.reduce(part, way, hop - 1).wait_recv()
            own = self.parts[part](self.target(part, way, hop))
            came = self.slot(part, way, hop - 1)
            own[...] = (own[...].astype(F32) + came[...].astype(F32)).astype(BF)
        self.reduce(part, way, hop).start()

    def reduce_end(self, part):
        total = self.parts[part](self.me)[...].astype(F32)
        for way in range(2):
            last = self.reach(part, way)
            self.reduce(part, way, last).wait_recv()
            total = total + self.slot(part, way, last)[...].astype(F32)
        return total

    def reduce_sends_done(self, part):
        for way in range(2):
            for hop in range(1, self.reach(part, way) + 1):
                self.reduce(part, way, hop).wait_send()


def part_views(attn, ffn, attn_cut, ffn_cut):
    views = []
    for low, high in attn_cut:
        views.append(lambda b, low=low, high=high: attn.at[b, :, pl.ds(low, high - low)])
    for chunk in range(ffn.shape[0]):
        for low, high in ffn_cut:
            views.append(
                lambda b, c=chunk, low=low, high=high: ffn.at[c, b, :, pl.ds(low, high - low)]
            )
    return views


def halves(cols, step=128):
    mid = cols // 2 // step * step
    return ((0, mid), (mid, cols))


def gather_kernel(n, attn_ref, ffn_ref, attn_out, ffn_out, local_sem, send_sem, recv_sem):
    parts = part_views(attn_out, ffn_out, halves(attn_ref.shape[-1]), halves(ffn_ref.shape[-1]))
    ring = Ring(n, parts, send_sem, recv_sem)
    mine = [
        pltpu.make_async_copy(attn_ref, attn_out.at[ring.me], local_sem.at[0]),
        pltpu.make_async_copy(ffn_ref, ffn_out.at[:, ring.me], local_sem.at[1]),
    ]
    for copy in mine:
        copy.start()
    barrier(ring.peer)
    for copy in mine:
        copy.wait()
    width = 4
    for low in range(0, len(parts), width):
        for hop in range(1, n // 2 + 2):
            for part in range(low, min(low + width, len(parts))):
                for way in range(2):
                    if hop <= ring.reach(part, way) + 1:
                        ring.gather_step(part, way, hop)
    for part in range(len(parts)):
        ring.gather_sends_done(part)


def reduce_kernel(n, attn_ref, ffn_ref, attn_out, ffn_out, attn_buf, ffn_buf, attn_land, ffn_land, local_sem, send_sem, recv_sem):
    acut, fcut = halves(attn_ref.shape[-1]), halves(ffn_ref.shape[-1])
    parts = part_views(attn_buf, ffn_buf, acut, fcut)
    landing = part_views(attn_land, ffn_land, acut, fcut)
    ring = Ring(n, parts, send_sem, recv_sem, lambda part, slot: landing[part](slot))
    load = [
        pltpu.make_async_copy(attn_ref, attn_buf, local_sem.at[0]),
        pltpu.make_async_copy(ffn_ref, ffn_buf, local_sem.at[1]),
    ]
    for copy in load:
        copy.start()
    barrier(ring.peer)
    for copy in load:
        copy.wait()
    width = 4
    for low in range(0, len(parts), width):
        for hop in range(1, n // 2 + 1):
            for part in range(low, min(low + width, len(parts))):
                for way in range(2):
                    ring.reduce_step(part, way, hop)
        for part in range(low, min(low + width, len(parts))):
            total = ring.reduce_end(part)
            if part < 2:
                attn_out[:, acut[part][0] : acut[part][1]] = total
            else:
                cut = fcut[part % 2]
                ffn_out[part // 2 - 1, :, cut[0] : cut[1]] = total
    for part in range(len(parts)):
        ring.reduce_sends_done(part)


VMEM_LIMIT = 60 * 2**20


def vmem_specs(count):
    return [pl.BlockSpec(memory_space=pltpu.VMEM)] * count


def any_specs(count):
    return [pl.BlockSpec(memory_space=pl.ANY)] * count


def ring_gather(n, attn, ffn):
    chunks = ffn.shape[0]
    sems = pltpu.SemaphoreType.DMA((2 * (chunks + 1), 2, n // 2))
    return pl.pallas_call(
        partial(gather_kernel, n),
        out_shape=(
            jax.ShapeDtypeStruct((n,) + attn.shape, BF),
            jax.ShapeDtypeStruct((chunks, n) + ffn.shape[1:], BF),
        ),
        in_specs=any_specs(2),
        out_specs=vmem_specs(2),
        scratch_shapes=[pltpu.SemaphoreType.DMA((2,)), sems, sems],
        compiler_params=pltpu.CompilerParams(
            collective_id=0, has_side_effects=True, vmem_limit_bytes=VMEM_LIMIT
        ),
    )(attn, ffn)


def ring_reduce(n, attn, ffn):
    chunks, _, rows, cols = ffn.shape
    sems = pltpu.SemaphoreType.DMA((2 * (chunks + 1), 2, n // 2))
    return pl.pallas_call(
        partial(reduce_kernel, n),
        out_shape=(
            jax.ShapeDtypeStruct(attn.shape[1:], F32),
            jax.ShapeDtypeStruct((chunks, rows, cols), F32),
        ),
        in_specs=any_specs(2),
        out_specs=vmem_specs(2),
        scratch_shapes=[
            pltpu.VMEM(attn.shape, BF),
            pltpu.VMEM(ffn.shape, BF),
            pltpu.VMEM((n - 1,) + attn.shape[1:], BF),
            pltpu.VMEM((chunks, n - 1, rows, cols), BF),
            pltpu.SemaphoreType.DMA((2,)),
            sems,
            sems,
        ],
        compiler_params=pltpu.CompilerParams(
            collective_id=1, has_side_effects=True, vmem_limit_bytes=VMEM_LIMIT
        ),
    )(attn, ffn)


CHUNK = 256


def pack_rows(array, rows):
    return jnp.pad(array, ((0, rows - array.shape[0]), (0, 0)))


def pack_ffn(gate, up, down_t, rows):
    width = gate.shape[1]
    chunks = -(-width // CHUNK)

    def cut(array):
        array = jnp.pad(array, ((0, rows - array.shape[0]), (0, chunks * CHUNK - width)))
        return array.reshape(rows, chunks, CHUNK).transpose(1, 0, 2)

    return jnp.concatenate([cut(gate), cut(up), cut(down_t)], axis=2)


def unpack_ffn(packed, width):
    chunks, rows = packed.shape[:2]
    out = []
    for k in range(3):
        piece = packed[:, :, k * CHUNK : (k + 1) * CHUNK]
        out.append(piece.transpose(1, 0, 2).reshape(rows, chunks * CHUNK)[:, :width])
    return out


def pack_blocks(array, n, rows):
    depth = array.shape[0] // n
    return jnp.pad(array.reshape(n, depth, -1), ((0, 0), (0, rows - depth), (0, 0)))


EPSILON = 1e-06
THETA = 1000000.0
NEG_LARGE = -1e30


def rms_scale(values, gain_vec):
    inverse = lax.rsqrt(jnp.mean(values * values, axis=-1, keepdims=True) + EPSILON)
    return values * inverse * gain_vec


def gelu_product(gate_proj, up_proj):
    return jax.nn.gelu(gate_proj, approximate=True) * up_proj


def rows_product(left, right):
    return lax.dot_general(
        left, right, (((0,), (0,)), ((), ())), preferred_element_type=jnp.float32
    )


def cols_product(left, right):
    return lax.dot_general(
        left, right, (((1,), (1,)), ((), ())), preferred_element_type=jnp.float32
    )


def plain_product(left, right):
    return jnp.dot(left, right, preferred_element_type=jnp.float32)


def rotary_tables(segments):
    count = segments.shape[0]
    row_index = jnp.arange(count, dtype=jnp.int32)
    previous = jnp.concatenate([jnp.full((1,), -1, jnp.int32), segments[:-1]])
    starts = jnp.where(segments != previous, row_index, jnp.zeros_like(row_index))
    seq_start = lax.cummax(starts, axis=0)
    position = (row_index - seq_start).astype(jnp.float32)
    half_width = HD // 2
    exponent = -2.0 * jnp.arange(half_width, dtype=jnp.float32) / HD
    inverse = jnp.power(jnp.float32(THETA), exponent)
    angles = position[:, None] * inverse[None, :]
    cosine = jnp.concatenate([jnp.cos(angles), jnp.cos(angles)], axis=1)
    sine_tab = jnp.concatenate([jnp.sin(angles), jnp.sin(angles)], axis=1)
    return (cosine, sine_tab)


def prepare(projection, gain_vec, cosine, sine_tab):
    normed = rms_scale(projection, gain_vec)
    half_width = HD // 2
    turned = jnp.concatenate([-normed[..., half_width:], normed[..., :half_width]], axis=-1)
    return normed * cosine[:, None, :] + turned * sine_tab[:, None, :]


def visible(segments):
    tile_count = segments.shape[0] // SEGMAX
    seg_tiles = segments.reshape(tile_count, SEGMAX)
    offsets = jnp.arange(SEGMAX, dtype=jnp.int32)
    same = seg_tiles[:, :, None] == seg_tiles[:, None, :]
    return same & (offsets[:, None] >= offsets[None, :])


def tile_scores(query_tiles, key_tiles, segments):
    head_width = key_tiles.shape[-1]
    scores = jnp.einsum(
        "tqhd,tkd->thqk", query_tiles, key_tiles, preferred_element_type=jnp.float32
    ) * head_width ** (-0.5)
    return jnp.where(visible(segments)[:, None], scores, NEG_LARGE)


def attend(query_ready, key_ready, value_b, segments):
    row_count, head_count, head_width = query_ready.shape
    tile_count = row_count // SEGMAX
    query_tiles = query_ready.reshape(tile_count, SEGMAX, head_count, head_width)
    key_tiles = key_ready.reshape(tile_count, SEGMAX, head_width)
    value_tiles = value_b.reshape(tile_count, SEGMAX, head_width)
    scores = tile_scores(query_tiles, key_tiles, segments)
    row_max = jnp.max(scores, axis=-1, keepdims=True)
    row_total = jnp.sum(jnp.exp(scores - row_max), axis=-1, keepdims=True)
    log_total = row_max + jnp.log(row_total)
    probs = jnp.exp(scores - log_total).astype(jnp.bfloat16)
    attended = jnp.einsum("thqk,tkd->tqhd", probs, value_tiles, preferred_element_type=jnp.float32)
    return (attended.reshape(row_count, head_count * head_width).astype(jnp.bfloat16), log_total)


def attend_back(query_ready, key_ready, value_b, segments, log_total, d_attended):
    row_count, head_count, head_width = query_ready.shape
    tile_count = row_count // SEGMAX
    query_tiles = query_ready.reshape(tile_count, SEGMAX, head_count, head_width)
    key_tiles = key_ready.reshape(tile_count, SEGMAX, head_width)
    value_tiles = value_b.reshape(tile_count, SEGMAX, head_width)
    grad_tiles = d_attended.reshape(tile_count, SEGMAX, head_count, head_width)
    scores = tile_scores(query_tiles, key_tiles, segments)
    prob_vals = jnp.exp(scores - log_total)
    prob_b = prob_vals.astype(jnp.bfloat16)
    d_value = jnp.einsum(
        "thqk,tqhd->tkd", prob_b, grad_tiles, preferred_element_type=jnp.float32
    ).reshape(row_count, head_width)
    d_probs = jnp.einsum(
        "tqhd,tkd->thqk", grad_tiles, value_tiles, preferred_element_type=jnp.float32
    )
    row_delta = jnp.sum(prob_vals * d_probs, axis=-1, keepdims=True)
    d_scores = (prob_vals * (d_probs - row_delta) * head_width ** (-0.5)).astype(jnp.bfloat16)
    d_query = jnp.einsum(
        "thqk,tkd->tqhd", d_scores, key_tiles, preferred_element_type=jnp.float32
    ).reshape(row_count, head_count, head_width)
    d_key = jnp.einsum(
        "thqk,tqhd->tkd", d_scores, query_tiles, preferred_element_type=jnp.float32
    ).reshape(row_count, head_width)
    return (d_query, d_key, d_value)


def local(
    inputs,
    segments,
    w_query,
    w_key,
    w_value,
    w_out,
    g_in,
    g_attn,
    g_query,
    g_key,
    w_gate,
    w_up,
    w_down,
    g_pre,
    g_post,
    cotangent,
):
    n = lax.axis_size("dp")
    depth = w_query.shape[0]
    rows = -(-depth // 16) * 16
    width = w_gate.shape[1]
    gains = jnp.stack([g_in, g_attn, g_pre, g_post], axis=1)
    attn_pack = jnp.concatenate(
        [w_query, w_key, w_value, w_out.T, jnp.pad(gains, ((0, 0), (0, 124)))], axis=1
    )
    attn_all, ffn_all = ring_gather(
        n, pack_rows(attn_pack, rows), pack_ffn(w_gate, w_up, w_down.T, rows)
    )
    attn_all = attn_all[:, :depth].reshape(n * depth, -1)
    ffn_all = ffn_all[:, :, :depth].reshape(ffn_all.shape[0], n * depth, -1)
    wq_full, wk_full, wv_full, wo_t = (attn_all[:, k * HD : (k + 1) * HD] for k in range(4))
    wo_full = wo_t.T
    gin_full, gattn_full, gpre_full, gpost_full = (attn_all[:, 4 * HD + k] for k in range(4))
    wg_full, wu_full, wd_t = unpack_ffn(ffn_all, width)
    wd_full = wd_t.T
    gain_in = gin_full.astype(jnp.float32)
    gain_attn = gattn_full.astype(jnp.float32)
    gain_query = g_query.astype(jnp.float32)
    gain_key = g_key.astype(jnp.float32)
    cosine, sine_tab = rotary_tables(segments)
    inputs_f = inputs.astype(jnp.float32)
    normed_shard = rms_scale(inputs_f, gain_in).astype(jnp.bfloat16)
    normed_in = lax.all_gather(normed_shard, "tensor", axis=0, tiled=True)
    row_count = normed_in.shape[0]
    head_count = wq_full.shape[1] // HD
    key_proj = plain_product(normed_in, wk_full)
    value_b = plain_product(normed_in, wv_full).astype(jnp.bfloat16)
    key_ready = prepare(key_proj[:, None, :], gain_key, cosine, sine_tab)[:, 0, :].astype(
        jnp.bfloat16
    )
    query_proj = plain_product(normed_in, wq_full).reshape(row_count, head_count, HD)
    query_ready = prepare(query_proj, gain_query, cosine, sine_tab).astype(jnp.bfloat16)
    attended, log_total = attend(query_ready, key_ready, value_b, segments)
    projected = lax.psum_scatter(
        plain_product(attended, wo_full), "tensor", scatter_dimension=0, tiled=True
    )
    residual_mid = inputs_f + rms_scale(projected, gain_attn)
    gain_pre = gpre_full.astype(jnp.float32)
    gain_post = gpost_full.astype(jnp.float32)
    normed_mid = lax.all_gather(
        rms_scale(residual_mid, gain_pre).astype(jnp.bfloat16), "tensor", axis=0, tiled=True
    )
    gate_proj = plain_product(normed_mid, wg_full)
    up_proj = plain_product(normed_mid, wu_full)
    hidden = gelu_product(gate_proj, up_proj).astype(jnp.bfloat16)
    feed = lax.psum_scatter(
        plain_product(hidden, wd_full), "tensor", scatter_dimension=0, tiled=True
    )
    output = (residual_mid + rms_scale(feed, gain_post)).astype(jnp.bfloat16)
    wg_back, wu_back, wd_back = wg_full, wu_full, wd_full
    grad_output = cotangent.astype(jnp.float32)
    d_feed_f, grad_g_post = jax.vjp(rms_scale, feed, gain_post)[1](grad_output)
    d_feed = lax.all_gather(d_feed_f.astype(jnp.bfloat16), "tensor", axis=0, tiled=True)
    d_hidden = cols_product(d_feed, wd_back)
    d_gate_f, d_up_f = jax.vjp(gelu_product, gate_proj, up_proj)[1](d_hidden)
    d_gate = d_gate_f.astype(jnp.bfloat16)
    d_up = d_up_f.astype(jnp.bfloat16)
    grad_gate = rows_product(normed_mid, d_gate)
    grad_up = rows_product(normed_mid, d_up)
    d_normed_mid = lax.psum_scatter(
        cols_product(d_gate, wg_back) + cols_product(d_up, wu_back),
        "tensor",
        scatter_dimension=0,
        tiled=True,
    )
    d_mid_n, grad_g_pre = jax.vjp(rms_scale, residual_mid, gain_pre)[1](d_normed_mid)
    d_mid = grad_output + d_mid_n
    d_proj_f, grad_g_attn = jax.vjp(rms_scale, projected, gain_attn)[1](d_mid)
    wq_back, wk_back, wv_back, wo_back = wq_full, wk_full, wv_full, wo_full
    d_proj = lax.all_gather(d_proj_f.astype(jnp.bfloat16), "tensor", axis=0, tiled=True)
    d_attended = cols_product(d_proj, wo_back).astype(jnp.bfloat16)
    d_query_ready, d_key_ready, d_value_f = attend_back(
        query_ready, key_ready, value_b, segments, log_total, d_attended
    )
    rotate_fn = partial(prepare, cosine=cosine, sine_tab=sine_tab)
    d_query_f, grad_g_query = jax.vjp(rotate_fn, query_proj, gain_query)[1](d_query_ready)
    d_key_f, grad_g_key = jax.vjp(rotate_fn, key_proj[:, None, :], gain_key)[1](
        d_key_ready[:, None, :]
    )
    d_query = d_query_f.reshape(row_count, head_count * HD).astype(jnp.bfloat16)
    d_key = d_key_f[:, 0, :].astype(jnp.bfloat16)
    d_value = d_value_f.astype(jnp.bfloat16)
    grad_query = rows_product(normed_in, d_query)
    grad_key = rows_product(normed_in, d_key)
    grad_value = rows_product(normed_in, d_value)
    d_normed_terms = (
        cols_product(d_query, wq_back)
        + cols_product(d_key, wk_back)
        + cols_product(d_value, wv_back)
    )
    d_normed_in = lax.psum_scatter(
        d_normed_terms.astype(jnp.bfloat16), "tensor", scatter_dimension=0, tiled=True
    ).astype(jnp.float32)
    d_in_n, grad_g_in = jax.vjp(rms_scale, inputs_f, gain_in)[1](d_normed_in)
    d_inputs = (d_mid + d_in_n).astype(jnp.bfloat16)
    attn_part = jnp.concatenate(
        [grad_query, grad_key, grad_value, rows_product(d_proj, attended)], axis=1
    ).astype(BF)
    attn_part = pack_blocks(attn_part, n, rows)
    ffn_part = pack_ffn(
        grad_gate.astype(BF), grad_up.astype(BF), rows_product(d_feed, hidden).astype(BF), n * depth
    )
    ffn_part = jax.vmap(lambda a: pack_blocks(a, n, rows))(ffn_part)
    attn_sum, ffn_sum = ring_reduce(n, attn_part, ffn_part)
    attn_sum, ffn_sum = attn_sum[:depth], ffn_sum[:, :depth]
    sum_gate, sum_up, sum_down_t = unpack_ffn(ffn_sum, width)
    split_grads = (
        attn_sum[:, :HD],
        attn_sum[:, 3 * HD : 4 * HD].T,
        sum_gate,
        sum_up,
        sum_down_t.T,
    )
    sum_key, sum_value = attn_sum[:, HD : 2 * HD], attn_sum[:, 2 * HD : 3 * HD]
    shared = (
        lax.psum_scatter(sum_key, "tensor", scatter_dimension=0, tiled=True),
        lax.psum_scatter(sum_value, "tensor", scatter_dimension=0, tiled=True),
        lax.psum_scatter(grad_g_in, ("dp", "tensor"), scatter_dimension=0, tiled=True),
        lax.psum_scatter(grad_g_attn, ("dp", "tensor"), scatter_dimension=0, tiled=True),
        lax.psum_scatter(grad_g_pre, ("dp", "tensor"), scatter_dimension=0, tiled=True),
        lax.psum_scatter(grad_g_post, ("dp", "tensor"), scatter_dimension=0, tiled=True),
        lax.psum_scatter(grad_g_query, ("dp", "tensor"), scatter_dimension=0, tiled=True),
        lax.psum_scatter(grad_g_key, ("dp", "tensor"), scatter_dimension=0, tiled=True),
    )
    return (
        output,
        d_inputs,
        split_grads[0],
        shared[0],
        shared[1],
        split_grads[1],
        shared[2],
        shared[3],
        shared[6],
        shared[7],
        split_grads[2],
        split_grads[3],
        split_grads[4],
        shared[4],
        shared[5],
    )


SCALE = HD**-0.5
ROOT = 0.7978845608028654
CUBIC = 0.044715


def dot_nn(a, b):
    return jnp.dot(a, b, preferred_element_type=F32)


def dot_nt(a, b):
    return lax.dot_general(a, b, (((1,), (1,)), ((), ())), preferred_element_type=F32)


def dot_tn(a, b):
    return lax.dot_general(a, b, (((0,), (0,)), ((), ())), preferred_element_type=F32)


def inverse_rms(values):
    return lax.rsqrt(jnp.mean(values * values, axis=-1, keepdims=True) + EPSILON)


def rms_back(values, gain_vec, grad):
    inverse = inverse_rms(values)
    unit = values * inverse
    scaled = grad * gain_vec
    back = inverse * (scaled - unit * jnp.mean(scaled * unit, axis=-1, keepdims=True))
    return back, grad * unit


def gelu_parts(gate):
    bent = jnp.tanh(ROOT * (gate + CUBIC * gate * gate * gate))
    return 0.5 * gate * (1.0 + bent), bent


class Quad:
    def __init__(self, part, near, far, gather_sems, reduce_sems):
        self.me = lax.axis_index("tensor")
        self.twin = self.me + 1 - 2 * (self.me % 2)
        self.across = (self.me + 2) % 4
        self.corner = (self.twin + 2) % 4
        self.part, self.near, self.far = part, near, far
        self.gather_sems, self.reduce_sems = gather_sems, reduce_sems

    def copy(self, src, dst, sems, use, k, peer):
        return pltpu.make_async_remote_copy(
            src,
            dst,
            sems[0].at[use, k],
            sems[1].at[use, k],
            device_id={"tensor": peer},
            device_id_type=MESH,
        )

    def gather(self, use, k, buf):
        block = buf.at[self.across if k == 2 else self.me]
        peer = self.across if k == 1 else self.twin
        return self.copy(block, block, self.gather_sems, use, k, peer)

    def gather_start(self, use, buf):
        self.gather(use, 1, buf).start()
        self.gather(use, 0, buf).start()

    def gather_relay(self, use, buf):
        self.gather(use, 1, buf).wait_recv()
        self.gather(use, 2, buf).start()

    def gather_end(self, use, buf):
        self.gather(use, 0, buf).wait_recv()
        self.gather(use, 2, buf).wait_recv()
        for k in range(3):
            self.gather(use, k, buf).wait_send()

    def reduce(self, use, k):
        block = self.part.at[(self.twin, self.corner, self.across)[k]]
        land = self.far if k == 2 else self.near.at[k]
        peer = self.across if k == 2 else self.twin
        return self.copy(block, land, self.reduce_sems, use, k, peer)

    def reduce_start(self, use):
        self.reduce(use, 1).start()
        self.reduce(use, 0).start()

    def reduce_relay(self, use):
        self.reduce(use, 1).wait_recv()
        for low in range(0, self.part.shape[1], 64):
            rows = pl.ds(low, 64)
            total = self.part[self.across, rows].astype(F32) + self.near[1, rows].astype(F32)
            self.part[self.across, rows] = total.astype(BF)
        self.reduce(use, 2).start()

    def reduce_end(self, use):
        self.reduce(use, 0).wait_recv()
        self.reduce(use, 2).wait_recv()
        for k in range(3):
            self.reduce(use, k).wait_send()


class Queue:
    def __init__(self):
        self.steps = []

    def add(self, tag, fn):
        self.steps.append((tag, fn))

    def run(self, count, ready=None):
        while count > 0 and self.steps:
            tag, fn = self.steps[0]
            if ready is not None and tag not in ready:
                return
            self.steps.pop(0)
            fn()
            count -= 1

    def until(self, tag):
        while any(t == tag for t, _ in self.steps):
            self.run(1)


def layer_kernel(
    n,
    x_ref,
    cot_ref,
    seg_row,
    freq_ref,
    gq_ref,
    gk_ref,
    attn_in,
    ffn_in,
    out_ref,
    dx_ref,
    sums_ref,
    ggate_hbm,
    gup_hbm,
    gdown_hbm,
    attn,
    ffn,
    attn_land,
    ffn_land,
    gate_buf,
    up_buf,
    hid_buf,
    acc,
    part,
    near,
    far,
    xa,
    nm,
    df,
    proj_s,
    res_s,
    gains,
    gsum,
    gqk,
    q_proj,
    k_proj,
    qr,
    kr,
    vb,
    att,
    probs,
    cos_s,
    sin_s,
    stage,
    kvg,
    kvg_land,
    local_sem,
    stage_sem,
    ag_send,
    ag_recv,
    rs_send,
    rs_recv,
    qg_send,
    qg_recv,
    qr_send,
    qr_recv,
    kv_send,
    kv_recv,
):
    chunks = ffn.shape[0]
    rows, width = x_ref.shape
    attn_cut = ((0, 2 * HD), (2 * HD, 4 * HD), (4 * HD, attn.shape[-1]))
    ffn_cut = halves(ffn.shape[-1])
    parts = part_views(attn, ffn, attn_cut, ffn_cut)
    landing = part_views(attn_land, ffn_land, attn_cut, ffn_cut)
    first = len(attn_cut)
    ring = Ring(n, parts, ag_send, ag_recv)
    back = Ring(n, parts, rs_send, rs_recv, lambda p, slot: landing[p](slot))
    quad = Quad(part, near, far, (qg_send, qg_recv), (qr_send, qr_recv))
    me = quad.me

    def of_chunk(c):
        return range(first + 2 * c, first + 2 * c + 2)

    def piece(c, k):
        return ffn[c, :, :, k * HD : (k + 1) * HD].reshape(width, HD)

    def attn_cols(low, high):
        return attn[:, :, low:high].reshape(width, high - low)

    mine = [
        pltpu.make_async_copy(attn_in, attn.at[ring.me], local_sem.at[0]),
        pltpu.make_async_copy(ffn_in, ffn.at[:, ring.me], local_sem.at[1]),
        pltpu.make_async_copy(x_ref, xa.at[me], local_sem.at[2]),
    ]
    for copy in mine:
        copy.start()
    barrier(ring.peer + [{"tensor": quad.twin}, {"tensor": quad.across}])
    for copy in mine:
        copy.wait()
    quad.gather_start(0, xa)

    queue = Queue()
    slots = [[] for _ in range(2 * chunks + n + 4)]
    for p in range(first):
        for hop in range(1, n // 2 + 2):
            slots[hop - 1].append((-1, p, hop))
    for c in range(chunks):
        for hop in range(1, n // 2 + 2):
            for p in of_chunk(c):
                slots[2 * (c + 1) + hop - 1].append((c, p, hop))
    for slot in slots:
        for c, p, hop in slot:
            for way in range(2):
                if hop <= ring.reach(p, way) + 1:
                    queue.add(c, partial(ring.gather_step, p, way, hop))

    queue.run(AHEAD[0])
    quarter = SEGMAX // 2

    def seg_column(seg_j, half):
        cut = seg_j[:, half * quarter : (half + 1) * quarter].astype(F32)
        return jnp.transpose(jnp.broadcast_to(cut, (128, quarter)))[:, :1]

    def tables(tile, _):
        seg_j = seg_row[pl.ds(tile, 1), :]
        for half in range(2):
            r = 2 * tile + half
            same = seg_column(seg_j, half) == seg_j.astype(F32)
            j = lax.broadcasted_iota(jnp.int32, (quarter, SEGMAX), 1)
            start = jnp.min(jnp.where(same, j, SEGMAX).astype(F32), axis=1, keepdims=True)
            i = lax.broadcasted_iota(jnp.int32, (quarter, 1), 0).astype(F32) + half * quarter
            angle = (i - start) * freq_ref[...]
            cos_s[r] = jnp.cos(angle)
            sin_s[r] = jnp.sin(angle)
        return 0

    for tile in range(N_TILES):
        tables(tile, 0)
        queue.run(AHEAD[1])
    quad.gather_relay(0, xa)
    queue.until(-1)
    flipped = jnp.transpose(attn_cols(4 * HD, 4 * HD + 128).astype(F32))
    gains[...] = flipped[:8]
    quad.gather_end(0, xa)
    queue.run(AHEAD[2])

    sub = 32
    per = rows // sub

    def normalize(i, _):
        b, at = i // per, pl.ds(pl.multiple_of(i % per * sub, sub), sub)
        values = xa[b, at].astype(F32)
        xa[b, at] = (values * inverse_rms(values) * gains[0:1, :]).astype(BF)
        return 0

    lax.fori_loop(0, 4 * per, normalize, 0)

    def rope(values, gain_vec, r):
        normed = values * inverse_rms(values) * gain_vec
        low, high = normed[:, : HD // 2], normed[:, HD // 2 :]
        cosine, sine = cos_s[r], sin_s[r]
        return jnp.concatenate([low * cosine - high * sine, high * cosine + low * sine], axis=1)

    queue.run(AHEAD[3])

    def project(r, _):
        block = xa[r]
        query = dot_nn(block, attn_cols(HD, 2 * HD))
        q_proj[r] = query.astype(BF)
        qr[r] = rope(query, gq_ref[...], r).astype(BF)
        key = dot_nn(block, attn_cols(2 * HD, 3 * HD))
        k_proj[r] = key.astype(BF)
        kr[r] = rope(key, gk_ref[...], r).astype(BF)
        vb[r] = dot_nn(block, attn_cols(3 * HD, 4 * HD)).astype(BF)
        return 0

    lax.fori_loop(0, 4, project, 0)
    queue.run(AHEAD[4])

    def attend_tile(tile, _):
        two = pl.ds(2 * tile, 2)
        keys = kr[two].reshape(SEGMAX, HD)
        values = vb[two].reshape(SEGMAX, HD)
        seg_j = seg_row[pl.ds(tile, 1), :]
        for half in range(2):
            r = 2 * tile + half
            scores = dot_nt(qr[r], keys) * SCALE
            j = lax.broadcasted_iota(jnp.int32, (quarter, SEGMAX), 1)
            i = lax.broadcasted_iota(jnp.int32, (quarter, SEGMAX), 0) + half * quarter
            seen = (seg_column(seg_j, half) == seg_j.astype(F32)) & (i >= j)
            scores = jnp.where(seen, scores, NEG_LARGE)
            powers = jnp.exp(scores - jnp.max(scores, axis=1, keepdims=True))
            weights = (powers / jnp.sum(powers, axis=1, keepdims=True)).astype(BF)
            probs[r] = weights
            att[r] = dot_nn(weights, values).astype(BF)
        return 0

    lax.fori_loop(0, N_TILES, attend_tile, 0)
    queue.run(AHEAD[5])

    def out_block(r, _):
        acc[r] = dot_nt(att[r], attn_cols(0, HD))
        part[r] = acc[r].astype(BF)
        return 0

    lax.fori_loop(0, 4, out_block, 0)
    quad.reduce_start(0)
    queue.run(AHEAD[6])
    quad.reduce_relay(0)
    queue.run(AHEAD[7])
    quad.reduce_end(0)

    def total(at):
        return acc[me, at] + near[0, at].astype(F32) + far[at].astype(F32)

    def at_rows(i):
        return pl.ds(pl.multiple_of(i * sub, sub), sub)

    def middle(i, _):
        at = at_rows(i)
        projected = total(at)
        proj_s[at] = projected.astype(BF)
        mid = x_ref[at].astype(F32) + projected * inverse_rms(projected) * gains[1:2, :]
        res_s[at] = mid
        nm[me, at] = (mid * inverse_rms(mid) * gains[2:3, :]).astype(BF)
        return 0

    lax.fori_loop(0, per, middle, 0)
    quad.gather_start(1, nm)
    queue.run(AHEAD[8])
    quad.gather_relay(1, nm)
    queue.run(AHEAD[9])
    quad.gather_end(1, nm)

    for c in range(chunks):
        queue.until(c)

        def ffn_block(r, _):
            block = nm[r]
            gate = dot_nn(block, piece(c, 0))
            up = dot_nn(block, piece(c, 1))
            gate_buf[c, r] = gate.astype(BF)
            up_buf[c, r] = up.astype(BF)
            hidden = (gelu_parts(gate)[0] * up).astype(BF)
            grown = dot_nt(hidden, piece(c, 2))
            if c > 0:
                grown = grown + acc[r]
            acc[r] = grown
            if c == chunks - 1:
                part[r] = grown.astype(BF)
            return 0

        for low in range(0, 4, 2):
            lax.fori_loop(low, low + 2, ffn_block, 0)
            queue.run(AHEAD[10])
    queue.run(10**6)
    quad.reduce_start(1)
    for p in range(len(parts)):
        ring.gather_sends_done(p)
    quad.reduce_relay(1)
    quad.reduce_end(1)
    eight = (8, width)

    def fold(values):
        return jnp.sum(values.reshape(sub // 8, 8, values.shape[-1]), axis=0)

    def after_feed(i, carry):
        at = at_rows(i)
        feed = total(at)
        out_ref[at] = (res_s[at] + feed * inverse_rms(feed) * gains[3:4, :]).astype(BF)
        grad, gain_part = rms_back(feed, gains[3:4, :], cot_ref[at].astype(F32))
        df[me, at] = grad.astype(BF)
        return carry + fold(gain_part)

    gain_sum = lax.fori_loop(0, per, after_feed, jnp.zeros(eight, F32))
    gsum[3:4, :] = jnp.sum(gain_sum, axis=0, keepdims=True)
    quad.gather_start(2, df)
    quad.gather_relay(2, df)
    quad.gather_end(2, df)

    queue = Queue()
    slots = [[] for _ in range(2 * (chunks + 3) + n)]
    for c in range(chunks):
        for hop in range(1, n // 2 + 1):
            for p in of_chunk(c):
                slots[2 * c + hop].append((c, p, hop))
    stage_count = [0]

    def finish(c, p):
        low = ffn_cut[(p - first) % 2]
        k = stage_count[0]
        stage_count[0] += 1
        copies = []
        for which, hbm in ((0, ggate_hbm), (1, gup_hbm), (2, gdown_hbm)):
            left = max(low[0], which * HD)
            right = min(low[1], (which + 1) * HD)
            if left < right:
                copies.append(
                    pltpu.make_async_copy(
                        stage.at[k % 2, :, pl.ds(left - low[0], right - left)],
                        hbm.at[:, pl.ds(c * HD + left - which * HD, right - left)],
                        stage_sem.at[k % 2, len(copies)],
                    )
                )
        if k >= 2:
            for copy in pending[k - 2]:
                copy.wait()
        stage[k % 2] = back.reduce_end(p)
        for copy in copies:
            copy.start()
        pending.append(copies)

    pending = []
    for s, slot in enumerate(slots):
        for c, p, hop in slot:
            for way in range(2):
                if hop <= back.reach(p, way):
                    queue.add(c, partial(back.reduce_step, p, way, hop))
        c = (s - n // 2 - 1) // 2
        if s >= n // 2 + 1 and (s - n // 2 - 1) % 2 == 0 and c < chunks:
            for p in of_chunk(c):
                queue.add(c, partial(finish, c, p))
    ready = set()

    for c in range(chunks):

        def back_block(r, _):
            grad = dot_nn(df[r], piece(c, 2))
            gate, up = gate_buf[c, r].astype(F32), up_buf[c, r].astype(F32)
            act, bent = gelu_parts(gate)
            slope = 0.5 * (1.0 + bent) + 0.5 * gate * (1.0 - bent * bent) * ROOT * (
                1.0 + 3.0 * CUBIC * gate * gate
            )
            d_gate = (grad * up * slope).astype(BF)
            d_up = (grad * act).astype(BF)
            hid_buf[r] = (act * up).astype(BF)
            gate_buf[c, r] = d_gate
            up_buf[c, r] = d_up
            grown = dot_nt(d_gate, piece(c, 0)) + dot_nt(d_up, piece(c, 1))
            if c > 0:
                grown = grown + acc[r]
            acc[r] = grown
            if c == chunks - 1:
                part[r] = grown.astype(BF)
            return 0

        lax.fori_loop(0, 4, back_block, 0)
        queue.run(PACE[0], ready)

        def grad_piece(k, left, right):
            value = dot_tn(left.reshape(4 * rows, width), right.reshape(4 * rows, HD))
            ffn[c, :, :, k * HD : (k + 1) * HD] = value.astype(BF).reshape(n, width // n, HD)

        grad_piece(2, df[...], hid_buf[...])
        if c == chunks - 1:
            quad.reduce_start(2)
        queue.run(PACE[1], ready)
        grad_piece(0, nm[...], gate_buf[c])
        queue.run(PACE[1], ready)
        if c == chunks - 1:
            quad.reduce_relay(2)
        grad_piece(1, nm[...], up_buf[c])
        ready.add(c)
        queue.run(PACE[1], ready)

    queue.run(PACE[2], ready)
    quad.reduce_end(2)

    def after_ffn(i, carry):
        at = at_rows(i)
        grad, pre_part = rms_back(res_s[at], gains[2:3, :], total(at))
        grad = cot_ref[at].astype(F32) + grad
        res_s[at] = grad
        grad, attn_part = rms_back(proj_s[at].astype(F32), gains[1:2, :], grad)
        df[me, at] = grad.astype(BF)
        return carry[0] + fold(pre_part), carry[1] + fold(attn_part)

    zero = jnp.zeros(eight, F32)
    pre_sum, attn_sum = lax.fori_loop(0, per, after_ffn, (zero, zero))
    gsum[2:3, :] = jnp.sum(pre_sum, axis=0, keepdims=True)
    gsum[1:2, :] = jnp.sum(attn_sum, axis=0, keepdims=True)
    quad.gather_start(3, df)
    queue.run(PACE[3], ready)
    quad.gather_relay(3, df)
    queue.run(PACE[4], ready)
    quad.gather_end(3, df)

    d_q, d_k, d_v, datt = (gate_buf.at[k] for k in range(4))
    def back_out(r, _):
        datt[r] = dot_nn(df[r], attn_cols(0, HD)).astype(BF)
        return 0

    lax.fori_loop(0, 4, back_out, 0)
    queue.run(PACE[5], ready)
    gqk[...] = jnp.zeros_like(gqk)

    def unrope(grad, projection, gain_vec, r, row):
        low, high = grad[:, : HD // 2], grad[:, HD // 2 :]
        cosine, sine = cos_s[r], sin_s[r]
        grad = jnp.concatenate([low * cosine + high * sine, high * cosine - low * sine], axis=1)
        grad, gain_part = rms_back(projection, gain_vec, grad)
        gqk[row : row + 1, :] += jnp.sum(gain_part, axis=0, keepdims=True)
        return grad.astype(BF)

    def back_tile(tile, _):
        two = pl.ds(2 * tile, 2)
        keys = kr[two].reshape(SEGMAX, HD)
        values = vb[two].reshape(SEGMAX, HD)
        d_key = jnp.zeros((SEGMAX, HD), F32)
        d_value = jnp.zeros((SEGMAX, HD), F32)
        for half in range(2):
            r = 2 * tile + half
            d_att = datt[r]
            weights = probs[r]
            d_value = d_value + dot_tn(weights, d_att)
            d_probs = dot_nt(d_att, values)
            weights = weights.astype(F32)
            delta = jnp.sum(weights * d_probs, axis=1, keepdims=True)
            d_scores = (weights * (d_probs - delta) * SCALE).astype(BF)
            d_key = d_key + dot_tn(d_scores, qr[r])
            d_query = dot_nn(d_scores, keys)
            d_q[r] = unrope(d_query, q_proj[r].astype(F32), gq_ref[...], r, 4)
        for half in range(2):
            r = 2 * tile + half
            cut = slice(half * quarter, (half + 1) * quarter)
            d_k[r] = unrope(d_key[cut], k_proj[r].astype(F32), gk_ref[...], r, 5)
            d_v[r] = d_value[cut].astype(BF)
        return 0

    lax.fori_loop(0, N_TILES, back_tile, 0)
    queue.run(PACE[5], ready)

    def back_in(r, _):
        grown = dot_nt(d_q[r], attn_cols(HD, 2 * HD))
        grown = grown + dot_nt(d_k[r], attn_cols(2 * HD, 3 * HD))
        grown = grown + dot_nt(d_v[r], attn_cols(3 * HD, 4 * HD))
        acc[r] = grown
        part[r] = grown.astype(BF)
        return 0

    lax.fori_loop(0, 4, back_in, 0)
    quad.reduce_start(3)
    queue.run(PACE[5], ready)

    def attn_grad(low, left, right):
        value = dot_tn(left.reshape(4 * rows, width), right.reshape(4 * rows, HD))
        attn[:, :, low : low + HD] = value.astype(BF).reshape(n, width // n, HD)

    attn_grad(0, df[...], att[...])
    quad.reduce_relay(3)
    for k, grad in enumerate((d_q, d_k, d_v)):
        attn_grad((k + 1) * HD, xa[...], grad[...])
        queue.run(PACE[5], ready)
    queue.run(PACE[6], ready)
    quad.reduce_end(3)

    def after_attn(i, carry):
        at = at_rows(i)
        grad, gain_part = rms_back(x_ref[at].astype(F32), gains[0:1, :], total(at))
        dx_ref[at] = (res_s[at] + grad).astype(BF)
        return carry + fold(gain_part)

    gain_sum = lax.fori_loop(0, per, after_attn, zero)
    gsum[0:1, :] = jnp.sum(gain_sum, axis=0, keepdims=True)
    gsum[4:8, :] = jnp.zeros((4, width), F32)
    tall = jnp.concatenate([gsum[...], jnp.zeros((120, width), F32)], axis=0)
    tall = jnp.transpose(tall).reshape(n, width // n, 128)
    short = jnp.concatenate([gqk[...], jnp.zeros((120, HD), F32)], axis=0)
    short = jnp.transpose(short).reshape(n, HD // n, 128)
    attn[:, :, 4 * HD : 4 * HD + 128] = tall.astype(BF)
    attn[:, : HD // n, 4 * HD : 4 * HD + 128] = (tall[:, : HD // n] + short).astype(BF)

    for hop in range(1, n // 2 + 1):
        for p in range(first):
            for way in range(2):
                if hop <= back.reach(p, way):
                    queue.add(-1, partial(back.reduce_step, p, way, hop))
    queue.run(10**6)
    sums_ref[:, : 2 * HD] = back.reduce_end(0)
    kvg[0, :, : 2 * HD] = back.reduce_end(1).astype(BF)
    kvg[0, :, 2 * HD :] = back.reduce_end(2).astype(BF)
    for k, peer in enumerate((quad.twin, quad.across)):
        copy = pltpu.make_async_remote_copy(
            kvg.at[k],
            kvg_land.at[k],
            kv_send.at[k],
            kv_recv.at[k],
            device_id={"tensor": peer},
            device_id_type=MESH,
        )
        copy.start()
        copy.wait()
        grown = kvg[k].astype(F32) + kvg_land[k].astype(F32)
        if k == 0:
            kvg[1] = grown.astype(BF)
        else:
            sums_ref[:, 2 * HD :] = grown
    for p in range(len(parts)):
        back.reduce_sends_done(p)
    for copies in pending[-2:]:
        for copy in copies:
            copy.wait()


AHEAD = (16, 8, 8, 6, 6, 6, 4, 12, 12, 4, 3)
PACE = (3, 2, 12, 12, 4, 4, 12)
N_TILES = 2


def run_layer(n, x, cot, segments, g_query, g_key, attn_pack, ffn_pack):
    rows, width = x.shape
    chunks, depth, cols = ffn_pack.shape
    tokens = segments.shape[0]
    wide = attn_pack.shape[1]
    parts = 3 + 2 * chunks
    exponent = -2.0 * jnp.arange(HD // 2, dtype=F32) / HD
    freq = jnp.power(jnp.float32(THETA), exponent)[None, :]
    vmem, dma = pltpu.VMEM, pltpu.SemaphoreType.DMA
    grown = chunks * HD
    return pl.pallas_call(
        partial(layer_kernel, n),
        out_shape=(
            jax.ShapeDtypeStruct((rows, width), BF),
            jax.ShapeDtypeStruct((rows, width), BF),
            jax.ShapeDtypeStruct((depth, wide), F32),
            jax.ShapeDtypeStruct((depth, grown), F32),
            jax.ShapeDtypeStruct((depth, grown), F32),
            jax.ShapeDtypeStruct((depth, grown), F32),
        ),
        in_specs=vmem_specs(6) + any_specs(2),
        out_specs=vmem_specs(3) + any_specs(3),
        scratch_shapes=[
            vmem((n, depth, wide), BF),
            vmem((chunks, n, depth, cols), BF),
            vmem((n - 1, depth, wide), BF),
            vmem((chunks, n - 1, depth, cols), BF),
            vmem((chunks, 4, rows, HD), BF),
            vmem((chunks, 4, rows, HD), BF),
            vmem((4, rows, HD), BF),
            vmem((4, rows, width), F32),
            vmem((4, rows, width), BF),
            vmem((2, rows, width), BF),
            vmem((rows, width), BF),
            vmem((4, rows, width), BF),
            vmem((4, rows, width), BF),
            vmem((4, rows, width), BF),
            vmem((rows, width), BF),
            vmem((rows, width), F32),
            vmem((8, width), F32),
            vmem((8, width), F32),
            vmem((8, HD), F32),
            vmem((4, rows, HD), BF),
            vmem((4, rows, HD), BF),
            vmem((4, rows, HD), BF),
            vmem((4, rows, HD), BF),
            vmem((4, rows, HD), BF),
            vmem((4, rows, HD), BF),
            vmem((4, rows, SEGMAX), BF),
            vmem((4, rows, HD // 2), F32),
            vmem((4, rows, HD // 2), F32),
            vmem((2, depth, cols // 2), F32),
            vmem((2, depth, wide - 2 * HD), BF),
            vmem((2, depth, wide - 2 * HD), BF),
            dma((3,)),
            dma((2, 2)),
            dma((parts, 2, n // 2)),
            dma((parts, 2, n // 2)),
            dma((parts, 2, n // 2)),
            dma((parts, 2, n // 2)),
            dma((4, 3)),
            dma((4, 3)),
            dma((4, 3)),
            dma((4, 3)),
            dma((2,)),
            dma((2,)),
        ],
        compiler_params=pltpu.CompilerParams(
            collective_id=2, has_side_effects=True, vmem_limit_bytes=67043328
        ),
    )(
        x,
        cot,
        segments.reshape(N_TILES, SEGMAX),
        freq,
        g_query.astype(F32)[None, :],
        g_key.astype(F32)[None, :],
        attn_pack,
        ffn_pack,
    )


def fused_local(
    inputs, segments, w_query, w_key, w_value, w_out, g_in, g_attn, g_query, g_key,
    w_gate, w_up, w_down, g_pre, g_post, cotangent,
):
    n = lax.axis_size("dp")
    depth = w_query.shape[0]
    width = w_gate.shape[1]
    gains = jnp.stack([g_in, g_attn, g_pre, g_post], axis=1)
    attn_pack = jnp.concatenate(
        [w_out.T, w_query, w_key, w_value, jnp.pad(gains, ((0, 0), (0, 124)))], axis=1
    )
    ffn_pack = pack_ffn(w_gate, w_up, w_down.T, depth)
    output, d_inputs, sums, g_gate, g_up, g_down = run_layer(
        n, inputs, cotangent, segments, g_query, g_key, attn_pack, ffn_pack
    )
    spot = lax.axis_index("tensor")
    part = depth // 4
    mine = lax.dynamic_slice_in_dim(sums[:, 2 * HD :], spot * part, part, 0)
    small = HD // n // 4
    few = lax.dynamic_slice_in_dim(sums[:, 4 * HD :], spot * small, small, 0)
    return (
        output,
        d_inputs,
        sums[:, HD : 2 * HD],
        mine[:, :HD],
        mine[:, HD : 2 * HD],
        sums[:, :HD].T,
        mine[:, 2 * HD],
        mine[:, 2 * HD + 1],
        few[:, 4],
        few[:, 5],
        g_gate[:, :width],
        g_up[:, :width],
        g_down[:, :width].T,
        mine[:, 2 * HD + 2],
        mine[:, 2 * HD + 3],
    )


def fits(mesh, depth, tokens, rows):
    return depth % 16 == 0 and mesh.shape["tensor"] == 4 and tokens == 2 * SEGMAX


def layer(mesh):
    def body(*args):
        inputs, segments, w_query = args[0], args[1], args[2]
        if fits(mesh, w_query.shape[0], segments.shape[0], inputs.shape[0]):
            return fused_local(*args)
        return local(*args)

    return body


def solution(mesh):
    return jax.shard_map(
        layer(mesh),
        mesh=mesh,
        in_specs=(
            P(("dp", "tensor"), None),
            P("dp"),
            P("dp", "tensor"),
            P("dp", None),
            P("dp", None),
            P("tensor", "dp"),
            P("dp"),
            P("dp"),
            P(),
            P(),
            P("dp", "tensor"),
            P("dp", "tensor"),
            P("tensor", "dp"),
            P("dp"),
            P("dp"),
            P(("dp", "tensor"), None),
        ),
        out_specs=(
            P(("dp", "tensor"), None),
            P(("dp", "tensor"), None),
            P("dp", "tensor"),
            P(("dp", "tensor"), None),
            P(("dp", "tensor"), None),
            P("tensor", "dp"),
            P(("dp", "tensor")),
            P(("dp", "tensor")),
            P(("dp", "tensor")),
            P(("dp", "tensor")),
            P("dp", "tensor"),
            P("dp", "tensor"),
            P("tensor", "dp"),
            P(("dp", "tensor")),
            P(("dp", "tensor")),
        ),
        check_vma=False,
    )
```

```python
from functools import partial

import jax
import jax.numpy as jnp
from jax import lax
from jax.experimental import pallas as pl
from jax.experimental.pallas import tpu as pltpu
from jax.sharding import PartitionSpec as P

HD = 256
SEGMAX = 512
MESH = pl.DeviceIdType.MESH
BF = jnp.bfloat16
F32 = jnp.float32


def ring_pos(dev, n):
    return (1 - dev % 2) * (dev // 2) + (dev % 2) * (n - 1 - dev // 2)


def ring_dev(pos, n):
    high = pos // (n // 2)
    return (1 - high) * (2 * pos) + high * (2 * (n - 1 - pos) + 1)


def barrier(peers):
    sem = pltpu.get_barrier_semaphore()
    for peer in peers:
        pl.semaphore_signal(sem, inc=1, device_id=peer, device_id_type=MESH)
    pl.semaphore_wait(sem, len(peers))


def reach(bias, way, n):
    return n // 2 if bias == way else n // 2 - 1


class Ring:
    def __init__(self, n, parts, send_sem, recv_sem, land=None):
        self.n, self.parts, self.land = n, parts, land
        self.send_sem, self.recv_sem = send_sem, recv_sem
        self.me = lax.axis_index("dp")
        self.pos = ring_pos(self.me, n)
        self.peer = [{"dp": self.dev(1)}, {"dp": self.dev(-1)}]

    def dev(self, offset):
        return ring_dev((self.pos + (offset + self.n) % self.n) % self.n, self.n)

    def reach(self, part, way):
        return reach(part % 2, way, self.n)

    def gather(self, part, way, hop, ahead):
        away = hop - 1 if ahead else hop
        block = self.parts[part](self.dev(-away if way == 0 else away))
        return pltpu.make_async_remote_copy(
            block,
            block,
            self.send_sem.at[part, way, hop - 1],
            self.recv_sem.at[part, way, hop - 1],
            device_id=self.peer[way],
            device_id_type=MESH,
        )

    def gather_step(self, part, way, hop):
        if hop > 1:
            self.gather(part, way, hop - 1, False).wait_recv()
        if hop <= self.reach(part, way):
            self.gather(part, way, hop, True).start()

    def gather_sends_done(self, part):
        for way in range(2):
            for hop in range(1, self.reach(part, way) + 1):
                self.gather(part, way, hop, True).wait_send()

    def target(self, part, way, hop):
        away = self.reach(part, way) - hop + 1
        return self.dev(away if way == 0 else -away)

    def slot(self, part, way, hop):
        return self.land(part, hop - 1 + (self.reach(part, 0) if way else 0))

    def reduce(self, part, way, hop):
        return pltpu.make_async_remote_copy(
            self.parts[part](self.target(part, way, hop)),
            self.slot(part, way, hop),
            self.send_sem.at[part, way, hop - 1],
            self.recv_sem.at[part, way, hop - 1],
            device_id=self.peer[way],
            device_id_type=MESH,
        )

    def reduce_step(self, part, way, hop):
        if hop > self.reach(part, way):
            return
        if hop > 1:
            self.reduce(part, way, hop - 1).wait_recv()
            own = self.parts[part](self.target(part, way, hop))
            came = self.slot(part, way, hop - 1)
            own[...] = (own[...].astype(F32) + came[...].astype(F32)).astype(BF)
        self.reduce(part, way, hop).start()

    def reduce_end(self, part):
        total = self.parts[part](self.me)[...].astype(F32)
        for way in range(2):
            last = self.reach(part, way)
            self.reduce(part, way, last).wait_recv()
            total = total + self.slot(part, way, last)[...].astype(F32)
        return total

    def reduce_sends_done(self, part):
        for way in range(2):
            for hop in range(1, self.reach(part, way) + 1):
                self.reduce(part, way, hop).wait_send()


def part_views(attn, attn_cut, ffn=None, ffn_cut=()):
    views = []
    for low, high in attn_cut:
        views.append(lambda b, low=low, high=high: attn.at[b, :, pl.ds(low, high - low)])
    for chunk in range(0 if ffn is None else ffn.shape[0]):
        for low, high in ffn_cut:
            views.append(
                lambda b, c=chunk, low=low, high=high: ffn.at[c, b, :, pl.ds(low, high - low)]
            )
    return views


def halves(cols, step=128):
    mid = cols // 2 // step * step
    return ((0, mid), (mid, cols))


def gather_kernel(n, attn_ref, ffn_ref, attn_out, ffn_out, local_sem, send_sem, recv_sem):
    parts = part_views(attn_out, halves(attn_ref.shape[-1]), ffn_out, halves(ffn_ref.shape[-1]))
    ring = Ring(n, parts, send_sem, recv_sem)
    mine = [
        pltpu.make_async_copy(attn_ref, attn_out.at[ring.me], local_sem.at[0]),
        pltpu.make_async_copy(ffn_ref, ffn_out.at[:, ring.me], local_sem.at[1]),
    ]
    for copy in mine:
        copy.start()
    barrier(ring.peer)
    for copy in mine:
        copy.wait()
    width = 4
    for low in range(0, len(parts), width):
        for hop in range(1, n // 2 + 2):
            for part in range(low, min(low + width, len(parts))):
                for way in range(2):
                    if hop <= ring.reach(part, way) + 1:
                        ring.gather_step(part, way, hop)
    for part in range(len(parts)):
        ring.gather_sends_done(part)


def reduce_kernel(n, attn_ref, ffn_ref, attn_out, ffn_out, attn_buf, ffn_buf, attn_land, ffn_land, local_sem, send_sem, recv_sem):
    acut, fcut = halves(attn_ref.shape[-1]), halves(ffn_ref.shape[-1])
    parts = part_views(attn_buf, acut, ffn_buf, fcut)
    landing = part_views(attn_land, acut, ffn_land, fcut)
    ring = Ring(n, parts, send_sem, recv_sem, lambda part, slot: landing[part](slot))
    load = [
        pltpu.make_async_copy(attn_ref, attn_buf, local_sem.at[0]),
        pltpu.make_async_copy(ffn_ref, ffn_buf, local_sem.at[1]),
    ]
    for copy in load:
        copy.start()
    barrier(ring.peer)
    for copy in load:
        copy.wait()
    width = 4
    for low in range(0, len(parts), width):
        for hop in range(1, n // 2 + 1):
            for part in range(low, min(low + width, len(parts))):
                for way in range(2):
                    ring.reduce_step(part, way, hop)
        for part in range(low, min(low + width, len(parts))):
            total = ring.reduce_end(part)
            if part < 2:
                attn_out[:, acut[part][0] : acut[part][1]] = total
            else:
                cut = fcut[part % 2]
                ffn_out[part // 2 - 1, :, cut[0] : cut[1]] = total
    for part in range(len(parts)):
        ring.reduce_sends_done(part)


VMEM_LIMIT = 60 * 2**20


def vmem_specs(count):
    return [pl.BlockSpec(memory_space=pltpu.VMEM)] * count


def any_specs(count):
    return [pl.BlockSpec(memory_space=pl.ANY)] * count


def ring_gather(n, attn, ffn):
    chunks = ffn.shape[0]
    sems = pltpu.SemaphoreType.DMA((2 * (chunks + 1), 2, n // 2))
    return pl.pallas_call(
        partial(gather_kernel, n),
        out_shape=(
            jax.ShapeDtypeStruct((n,) + attn.shape, BF),
            jax.ShapeDtypeStruct((chunks, n) + ffn.shape[1:], BF),
        ),
        in_specs=any_specs(2),
        out_specs=vmem_specs(2),
        scratch_shapes=[pltpu.SemaphoreType.DMA((2,)), sems, sems],
        compiler_params=pltpu.CompilerParams(
            collective_id=0, has_side_effects=True, vmem_limit_bytes=VMEM_LIMIT
        ),
    )(attn, ffn)


def ring_reduce(n, attn, ffn):
    chunks, _, rows, cols = ffn.shape
    sems = pltpu.SemaphoreType.DMA((2 * (chunks + 1), 2, n // 2))
    return pl.pallas_call(
        partial(reduce_kernel, n),
        out_shape=(
            jax.ShapeDtypeStruct(attn.shape[1:], F32),
            jax.ShapeDtypeStruct((chunks, rows, cols), F32),
        ),
        in_specs=any_specs(2),
        out_specs=vmem_specs(2),
        scratch_shapes=[
            pltpu.VMEM(attn.shape, BF),
            pltpu.VMEM(ffn.shape, BF),
            pltpu.VMEM((n - 1,) + attn.shape[1:], BF),
            pltpu.VMEM((chunks, n - 1, rows, cols), BF),
            pltpu.SemaphoreType.DMA((2,)),
            sems,
            sems,
        ],
        compiler_params=pltpu.CompilerParams(
            collective_id=1, has_side_effects=True, vmem_limit_bytes=VMEM_LIMIT
        ),
    )(attn, ffn)


CHUNK = 256


def pack_rows(array, rows):
    return jnp.pad(array, ((0, rows - array.shape[0]), (0, 0)))


def pack_ffn(gate, up, down_t, rows, step=CHUNK):
    width = gate.shape[1]
    chunks = -(-width // step)
    chunks += chunks % 2 if step != CHUNK else 0

    def cut(array):
        array = jnp.pad(array, ((0, rows - array.shape[0]), (0, chunks * step - width)))
        return array.reshape(rows, chunks, step).transpose(1, 0, 2)

    return jnp.concatenate([cut(gate), cut(up), cut(down_t)], axis=2)


def unpack_ffn(packed, width):
    chunks, rows = packed.shape[:2]
    out = []
    for k in range(3):
        piece = packed[:, :, k * CHUNK : (k + 1) * CHUNK]
        out.append(piece.transpose(1, 0, 2).reshape(rows, chunks * CHUNK)[:, :width])
    return out


def pack_blocks(array, n, rows):
    depth = array.shape[0] // n
    return jnp.pad(array.reshape(n, depth, -1), ((0, 0), (0, rows - depth), (0, 0)))


EPSILON = 1e-06
THETA = 1000000.0
NEG_LARGE = -1e30


def rms_scale(values, gain_vec):
    inverse = lax.rsqrt(jnp.mean(values * values, axis=-1, keepdims=True) + EPSILON)
    return values * inverse * gain_vec


def gelu_product(gate_proj, up_proj):
    return jax.nn.gelu(gate_proj, approximate=True) * up_proj


def rows_product(left, right):
    return lax.dot_general(
        left, right, (((0,), (0,)), ((), ())), preferred_element_type=jnp.float32
    )


def cols_product(left, right):
    return lax.dot_general(
        left, right, (((1,), (1,)), ((), ())), preferred_element_type=jnp.float32
    )


def plain_product(left, right):
    return jnp.dot(left, right, preferred_element_type=jnp.float32)


def rotary_tables(segments):
    count = segments.shape[0]
    row_index = jnp.arange(count, dtype=jnp.int32)
    previous = jnp.concatenate([jnp.full((1,), -1, jnp.int32), segments[:-1]])
    starts = jnp.where(segments != previous, row_index, jnp.zeros_like(row_index))
    seq_start = lax.cummax(starts, axis=0)
    position = (row_index - seq_start).astype(jnp.float32)
    half_width = HD // 2
    exponent = -2.0 * jnp.arange(half_width, dtype=jnp.float32) / HD
    inverse = jnp.power(jnp.float32(THETA), exponent)
    angles = position[:, None] * inverse[None, :]
    cosine = jnp.concatenate([jnp.cos(angles), jnp.cos(angles)], axis=1)
    sine_tab = jnp.concatenate([jnp.sin(angles), jnp.sin(angles)], axis=1)
    return (cosine, sine_tab)


def prepare(projection, gain_vec, cosine, sine_tab):
    normed = rms_scale(projection, gain_vec)
    half_width = HD // 2
    turned = jnp.concatenate([-normed[..., half_width:], normed[..., :half_width]], axis=-1)
    return normed * cosine[:, None, :] + turned * sine_tab[:, None, :]


def visible(segments):
    tile_count = segments.shape[0] // SEGMAX
    seg_tiles = segments.reshape(tile_count, SEGMAX)
    offsets = jnp.arange(SEGMAX, dtype=jnp.int32)
    same = seg_tiles[:, :, None] == seg_tiles[:, None, :]
    return same & (offsets[:, None] >= offsets[None, :])


def tile_scores(query_tiles, key_tiles, segments):
    head_width = key_tiles.shape[-1]
    scores = jnp.einsum(
        "tqhd,tkd->thqk", query_tiles, key_tiles, preferred_element_type=jnp.float32
    ) * head_width ** (-0.5)
    return jnp.where(visible(segments)[:, None], scores, NEG_LARGE)


def attend(query_ready, key_ready, value_b, segments):
    row_count, head_count, head_width = query_ready.shape
    tile_count = row_count // SEGMAX
    query_tiles = query_ready.reshape(tile_count, SEGMAX, head_count, head_width)
    key_tiles = key_ready.reshape(tile_count, SEGMAX, head_width)
    value_tiles = value_b.reshape(tile_count, SEGMAX, head_width)
    scores = tile_scores(query_tiles, key_tiles, segments)
    row_max = jnp.max(scores, axis=-1, keepdims=True)
    row_total = jnp.sum(jnp.exp(scores - row_max), axis=-1, keepdims=True)
    log_total = row_max + jnp.log(row_total)
    probs = jnp.exp(scores - log_total).astype(jnp.bfloat16)
    attended = jnp.einsum("thqk,tkd->tqhd", probs, value_tiles, preferred_element_type=jnp.float32)
    return (attended.reshape(row_count, head_count * head_width).astype(jnp.bfloat16), log_total)


def attend_back(query_ready, key_ready, value_b, segments, log_total, d_attended):
    row_count, head_count, head_width = query_ready.shape
    tile_count = row_count // SEGMAX
    query_tiles = query_ready.reshape(tile_count, SEGMAX, head_count, head_width)
    key_tiles = key_ready.reshape(tile_count, SEGMAX, head_width)
    value_tiles = value_b.reshape(tile_count, SEGMAX, head_width)
    grad_tiles = d_attended.reshape(tile_count, SEGMAX, head_count, head_width)
    scores = tile_scores(query_tiles, key_tiles, segments)
    prob_vals = jnp.exp(scores - log_total)
    prob_b = prob_vals.astype(jnp.bfloat16)
    d_value = jnp.einsum(
        "thqk,tqhd->tkd", prob_b, grad_tiles, preferred_element_type=jnp.float32
    ).reshape(row_count, head_width)
    d_probs = jnp.einsum(
        "tqhd,tkd->thqk", grad_tiles, value_tiles, preferred_element_type=jnp.float32
    )
    row_delta = jnp.sum(prob_vals * d_probs, axis=-1, keepdims=True)
    d_scores = (prob_vals * (d_probs - row_delta) * head_width ** (-0.5)).astype(jnp.bfloat16)
    d_query = jnp.einsum(
        "thqk,tkd->tqhd", d_scores, key_tiles, preferred_element_type=jnp.float32
    ).reshape(row_count, head_count, head_width)
    d_key = jnp.einsum(
        "thqk,tqhd->tkd", d_scores, query_tiles, preferred_element_type=jnp.float32
    ).reshape(row_count, head_width)
    return (d_query, d_key, d_value)


def local(
    inputs,
    segments,
    w_query,
    w_key,
    w_value,
    w_out,
    g_in,
    g_attn,
    g_query,
    g_key,
    w_gate,
    w_up,
    w_down,
    g_pre,
    g_post,
    cotangent,
):
    n = lax.axis_size("dp")
    depth = w_query.shape[0]
    rows = -(-depth // 16) * 16
    width = w_gate.shape[1]
    gains = jnp.stack([g_in, g_attn, g_pre, g_post], axis=1)
    attn_pack = jnp.concatenate(
        [w_query, w_key, w_value, w_out.T, jnp.pad(gains, ((0, 0), (0, 124)))], axis=1
    )
    attn_all, ffn_all = ring_gather(
        n, pack_rows(attn_pack, rows), pack_ffn(w_gate, w_up, w_down.T, rows)
    )
    attn_all = attn_all[:, :depth].reshape(n * depth, -1)
    ffn_all = ffn_all[:, :, :depth].reshape(ffn_all.shape[0], n * depth, -1)
    wq_full, wk_full, wv_full, wo_t = (attn_all[:, k * HD : (k + 1) * HD] for k in range(4))
    wo_full = wo_t.T
    gin_full, gattn_full, gpre_full, gpost_full = (attn_all[:, 4 * HD + k] for k in range(4))
    wg_full, wu_full, wd_t = unpack_ffn(ffn_all, width)
    wd_full = wd_t.T
    gain_in = gin_full.astype(jnp.float32)
    gain_attn = gattn_full.astype(jnp.float32)
    gain_query = g_query.astype(jnp.float32)
    gain_key = g_key.astype(jnp.float32)
    cosine, sine_tab = rotary_tables(segments)
    inputs_f = inputs.astype(jnp.float32)
    normed_shard = rms_scale(inputs_f, gain_in).astype(jnp.bfloat16)
    normed_in = lax.all_gather(normed_shard, "tensor", axis=0, tiled=True)
    row_count = normed_in.shape[0]
    head_count = wq_full.shape[1] // HD
    key_proj = plain_product(normed_in, wk_full)
    value_b = plain_product(normed_in, wv_full).astype(jnp.bfloat16)
    key_ready = prepare(key_proj[:, None, :], gain_key, cosine, sine_tab)[:, 0, :].astype(
        jnp.bfloat16
    )
    query_proj = plain_product(normed_in, wq_full).reshape(row_count, head_count, HD)
    query_ready = prepare(query_proj, gain_query, cosine, sine_tab).astype(jnp.bfloat16)
    attended, log_total = attend(query_ready, key_ready, value_b, segments)
    projected = lax.psum_scatter(
        plain_product(attended, wo_full), "tensor", scatter_dimension=0, tiled=True
    )
    residual_mid = inputs_f + rms_scale(projected, gain_attn)
    gain_pre = gpre_full.astype(jnp.float32)
    gain_post = gpost_full.astype(jnp.float32)
    normed_mid = lax.all_gather(
        rms_scale(residual_mid, gain_pre).astype(jnp.bfloat16), "tensor", axis=0, tiled=True
    )
    gate_proj = plain_product(normed_mid, wg_full)
    up_proj = plain_product(normed_mid, wu_full)
    hidden = gelu_product(gate_proj, up_proj).astype(jnp.bfloat16)
    feed = lax.psum_scatter(
        plain_product(hidden, wd_full), "tensor", scatter_dimension=0, tiled=True
    )
    output = (residual_mid + rms_scale(feed, gain_post)).astype(jnp.bfloat16)
    wg_back, wu_back, wd_back = wg_full, wu_full, wd_full
    grad_output = cotangent.astype(jnp.float32)
    d_feed_f, grad_g_post = jax.vjp(rms_scale, feed, gain_post)[1](grad_output)
    d_feed = lax.all_gather(d_feed_f.astype(jnp.bfloat16), "tensor", axis=0, tiled=True)
    d_hidden = cols_product(d_feed, wd_back)
    d_gate_f, d_up_f = jax.vjp(gelu_product, gate_proj, up_proj)[1](d_hidden)
    d_gate = d_gate_f.astype(jnp.bfloat16)
    d_up = d_up_f.astype(jnp.bfloat16)
    grad_gate = rows_product(normed_mid, d_gate)
    grad_up = rows_product(normed_mid, d_up)
    d_normed_mid = lax.psum_scatter(
        cols_product(d_gate, wg_back) + cols_product(d_up, wu_back),
        "tensor",
        scatter_dimension=0,
        tiled=True,
    )
    d_mid_n, grad_g_pre = jax.vjp(rms_scale, residual_mid, gain_pre)[1](d_normed_mid)
    d_mid = grad_output + d_mid_n
    d_proj_f, grad_g_attn = jax.vjp(rms_scale, projected, gain_attn)[1](d_mid)
    wq_back, wk_back, wv_back, wo_back = wq_full, wk_full, wv_full, wo_full
    d_proj = lax.all_gather(d_proj_f.astype(jnp.bfloat16), "tensor", axis=0, tiled=True)
    d_attended = cols_product(d_proj, wo_back).astype(jnp.bfloat16)
    d_query_ready, d_key_ready, d_value_f = attend_back(
        query_ready, key_ready, value_b, segments, log_total, d_attended
    )
    rotate_fn = partial(prepare, cosine=cosine, sine_tab=sine_tab)
    d_query_f, grad_g_query = jax.vjp(rotate_fn, query_proj, gain_query)[1](d_query_ready)
    d_key_f, grad_g_key = jax.vjp(rotate_fn, key_proj[:, None, :], gain_key)[1](
        d_key_ready[:, None, :]
    )
    d_query = d_query_f.reshape(row_count, head_count * HD).astype(jnp.bfloat16)
    d_key = d_key_f[:, 0, :].astype(jnp.bfloat16)
    d_value = d_value_f.astype(jnp.bfloat16)
    grad_query = rows_product(normed_in, d_query)
    grad_key = rows_product(normed_in, d_key)
    grad_value = rows_product(normed_in, d_value)
    d_normed_terms = (
        cols_product(d_query, wq_back)
        + cols_product(d_key, wk_back)
        + cols_product(d_value, wv_back)
    )
    d_normed_in = lax.psum_scatter(
        d_normed_terms.astype(jnp.bfloat16), "tensor", scatter_dimension=0, tiled=True
    ).astype(jnp.float32)
    d_in_n, grad_g_in = jax.vjp(rms_scale, inputs_f, gain_in)[1](d_normed_in)
    d_inputs = (d_mid + d_in_n).astype(jnp.bfloat16)
    attn_part = jnp.concatenate(
        [grad_query, grad_key, grad_value, rows_product(d_proj, attended)], axis=1
    ).astype(BF)
    attn_part = pack_blocks(attn_part, n, rows)
    ffn_part = pack_ffn(
        grad_gate.astype(BF), grad_up.astype(BF), rows_product(d_feed, hidden).astype(BF), n * depth
    )
    ffn_part = jax.vmap(lambda a: pack_blocks(a, n, rows))(ffn_part)
    attn_sum, ffn_sum = ring_reduce(n, attn_part, ffn_part)
    attn_sum, ffn_sum = attn_sum[:depth], ffn_sum[:, :depth]
    sum_gate, sum_up, sum_down_t = unpack_ffn(ffn_sum, width)
    split_grads = (
        attn_sum[:, :HD],
        attn_sum[:, 3 * HD : 4 * HD].T,
        sum_gate,
        sum_up,
        sum_down_t.T,
    )
    sum_key, sum_value = attn_sum[:, HD : 2 * HD], attn_sum[:, 2 * HD : 3 * HD]
    shared = (
        lax.psum_scatter(sum_key, "tensor", scatter_dimension=0, tiled=True),
        lax.psum_scatter(sum_value, "tensor", scatter_dimension=0, tiled=True),
        lax.psum_scatter(grad_g_in, ("dp", "tensor"), scatter_dimension=0, tiled=True),
        lax.psum_scatter(grad_g_attn, ("dp", "tensor"), scatter_dimension=0, tiled=True),
        lax.psum_scatter(grad_g_pre, ("dp", "tensor"), scatter_dimension=0, tiled=True),
        lax.psum_scatter(grad_g_post, ("dp", "tensor"), scatter_dimension=0, tiled=True),
        lax.psum_scatter(grad_g_query, ("dp", "tensor"), scatter_dimension=0, tiled=True),
        lax.psum_scatter(grad_g_key, ("dp", "tensor"), scatter_dimension=0, tiled=True),
    )
    return (
        output,
        d_inputs,
        split_grads[0],
        shared[0],
        shared[1],
        split_grads[1],
        shared[2],
        shared[3],
        shared[6],
        shared[7],
        split_grads[2],
        split_grads[3],
        split_grads[4],
        shared[4],
        shared[5],
    )


SCALE = HD**-0.5
ROOT = 0.7978845608028654
CUBIC = 0.044715


def dot_nn(a, b):
    return jnp.dot(a, b, preferred_element_type=F32)


def dot_nt(a, b):
    return lax.dot_general(a, b, (((1,), (1,)), ((), ())), preferred_element_type=F32)


def dot_tn(a, b):
    return lax.dot_general(a, b, (((0,), (0,)), ((), ())), preferred_element_type=F32)


def inverse_rms(values):
    return lax.rsqrt(jnp.mean(values * values, axis=-1, keepdims=True) + EPSILON)


def rms_back(values, gain_vec, grad):
    inverse = inverse_rms(values)
    unit = values * inverse
    scaled = grad * gain_vec
    back = inverse * (scaled - unit * jnp.mean(scaled * unit, axis=-1, keepdims=True))
    return back, grad * unit


def gelu_parts(gate):
    bent = jnp.tanh(ROOT * (gate + CUBIC * gate * gate * gate))
    return 0.5 * gate * (1.0 + bent), bent


class Quad:
    def __init__(self, part, near, far, gather_sems, reduce_sems):
        self.me = lax.axis_index("tensor")
        self.twin = self.me + 1 - 2 * (self.me % 2)
        self.across = (self.me + 2) % 4
        self.corner = (self.twin + 2) % 4
        self.part, self.near, self.far = part, near, far
        self.gather_sems, self.reduce_sems = gather_sems, reduce_sems

    def copy(self, src, dst, sems, use, k, peer):
        return pltpu.make_async_remote_copy(
            src,
            dst,
            sems[0].at[use, k],
            sems[1].at[use, k],
            device_id={"tensor": peer},
            device_id_type=MESH,
        )

    def gather(self, use, k, buf):
        block = buf.at[self.across if k == 2 else self.me]
        peer = self.across if k == 1 else self.twin
        return self.copy(block, block, self.gather_sems, use, k, peer)

    def gather_start(self, use, buf):
        self.gather(use, 1, buf).start()
        self.gather(use, 0, buf).start()

    def gather_relay(self, use, buf):
        self.gather(use, 1, buf).wait_recv()
        self.gather(use, 2, buf).start()

    def gather_end(self, use, buf):
        self.gather(use, 0, buf).wait_recv()
        self.gather(use, 2, buf).wait_recv()
        for k in range(3):
            self.gather(use, k, buf).wait_send()

    def reduce(self, use, k):
        block = self.part.at[(self.twin, self.corner, self.across)[k]]
        land = self.far if k == 2 else self.near.at[k]
        peer = self.across if k == 2 else self.twin
        return self.copy(block, land, self.reduce_sems, use, k, peer)

    def reduce_start(self, use):
        self.reduce(use, 1).start()
        self.reduce(use, 0).start()

    def reduce_relay(self, use):
        self.reduce(use, 1).wait_recv()
        for low in range(0, self.part.shape[1], 64):
            rows = pl.ds(low, 64)
            total = self.part[self.across, rows].astype(F32) + self.near[1, rows].astype(F32)
            self.part[self.across, rows] = total.astype(BF)
        self.reduce(use, 2).start()

    def reduce_end(self, use):
        self.reduce(use, 0).wait_recv()
        self.reduce(use, 2).wait_recv()
        for k in range(3):
            self.reduce(use, k).wait_send()


class Octet:
    def __init__(self, part, near, far, bend, gather_sems, reduce_sems):
        tensor, dp = lax.axis_index("tensor"), lax.axis_index("dp")
        z = dp // 2
        self.low, self.x, self.core = z % 2, tensor // 2, tensor % 2
        self.twin = {"tensor": tensor + 1 - 2 * self.core}
        self.across = {"tensor": (tensor + 2) % 4}
        self.pair = {"dp": dp + 2 - 4 * self.low}
        self.part, self.near, self.far, self.bend = part, near, far, bend
        self.gather_sems, self.reduce_sems = gather_sems, reduce_sems

    def block(self, p, other=0):
        core = (self.core + other) % 2
        return (self.low + p // 2) % 2 * 4 + (self.x + p % 2) % 2 * 2 + core

    def copy(self, src, dst, sems, use, k, peer):
        return pltpu.make_async_remote_copy(
            src, dst, sems[0].at[use, k], sems[1].at[use, k], device_id=peer, device_id_type=MESH
        )

    def gather(self, use, k, buf, come=False):
        half = buf.shape[1] // 2
        if k < 2:
            place, peer = (k + 1 if come else 0), (self.across, self.pair)[k]
            ref = buf.at[self.block(place)]
        elif k < 6:
            ref = buf.at[self.block(k - 2, 1 if come else 0)]
            peer = self.twin
        else:
            place = 3 if come else k - 5
            ref = buf.at[self.block(place), pl.ds((k - 6) * half, half)]
            peer = (self.pair, self.across)[k - 6]
        return self.copy(ref, ref, self.gather_sems, use, k, peer)

    def gather_start(self, use, buf):
        for k in range(3):
            self.gather(use, k, buf).start()

    def gather_relay(self, use, buf, k):
        self.gather(use, k, buf, True).wait_recv()
        self.gather(use, 6 + k, buf).start()
        self.gather(use, 3 + k, buf).start()

    def gather_corner(self, use, buf):
        for k in (6, 7):
            self.gather(use, k, buf, True).wait_recv()
        self.gather(use, 5, buf).start()

    def gather_end(self, use, buf):
        for k in range(2, 6):
            self.gather(use, k, buf, True).wait_recv()
        for k in range(8):
            self.gather(use, k, buf).wait_send()

    def reduce(self, use, k):
        half = self.part.shape[1] // 2
        if k < 4:
            return self.copy(
                self.part.at[self.block(k, 1)], self.near.at[k], self.reduce_sems, use, k, self.twin
            )
        peer = (self.across, self.pair)[k % 2]
        if k < 6:
            src, dst = self.part.at[self.block(3), pl.ds((k - 4) * half, half)], self.bend.at[k - 4]
        else:
            src, dst = self.part.at[self.block(k - 5)], self.far.at[k - 6]
        return self.copy(src, dst, self.reduce_sems, use, k, peer)

    def add(self, place, low, count, came):
        step = 32

        def body(i, _):
            at = pl.multiple_of(i * step, step)
            rows = pl.ds(low + at, step)
            total = self.part[self.block(place), rows].astype(F32) + came[pl.ds(at, step)].astype(F32)
            self.part[self.block(place), rows] = total.astype(BF)
            return 0

        lax.fori_loop(0, count // step, body, 0)

    def reduce_start(self, use):
        for k in (3, 2, 1, 0):
            self.reduce(use, k).start()

    def reduce_corner(self, use):
        rows = self.part.shape[1]
        self.reduce(use, 3).wait_recv()
        self.add(3, 0, rows, self.near.at[3])
        self.reduce(use, 4).start()
        self.reduce(use, 5).start()
        for place in (2, 1):
            self.reduce(use, place).wait_recv()
            self.add(place, 0, rows, self.near.at[place])

    def reduce_relay(self, use):
        half = self.part.shape[1] // 2
        for k in range(2):
            self.reduce(use, 4 + k).wait_recv()
            self.add(2 - k, k * half, half, self.bend.at[k])
            self.reduce(use, 7 - k).start()

    def reduce_end(self, use):
        for k in (0, 6, 7):
            self.reduce(use, k).wait_recv()
        for k in range(8):
            self.reduce(use, k).wait_send()


class Columns:
    def __init__(self, ffn, other, land, gather_sems, reduce_sems):
        dp = lax.axis_index("dp")
        z, y = dp // 2, dp % 2
        self.low = z % 2
        self.inner = z * (3 - z) > 0
        self.outer = z * (3 - z) < 1
        ranks = (z, z + 1 - 2 * (z % 2), (z + 2) % 4, 3 - z)
        self.mine = [rank * 2 + y for rank in ranks]
        self.theirs = [rank * 2 + 1 - y for rank in ranks]
        self.ffn, self.other, self.land = ffn, other, land
        self.gather_sems, self.reduce_sems = gather_sems, reduce_sems

    def copy(self, src, dst, sems, u, send, recv, peer):
        return pltpu.make_async_remote_copy(
            src,
            dst,
            sems[0].at[u, send],
            sems[1].at[u, recv],
            device_id={"dp": peer},
            device_id_type=MESH,
        )

    def gather(self, u, k):
        own = self.ffn.at[u, self.mine[0]]
        sems = self.gather_sems
        if k == 0:
            return self.copy(own, own, sems, u, 0, 0, self.mine[2])
        if k == 1:
            return self.copy(self.other.at[u], own, sems, u, 1, 1, self.mine[1])
        if k == 2:
            return self.copy(self.other.at[u], own, sems, u, 2, 2, self.mine[3])
        if k == 3:
            block = self.ffn.at[u, self.mine[1]]
            return self.copy(block, block, sems, u, 3, 2, self.mine[2])
        block = self.ffn.at[u, self.mine[k - 4]]
        return self.copy(block, block, sems, u, k, k, self.theirs[0])

    def come(self, u, k):
        place = self.theirs[k - 4] if k >= 4 else self.mine[(2, 1, 3)[k]]
        block = self.ffn.at[u, place]
        self.copy(block, block, self.gather_sems, u, k, k, place).wait_recv()

    def gather_step(self, u, step):
        if step == 0:
            self.gather(u, 0).start()
            self.gather(u, 1).start()
            pl.when(self.inner)(lambda: self.gather(u, 2).start())
            self.gather(u, 4).start()
        elif step == 1:
            self.come(u, 1)
            pl.when(self.inner)(lambda: self.gather(u, 3).start())
            self.gather(u, 5).start()
        elif step == 2:
            self.come(u, 0)
            self.gather(u, 6).start()
        elif step == 3:
            self.come(u, 2)
            self.gather(u, 7).start()
        else:
            for k in range(4, 8):
                self.come(u, k)

    def gather_sends_done(self, u):
        for k in (0, 1, 4, 5, 6, 7):
            self.gather(u, k).wait_send()

        @pl.when(self.inner)
        def _():
            self.gather(u, 2).wait_send()
            self.gather(u, 3).wait_send()

    def piece(self, item, place):
        unit, count, lane, lanes = item[1:]
        return self.ffn.at[pl.ds(unit, count), place, :, pl.ds(lane, lanes)]

    def reduce(self, item, k):
        if k < 4:
            place, peer = self.theirs[k], self.theirs[0]
        else:
            place = self.mine[(2, 1, 3, 3)[k - 4]]
            peer = self.mine[(2, 1, 3, 2)[k - 4]]
        unit, count, lane, lanes = item[1:]
        land = self.land.at[pl.ds(unit, count), k, :, pl.ds(lane, lanes)]
        return self.copy(
            self.piece(item, place), land, self.reduce_sems, item[0], min(k, 6), k, peer
        )

    def came(self, item, k):
        unit, count, lane, lanes = item[1:]
        return [
            self.land[u, k, :, lane : lane + lanes].astype(F32) for u in range(unit, unit + count)
        ]

    def own(self, item, place):
        unit, count, lane, lanes = item[1:]
        return [
            self.ffn.at[u, self.mine[place], :, pl.ds(lane, lanes)]
            for u in range(unit, unit + count)
        ]

    def add(self, item, place, k):
        self.reduce(item, k).wait_recv()
        for own, came in zip(self.own(item, place), self.came(item, k), strict=True):
            own[...] = (own[...].astype(F32) + came).astype(BF)

    def reduce_step(self, item, step):
        if step == 0:
            for k in (3, 2, 1, 0):
                self.reduce(item, k).start()
        elif step == 1:
            self.add(item, 3, 3)
            pl.when(self.inner)(lambda: self.reduce(item, 6).start())
            pl.when(self.outer)(lambda: self.reduce(item, 7).start())
        elif step == 2:
            self.add(item, 2, 2)
            self.reduce(item, 4).start()
        else:
            self.add(item, 1, 1)
            pl.when(self.inner)(lambda: self.add(item, 1, 7))
            self.reduce(item, 5).start()

    def sum_own(self, item, out):
        for k in (0, 4):
            self.reduce(item, k).wait_recv()
        lanes = item[4]
        for i, (own, one, two) in enumerate(
            zip(self.own(item, 0), self.came(item, 0), self.came(item, 4), strict=True)
        ):
            out[:, i * lanes : (i + 1) * lanes] = own[...].astype(F32) + one + two

    def sum_other(self, item, out):
        self.reduce(item, 5).wait_recv()
        lanes = item[4]
        for i, came in enumerate(self.came(item, 5)):
            out[:, i * lanes : (i + 1) * lanes] = came

        @pl.when(self.inner)
        def _():
            self.reduce(item, 6).wait_recv()
            for i, came in enumerate(self.came(item, 6)):
                out[:, i * lanes : (i + 1) * lanes] += came

    def reduce_sends_done(self, item):
        for k in range(7):
            self.reduce(item, k).wait_send()


class Queue:
    def __init__(self):
        self.steps = []

    def add(self, tag, fn):
        self.steps.append((tag, fn))

    def run(self, count, ready=None):
        while count > 0 and self.steps:
            tag, fn = self.steps[0]
            if ready is not None and tag not in ready:
                return
            self.steps.pop(0)
            fn()
            count -= 1

    def until(self, tag):
        while any(t == tag for t, _ in self.steps):
            self.run(1)


def layer_kernel(
    n,
    x_ref,
    cot_ref,
    seg_row,
    freq_ref,
    gq_ref,
    gk_ref,
    attn_in,
    ffn_in,
    dx_ref,
    sums_ref,
    out_hbm,
    ggate_hbm,
    gup_hbm,
    gdown_hbm,
    attn,
    ffn,
    other,
    attn_land,
    ffn_land,
    gate_buf,
    up_buf,
    hid_buf,
    part,
    near,
    far,
    bend,
    xa,
    nm,
    df,
    dp_buf,
    proj_s,
    res_s,
    gains,
    gsum,
    gqk,
    q_proj,
    k_proj,
    qr,
    kr,
    vb,
    att,
    probs,
    cos_s,
    sin_s,
    stage,
    kvg,
    kvg_land,
    local_sem,
    stage_sem,
    ag_send,
    ag_recv,
    rs_send,
    rs_recv,
    cg_send,
    cg_recv,
    cr_send,
    cr_recv,
    og_send,
    og_recv,
    or_send,
    or_recv,
    qg_send,
    qg_recv,
    qr_send,
    qr_recv,
    kv_send,
    kv_recv,
):
    units, _, depth, cols = ffn.shape
    rows, width = x_ref.shape
    attn_cut = ((0, HD), (HD, 2 * HD), (2 * HD, 4 * HD), (4 * HD, attn.shape[-1]))
    parts = part_views(attn, attn_cut)
    landing = part_views(attn_land, attn_cut)
    first = len(attn_cut)
    ring = Ring(n, parts, ag_send, ag_recv)
    back = Ring(n, parts, rs_send, rs_recv, lambda p, slot: landing[p](slot))
    quad = Quad(part, near, far.at[0], (qg_send, qg_recv), (qr_send, qr_recv))
    octet = Octet(part, near, far, bend, (og_send, og_recv), (or_send, or_recv))
    columns = Columns(ffn, other, ffn_land, (cg_send, cg_recv), (cr_send, cr_recv))
    me, spot = quad.me, octet.block(0)

    def attn_cols(low, high):
        return attn[:, :, low:high].reshape(width, high - low)

    def unit_cols(u, k, count=1):
        return ffn[u, :, :, k * UNIT : (k + count) * UNIT].reshape(width, count * UNIT)

    def across_units(k, low=0, high=units):
        return jnp.concatenate([unit_cols(u, k) for u in range(low, high)], axis=1)

    mine = [
        pltpu.make_async_copy(attn_in, attn.at[ring.me], local_sem.at[0]),
        pltpu.make_async_copy(
            ffn_in.at[pl.ds(columns.low * units, units)], ffn.at[:, ring.me], local_sem.at[1]
        ),
        pltpu.make_async_copy(x_ref, xa.at[me], local_sem.at[2]),
        pltpu.make_async_copy(
            ffn_in.at[pl.ds((1 - columns.low) * units, units)], other, local_sem.at[3]
        ),
    ]
    for copy in mine:
        copy.start()
    barrier(
        [{"dp": peer} for peer in columns.mine[1:] + columns.theirs[:1]]
        + [{"tensor": quad.twin}, {"tensor": quad.across}]
    )
    for copy in mine:
        copy.wait()
    quad.gather_start(0, xa)

    queue = Queue()
    def ring_gather_step(parts, hop, tag):
        for p in parts:
            for way in range(2):
                if 0 < hop <= ring.reach(p, way) + 1:
                    queue.add(tag, partial(ring.gather_step, p, way, hop))

    for hop in range(1, n // 2 + 2):
        ring_gather_step((3, 1, 2), hop, -1)
        ring_gather_step((0,), hop - 2, -1)
        if hop == 3:
            queue.add(-1, partial(quad.gather_relay, 0, xa))
            queue.add(-1, partial(columns.gather_step, 0, 0))
    for hop in (n // 2, n // 2 + 1):
        ring_gather_step((0,), hop, -3)
        if hop == n // 2:
            for u in range(1, EARLY):
                queue.add(-3, partial(columns.gather_step, u, 0))
    for u in range(units):
        for step in range(1, 4):
            queue.add(-2, partial(columns.gather_step, u, step))
        if u + EARLY < units:
            queue.add(-2, partial(columns.gather_step, u + EARLY, 0))
        if u > 0:
            queue.add(u - 1, partial(columns.gather_step, u - 1, 4))
    queue.add(units - 1, partial(columns.gather_step, units - 1, 4))

    queue.run(AHEAD[0])
    quarter = SEGMAX // 2

    def seg_column(seg_j, half):
        cut = seg_j[:, half * quarter : (half + 1) * quarter].astype(F32)
        return jnp.transpose(jnp.broadcast_to(cut, (128, quarter)))[:, :1]

    def tables(tile, _):
        seg_j = seg_row[pl.ds(tile, 1), :]
        for half in range(2):
            r = 2 * tile + half
            same = seg_column(seg_j, half) == seg_j.astype(F32)
            j = lax.broadcasted_iota(jnp.int32, (quarter, SEGMAX), 1)
            start = jnp.min(jnp.where(same, j, SEGMAX).astype(F32), axis=1, keepdims=True)
            i = lax.broadcasted_iota(jnp.int32, (quarter, 1), 0).astype(F32) + half * quarter
            angle = (i - start) * freq_ref[...]
            cos_s[r] = jnp.cos(angle)
            sin_s[r] = jnp.sin(angle)
        return 0

    for tile in range(N_TILES):
        tables(tile, 0)
        queue.run(AHEAD[1])
    queue.until(-1)
    flipped = jnp.transpose(attn_cols(4 * HD, 4 * HD + 128).astype(F32))
    gains[...] = flipped[:8]
    quad.gather_end(0, xa)
    queue.run(AHEAD[2])

    sub = 32
    per = rows // sub

    def normalize(i, _):
        b, at = i // per, pl.ds(pl.multiple_of(i % per * sub, sub), sub)
        values = xa[b, at].astype(F32)
        xa[b, at] = (values * inverse_rms(values) * gains[0:1, :]).astype(BF)
        return 0

    lax.fori_loop(0, 4 * per, normalize, 0)

    def rope(values, gain_vec, r):
        normed = values * inverse_rms(values) * gain_vec
        low, high = normed[:, : HD // 2], normed[:, HD // 2 :]
        cosine, sine = cos_s[r], sin_s[r]
        return jnp.concatenate([low * cosine - high * sine, high * cosine + low * sine], axis=1)

    queue.run(AHEAD[3])

    def project(r, _):
        block = xa[r]
        query = dot_nn(block, attn_cols(HD, 2 * HD))
        q_proj[r] = query.astype(BF)
        qr[r] = rope(query, gq_ref[...], r).astype(BF)
        key = dot_nn(block, attn_cols(2 * HD, 3 * HD))
        k_proj[r] = key.astype(BF)
        kr[r] = rope(key, gk_ref[...], r).astype(BF)
        vb[r] = dot_nn(block, attn_cols(3 * HD, 4 * HD)).astype(BF)
        return 0

    lax.fori_loop(0, 4, project, 0)
    queue.run(AHEAD[4])

    def attend_tile(tile, _):
        two = pl.ds(2 * tile, 2)
        keys = kr[two].reshape(SEGMAX, HD)
        values = vb[two].reshape(SEGMAX, HD)
        seg_j = seg_row[pl.ds(tile, 1), :]
        for half in range(2):
            r = 2 * tile + half
            scores = dot_nt(qr[r], keys) * SCALE
            j = lax.broadcasted_iota(jnp.int32, (quarter, SEGMAX), 1)
            i = lax.broadcasted_iota(jnp.int32, (quarter, SEGMAX), 0) + half * quarter
            seen = (seg_column(seg_j, half) == seg_j.astype(F32)) & (i >= j)
            scores = jnp.where(seen, scores, NEG_LARGE)
            powers = jnp.exp(scores - jnp.max(scores, axis=1, keepdims=True))
            weights = (powers / jnp.sum(powers, axis=1, keepdims=True)).astype(BF)
            probs[r] = weights
            att[r] = dot_nn(weights, values).astype(BF)
        return 0

    lax.fori_loop(0, N_TILES, attend_tile, 0)
    queue.run(AHEAD[5])

    queue.until(-3)

    def out_block(r, _):
        part[r] = dot_nt(att[r], attn_cols(0, HD)).astype(BF)
        return 0

    lax.fori_loop(0, 4, out_block, 0)
    quad.reduce_start(0)
    queue.run(AHEAD[6])
    quad.reduce_relay(0)
    queue.run(AHEAD[7])
    quad.reduce_end(0)

    def total(at):
        return part[me, at].astype(F32) + near[0, at].astype(F32) + far[0, at].astype(F32)

    def total_ffn(at):
        return part[spot, at].astype(F32) + near[0, at].astype(F32) + (
            far[0, at].astype(F32) + far[1, at].astype(F32)
        )

    def at_rows(i):
        return pl.ds(pl.multiple_of(i * sub, sub), sub)

    def middle(i, _):
        at = at_rows(i)
        projected = total(at)
        proj_s[at] = projected.astype(BF)
        mid = x_ref[at].astype(F32) + projected * inverse_rms(projected) * gains[1:2, :]
        res_s[at] = mid
        nm[spot, at] = (mid * inverse_rms(mid) * gains[2:3, :]).astype(BF)
        return 0

    lax.fori_loop(0, per, middle, 0)
    octet.gather_start(0, nm)
    queue.run(AHEAD[8])
    octet.gather_relay(0, nm, 0)
    octet.gather_relay(0, nm, 1)
    queue.run(AHEAD[9])
    octet.gather_corner(0, nm)
    queue.run(AHEAD[9])
    octet.gather_end(0, nm)

    for u in range(units):
        queue.until(u)
        lanes = slice(u * UNIT, (u + 1) * UNIT)

        def ffn_block(r, _):
            both = dot_nn(nm[r], unit_cols(u, 0, 2))
            gate, up = both[:, :UNIT], both[:, UNIT:]
            gate_buf[r, :, lanes] = gate.astype(BF)
            up_buf[r, :, lanes] = up.astype(BF)
            hid_buf[r, :, lanes] = (gelu_parts(gate)[0] * up).astype(BF)
            return 0

        for low in range(0, 8, 4):
            lax.fori_loop(low, low + 4, ffn_block, 0)
            queue.run(AHEAD[10])
    queue.run(10**6)

    def feed_block(i, other):
        b = octet.block(3 - i, other)
        part[b] = dot_nt(hid_buf[b], across_units(2)).astype(BF)

    def feed_half(other):
        def body(i, _):
            feed_block(i, other)
            return 0

        lax.fori_loop(0, 4, body, 0)

    feed_half(1)
    octet.reduce_start(0)
    feed_half(0)
    octet.reduce_corner(0)
    for p in range(first):
        ring.gather_sends_done(p)
    for u in range(units):
        columns.gather_sends_done(u)
    octet.reduce_relay(0)
    octet.reduce_end(0)
    eight = (8, width)

    def fold(values):
        return jnp.sum(values.reshape(sub // 8, 8, values.shape[-1]), axis=0)

    def after_feed(i, carry):
        at = at_rows(i)
        feed = total_ffn(at)
        dx_ref[at] = (res_s[at] + feed * inverse_rms(feed) * gains[3:4, :]).astype(BF)
        grad, gain_part = rms_back(feed, gains[3:4, :], cot_ref[at].astype(F32))
        df[spot, at] = grad.astype(BF)
        return carry + fold(gain_part)

    gain_sum = lax.fori_loop(0, per, after_feed, jnp.zeros(eight, F32))
    gsum[3:4, :] = jnp.sum(gain_sum, axis=0, keepdims=True)
    put_out = pltpu.make_async_copy(dx_ref, out_hbm, local_sem.at[0])
    put_out.start()
    octet.gather_start(1, df)
    octet.gather_relay(1, df, 0)
    octet.gather_relay(1, df, 1)
    octet.gather_corner(1, df)
    octet.gather_end(1, df)

    queue = Queue()
    pending = []

    def finish(item, other):
        k = len(pending)
        if k >= 2:
            for copy in pending[k - 2]:
                copy.wait()
        (columns.sum_other if other else columns.sum_own)(item, stage.at[k % 2])
        half = 1 - columns.low if other else columns.low
        unit, count, lane, lanes = item[1:]
        at = pl.multiple_of(half * (units * UNIT) + unit * UNIT, UNIT)
        outs = ((ggate_hbm, UNIT), (gup_hbm, UNIT)) if lane == 0 else ((gdown_hbm, count * UNIT),)
        copies = [
            pltpu.make_async_copy(
                stage.at[k % 2, :, pl.ds(which * UNIT, wide)],
                hbm.at[:, pl.ds(at, wide)],
                stage_sem.at[k % 2, which],
            )
            for which, (hbm, wide) in enumerate(outs)
        ]
        for copy in copies:
            copy.start()
        pending.append(copies)

    pairs = [(low, min(low + 2, units)) for low in range(0, units, 2)]
    items = [(k, low, high - low, 2 * UNIT, UNIT) for k, (low, high) in enumerate(pairs)]
    items += [(len(pairs) + u, u, 1, 0, 2 * UNIT) for u in range(units)]
    queue.add(0, partial(columns.reduce_step, items[0], 0))
    for k, item in enumerate(items):
        if k + 1 < len(items):
            queue.add(k + 1, partial(columns.reduce_step, items[k + 1], 0))
        for step in range(1, 4):
            queue.add(k, partial(columns.reduce_step, item, step))
        if k > 0:
            queue.add(k - 1, partial(finish, items[k - 1], False))
            queue.add(k - 1, partial(finish, items[k - 1], True))
    queue.add(len(items) - 1, partial(finish, items[-1], False))
    queue.add(len(items) - 1, partial(finish, items[-1], True))
    ready = set()
    def tall(ref, lanes):
        return ref[:, :, lanes].reshape(8 * rows, lanes.stop - lanes.start)

    def down_grad(low, high):
        value = dot_tn(df[...].reshape(8 * rows, width), tall(hid_buf, slice(low * UNIT, high * UNIT)))
        value = value.astype(BF)
        for u in range(low, high):
            piece = value[:, (u - low) * UNIT : (u - low + 1) * UNIT]
            ffn[u, :, :, 2 * UNIT :] = piece.reshape(n, depth, UNIT)
        ready.add(low // 2)

    for low, high in pairs:
        lanes = slice(low * UNIT, high * UNIT)

        def back_block(r, _):
            grad = dot_nn(df[r], across_units(2, low, high))
            gate, up = gate_buf[r, :, lanes].astype(F32), up_buf[r, :, lanes].astype(F32)
            act, bent = gelu_parts(gate)
            slope = 0.5 * (1.0 + bent) + 0.5 * gate * (1.0 - bent * bent) * ROOT * (
                1.0 + 3.0 * CUBIC * gate * gate
            )
            gate_buf[r, :, lanes] = (grad * up * slope).astype(BF)
            up_buf[r, :, lanes] = (grad * act).astype(BF)
            return 0

        for start in (0, 4):
            lax.fori_loop(start, start + 4, back_block, 0)
            queue.run(PACE[0], ready)
        down_grad(low, high)
        queue.run(PACE[0], ready)

    def back_half(other):
        def body(i, _):
            b = octet.block(3 - i, other)
            grown = dot_nt(gate_buf[b], across_units(0)) + dot_nt(up_buf[b], across_units(1))
            part[b] = grown.astype(BF)
            return 0

        for start in (0, 2):
            lax.fori_loop(start, start + 2, body, 0)
            queue.run(PACE[0], ready)

    def gate_grad(u):
        lanes = slice(u * UNIT, (u + 1) * UNIT)
        both = jnp.concatenate([tall(gate_buf, lanes), tall(up_buf, lanes)], axis=1)
        value = dot_tn(nm[...].reshape(8 * rows, width), both)
        ffn[u, :, :, : 2 * UNIT] = value.astype(BF).reshape(n, depth, 2 * UNIT)
        ready.add(len(pairs) + u)

    work = [partial(gate_grad, u) for u in range(units)]

    def do_work(count):
        for _ in range(count):
            if work:
                work.pop(0)()
                queue.run(PACE[1], ready)

    back_half(1)
    octet.reduce_start(1)
    back_half(0)
    octet.reduce_corner(1)
    do_work(WORK[0])
    octet.reduce_relay(1)
    do_work(WORK[1])
    queue.run(PACE[2], ready)
    octet.reduce_end(1)

    def after_ffn(i, carry):
        at = at_rows(i)
        grad, pre_part = rms_back(res_s[at], gains[2:3, :], total_ffn(at))
        grad = cot_ref[at].astype(F32) + grad
        res_s[at] = grad
        grad, attn_part = rms_back(proj_s[at].astype(F32), gains[1:2, :], grad)
        dp_buf[me, at] = grad.astype(BF)
        return carry[0] + fold(pre_part), carry[1] + fold(attn_part)

    zero = jnp.zeros(eight, F32)
    pre_sum, attn_sum = lax.fori_loop(0, per, after_ffn, (zero, zero))
    gsum[2:3, :] = jnp.sum(pre_sum, axis=0, keepdims=True)
    gsum[1:2, :] = jnp.sum(attn_sum, axis=0, keepdims=True)
    quad.gather_start(1, dp_buf)
    do_work(WORK[2])
    queue.run(PACE[3], ready)
    quad.gather_relay(1, dp_buf)
    do_work(len(work))
    queue.run(PACE[4], ready)
    quad.gather_end(1, dp_buf)

    d_q, d_k, d_v = (gate_buf.at[pl.ds(0, 4), :, pl.ds(k * HD, HD)] for k in range(3))
    datt = up_buf.at[pl.ds(0, 4), :, pl.ds(0, HD)]

    def attn_grad(low, left, right):
        value = dot_tn(left.reshape(4 * rows, width), right.reshape(4 * rows, HD))
        attn[:, :, low : low + HD] = value.astype(BF).reshape(n, width // n, HD)

    def ring_steps(*some):
        for hop in range(1, n // 2 + 1):
            for p in some:
                for way in range(2):
                    if hop <= back.reach(p, way):
                        queue.add(-1, partial(back.reduce_step, p, way, hop))

    ready.add(-1)
    def back_out(r, _):
        datt[r] = dot_nn(dp_buf[r], attn_cols(0, HD)).astype(BF)
        return 0

    lax.fori_loop(0, 4, back_out, 0)
    attn_grad(0, dp_buf[...], att[...])
    ring_steps(0)
    queue.run(PACE[5], ready)
    gqk[...] = jnp.zeros_like(gqk)

    def unrope(grad, projection, gain_vec, r, row):
        low, high = grad[:, : HD // 2], grad[:, HD // 2 :]
        cosine, sine = cos_s[r], sin_s[r]
        grad = jnp.concatenate([low * cosine + high * sine, high * cosine - low * sine], axis=1)
        grad, gain_part = rms_back(projection, gain_vec, grad)
        gqk[row : row + 1, :] += jnp.sum(gain_part, axis=0, keepdims=True)
        return grad.astype(BF)

    def back_tile(tile, _):
        two = pl.ds(2 * tile, 2)
        keys = kr[two].reshape(SEGMAX, HD)
        values = vb[two].reshape(SEGMAX, HD)
        d_key = jnp.zeros((SEGMAX, HD), F32)
        d_value = jnp.zeros((SEGMAX, HD), F32)
        for half in range(2):
            r = 2 * tile + half
            d_att = datt[r]
            weights = probs[r]
            d_value = d_value + dot_tn(weights, d_att)
            d_probs = dot_nt(d_att, values)
            weights = weights.astype(F32)
            delta = jnp.sum(weights * d_probs, axis=1, keepdims=True)
            d_scores = (weights * (d_probs - delta) * SCALE).astype(BF)
            d_key = d_key + dot_tn(d_scores, qr[r])
            d_query = dot_nn(d_scores, keys)
            d_q[r] = unrope(d_query, q_proj[r].astype(F32), gq_ref[...], r, 4)
        for half in range(2):
            r = 2 * tile + half
            cut = slice(half * quarter, (half + 1) * quarter)
            d_k[r] = unrope(d_key[cut], k_proj[r].astype(F32), gk_ref[...], r, 5)
            d_v[r] = d_value[cut].astype(BF)
        return 0

    for tile in range(N_TILES):
        back_tile(tile, 0)
        queue.run(PACE[5], ready)

    def back_in(r, _):
        grown = dot_nt(d_q[r], attn_cols(HD, 2 * HD))
        grown = grown + dot_nt(d_k[r], attn_cols(2 * HD, 3 * HD))
        grown = grown + dot_nt(d_v[r], attn_cols(3 * HD, 4 * HD))
        part[r] = grown.astype(BF)
        return 0

    lax.fori_loop(0, 4, back_in, 0)
    quad.reduce_start(1)
    queue.run(PACE[5], ready)

    for k, grad in enumerate((d_q, d_k, d_v)):
        attn_grad((k + 1) * HD, xa[...], grad[...])
        queue.run(PACE[5], ready)
    def input_gain(i, carry):
        b, at = i // per, pl.ds(pl.multiple_of(i % per * sub, sub), sub)
        return carry + fold(part[b, at].astype(F32) * xa[b, at].astype(F32))

    gain_sum = lax.fori_loop(0, 4 * per, input_gain, zero)
    gsum[0:1, :] = jnp.sum(gain_sum, axis=0, keepdims=True) / gains[0:1, :]
    gsum[4:8, :] = jnp.zeros((4, width), F32)
    long = jnp.concatenate([gsum[...], jnp.zeros((120, width), F32)], axis=0)
    long = jnp.transpose(long).reshape(n, width // n, 128)
    short = jnp.concatenate([gqk[...], jnp.zeros((120, HD), F32)], axis=0)
    short = jnp.transpose(short).reshape(n, HD // n, 128)
    attn[:, :, 4 * HD : 4 * HD + 128] = long.astype(BF)
    attn[:, : HD // n, 4 * HD : 4 * HD + 128] = (long[:, : HD // n] + short).astype(BF)

    ring_steps(3, 1, 2)
    queue.run(PACE[6], ready)
    quad.reduce_relay(1)
    queue.run(PACE[7], ready)
    quad.reduce_end(1)
    put_out.wait()

    def after_attn(i, _):
        at = at_rows(i)
        grad, _ = rms_back(x_ref[at].astype(F32), gains[0:1, :], total(at))
        dx_ref[at] = (res_s[at] + grad).astype(BF)
        return 0

    lax.fori_loop(0, per, after_attn, 0)
    queue.run(10**6)
    for p in range(2):
        sums_ref[:, p * HD : (p + 1) * HD] = back.reduce_end(p)
    kvg[0, :, : 2 * HD] = back.reduce_end(2).astype(BF)
    kvg[0, :, 2 * HD :] = back.reduce_end(3).astype(BF)
    for k, peer in enumerate((quad.twin, quad.across)):
        copy = pltpu.make_async_remote_copy(
            kvg.at[k],
            kvg_land.at[k],
            kv_send.at[k],
            kv_recv.at[k],
            device_id={"tensor": peer},
            device_id_type=MESH,
        )
        copy.start()
        copy.wait()
        grown = kvg[k].astype(F32) + kvg_land[k].astype(F32)
        if k == 0:
            kvg[1] = grown.astype(BF)
        else:
            sums_ref[:, 2 * HD :] = grown
    for p in range(len(parts)):
        back.reduce_sends_done(p)
    for item in items:
        columns.reduce_sends_done(item)
    for copies in pending[-2:]:
        for copy in copies:
            copy.wait()


AHEAD = (8, 6, 0, 2, 2, 2, 0, 6, 4, 4, 1)
PACE = (2, 2, 4, 5, 4, 3, 4, 6)
WORK = (2, 3, 2)
EARLY = 2
UNIT = 128
N_TILES = 2


def run_layer(n, x, cot, segments, g_query, g_key, attn_pack, ffn_pack):
    rows, width = x.shape
    both, depth, cols = ffn_pack.shape
    units = both // 2
    tokens = segments.shape[0]
    wide = attn_pack.shape[1]
    parts = 4
    exponent = -2.0 * jnp.arange(HD // 2, dtype=F32) / HD
    freq = jnp.power(jnp.float32(THETA), exponent)[None, :]
    vmem, dma = pltpu.VMEM, pltpu.SemaphoreType.DMA
    grown = both * UNIT
    return pl.pallas_call(
        partial(layer_kernel, n),
        out_shape=(
            jax.ShapeDtypeStruct((rows, width), BF),
            jax.ShapeDtypeStruct((depth, wide), F32),
            jax.ShapeDtypeStruct((rows, width), BF),
            jax.ShapeDtypeStruct((depth, grown), F32),
            jax.ShapeDtypeStruct((depth, grown), F32),
            jax.ShapeDtypeStruct((depth, grown), F32),
        ),
        in_specs=vmem_specs(6) + any_specs(2),
        out_specs=vmem_specs(2) + any_specs(4),
        scratch_shapes=[
            vmem((n, depth, wide), BF),
            vmem((units, n, depth, cols), BF),
            vmem((units, depth, cols), BF),
            vmem((n - 1, depth, wide), BF),
            vmem((units, 8, depth, cols), BF),
            vmem((8, rows, units * UNIT), BF),
            vmem((8, rows, units * UNIT), BF),
            vmem((8, rows, units * UNIT), BF),
            vmem((8, rows, width), BF),
            vmem((4, rows, width), BF),
            vmem((2, rows, width), BF),
            vmem((2, rows // 2, width), BF),
            vmem((4, rows, width), BF),
            vmem((8, rows, width), BF),
            vmem((8, rows, width), BF),
            vmem((4, rows, width), BF),
            vmem((rows, width), BF),
            vmem((rows, width), F32),
            vmem((8, width), F32),
            vmem((8, width), F32),
            vmem((8, HD), F32),
            vmem((4, rows, HD), BF),
            vmem((4, rows, HD), BF),
            vmem((4, rows, HD), BF),
            vmem((4, rows, HD), BF),
            vmem((4, rows, HD), BF),
            vmem((4, rows, HD), BF),
            vmem((4, rows, SEGMAX), BF),
            vmem((4, rows, HD // 2), F32),
            vmem((4, rows, HD // 2), F32),
            vmem((2, depth, 2 * UNIT), F32),
            vmem((2, depth, wide - 2 * HD), BF),
            vmem((2, depth, wide - 2 * HD), BF),
            dma((4,)),
            dma((2, 3)),
            dma((parts, 2, n // 2)),
            dma((parts, 2, n // 2)),
            dma((parts, 2, n // 2)),
            dma((parts, 2, n // 2)),
            dma((units, 8)),
            dma((units, 8)),
            dma((units + (units + 1) // 2, 8)),
            dma((units + (units + 1) // 2, 8)),
            dma((2, 8)),
            dma((2, 8)),
            dma((2, 8)),
            dma((2, 8)),
            dma((2, 3)),
            dma((2, 3)),
            dma((2, 3)),
            dma((2, 3)),
            dma((2,)),
            dma((2,)),
        ],
        compiler_params=pltpu.CompilerParams(
            collective_id=2, has_side_effects=True, vmem_limit_bytes=67043328
        ),
    )(
        x,
        cot,
        segments.reshape(N_TILES, SEGMAX),
        freq,
        g_query.astype(F32)[None, :],
        g_key.astype(F32)[None, :],
        attn_pack,
        ffn_pack,
    )


def fused_local(
    inputs, segments, w_query, w_key, w_value, w_out, g_in, g_attn, g_query, g_key,
    w_gate, w_up, w_down, g_pre, g_post, cotangent,
):
    n = lax.axis_size("dp")
    depth = w_query.shape[0]
    width = w_gate.shape[1]
    gains = jnp.stack([g_in, g_attn, g_pre, g_post], axis=1)
    attn_pack = jnp.concatenate(
        [w_out.T, w_query, w_key, w_value, jnp.pad(gains, ((0, 0), (0, 124)))], axis=1
    )
    ffn_pack = pack_ffn(w_gate, w_up, w_down.T, depth, UNIT)
    d_inputs, sums, output, g_gate, g_up, g_down = run_layer(
        n, inputs, cotangent, segments, g_query, g_key, attn_pack, ffn_pack
    )
    spot = lax.axis_index("tensor")
    part = depth // 4
    mine = lax.dynamic_slice_in_dim(sums[:, 2 * HD :], spot * part, part, 0)
    small = HD // n // 4
    few = lax.dynamic_slice_in_dim(sums[:, 4 * HD :], spot * small, small, 0)
    return (
        output,
        d_inputs,
        sums[:, HD : 2 * HD],
        mine[:, :HD],
        mine[:, HD : 2 * HD],
        sums[:, :HD].T,
        mine[:, 2 * HD],
        mine[:, 2 * HD + 1],
        few[:, 4],
        few[:, 5],
        g_gate[:, :width],
        g_up[:, :width],
        g_down[:, :width].T,
        mine[:, 2 * HD + 2],
        mine[:, 2 * HD + 3],
    )


def fits(mesh, depth, tokens, rows):
    return mesh.shape["dp"] == 8 and depth % 16 == 0 and mesh.shape["tensor"] == 4 and tokens == 2 * SEGMAX


def layer(mesh):
    def body(*args):
        inputs, segments, w_query = args[0], args[1], args[2]
        if fits(mesh, w_query.shape[0], segments.shape[0], inputs.shape[0]):
            return fused_local(*args)
        return local(*args)

    return body


def solution(mesh):
    return jax.shard_map(
        layer(mesh),
        mesh=mesh,
        in_specs=(
            P(("dp", "tensor"), None),
            P("dp"),
            P("dp", "tensor"),
            P("dp", None),
            P("dp", None),
            P("tensor", "dp"),
            P("dp"),
            P("dp"),
            P(),
            P(),
            P("dp", "tensor"),
            P("dp", "tensor"),
            P("tensor", "dp"),
            P("dp"),
            P("dp"),
            P(("dp", "tensor"), None),
        ),
        out_specs=(
            P(("dp", "tensor"), None),
            P(("dp", "tensor"), None),
            P("dp", "tensor"),
            P(("dp", "tensor"), None),
            P(("dp", "tensor"), None),
            P("tensor", "dp"),
            P(("dp", "tensor")),
            P(("dp", "tensor")),
            P(("dp", "tensor")),
            P(("dp", "tensor")),
            P("dp", "tensor"),
            P("dp", "tensor"),
            P("tensor", "dp"),
            P(("dp", "tensor")),
            P(("dp", "tensor")),
        ),
        check_vma=False,
    )
```

```python
from functools import partial

import jax
import jax.numpy as jnp
from jax import lax
from jax.experimental import pallas as pl
from jax.experimental.pallas import tpu as pltpu
from jax.sharding import PartitionSpec as P

HD = 256
SEGMAX = 512
MESH = pl.DeviceIdType.MESH
BF = jnp.bfloat16
F32 = jnp.float32


def ring_pos(dev, n):
    return (1 - dev % 2) * (dev // 2) + (dev % 2) * (n - 1 - dev // 2)


def ring_dev(pos, n):
    high = pos // (n // 2)
    return (1 - high) * (2 * pos) + high * (2 * (n - 1 - pos) + 1)


def barrier(peers):
    sem = pltpu.get_barrier_semaphore()
    for peer in peers:
        pl.semaphore_signal(sem, inc=1, device_id=peer, device_id_type=MESH)
    pl.semaphore_wait(sem, len(peers))


def reach(bias, way, n):
    return n // 2 if bias == way else n // 2 - 1


class Ring:
    def __init__(self, n, parts, send_sem, recv_sem, land=None):
        self.n, self.parts, self.land = n, parts, land
        self.send_sem, self.recv_sem = send_sem, recv_sem
        self.me = lax.axis_index("dp")
        self.pos = ring_pos(self.me, n)
        self.peer = [{"dp": self.dev(1)}, {"dp": self.dev(-1)}]

    def dev(self, offset):
        return ring_dev((self.pos + (offset + self.n) % self.n) % self.n, self.n)

    def reach(self, part, way):
        return reach(part % 2, way, self.n)

    def gather(self, part, way, hop, ahead):
        away = hop - 1 if ahead else hop
        block = self.parts[part](self.dev(-away if way == 0 else away))
        return pltpu.make_async_remote_copy(
            block,
            block,
            self.send_sem.at[part, way, hop - 1],
            self.recv_sem.at[part, way, hop - 1],
            device_id=self.peer[way],
            device_id_type=MESH,
        )

    def gather_step(self, part, way, hop):
        if hop > 1:
            self.gather(part, way, hop - 1, False).wait_recv()
        if hop <= self.reach(part, way):
            self.gather(part, way, hop, True).start()

    def gather_sends_done(self, part):
        for way in range(2):
            for hop in range(1, self.reach(part, way) + 1):
                self.gather(part, way, hop, True).wait_send()

    def target(self, part, way, hop):
        away = self.reach(part, way) - hop + 1
        return self.dev(away if way == 0 else -away)

    def slot(self, part, way, hop):
        return self.land(part, hop - 1 + (self.reach(part, 0) if way else 0))

    def reduce(self, part, way, hop):
        return pltpu.make_async_remote_copy(
            self.parts[part](self.target(part, way, hop)),
            self.slot(part, way, hop),
            self.send_sem.at[part, way, hop - 1],
            self.recv_sem.at[part, way, hop - 1],
            device_id=self.peer[way],
            device_id_type=MESH,
        )

    def reduce_step(self, part, way, hop):
        if hop > self.reach(part, way):
            return
        if hop > 1:
            self.reduce(part, way, hop - 1).wait_recv()
            own = self.parts[part](self.target(part, way, hop))
            came = self.slot(part, way, hop - 1)
            own[...] = (own[...].astype(F32) + came[...].astype(F32)).astype(BF)
        self.reduce(part, way, hop).start()

    def reduce_end(self, part):
        total = self.parts[part](self.me)[...].astype(F32)
        for way in range(2):
            last = self.reach(part, way)
            self.reduce(part, way, last).wait_recv()
            total = total + self.slot(part, way, last)[...].astype(F32)
        return total

    def reduce_sends_done(self, part):
        for way in range(2):
            for hop in range(1, self.reach(part, way) + 1):
                self.reduce(part, way, hop).wait_send()


def part_views(attn, attn_cut, ffn=None, ffn_cut=()):
    views = []
    for low, high in attn_cut:
        views.append(lambda b, low=low, high=high: attn.at[b, :, pl.ds(low, high - low)])
    for chunk in range(0 if ffn is None else ffn.shape[0]):
        for low, high in ffn_cut:
            views.append(
                lambda b, c=chunk, low=low, high=high: ffn.at[c, b, :, pl.ds(low, high - low)]
            )
    return views


def halves(cols, step=128):
    mid = cols // 2 // step * step
    return ((0, mid), (mid, cols))


def gather_kernel(n, attn_ref, ffn_ref, attn_out, ffn_out, local_sem, send_sem, recv_sem):
    parts = part_views(attn_out, halves(attn_ref.shape[-1]), ffn_out, halves(ffn_ref.shape[-1]))
    ring = Ring(n, parts, send_sem, recv_sem)
    mine = [
        pltpu.make_async_copy(attn_ref, attn_out.at[ring.me], local_sem.at[0]),
        pltpu.make_async_copy(ffn_ref, ffn_out.at[:, ring.me], local_sem.at[1]),
    ]
    for copy in mine:
        copy.start()
    barrier(ring.peer)
    for copy in mine:
        copy.wait()
    width = 4
    for low in range(0, len(parts), width):
        for hop in range(1, n // 2 + 2):
            for part in range(low, min(low + width, len(parts))):
                for way in range(2):
                    if hop <= ring.reach(part, way) + 1:
                        ring.gather_step(part, way, hop)
    for part in range(len(parts)):
        ring.gather_sends_done(part)


def reduce_kernel(n, attn_ref, ffn_ref, attn_out, ffn_out, attn_buf, ffn_buf, attn_land, ffn_land, local_sem, send_sem, recv_sem):
    acut, fcut = halves(attn_ref.shape[-1]), halves(ffn_ref.shape[-1])
    parts = part_views(attn_buf, acut, ffn_buf, fcut)
    landing = part_views(attn_land, acut, ffn_land, fcut)
    ring = Ring(n, parts, send_sem, recv_sem, lambda part, slot: landing[part](slot))
    load = [
        pltpu.make_async_copy(attn_ref, attn_buf, local_sem.at[0]),
        pltpu.make_async_copy(ffn_ref, ffn_buf, local_sem.at[1]),
    ]
    for copy in load:
        copy.start()
    barrier(ring.peer)
    for copy in load:
        copy.wait()
    width = 4
    for low in range(0, len(parts), width):
        for hop in range(1, n // 2 + 1):
            for part in range(low, min(low + width, len(parts))):
                for way in range(2):
                    ring.reduce_step(part, way, hop)
        for part in range(low, min(low + width, len(parts))):
            total = ring.reduce_end(part)
            if part < 2:
                attn_out[:, acut[part][0] : acut[part][1]] = total
            else:
                cut = fcut[part % 2]
                ffn_out[part // 2 - 1, :, cut[0] : cut[1]] = total
    for part in range(len(parts)):
        ring.reduce_sends_done(part)


VMEM_LIMIT = 60 * 2**20


def vmem_specs(count):
    return [pl.BlockSpec(memory_space=pltpu.VMEM)] * count


def any_specs(count):
    return [pl.BlockSpec(memory_space=pl.ANY)] * count


def ring_gather(n, attn, ffn):
    chunks = ffn.shape[0]
    sems = pltpu.SemaphoreType.DMA((2 * (chunks + 1), 2, n // 2))
    return pl.pallas_call(
        partial(gather_kernel, n),
        out_shape=(
            jax.ShapeDtypeStruct((n,) + attn.shape, BF),
            jax.ShapeDtypeStruct((chunks, n) + ffn.shape[1:], BF),
        ),
        in_specs=any_specs(2),
        out_specs=vmem_specs(2),
        scratch_shapes=[pltpu.SemaphoreType.DMA((2,)), sems, sems],
        compiler_params=pltpu.CompilerParams(
            collective_id=0, has_side_effects=True, vmem_limit_bytes=VMEM_LIMIT
        ),
    )(attn, ffn)


def ring_reduce(n, attn, ffn):
    chunks, _, rows, cols = ffn.shape
    sems = pltpu.SemaphoreType.DMA((2 * (chunks + 1), 2, n // 2))
    return pl.pallas_call(
        partial(reduce_kernel, n),
        out_shape=(
            jax.ShapeDtypeStruct(attn.shape[1:], F32),
            jax.ShapeDtypeStruct((chunks, rows, cols), F32),
        ),
        in_specs=any_specs(2),
        out_specs=vmem_specs(2),
        scratch_shapes=[
            pltpu.VMEM(attn.shape, BF),
            pltpu.VMEM(ffn.shape, BF),
            pltpu.VMEM((n - 1,) + attn.shape[1:], BF),
            pltpu.VMEM((chunks, n - 1, rows, cols), BF),
            pltpu.SemaphoreType.DMA((2,)),
            sems,
            sems,
        ],
        compiler_params=pltpu.CompilerParams(
            collective_id=1, has_side_effects=True, vmem_limit_bytes=VMEM_LIMIT
        ),
    )(attn, ffn)


CHUNK = 256


def pack_rows(array, rows):
    return jnp.pad(array, ((0, rows - array.shape[0]), (0, 0)))


def pack_ffn(gate, up, down_t, rows, step=CHUNK):
    width = gate.shape[1]
    chunks = -(-width // step)
    chunks += chunks % 2 if step != CHUNK else 0

    def cut(array):
        array = jnp.pad(array, ((0, rows - array.shape[0]), (0, chunks * step - width)))
        return array.reshape(rows, chunks, step).transpose(1, 0, 2)

    return jnp.concatenate([cut(gate), cut(up), cut(down_t)], axis=2)


def unpack_ffn(packed, width):
    chunks, rows = packed.shape[:2]
    out = []
    for k in range(3):
        piece = packed[:, :, k * CHUNK : (k + 1) * CHUNK]
        out.append(piece.transpose(1, 0, 2).reshape(rows, chunks * CHUNK)[:, :width])
    return out


def pack_blocks(array, n, rows):
    depth = array.shape[0] // n
    return jnp.pad(array.reshape(n, depth, -1), ((0, 0), (0, rows - depth), (0, 0)))


EPSILON = 1e-06
THETA = 1000000.0
NEG_LARGE = -1e30


def rms_scale(values, gain_vec):
    inverse = lax.rsqrt(jnp.mean(values * values, axis=-1, keepdims=True) + EPSILON)
    return values * inverse * gain_vec


def gelu_product(gate_proj, up_proj):
    return jax.nn.gelu(gate_proj, approximate=True) * up_proj


def rows_product(left, right):
    return lax.dot_general(
        left, right, (((0,), (0,)), ((), ())), preferred_element_type=jnp.float32
    )


def cols_product(left, right):
    return lax.dot_general(
        left, right, (((1,), (1,)), ((), ())), preferred_element_type=jnp.float32
    )


def plain_product(left, right):
    return jnp.dot(left, right, preferred_element_type=jnp.float32)


def rotary_tables(segments):
    count = segments.shape[0]
    row_index = jnp.arange(count, dtype=jnp.int32)
    previous = jnp.concatenate([jnp.full((1,), -1, jnp.int32), segments[:-1]])
    starts = jnp.where(segments != previous, row_index, jnp.zeros_like(row_index))
    seq_start = lax.cummax(starts, axis=0)
    position = (row_index - seq_start).astype(jnp.float32)
    half_width = HD // 2
    exponent = -2.0 * jnp.arange(half_width, dtype=jnp.float32) / HD
    inverse = jnp.power(jnp.float32(THETA), exponent)
    angles = position[:, None] * inverse[None, :]
    cosine = jnp.concatenate([jnp.cos(angles), jnp.cos(angles)], axis=1)
    sine_tab = jnp.concatenate([jnp.sin(angles), jnp.sin(angles)], axis=1)
    return (cosine, sine_tab)


def prepare(projection, gain_vec, cosine, sine_tab):
    normed = rms_scale(projection, gain_vec)
    half_width = HD // 2
    turned = jnp.concatenate([-normed[..., half_width:], normed[..., :half_width]], axis=-1)
    return normed * cosine[:, None, :] + turned * sine_tab[:, None, :]


def visible(segments):
    tile_count = segments.shape[0] // SEGMAX
    seg_tiles = segments.reshape(tile_count, SEGMAX)
    offsets = jnp.arange(SEGMAX, dtype=jnp.int32)
    same = seg_tiles[:, :, None] == seg_tiles[:, None, :]
    return same & (offsets[:, None] >= offsets[None, :])


def tile_scores(query_tiles, key_tiles, segments):
    head_width = key_tiles.shape[-1]
    scores = jnp.einsum(
        "tqhd,tkd->thqk", query_tiles, key_tiles, preferred_element_type=jnp.float32
    ) * head_width ** (-0.5)
    return jnp.where(visible(segments)[:, None], scores, NEG_LARGE)


def attend(query_ready, key_ready, value_b, segments):
    row_count, head_count, head_width = query_ready.shape
    tile_count = row_count // SEGMAX
    query_tiles = query_ready.reshape(tile_count, SEGMAX, head_count, head_width)
    key_tiles = key_ready.reshape(tile_count, SEGMAX, head_width)
    value_tiles = value_b.reshape(tile_count, SEGMAX, head_width)
    scores = tile_scores(query_tiles, key_tiles, segments)
    row_max = jnp.max(scores, axis=-1, keepdims=True)
    row_total = jnp.sum(jnp.exp(scores - row_max), axis=-1, keepdims=True)
    log_total = row_max + jnp.log(row_total)
    probs = jnp.exp(scores - log_total).astype(jnp.bfloat16)
    attended = jnp.einsum("thqk,tkd->tqhd", probs, value_tiles, preferred_element_type=jnp.float32)
    return (attended.reshape(row_count, head_count * head_width).astype(jnp.bfloat16), log_total)


def attend_back(query_ready, key_ready, value_b, segments, log_total, d_attended):
    row_count, head_count, head_width = query_ready.shape
    tile_count = row_count // SEGMAX
    query_tiles = query_ready.reshape(tile_count, SEGMAX, head_count, head_width)
    key_tiles = key_ready.reshape(tile_count, SEGMAX, head_width)
    value_tiles = value_b.reshape(tile_count, SEGMAX, head_width)
    grad_tiles = d_attended.reshape(tile_count, SEGMAX, head_count, head_width)
    scores = tile_scores(query_tiles, key_tiles, segments)
    prob_vals = jnp.exp(scores - log_total)
    prob_b = prob_vals.astype(jnp.bfloat16)
    d_value = jnp.einsum(
        "thqk,tqhd->tkd", prob_b, grad_tiles, preferred_element_type=jnp.float32
    ).reshape(row_count, head_width)
    d_probs = jnp.einsum(
        "tqhd,tkd->thqk", grad_tiles, value_tiles, preferred_element_type=jnp.float32
    )
    row_delta = jnp.sum(prob_vals * d_probs, axis=-1, keepdims=True)
    d_scores = (prob_vals * (d_probs - row_delta) * head_width ** (-0.5)).astype(jnp.bfloat16)
    d_query = jnp.einsum(
        "thqk,tkd->tqhd", d_scores, key_tiles, preferred_element_type=jnp.float32
    ).reshape(row_count, head_count, head_width)
    d_key = jnp.einsum(
        "thqk,tqhd->tkd", d_scores, query_tiles, preferred_element_type=jnp.float32
    ).reshape(row_count, head_width)
    return (d_query, d_key, d_value)


def local(
    inputs,
    segments,
    w_query,
    w_key,
    w_value,
    w_out,
    g_in,
    g_attn,
    g_query,
    g_key,
    w_gate,
    w_up,
    w_down,
    g_pre,
    g_post,
    cotangent,
):
    n = lax.axis_size("dp")
    depth = w_query.shape[0]
    rows = -(-depth // 16) * 16
    width = w_gate.shape[1]
    gains = jnp.stack([g_in, g_attn, g_pre, g_post], axis=1)
    attn_pack = jnp.concatenate(
        [w_query, w_key, w_value, w_out.T, jnp.pad(gains, ((0, 0), (0, 124)))], axis=1
    )
    attn_all, ffn_all = ring_gather(
        n, pack_rows(attn_pack, rows), pack_ffn(w_gate, w_up, w_down.T, rows)
    )
    attn_all = attn_all[:, :depth].reshape(n * depth, -1)
    ffn_all = ffn_all[:, :, :depth].reshape(ffn_all.shape[0], n * depth, -1)
    wq_full, wk_full, wv_full, wo_t = (attn_all[:, k * HD : (k + 1) * HD] for k in range(4))
    wo_full = wo_t.T
    gin_full, gattn_full, gpre_full, gpost_full = (attn_all[:, 4 * HD + k] for k in range(4))
    wg_full, wu_full, wd_t = unpack_ffn(ffn_all, width)
    wd_full = wd_t.T
    gain_in = gin_full.astype(jnp.float32)
    gain_attn = gattn_full.astype(jnp.float32)
    gain_query = g_query.astype(jnp.float32)
    gain_key = g_key.astype(jnp.float32)
    cosine, sine_tab = rotary_tables(segments)
    inputs_f = inputs.astype(jnp.float32)
    normed_shard = rms_scale(inputs_f, gain_in).astype(jnp.bfloat16)
    normed_in = lax.all_gather(normed_shard, "tensor", axis=0, tiled=True)
    row_count = normed_in.shape[0]
    head_count = wq_full.shape[1] // HD
    key_proj = plain_product(normed_in, wk_full)
    value_b = plain_product(normed_in, wv_full).astype(jnp.bfloat16)
    key_ready = prepare(key_proj[:, None, :], gain_key, cosine, sine_tab)[:, 0, :].astype(
        jnp.bfloat16
    )
    query_proj = plain_product(normed_in, wq_full).reshape(row_count, head_count, HD)
    query_ready = prepare(query_proj, gain_query, cosine, sine_tab).astype(jnp.bfloat16)
    attended, log_total = attend(query_ready, key_ready, value_b, segments)
    projected = lax.psum_scatter(
        plain_product(attended, wo_full), "tensor", scatter_dimension=0, tiled=True
    )
    residual_mid = inputs_f + rms_scale(projected, gain_attn)
    gain_pre = gpre_full.astype(jnp.float32)
    gain_post = gpost_full.astype(jnp.float32)
    normed_mid = lax.all_gather(
        rms_scale(residual_mid, gain_pre).astype(jnp.bfloat16), "tensor", axis=0, tiled=True
    )
    gate_proj = plain_product(normed_mid, wg_full)
    up_proj = plain_product(normed_mid, wu_full)
    hidden = gelu_product(gate_proj, up_proj).astype(jnp.bfloat16)
    feed = lax.psum_scatter(
        plain_product(hidden, wd_full), "tensor", scatter_dimension=0, tiled=True
    )
    output = (residual_mid + rms_scale(feed, gain_post)).astype(jnp.bfloat16)
    wg_back, wu_back, wd_back = wg_full, wu_full, wd_full
    grad_output = cotangent.astype(jnp.float32)
    d_feed_f, grad_g_post = jax.vjp(rms_scale, feed, gain_post)[1](grad_output)
    d_feed = lax.all_gather(d_feed_f.astype(jnp.bfloat16), "tensor", axis=0, tiled=True)
    d_hidden = cols_product(d_feed, wd_back)
    d_gate_f, d_up_f = jax.vjp(gelu_product, gate_proj, up_proj)[1](d_hidden)
    d_gate = d_gate_f.astype(jnp.bfloat16)
    d_up = d_up_f.astype(jnp.bfloat16)
    grad_gate = rows_product(normed_mid, d_gate)
    grad_up = rows_product(normed_mid, d_up)
    d_normed_mid = lax.psum_scatter(
        cols_product(d_gate, wg_back) + cols_product(d_up, wu_back),
        "tensor",
        scatter_dimension=0,
        tiled=True,
    )
    d_mid_n, grad_g_pre = jax.vjp(rms_scale, residual_mid, gain_pre)[1](d_normed_mid)
    d_mid = grad_output + d_mid_n
    d_proj_f, grad_g_attn = jax.vjp(rms_scale, projected, gain_attn)[1](d_mid)
    wq_back, wk_back, wv_back, wo_back = wq_full, wk_full, wv_full, wo_full
    d_proj = lax.all_gather(d_proj_f.astype(jnp.bfloat16), "tensor", axis=0, tiled=True)
    d_attended = cols_product(d_proj, wo_back).astype(jnp.bfloat16)
    d_query_ready, d_key_ready, d_value_f = attend_back(
        query_ready, key_ready, value_b, segments, log_total, d_attended
    )
    rotate_fn = partial(prepare, cosine=cosine, sine_tab=sine_tab)
    d_query_f, grad_g_query = jax.vjp(rotate_fn, query_proj, gain_query)[1](d_query_ready)
    d_key_f, grad_g_key = jax.vjp(rotate_fn, key_proj[:, None, :], gain_key)[1](
        d_key_ready[:, None, :]
    )
    d_query = d_query_f.reshape(row_count, head_count * HD).astype(jnp.bfloat16)
    d_key = d_key_f[:, 0, :].astype(jnp.bfloat16)
    d_value = d_value_f.astype(jnp.bfloat16)
    grad_query = rows_product(normed_in, d_query)
    grad_key = rows_product(normed_in, d_key)
    grad_value = rows_product(normed_in, d_value)
    d_normed_terms = (
        cols_product(d_query, wq_back)
        + cols_product(d_key, wk_back)
        + cols_product(d_value, wv_back)
    )
    d_normed_in = lax.psum_scatter(
        d_normed_terms.astype(jnp.bfloat16), "tensor", scatter_dimension=0, tiled=True
    ).astype(jnp.float32)
    d_in_n, grad_g_in = jax.vjp(rms_scale, inputs_f, gain_in)[1](d_normed_in)
    d_inputs = (d_mid + d_in_n).astype(jnp.bfloat16)
    attn_part = jnp.concatenate(
        [grad_query, grad_key, grad_value, rows_product(d_proj, attended)], axis=1
    ).astype(BF)
    attn_part = pack_blocks(attn_part, n, rows)
    ffn_part = pack_ffn(
        grad_gate.astype(BF), grad_up.astype(BF), rows_product(d_feed, hidden).astype(BF), n * depth
    )
    ffn_part = jax.vmap(lambda a: pack_blocks(a, n, rows))(ffn_part)
    attn_sum, ffn_sum = ring_reduce(n, attn_part, ffn_part)
    attn_sum, ffn_sum = attn_sum[:depth], ffn_sum[:, :depth]
    sum_gate, sum_up, sum_down_t = unpack_ffn(ffn_sum, width)
    split_grads = (
        attn_sum[:, :HD],
        attn_sum[:, 3 * HD : 4 * HD].T,
        sum_gate,
        sum_up,
        sum_down_t.T,
    )
    sum_key, sum_value = attn_sum[:, HD : 2 * HD], attn_sum[:, 2 * HD : 3 * HD]
    shared = (
        lax.psum_scatter(sum_key, "tensor", scatter_dimension=0, tiled=True),
        lax.psum_scatter(sum_value, "tensor", scatter_dimension=0, tiled=True),
        lax.psum_scatter(grad_g_in, ("dp", "tensor"), scatter_dimension=0, tiled=True),
        lax.psum_scatter(grad_g_attn, ("dp", "tensor"), scatter_dimension=0, tiled=True),
        lax.psum_scatter(grad_g_pre, ("dp", "tensor"), scatter_dimension=0, tiled=True),
        lax.psum_scatter(grad_g_post, ("dp", "tensor"), scatter_dimension=0, tiled=True),
        lax.psum_scatter(grad_g_query, ("dp", "tensor"), scatter_dimension=0, tiled=True),
        lax.psum_scatter(grad_g_key, ("dp", "tensor"), scatter_dimension=0, tiled=True),
    )
    return (
        output,
        d_inputs,
        split_grads[0],
        shared[0],
        shared[1],
        split_grads[1],
        shared[2],
        shared[3],
        shared[6],
        shared[7],
        split_grads[2],
        split_grads[3],
        split_grads[4],
        shared[4],
        shared[5],
    )


SCALE = HD**-0.5
ROOT = 0.7978845608028654
CUBIC = 0.044715


def dot_nn(a, b):
    return jnp.dot(a, b, preferred_element_type=F32)


def dot_nt(a, b):
    return lax.dot_general(a, b, (((1,), (1,)), ((), ())), preferred_element_type=F32)


def dot_tn(a, b):
    return lax.dot_general(a, b, (((0,), (0,)), ((), ())), preferred_element_type=F32)


def inverse_rms(values):
    return lax.rsqrt(jnp.mean(values * values, axis=-1, keepdims=True) + EPSILON)


def rms_back(values, gain_vec, grad):
    inverse = inverse_rms(values)
    unit = values * inverse
    scaled = grad * gain_vec
    back = inverse * (scaled - unit * jnp.mean(scaled * unit, axis=-1, keepdims=True))
    return back, grad * unit


def gelu_parts(gate):
    bent = jnp.tanh(ROOT * (gate + CUBIC * gate * gate * gate))
    return 0.5 * gate * (1.0 + bent), bent


class Quad:
    def __init__(self, part, near, far, gather_sems, reduce_sems):
        self.me = lax.axis_index("tensor")
        self.twin = self.me + 1 - 2 * (self.me % 2)
        self.across = (self.me + 2) % 4
        self.corner = (self.twin + 2) % 4
        self.part, self.near, self.far = part, near, far
        self.gather_sems, self.reduce_sems = gather_sems, reduce_sems

    def copy(self, src, dst, sems, use, k, peer):
        return pltpu.make_async_remote_copy(
            src,
            dst,
            sems[0].at[use, k],
            sems[1].at[use, k],
            device_id={"tensor": peer},
            device_id_type=MESH,
        )

    def gather(self, use, k, buf):
        place = self.across if k == 2 else self.me
        block = buf(place) if callable(buf) else buf.at[place]
        peer = self.across if k == 1 else self.twin
        return self.copy(block, block, self.gather_sems, use, k, peer)

    def gather_start(self, use, buf):
        self.gather(use, 1, buf).start()
        self.gather(use, 0, buf).start()

    def gather_relay(self, use, buf):
        self.gather(use, 1, buf).wait_recv()
        self.gather(use, 2, buf).start()

    def gather_end(self, use, buf):
        self.gather(use, 0, buf).wait_recv()
        self.gather(use, 2, buf).wait_recv()
        for k in range(3):
            self.gather(use, k, buf).wait_send()

    def reduce(self, use, k):
        block = self.part.at[(self.twin, self.corner, self.across)[k]]
        land = self.far if k == 2 else self.near.at[k]
        peer = self.across if k == 2 else self.twin
        return self.copy(block, land, self.reduce_sems, use, k, peer)

    def reduce_start(self, use):
        self.reduce(use, 1).start()
        self.reduce(use, 0).start()

    def reduce_relay(self, use):
        self.reduce(use, 1).wait_recv()
        for low in range(0, self.part.shape[1], 64):
            rows = pl.ds(low, 64)
            total = self.part[self.across, rows].astype(F32) + self.near[1, rows].astype(F32)
            self.part[self.across, rows] = total.astype(BF)
        self.reduce(use, 2).start()

    def reduce_end(self, use):
        self.reduce(use, 0).wait_recv()
        self.reduce(use, 2).wait_recv()
        for k in range(3):
            self.reduce(use, k).wait_send()


class Octet:
    def __init__(self, part, near, far, bend, gather_sems, reduce_sems):
        tensor, dp = lax.axis_index("tensor"), lax.axis_index("dp")
        z = dp // 2
        self.low, self.x, self.core = z % 2, tensor // 2, tensor % 2
        self.twin = {"tensor": tensor + 1 - 2 * self.core}
        self.across = {"tensor": (tensor + 2) % 4}
        self.pair = {"dp": dp + 2 - 4 * self.low}
        self.part, self.near, self.far, self.bend = part, near, far, bend
        self.gather_sems, self.reduce_sems = gather_sems, reduce_sems

    def block(self, p, other=0):
        core = (self.core + other) % 2
        return (self.low + p // 2) % 2 * 4 + (self.x + p % 2) % 2 * 2 + core

    def copy(self, src, dst, sems, use, k, peer):
        return pltpu.make_async_remote_copy(
            src, dst, sems[0].at[use, k], sems[1].at[use, k], device_id=peer, device_id_type=MESH
        )

    def gather(self, use, k, buf, come=False):
        half = buf.shape[1] // 2
        if k < 2:
            place, peer = (k + 1 if come else 0), (self.across, self.pair)[k]
            ref = buf.at[self.block(place)]
        elif k < 6:
            ref = buf.at[self.block(k - 2, 1 if come else 0)]
            peer = self.twin
        else:
            place = 3 if come else k - 5
            ref = buf.at[self.block(place), pl.ds((k - 6) * half, half)]
            peer = (self.pair, self.across)[k - 6]
        return self.copy(ref, ref, self.gather_sems, use, k, peer)

    def gather_start(self, use, buf):
        for k in range(3):
            self.gather(use, k, buf).start()

    def gather_relay(self, use, buf, k):
        self.gather(use, k, buf, True).wait_recv()
        self.gather(use, 6 + k, buf).start()
        self.gather(use, 3 + k, buf).start()

    def gather_corner(self, use, buf):
        for k in (6, 7):
            self.gather(use, k, buf, True).wait_recv()
        self.gather(use, 5, buf).start()

    def gather_end(self, use, buf):
        for k in range(2, 6):
            self.gather(use, k, buf, True).wait_recv()
        for k in range(8):
            self.gather(use, k, buf).wait_send()

    def reduce(self, use, k):
        half = self.part.shape[1] // 2
        if k < 4:
            return self.copy(
                self.part.at[self.block(k, 1)], self.near.at[k], self.reduce_sems, use, k, self.twin
            )
        peer = (self.across, self.pair)[k % 2]
        if k < 6:
            src, dst = self.part.at[self.block(3), pl.ds((k - 4) * half, half)], self.bend.at[k - 4]
        else:
            src, dst = self.part.at[self.block(k - 5)], self.far.at[k - 6]
        return self.copy(src, dst, self.reduce_sems, use, k, peer)

    def add(self, place, low, count, came):
        step = 32

        def body(i, _):
            at = pl.multiple_of(i * step, step)
            rows = pl.ds(low + at, step)
            total = self.part[self.block(place), rows].astype(F32) + came[pl.ds(at, step)].astype(F32)
            self.part[self.block(place), rows] = total.astype(BF)
            return 0

        lax.fori_loop(0, count // step, body, 0)

    def reduce_near(self, use, place):
        self.reduce(use, place).wait_recv()
        self.add(place, 0, self.part.shape[1], self.near.at[place])

    def reduce_relay(self, use):
        half = self.part.shape[1] // 2
        for k in range(2):
            self.reduce(use, 4 + k).wait_recv()
            self.add(2 - k, k * half, half, self.bend.at[k])
            self.reduce(use, 7 - k).start()

    def reduce_after(self, use, i):
        for k in range(4):
            pl.when(i == 6 - 2 * k)(lambda k=k: self.reduce(use, k).start())
        for k in (1, 2):
            pl.when(i == 7 - 2 * k)(lambda k=k: self.reduce_near(use, k))
        pl.when(i == 6)(lambda: self.reduce_relay(use))

        @pl.when(i == 1)
        def _():
            self.reduce_near(use, 3)
            self.reduce(use, 4).start()
            self.reduce(use, 5).start()

    @staticmethod
    def arrival(j):
        a, b = j // 2, j % 2
        up = (a + 1) // 2
        mid = up * (2 - up)
        return up + mid * b + a // 3, (1 - mid) * b + mid * (a // 2)

    def gather_before(self, use, buf, j):
        for at, k in ((1, 2), (4, 3), (5, 4), (7, 5)):
            pl.when(j == at)(lambda k=k: self.gather(use, k, buf, True).wait_recv())

        @pl.when(j == 2)
        def _():
            self.gather_relay(use, buf, 0)
            self.gather_relay(use, buf, 1)

        pl.when(j == 6)(lambda: self.gather_corner(use, buf))

    def gather_sends_done(self, use, buf):
        for k in range(8):
            self.gather(use, k, buf).wait_send()

    def reduce_end(self, use):
        for k in (0, 6, 7):
            self.reduce(use, k).wait_recv()
        for k in range(8):
            self.reduce(use, k).wait_send()


class Columns:
    def __init__(self, ffn, other, land, gather_sems, reduce_sems):
        dp = lax.axis_index("dp")
        z, y = dp // 2, dp % 2
        self.low = z % 2
        self.inner = z * (3 - z) > 0
        self.outer = z * (3 - z) < 1
        ranks = (z, z + 1 - 2 * (z % 2), (z + 2) % 4, 3 - z)
        self.mine = [rank * 2 + y for rank in ranks]
        self.theirs = [rank * 2 + 1 - y for rank in ranks]
        self.ffn, self.other, self.land = ffn, other, land
        self.gather_sems, self.reduce_sems = gather_sems, reduce_sems

    def copy(self, src, dst, sems, u, send, recv, peer):
        return pltpu.make_async_remote_copy(
            src,
            dst,
            sems[0].at[u, send],
            sems[1].at[u, recv],
            device_id={"dp": peer},
            device_id_type=MESH,
        )

    def gather(self, u, k):
        own = self.ffn.at[u, self.mine[0]]
        sems = self.gather_sems
        if k == 0:
            return self.copy(own, own, sems, u, 0, 0, self.mine[2])
        if k == 1:
            return self.copy(self.other.at[u], own, sems, u, 1, 1, self.mine[1])
        if k == 2:
            return self.copy(self.other.at[u], own, sems, u, 2, 2, self.mine[3])
        if k == 3:
            block = self.ffn.at[u, self.mine[1]]
            return self.copy(block, block, sems, u, 3, 2, self.mine[2])
        block = self.ffn.at[u, self.mine[k - 4]]
        return self.copy(block, block, sems, u, k, k, self.theirs[0])

    def come(self, u, k):
        place = self.theirs[k - 4] if k >= 4 else self.mine[(2, 1, 3)[k]]
        block = self.ffn.at[u, place]
        self.copy(block, block, self.gather_sems, u, k, k, place).wait_recv()

    def gather_step(self, u, step):
        if step == 0:
            self.gather(u, 0).start()
            self.gather(u, 1).start()
            pl.when(self.inner)(lambda: self.gather(u, 2).start())
            self.gather(u, 4).start()
        elif step == 1:
            self.come(u, 1)
            pl.when(self.inner)(lambda: self.gather(u, 3).start())
            self.gather(u, 5).start()
        elif step == 2:
            self.come(u, 0)
            self.gather(u, 6).start()
        elif step == 3:
            self.come(u, 2)
            self.gather(u, 7).start()
        else:
            for k in range(4, 8):
                self.come(u, k)

    def gather_sends_done(self, u):
        for k in (0, 1, 4, 5, 6, 7):
            self.gather(u, k).wait_send()

        @pl.when(self.inner)
        def _():
            self.gather(u, 2).wait_send()
            self.gather(u, 3).wait_send()

    def piece(self, item, place):
        unit, count, lane, lanes = item[1:]
        return self.ffn.at[pl.ds(unit, count), place, :, pl.ds(lane, lanes)]

    def reduce(self, item, k):
        if k < 4:
            place, peer = self.theirs[k], self.theirs[0]
        else:
            place = self.mine[(2, 1, 3, 3)[k - 4]]
            peer = self.mine[(2, 1, 3, 2)[k - 4]]
        unit, count, lane, lanes = item[1:]
        land = self.land.at[pl.ds(unit, count), k, :, pl.ds(lane, lanes)]
        return self.copy(
            self.piece(item, place), land, self.reduce_sems, item[0], min(k, 6), k, peer
        )

    def came(self, item, k):
        unit, count, lane, lanes = item[1:]
        return [
            self.land[u, k, :, lane : lane + lanes].astype(F32) for u in range(unit, unit + count)
        ]

    def own(self, item, place):
        unit, count, lane, lanes = item[1:]
        return [
            self.ffn.at[u, self.mine[place], :, pl.ds(lane, lanes)]
            for u in range(unit, unit + count)
        ]

    def add(self, item, place, k):
        self.reduce(item, k).wait_recv()
        for own, came in zip(self.own(item, place), self.came(item, k), strict=True):
            own[...] = (own[...].astype(F32) + came).astype(BF)

    def reduce_step(self, item, step):
        if step == 0:
            for k in (3, 2, 1, 0):
                self.reduce(item, k).start()
        elif step == 1:
            self.add(item, 3, 3)
            pl.when(self.inner)(lambda: self.reduce(item, 6).start())
            pl.when(self.outer)(lambda: self.reduce(item, 7).start())
        elif step == 2:
            self.add(item, 2, 2)
            self.reduce(item, 4).start()
        else:
            self.add(item, 1, 1)
            pl.when(self.inner)(lambda: self.add(item, 1, 7))
            self.reduce(item, 5).start()

    def sum_own(self, item, out):
        for k in (0, 4):
            self.reduce(item, k).wait_recv()
        lanes = item[4]
        for i, (own, one, two) in enumerate(
            zip(self.own(item, 0), self.came(item, 0), self.came(item, 4), strict=True)
        ):
            out[:, i * lanes : (i + 1) * lanes] = own[...].astype(F32) + one + two

    def sum_other(self, item, out):
        self.reduce(item, 5).wait_recv()
        lanes = item[4]
        for i, came in enumerate(self.came(item, 5)):
            out[:, i * lanes : (i + 1) * lanes] = came

        @pl.when(self.inner)
        def _():
            self.reduce(item, 6).wait_recv()
            for i, came in enumerate(self.came(item, 6)):
                out[:, i * lanes : (i + 1) * lanes] += came

    def reduce_sends_done(self, item):
        for k in range(7):
            self.reduce(item, k).wait_send()


class Queue:
    def __init__(self):
        self.steps = []

    def add(self, tag, fn):
        self.steps.append((tag, fn))

    def run(self, count, ready=None):
        while count > 0 and self.steps:
            tag, fn = self.steps[0]
            if ready is not None and tag not in ready:
                return
            self.steps.pop(0)
            fn()
            count -= 1

    def until(self, tag):
        while any(t == tag for t, _ in self.steps):
            self.run(1)


def layer_kernel(
    n,
    x_ref,
    cot_ref,
    seg_row,
    small_ref,
    wo_in,
    wq_in,
    wk_in,
    wv_in,
    gain_in,
    ffn_in,
    dx_ref,
    sums_ref,
    out_hbm,
    ggate_hbm,
    gup_hbm,
    gdown_hbm,
    attn,
    ffn,
    other,
    attn_land,
    ffn_land,
    gate_buf,
    up_buf,
    hid_buf,
    part,
    near,
    far,
    bend,
    xa,
    nm,
    df,
    dp_buf,
    proj_s,
    res_s,
    gains,
    gsum,
    gqk,
    q_proj,
    k_proj,
    qr,
    kr,
    vb,
    att,
    probs,
    cos_s,
    sin_s,
    stage,
    kvg,
    kvg_land,
    local_sem,
    stage_sem,
    ag_send,
    ag_recv,
    rs_send,
    rs_recv,
    cg_send,
    cg_recv,
    cr_send,
    cr_recv,
    og_send,
    og_recv,
    or_send,
    or_recv,
    qg_send,
    qg_recv,
    qr_send,
    qr_recv,
    kv_send,
    kv_recv,
):
    units, _, depth, cols = ffn.shape
    rows, width = x_ref.shape
    attn_cut = ((0, HD), (HD, 2 * HD), (2 * HD, 4 * HD), (4 * HD, attn.shape[-1]))
    parts = part_views(attn, attn_cut)
    landing = part_views(attn_land, attn_cut)
    first = len(attn_cut)
    spot4 = lax.axis_index("tensor")

    def quarter_of(t):
        return attn.at[:, :, pl.ds(pl.multiple_of(2 * HD + t * 128, 128), 128)]

    gathered = list(parts)
    gathered[2] = lambda b: attn.at[
        b, :, pl.ds(pl.multiple_of(2 * HD + spot4 * 128, 128), 128)
    ]
    ring = Ring(n, gathered, ag_send, ag_recv)
    back = Ring(n, parts, rs_send, rs_recv, lambda p, slot: landing[p](slot))
    quad = Quad(part, near, far.at[0], (qg_send, qg_recv), (qr_send, qr_recv))
    octet = Octet(part, near, far, bend, (og_send, og_recv), (or_send, or_recv))
    columns = Columns(ffn, other, ffn_land, (cg_send, cg_recv), (cr_send, cr_recv))
    me, spot = quad.me, octet.block(0)
    gq_ref, gk_ref = small_ref.at[0:1], small_ref.at[1:2]
    freq_ref = small_ref.at[2:3, pl.ds(0, HD // 2)]

    def attn_cols(low, high):
        return attn[:, :, low:high].reshape(width, high - low)

    def unit_cols(u, k, count=1):
        return ffn[u, :, :, k * UNIT : (k + count) * UNIT].reshape(width, count * UNIT)

    def across_units(k, low=0, high=units):
        return jnp.concatenate([unit_cols(u, k) for u in range(low, high)], axis=1)

    mine = [
        pltpu.make_async_copy(wo_in, attn.at[ring.me, :, pl.ds(0, HD)], local_sem.at[0]),
        pltpu.make_async_copy(wq_in, attn.at[ring.me, :, pl.ds(HD, HD)], local_sem.at[4]),
        pltpu.make_async_copy(gain_in, attn.at[ring.me, :, pl.ds(4 * HD, 128)], local_sem.at[5]),
        pltpu.make_async_copy(
            ffn_in.at[pl.ds(columns.low * units, units)], ffn.at[:, ring.me], local_sem.at[1]
        ),
        pltpu.make_async_copy(x_ref, xa.at[me], local_sem.at[2]),
        pltpu.make_async_copy(
            ffn_in.at[pl.ds((1 - columns.low) * units, units)], other, local_sem.at[3]
        ),
    ]
    for copy in mine:
        copy.start()

    def quarter_copy(source):
        cols = pl.ds(pl.multiple_of(me % 2 * 128, 128), 128)
        return pltpu.make_async_copy(
            source.at[:, cols], quarter_of(me).at[ring.me], local_sem.at[6]
        )

    pl.when(me < 2)(lambda: quarter_copy(wk_in).start())
    pl.when(me > 1)(lambda: quarter_copy(wv_in).start())
    greet = [{"dp": peer} for peer in columns.mine[1:] + columns.theirs[:1]]
    greet += [{"tensor": quad.twin}, {"tensor": quad.across}]
    barrier(greet)
    for copy in mine:
        copy.wait()
    quarter_copy(wk_in).wait()
    quad.gather_start(0, xa)

    queue = Queue()
    def ring_gather_step(parts, hop, tag):
        for p in parts:
            for way in range(2):
                if 0 < hop <= ring.reach(p, way) + 1:
                    queue.add(tag, partial(ring.gather_step, p, way, hop))

    for hop in range(1, n // 2 + 1):
        ring_gather_step((2, 3, 1), hop, -1)
        ring_gather_step((0,), hop - 2, -1)
    ring_gather_step((2, 3), n // 2 + 1, -1)
    queue.add(-1, partial(quad.gather_start, 2, quarter_of))
    queue.add(-1, partial(quad.gather_relay, 0, xa))
    queue.add(-1, partial(columns.gather_step, 0, 0))
    ring_gather_step((1,), n // 2 + 1, -1)
    ring_gather_step((0,), n // 2 - 1, -1)
    queue.add(-1, partial(quad.gather_relay, 2, quarter_of))
    ring_gather_step((0,), n // 2, -3)
    for u in range(1, EARLY):
        queue.add(-3, partial(columns.gather_step, u, 0))
    ring_gather_step((0,), n // 2 + 1, -3)
    for u in range(units + 2):
        if u < units:
            queue.add(-2, partial(columns.gather_step, u, 1))
            queue.add(-2, partial(columns.gather_step, u, 2))
        if u + EARLY < units:
            queue.add(-2, partial(columns.gather_step, u + EARLY, 0))
        if 0 < u <= units:
            queue.add(-2, partial(columns.gather_step, u - 1, 3))
        if u > 1:
            queue.add(u - 2, partial(columns.gather_step, u - 2, 4))

    queue.run(AHEAD[0])
    quarter = SEGMAX // 2

    def seg_column(seg_j, half):
        cut = seg_j[:, half * quarter : (half + 1) * quarter].astype(F32)
        return jnp.transpose(jnp.broadcast_to(cut, (128, quarter)))[:, :1]

    def tables(tile, _):
        seg_j = seg_row[pl.ds(tile, 1), :]
        for half in range(2):
            r = 2 * tile + half
            same = seg_column(seg_j, half) == seg_j.astype(F32)
            j = lax.broadcasted_iota(jnp.int32, (quarter, SEGMAX), 1)
            start = jnp.min(jnp.where(same, j, SEGMAX).astype(F32), axis=1, keepdims=True)
            i = lax.broadcasted_iota(jnp.int32, (quarter, 1), 0).astype(F32) + half * quarter
            angle = (i - start) * freq_ref[...]
            cos_s[r] = jnp.cos(angle)
            sin_s[r] = jnp.sin(angle)
        return 0

    lax.fori_loop(0, N_TILES, tables, 0)
    queue.until(-1)
    flipped = jnp.transpose(attn_cols(4 * HD, 4 * HD + 128).astype(F32))
    gains[...] = flipped[:8]
    quad.gather_end(0, xa)
    queue.run(AHEAD[2])

    sub = 32
    per = rows // sub

    def normalize(i, _):
        b, at = i // per, pl.ds(pl.multiple_of(i % per * sub, sub), sub)
        values = xa[b, at].astype(F32)
        xa[b, at] = (values * inverse_rms(values) * gains[0:1, :]).astype(BF)
        return 0

    lax.fori_loop(0, 4 * per, normalize, 0)

    def rope(values, gain_vec, r):
        normed = values * inverse_rms(values) * gain_vec
        low, high = normed[:, : HD // 2], normed[:, HD // 2 :]
        cosine, sine = cos_s[r], sin_s[r]
        return jnp.concatenate([low * cosine - high * sine, high * cosine + low * sine], axis=1)

    queue.run(AHEAD[3])

    quad.gather_end(2, quarter_of)

    def project(r, _):
        block = xa[r]
        query = dot_nn(block, attn_cols(HD, 2 * HD))
        q_proj[r] = query.astype(BF)
        qr[r] = rope(query, gq_ref[...], r).astype(BF)
        key = dot_nn(block, attn_cols(2 * HD, 3 * HD))
        k_proj[r] = key.astype(BF)
        kr[r] = rope(key, gk_ref[...], r).astype(BF)
        vb[r] = dot_nn(block, attn_cols(3 * HD, 4 * HD)).astype(BF)
        return 0

    lax.fori_loop(0, 4, project, 0)
    queue.run(AHEAD[4])

    def attend_tile(tile, _):
        two = pl.ds(2 * tile, 2)
        keys = kr[two].reshape(SEGMAX, HD)
        values = vb[two].reshape(SEGMAX, HD)
        seg_j = seg_row[pl.ds(tile, 1), :]
        for half in range(2):
            r = 2 * tile + half
            scores = dot_nt(qr[r], keys) * SCALE
            j = lax.broadcasted_iota(jnp.int32, (quarter, SEGMAX), 1)
            i = lax.broadcasted_iota(jnp.int32, (quarter, SEGMAX), 0) + half * quarter
            seen = (seg_column(seg_j, half) == seg_j.astype(F32)) & (i >= j)
            scores = jnp.where(seen, scores, NEG_LARGE)
            powers = jnp.exp(scores - jnp.max(scores, axis=1, keepdims=True))
            weights = (powers / jnp.sum(powers, axis=1, keepdims=True)).astype(BF)
            probs[r] = weights
            att[r] = dot_nn(weights, values).astype(BF)
        return 0

    lax.fori_loop(0, N_TILES, attend_tile, 0)
    queue.run(AHEAD[5])

    queue.until(-3)

    def out_block(r, _):
        part[r] = dot_nt(att[r], attn_cols(0, HD)).astype(BF)
        return 0

    lax.fori_loop(0, 4, out_block, 0)
    quad.reduce_start(0)
    queue.run(AHEAD[6])
    quad.reduce_relay(0)
    queue.run(AHEAD[7])
    quad.reduce_end(0)

    def total(at):
        return part[me, at].astype(F32) + near[0, at].astype(F32) + far[0, at].astype(F32)

    def total_ffn(at):
        return part[spot, at].astype(F32) + near[0, at].astype(F32) + (
            far[0, at].astype(F32) + far[1, at].astype(F32)
        )

    def at_rows(i):
        return pl.ds(pl.multiple_of(i * sub, sub), sub)

    def middle(i, _):
        at = at_rows(i)
        projected = total(at)
        proj_s[at] = projected.astype(BF)
        mid = x_ref[at].astype(F32) + projected * inverse_rms(projected) * gains[1:2, :]
        res_s[at] = mid
        nm[spot, at] = (mid * inverse_rms(mid) * gains[2:3, :]).astype(BF)
        return 0

    lax.fori_loop(0, per, middle, 0)
    octet.gather_start(0, nm)
    queue.run(AHEAD[8])
    octet.gather_relay(0, nm, 0)
    octet.gather_relay(0, nm, 1)
    queue.run(AHEAD[9])
    octet.gather_corner(0, nm)
    queue.run(AHEAD[9])
    octet.gather_end(0, nm)

    for u in range(units):
        queue.until(u)
        lanes = slice(u * UNIT, (u + 1) * UNIT)

        def ffn_block(r, _):
            both = dot_nn(nm[r], unit_cols(u, 0, 2))
            gate, up = both[:, :UNIT], both[:, UNIT:]
            gate_buf[r, :, lanes] = gate.astype(BF)
            up_buf[r, :, lanes] = up.astype(BF)
            hid_buf[r, :, lanes] = (gelu_parts(gate)[0] * up).astype(BF)
            return 0

        lax.fori_loop(0, 8, ffn_block, 0)
        queue.run(AHEAD[10])
    queue.run(10**6)

    def feed_block(i, _):
        b = octet.block(3 - i // 2, 1 - i % 2)
        part[b] = dot_nt(hid_buf[b], across_units(2)).astype(BF)
        octet.reduce_after(0, i)
        return 0

    lax.fori_loop(0, 8, feed_block, 0)
    for p in range(first):
        ring.gather_sends_done(p)
    for u in range(units):
        columns.gather_sends_done(u)
    octet.reduce_end(0)
    eight = (8, width)

    def fold(values):
        return jnp.sum(values.reshape(sub // 8, 8, values.shape[-1]), axis=0)

    def after_feed(i, carry):
        at = at_rows(i)
        feed = total_ffn(at)
        dx_ref[at] = (res_s[at] + feed * inverse_rms(feed) * gains[3:4, :]).astype(BF)
        grad, gain_part = rms_back(feed, gains[3:4, :], cot_ref[at].astype(F32))
        df[spot, at] = grad.astype(BF)
        return carry + fold(gain_part)

    gain_sum = lax.fori_loop(0, per, after_feed, jnp.zeros(eight, F32))
    gsum[3:4, :] = jnp.sum(gain_sum, axis=0, keepdims=True)
    put_out = pltpu.make_async_copy(dx_ref, out_hbm, local_sem.at[0])
    put_out.start()
    octet.gather_start(1, df)

    queue = Queue()
    pending = []

    def finish(item, other):
        k = len(pending)
        if k >= 2:
            for copy in pending[k - 2]:
                copy.wait()
        (columns.sum_other if other else columns.sum_own)(item, stage.at[k % 2])
        half = 1 - columns.low if other else columns.low
        unit, count, lane, lanes = item[1:]
        at = pl.multiple_of(half * (units * UNIT) + unit * UNIT, UNIT)
        outs = ((ggate_hbm, UNIT), (gup_hbm, UNIT)) if lane == 0 else ((gdown_hbm, count * UNIT),)
        copies = [
            pltpu.make_async_copy(
                stage.at[k % 2, :, pl.ds(which * UNIT, wide)],
                hbm.at[:, pl.ds(at, wide)],
                stage_sem.at[k % 2, which],
            )
            for which, (hbm, wide) in enumerate(outs)
        ]
        for copy in copies:
            copy.start()
        pending.append(copies)

    pairs = [(low, min(low + 2, units)) for low in range(0, units, 2)]
    items = [(k, low, high - low, 2 * UNIT, UNIT) for k, (low, high) in enumerate(pairs)]
    items += [(len(pairs) + u, u, 1, 0, 2 * UNIT) for u in range(units)]
    count = len(items)
    queue.add(0, partial(columns.reduce_step, items[0], 0))
    for k in range(count + 2):
        if k + 1 < count:
            queue.add(k + 1, partial(columns.reduce_step, items[k + 1], 0))
        if k < count:
            for step in range(1, 4):
                queue.add(k, partial(columns.reduce_step, items[k], step))
        if k > 1:
            queue.add(k - 2, partial(finish, items[k - 2], False))
            queue.add(k - 2, partial(finish, items[k - 2], True))
    ready = set()
    def tall(ref, lanes):
        return ref[:, :, lanes].reshape(8 * rows, lanes.stop - lanes.start)

    def down_grad(low, high):
        value = dot_tn(df[...].reshape(8 * rows, width), tall(hid_buf, slice(low * UNIT, high * UNIT)))
        value = value.astype(BF)
        for u in range(low, high):
            piece = value[:, (u - low) * UNIT : (u - low + 1) * UNIT]
            ffn[u, :, :, 2 * UNIT :] = piece.reshape(n, depth, UNIT)
        ready.add(low // 2)

    def back_block(j, _):
        octet.gather_before(1, df, j)
        b = octet.block(*octet.arrival(j))
        for low, high in pairs:
            lanes = slice(low * UNIT, high * UNIT)
            grad = dot_nn(df[b], across_units(2, low, high))
            gate, up = gate_buf[b, :, lanes].astype(F32), up_buf[b, :, lanes].astype(F32)
            act, bent = gelu_parts(gate)
            slope = 0.5 * (1.0 + bent) + 0.5 * gate * (1.0 - bent * bent) * ROOT * (
                1.0 + 3.0 * CUBIC * gate * gate
            )
            gate_buf[b, :, lanes] = (grad * up * slope).astype(BF)
            up_buf[b, :, lanes] = (grad * act).astype(BF)
        return 0

    lax.fori_loop(0, 8, back_block, 0)
    octet.gather_sends_done(1, df)

    def down_grads(some):
        for low, high in some:
            down_grad(low, high)
            queue.run(PACE[0], ready)

    down_grads(pairs[: WORK[3]])

    def back_part(i, _):
        b = octet.block(3 - i // 2, 1 - i % 2)
        grown = dot_nt(gate_buf[b], across_units(0)) + dot_nt(up_buf[b], across_units(1))
        part[b] = grown.astype(BF)
        octet.reduce_after(1, i)
        return 0

    def gate_grad(u, _):
        lanes = pl.ds(pl.multiple_of(u * UNIT, UNIT), UNIT)
        both = jnp.concatenate(
            [ref[:, :, lanes].reshape(8 * rows, UNIT) for ref in (gate_buf, up_buf)], axis=1
        )
        value = dot_tn(nm[...].reshape(8 * rows, width), both)
        ffn[u, :, :, : 2 * UNIT] = value.astype(BF).reshape(n, depth, 2 * UNIT)
        return 0

    done = [0]

    def do_work(count):
        low, done[0] = done[0], min(units, done[0] + count)
        if low < done[0]:
            lax.fori_loop(low, done[0], gate_grad, 0)
            ready.update(range(len(pairs) + low, len(pairs) + done[0]))
            queue.run(PACE[1] * (done[0] - low), ready)

    lax.fori_loop(0, 4, back_part, 0)
    queue.run(2 * PACE[0], ready)
    lax.fori_loop(4, 8, back_part, 0)
    down_grads(pairs[WORK[3] :])
    do_work(WORK[0])
    do_work(WORK[1])
    queue.run(PACE[2], ready)
    octet.reduce_end(1)

    def after_ffn(i, carry):
        at = at_rows(i)
        grad, pre_part = rms_back(res_s[at], gains[2:3, :], total_ffn(at))
        grad = cot_ref[at].astype(F32) + grad
        res_s[at] = grad
        grad, attn_part = rms_back(proj_s[at].astype(F32), gains[1:2, :], grad)
        dp_buf[me, at] = grad.astype(BF)
        return carry[0] + fold(pre_part), carry[1] + fold(attn_part)

    zero = jnp.zeros(eight, F32)
    pre_sum, attn_sum = lax.fori_loop(0, per, after_ffn, (zero, zero))
    gsum[2:3, :] = jnp.sum(pre_sum, axis=0, keepdims=True)
    gsum[1:2, :] = jnp.sum(attn_sum, axis=0, keepdims=True)
    quad.gather_start(1, dp_buf)
    do_work(WORK[2])
    queue.run(PACE[3], ready)
    quad.gather_relay(1, dp_buf)
    do_work(units)
    queue.run(PACE[4], ready)
    quad.gather_end(1, dp_buf)

    d_q, d_k, d_v = (gate_buf.at[pl.ds(0, 4), :, pl.ds(k * HD, HD)] for k in range(3))
    datt = up_buf.at[pl.ds(0, 4), :, pl.ds(0, HD)]

    def attn_grad(low, left, right):
        value = dot_tn(left.reshape(4 * rows, width), right.reshape(4 * rows, HD))
        attn[:, :, low : low + HD] = value.astype(BF).reshape(n, width // n, HD)

    def ring_hop(hop, *some):
        for p in some:
            for way in range(2):
                back.reduce_step(p, way, hop)

    ready.add(-1)
    def back_out(r, _):
        datt[r] = dot_nn(dp_buf[r], attn_cols(0, HD)).astype(BF)
        return 0

    lax.fori_loop(0, 4, back_out, 0)
    attn_grad(0, dp_buf[...], att[...])
    ring_hop(1, 0)
    queue.run(PACE[5], ready)
    gqk[...] = jnp.zeros_like(gqk)

    def unrope(grad, projection, gain_vec, r, row):
        low, high = grad[:, : HD // 2], grad[:, HD // 2 :]
        cosine, sine = cos_s[r], sin_s[r]
        grad = jnp.concatenate([low * cosine + high * sine, high * cosine - low * sine], axis=1)
        grad, gain_part = rms_back(projection, gain_vec, grad)
        gqk[row : row + 1, :] += jnp.sum(gain_part, axis=0, keepdims=True)
        return grad.astype(BF)

    def back_tile(tile, _):
        two = pl.ds(2 * tile, 2)
        keys = kr[two].reshape(SEGMAX, HD)
        values = vb[two].reshape(SEGMAX, HD)
        d_key = jnp.zeros((SEGMAX, HD), F32)
        d_value = jnp.zeros((SEGMAX, HD), F32)
        for half in range(2):
            r = 2 * tile + half
            d_att = datt[r]
            weights = probs[r]
            d_value = d_value + dot_tn(weights, d_att)
            d_probs = dot_nt(d_att, values)
            weights = weights.astype(F32)
            delta = jnp.sum(weights * d_probs, axis=1, keepdims=True)
            d_scores = (weights * (d_probs - delta) * SCALE).astype(BF)
            d_key = d_key + dot_tn(d_scores, qr[r])
            d_query = dot_nn(d_scores, keys)
            d_q[r] = unrope(d_query, q_proj[r].astype(F32), gq_ref[...], r, 4)
        for half in range(2):
            r = 2 * tile + half
            cut = slice(half * quarter, (half + 1) * quarter)
            d_k[r] = unrope(d_key[cut], k_proj[r].astype(F32), gk_ref[...], r, 5)
            d_v[r] = d_value[cut].astype(BF)
        return 0

    lax.fori_loop(0, N_TILES, back_tile, 0)
    ring_hop(2, 0)
    queue.run(PACE[5], ready)

    def back_in(r, _):
        grown = dot_nt(d_q[r], attn_cols(HD, 2 * HD))
        grown = grown + dot_nt(d_k[r], attn_cols(2 * HD, 3 * HD))
        grown = grown + dot_nt(d_v[r], attn_cols(3 * HD, 4 * HD))
        part[r] = grown.astype(BF)
        return 0

    lax.fori_loop(0, 4, back_in, 0)
    quad.reduce_start(1)
    ring_hop(3, 0)
    queue.run(PACE[5], ready)

    def three_grads(k, _):
        grad = gate_buf[0:4, :, pl.ds(pl.multiple_of(k * HD, HD), HD)]
        value = dot_tn(xa[...].reshape(4 * rows, width), grad.reshape(4 * rows, HD))
        low = pl.multiple_of((k + 1) * HD, HD)
        attn[:, :, pl.ds(low, HD)] = value.astype(BF).reshape(n, depth, HD)
        return 0

    lax.fori_loop(0, 3, three_grads, 0)
    def input_gain(i, carry):
        b, at = i // per, pl.ds(pl.multiple_of(i % per * sub, sub), sub)
        return carry + fold(part[b, at].astype(F32) * xa[b, at].astype(F32))

    gain_sum = lax.fori_loop(0, 4 * per, input_gain, zero)
    gsum[0:1, :] = jnp.sum(gain_sum, axis=0, keepdims=True) / gains[0:1, :]
    gsum[4:8, :] = jnp.zeros((4, width), F32)
    long = jnp.concatenate([gsum[...], jnp.zeros((120, width), F32)], axis=0)
    long = jnp.transpose(long).reshape(n, width // n, 128)
    short = jnp.concatenate([gqk[...], jnp.zeros((120, HD), F32)], axis=0)
    short = jnp.transpose(short).reshape(n, HD // n, 128)
    attn[:, :, 4 * HD : 4 * HD + 128] = long.astype(BF)
    attn[:, : HD // n, 4 * HD : 4 * HD + 128] = (long[:, : HD // n] + short).astype(BF)

    ring_hop(1, 2, 1, 3)
    ring_hop(4, 0)
    quad.reduce_relay(1)
    queue.run(PACE[6], ready)
    for hop in range(2, n // 2 + 1):
        ring_hop(hop, 2, 1, 3)
        queue.run(PACE[7], ready)
    quad.reduce_end(1)
    put_out.wait()

    def after_attn(i, _):
        at = at_rows(i)
        grad, _ = rms_back(x_ref[at].astype(F32), gains[0:1, :], total(at))
        dx_ref[at] = (res_s[at] + grad).astype(BF)
        return 0

    lax.fori_loop(0, per, after_attn, 0)
    queue.run(10**6)
    for p in range(2):
        sums_ref[:, p * HD : (p + 1) * HD] = back.reduce_end(p)
    kvg[0, :, : 2 * HD] = back.reduce_end(2).astype(BF)
    kvg[0, :, 2 * HD :] = back.reduce_end(3).astype(BF)
    for k, peer in enumerate((quad.twin, quad.across)):
        copy = pltpu.make_async_remote_copy(
            kvg.at[k],
            kvg_land.at[k],
            kv_send.at[k],
            kv_recv.at[k],
            device_id={"tensor": peer},
            device_id_type=MESH,
        )
        copy.start()
        copy.wait()
        grown = kvg[k].astype(F32) + kvg_land[k].astype(F32)
        if k == 0:
            kvg[1] = grown.astype(BF)
        else:
            sums_ref[:, 2 * HD :] = grown
    for p in range(len(parts)):
        back.reduce_sends_done(p)
    for item in items:
        columns.reduce_sends_done(item)
    for copies in pending[-2:]:
        for copy in copies:
            copy.wait()


AHEAD = (14, 0, 0, 2, 3, 3, 0, 6, 5, 4, 2)
PACE = (2, 2, 6, 6, 4, 3, 2, 3)
WORK = (2, 3, 2, 2)
EARLY = 3
UNIT = 128
N_TILES = 2


def run_layer(n, x, cot, segments, small, attn_weights, ffn_pack):
    rows, width = x.shape
    both, depth, cols = ffn_pack.shape
    units = both // 2
    tokens = segments.shape[0]
    wide = 4 * HD + 128
    parts = 4
    vmem, dma = pltpu.VMEM, pltpu.SemaphoreType.DMA
    grown = both * UNIT
    return pl.pallas_call(
        partial(layer_kernel, n),
        out_shape=(
            jax.ShapeDtypeStruct((rows, width), BF),
            jax.ShapeDtypeStruct((depth, wide), F32),
            jax.ShapeDtypeStruct((rows, width), BF),
            jax.ShapeDtypeStruct((depth, grown), F32),
            jax.ShapeDtypeStruct((depth, grown), F32),
            jax.ShapeDtypeStruct((depth, grown), F32),
        ),
        in_specs=vmem_specs(4) + any_specs(6),
        out_specs=vmem_specs(2) + any_specs(4),
        scratch_shapes=[
            vmem((n, depth, wide), BF),
            vmem((units, n, depth, cols), BF),
            vmem((units, depth, cols), BF),
            vmem((n - 1, depth, wide), BF),
            vmem((units, 8, depth, cols), BF),
            vmem((8, rows, units * UNIT), BF),
            vmem((8, rows, units * UNIT), BF),
            vmem((8, rows, units * UNIT), BF),
            vmem((8, rows, width), BF),
            vmem((4, rows, width), BF),
            vmem((2, rows, width), BF),
            vmem((2, rows // 2, width), BF),
            vmem((4, rows, width), BF),
            vmem((8, rows, width), BF),
            vmem((8, rows, width), BF),
            vmem((4, rows, width), BF),
            vmem((rows, width), BF),
            vmem((rows, width), F32),
            vmem((8, width), F32),
            vmem((8, width), F32),
            vmem((8, HD), F32),
            vmem((4, rows, HD), BF),
            vmem((4, rows, HD), BF),
            vmem((4, rows, HD), BF),
            vmem((4, rows, HD), BF),
            vmem((4, rows, HD), BF),
            vmem((4, rows, HD), BF),
            vmem((4, rows, SEGMAX), BF),
            vmem((4, rows, HD // 2), F32),
            vmem((4, rows, HD // 2), F32),
            vmem((2, depth, 2 * UNIT), F32),
            vmem((2, depth, wide - 2 * HD), BF),
            vmem((2, depth, wide - 2 * HD), BF),
            dma((7,)),
            dma((2, 3)),
            dma((parts, 2, n // 2)),
            dma((parts, 2, n // 2)),
            dma((parts, 2, n // 2)),
            dma((parts, 2, n // 2)),
            dma((units, 8)),
            dma((units, 8)),
            dma((units + (units + 1) // 2, 8)),
            dma((units + (units + 1) // 2, 8)),
            dma((2, 8)),
            dma((2, 8)),
            dma((2, 8)),
            dma((2, 8)),
            dma((3, 3)),
            dma((3, 3)),
            dma((2, 3)),
            dma((2, 3)),
            dma((2,)),
            dma((2,)),
        ],
        compiler_params=pltpu.CompilerParams(
            collective_id=2, has_side_effects=True, vmem_limit_bytes=67043328
        ),
    )(
        x,
        cot,
        segments.reshape(N_TILES, SEGMAX),
        small,
        *attn_weights,
        ffn_pack,
    )


def fused_local(
    inputs, segments, w_query, w_key, w_value, w_out, g_in, g_attn, g_query, g_key,
    w_gate, w_up, w_down, g_pre, g_post, cotangent,
):
    n = lax.axis_size("dp")
    depth = w_query.shape[0]
    width = w_gate.shape[1]
    lane = lax.broadcasted_iota(jnp.int32, (depth, 128), 1)
    gains = jnp.zeros((depth, 128), BF)
    for k, gain in enumerate((g_in, g_attn, g_pre, g_post)):
        gains = jnp.where(lane == k, gain[:, None], gains)
    exponent = -2.0 * (jnp.arange(HD) % (HD // 2)).astype(F32) / HD
    freq = jnp.power(jnp.float32(THETA), exponent)
    line = lax.broadcasted_iota(jnp.int32, (3, HD), 0)
    small = jnp.where(line == 0, g_query.astype(F32)[None, :], freq[None, :])
    small = jnp.where(line == 1, g_key.astype(F32)[None, :], small)
    ffn_pack = pack_ffn(w_gate, w_up, w_down.T, depth, UNIT)
    d_inputs, sums, output, g_gate, g_up, g_down = run_layer(
        n, inputs, cotangent, segments, small, (w_out.T, w_query, w_key, w_value, gains), ffn_pack
    )
    spot = lax.axis_index("tensor")
    part = depth // 4
    mine = lax.dynamic_slice_in_dim(sums[:, 2 * HD :], spot * part, part, 0)
    small = HD // n // 4
    few = lax.dynamic_slice_in_dim(sums[:, 4 * HD :], spot * small, small, 0)
    return (
        output,
        d_inputs,
        sums[:, HD : 2 * HD],
        mine[:, :HD],
        mine[:, HD : 2 * HD],
        sums[:, :HD].T,
        mine[:, 2 * HD],
        mine[:, 2 * HD + 1],
        few[:, 4],
        few[:, 5],
        g_gate[:, :width],
        g_up[:, :width],
        g_down[:, :width].T,
        mine[:, 2 * HD + 2],
        mine[:, 2 * HD + 3],
    )


def fits(mesh, depth, tokens, rows):
    return mesh.shape["dp"] == 8 and depth % 16 == 0 and mesh.shape["tensor"] == 4 and tokens == 2 * SEGMAX


def layer(mesh):
    def body(*args):
        inputs, segments, w_query = args[0], args[1], args[2]
        if fits(mesh, w_query.shape[0], segments.shape[0], inputs.shape[0]):
            return fused_local(*args)
        return local(*args)

    return body


def solution(mesh):
    return jax.shard_map(
        layer(mesh),
        mesh=mesh,
        in_specs=(
            P(("dp", "tensor"), None),
            P("dp"),
            P("dp", "tensor"),
            P("dp", None),
            P("dp", None),
            P("tensor", "dp"),
            P("dp"),
            P("dp"),
            P(),
            P(),
            P("dp", "tensor"),
            P("dp", "tensor"),
            P("tensor", "dp"),
            P("dp"),
            P("dp"),
            P(("dp", "tensor"), None),
        ),
        out_specs=(
            P(("dp", "tensor"), None),
            P(("dp", "tensor"), None),
            P("dp", "tensor"),
            P(("dp", "tensor"), None),
            P(("dp", "tensor"), None),
            P("tensor", "dp"),
            P(("dp", "tensor")),
            P(("dp", "tensor")),
            P(("dp", "tensor")),
            P(("dp", "tensor")),
            P("dp", "tensor"),
            P("dp", "tensor"),
            P("tensor", "dp"),
            P(("dp", "tensor")),
            P(("dp", "tensor")),
        ),
        check_vma=False,
    )
```

```python
from functools import partial

import jax
import jax.numpy as jnp
from jax import lax
from jax.experimental import pallas as pl
from jax.experimental.pallas import tpu as pltpu
from jax.sharding import PartitionSpec as P

HD = 256
SEGMAX = 512
MESH = pl.DeviceIdType.MESH
BF = jnp.bfloat16
F32 = jnp.float32


def ring_pos(dev, n):
    return (1 - dev % 2) * (dev // 2) + (dev % 2) * (n - 1 - dev // 2)


def ring_dev(pos, n):
    high = pos // (n // 2)
    return (1 - high) * (2 * pos) + high * (2 * (n - 1 - pos) + 1)


def barrier(peers):
    sem = pltpu.get_barrier_semaphore()
    for peer in peers:
        pl.semaphore_signal(sem, inc=1, device_id=peer, device_id_type=MESH)
    pl.semaphore_wait(sem, len(peers))


def reach(bias, way, n):
    return n // 2 if bias == way else n // 2 - 1


class Ring:
    def __init__(self, n, parts, send_sem, recv_sem, land=None):
        self.n, self.parts, self.land = n, parts, land
        self.send_sem, self.recv_sem = send_sem, recv_sem
        self.me = lax.axis_index("dp")
        self.pos = ring_pos(self.me, n)
        self.peer = [{"dp": self.dev(1)}, {"dp": self.dev(-1)}]

    def dev(self, offset):
        return ring_dev((self.pos + (offset + self.n) % self.n) % self.n, self.n)

    def reach(self, part, way):
        return reach(part % 2, way, self.n)

    def gather(self, part, way, hop, ahead):
        away = hop - 1 if ahead else hop
        block = self.parts[part](self.dev(-away if way == 0 else away))
        return pltpu.make_async_remote_copy(
            block,
            block,
            self.send_sem.at[part, way, hop - 1],
            self.recv_sem.at[part, way, hop - 1],
            device_id=self.peer[way],
            device_id_type=MESH,
        )

    def gather_step(self, part, way, hop):
        if hop > 1:
            self.gather(part, way, hop - 1, False).wait_recv()
        if hop <= self.reach(part, way):
            self.gather(part, way, hop, True).start()

    def gather_sends_done(self, part):
        for way in range(2):
            for hop in range(1, self.reach(part, way) + 1):
                self.gather(part, way, hop, True).wait_send()

    def target(self, part, way, hop):
        away = self.reach(part, way) - hop + 1
        return self.dev(away if way == 0 else -away)

    def slot(self, part, way, hop):
        return self.land(part, hop - 1 + (self.reach(part, 0) if way else 0))

    def reduce(self, part, way, hop):
        return pltpu.make_async_remote_copy(
            self.parts[part](self.target(part, way, hop)),
            self.slot(part, way, hop),
            self.send_sem.at[part, way, hop - 1],
            self.recv_sem.at[part, way, hop - 1],
            device_id=self.peer[way],
            device_id_type=MESH,
        )

    def reduce_step(self, part, way, hop):
        if hop > self.reach(part, way):
            return
        if hop > 1:
            self.reduce(part, way, hop - 1).wait_recv()
            own = self.parts[part](self.target(part, way, hop))
            came = self.slot(part, way, hop - 1)
            own[...] = (own[...].astype(F32) + came[...].astype(F32)).astype(BF)
        self.reduce(part, way, hop).start()

    def reduce_end(self, part):
        total = self.parts[part](self.me)[...].astype(F32)
        for way in range(2):
            last = self.reach(part, way)
            self.reduce(part, way, last).wait_recv()
            total = total + self.slot(part, way, last)[...].astype(F32)
        return total

    def reduce_sends_done(self, part):
        for way in range(2):
            for hop in range(1, self.reach(part, way) + 1):
                self.reduce(part, way, hop).wait_send()


def part_views(attn, attn_cut, ffn=None, ffn_cut=()):
    views = []
    for low, high in attn_cut:
        views.append(lambda b, low=low, high=high: attn.at[b, :, pl.ds(low, high - low)])
    for chunk in range(0 if ffn is None else ffn.shape[0]):
        for low, high in ffn_cut:
            views.append(
                lambda b, c=chunk, low=low, high=high: ffn.at[c, b, :, pl.ds(low, high - low)]
            )
    return views


def halves(cols, step=128):
    mid = cols // 2 // step * step
    return ((0, mid), (mid, cols))


def gather_kernel(n, attn_ref, ffn_ref, attn_out, ffn_out, local_sem, send_sem, recv_sem):
    parts = part_views(attn_out, halves(attn_ref.shape[-1]), ffn_out, halves(ffn_ref.shape[-1]))
    ring = Ring(n, parts, send_sem, recv_sem)
    mine = [
        pltpu.make_async_copy(attn_ref, attn_out.at[ring.me], local_sem.at[0]),
        pltpu.make_async_copy(ffn_ref, ffn_out.at[:, ring.me], local_sem.at[1]),
    ]
    for copy in mine:
        copy.start()
    barrier(ring.peer)
    for copy in mine:
        copy.wait()
    width = 4
    for low in range(0, len(parts), width):
        for hop in range(1, n // 2 + 2):
            for part in range(low, min(low + width, len(parts))):
                for way in range(2):
                    if hop <= ring.reach(part, way) + 1:
                        ring.gather_step(part, way, hop)
    for part in range(len(parts)):
        ring.gather_sends_done(part)


def reduce_kernel(n, attn_ref, ffn_ref, attn_out, ffn_out, attn_buf, ffn_buf, attn_land, ffn_land, local_sem, send_sem, recv_sem):
    acut, fcut = halves(attn_ref.shape[-1]), halves(ffn_ref.shape[-1])
    parts = part_views(attn_buf, acut, ffn_buf, fcut)
    landing = part_views(attn_land, acut, ffn_land, fcut)
    ring = Ring(n, parts, send_sem, recv_sem, lambda part, slot: landing[part](slot))
    load = [
        pltpu.make_async_copy(attn_ref, attn_buf, local_sem.at[0]),
        pltpu.make_async_copy(ffn_ref, ffn_buf, local_sem.at[1]),
    ]
    for copy in load:
        copy.start()
    barrier(ring.peer)
    for copy in load:
        copy.wait()
    width = 4
    for low in range(0, len(parts), width):
        for hop in range(1, n // 2 + 1):
            for part in range(low, min(low + width, len(parts))):
                for way in range(2):
                    ring.reduce_step(part, way, hop)
        for part in range(low, min(low + width, len(parts))):
            total = ring.reduce_end(part)
            if part < 2:
                attn_out[:, acut[part][0] : acut[part][1]] = total
            else:
                cut = fcut[part % 2]
                ffn_out[part // 2 - 1, :, cut[0] : cut[1]] = total
    for part in range(len(parts)):
        ring.reduce_sends_done(part)


VMEM_LIMIT = 60 * 2**20


def vmem_specs(count):
    return [pl.BlockSpec(memory_space=pltpu.VMEM)] * count


def any_specs(count):
    return [pl.BlockSpec(memory_space=pl.ANY)] * count


def ring_gather(n, attn, ffn):
    chunks = ffn.shape[0]
    sems = pltpu.SemaphoreType.DMA((2 * (chunks + 1), 2, n // 2))
    return pl.pallas_call(
        partial(gather_kernel, n),
        out_shape=(
            jax.ShapeDtypeStruct((n,) + attn.shape, BF),
            jax.ShapeDtypeStruct((chunks, n) + ffn.shape[1:], BF),
        ),
        in_specs=any_specs(2),
        out_specs=vmem_specs(2),
        scratch_shapes=[pltpu.SemaphoreType.DMA((2,)), sems, sems],
        compiler_params=pltpu.CompilerParams(
            collective_id=0, has_side_effects=True, vmem_limit_bytes=VMEM_LIMIT
        ),
    )(attn, ffn)


def ring_reduce(n, attn, ffn):
    chunks, _, rows, cols = ffn.shape
    sems = pltpu.SemaphoreType.DMA((2 * (chunks + 1), 2, n // 2))
    return pl.pallas_call(
        partial(reduce_kernel, n),
        out_shape=(
            jax.ShapeDtypeStruct(attn.shape[1:], F32),
            jax.ShapeDtypeStruct((chunks, rows, cols), F32),
        ),
        in_specs=any_specs(2),
        out_specs=vmem_specs(2),
        scratch_shapes=[
            pltpu.VMEM(attn.shape, BF),
            pltpu.VMEM(ffn.shape, BF),
            pltpu.VMEM((n - 1,) + attn.shape[1:], BF),
            pltpu.VMEM((chunks, n - 1, rows, cols), BF),
            pltpu.SemaphoreType.DMA((2,)),
            sems,
            sems,
        ],
        compiler_params=pltpu.CompilerParams(
            collective_id=1, has_side_effects=True, vmem_limit_bytes=VMEM_LIMIT
        ),
    )(attn, ffn)


CHUNK = 256


def pack_rows(array, rows):
    return jnp.pad(array, ((0, rows - array.shape[0]), (0, 0)))


def pack_ffn(gate, up, down_t, rows, step=CHUNK):
    width = gate.shape[1]
    chunks = -(-width // step)
    chunks += chunks % 2 if step != CHUNK else 0

    def cut(array):
        array = jnp.pad(array, ((0, rows - array.shape[0]), (0, chunks * step - width)))
        return array.reshape(rows, chunks, step).transpose(1, 0, 2)

    return jnp.concatenate([cut(gate), cut(up), cut(down_t)], axis=2)


def unpack_ffn(packed, width):
    chunks, rows = packed.shape[:2]
    out = []
    for k in range(3):
        piece = packed[:, :, k * CHUNK : (k + 1) * CHUNK]
        out.append(piece.transpose(1, 0, 2).reshape(rows, chunks * CHUNK)[:, :width])
    return out


def pack_blocks(array, n, rows):
    depth = array.shape[0] // n
    return jnp.pad(array.reshape(n, depth, -1), ((0, 0), (0, rows - depth), (0, 0)))


EPSILON = 1e-06
THETA = 1000000.0
NEG_LARGE = -1e30


def rms_scale(values, gain_vec):
    inverse = lax.rsqrt(jnp.mean(values * values, axis=-1, keepdims=True) + EPSILON)
    return values * inverse * gain_vec


def gelu_product(gate_proj, up_proj):
    return jax.nn.gelu(gate_proj, approximate=True) * up_proj


def rows_product(left, right):
    return lax.dot_general(
        left, right, (((0,), (0,)), ((), ())), preferred_element_type=jnp.float32
    )


def cols_product(left, right):
    return lax.dot_general(
        left, right, (((1,), (1,)), ((), ())), preferred_element_type=jnp.float32
    )


def plain_product(left, right):
    return jnp.dot(left, right, preferred_element_type=jnp.float32)


def rotary_tables(segments):
    count = segments.shape[0]
    row_index = jnp.arange(count, dtype=jnp.int32)
    previous = jnp.concatenate([jnp.full((1,), -1, jnp.int32), segments[:-1]])
    starts = jnp.where(segments != previous, row_index, jnp.zeros_like(row_index))
    seq_start = lax.cummax(starts, axis=0)
    position = (row_index - seq_start).astype(jnp.float32)
    half_width = HD // 2
    exponent = -2.0 * jnp.arange(half_width, dtype=jnp.float32) / HD
    inverse = jnp.power(jnp.float32(THETA), exponent)
    angles = position[:, None] * inverse[None, :]
    cosine = jnp.concatenate([jnp.cos(angles), jnp.cos(angles)], axis=1)
    sine_tab = jnp.concatenate([jnp.sin(angles), jnp.sin(angles)], axis=1)
    return (cosine, sine_tab)


def prepare(projection, gain_vec, cosine, sine_tab):
    normed = rms_scale(projection, gain_vec)
    half_width = HD // 2
    turned = jnp.concatenate([-normed[..., half_width:], normed[..., :half_width]], axis=-1)
    return normed * cosine[:, None, :] + turned * sine_tab[:, None, :]


def visible(segments):
    tile_count = segments.shape[0] // SEGMAX
    seg_tiles = segments.reshape(tile_count, SEGMAX)
    offsets = jnp.arange(SEGMAX, dtype=jnp.int32)
    same = seg_tiles[:, :, None] == seg_tiles[:, None, :]
    return same & (offsets[:, None] >= offsets[None, :])


def tile_scores(query_tiles, key_tiles, segments):
    head_width = key_tiles.shape[-1]
    scores = jnp.einsum(
        "tqhd,tkd->thqk", query_tiles, key_tiles, preferred_element_type=jnp.float32
    ) * head_width ** (-0.5)
    return jnp.where(visible(segments)[:, None], scores, NEG_LARGE)


def attend(query_ready, key_ready, value_b, segments):
    row_count, head_count, head_width = query_ready.shape
    tile_count = row_count // SEGMAX
    query_tiles = query_ready.reshape(tile_count, SEGMAX, head_count, head_width)
    key_tiles = key_ready.reshape(tile_count, SEGMAX, head_width)
    value_tiles = value_b.reshape(tile_count, SEGMAX, head_width)
    scores = tile_scores(query_tiles, key_tiles, segments)
    row_max = jnp.max(scores, axis=-1, keepdims=True)
    row_total = jnp.sum(jnp.exp(scores - row_max), axis=-1, keepdims=True)
    log_total = row_max + jnp.log(row_total)
    probs = jnp.exp(scores - log_total).astype(jnp.bfloat16)
    attended = jnp.einsum("thqk,tkd->tqhd", probs, value_tiles, preferred_element_type=jnp.float32)
    return (attended.reshape(row_count, head_count * head_width).astype(jnp.bfloat16), log_total)


def attend_back(query_ready, key_ready, value_b, segments, log_total, d_attended):
    row_count, head_count, head_width = query_ready.shape
    tile_count = row_count // SEGMAX
    query_tiles = query_ready.reshape(tile_count, SEGMAX, head_count, head_width)
    key_tiles = key_ready.reshape(tile_count, SEGMAX, head_width)
    value_tiles = value_b.reshape(tile_count, SEGMAX, head_width)
    grad_tiles = d_attended.reshape(tile_count, SEGMAX, head_count, head_width)
    scores = tile_scores(query_tiles, key_tiles, segments)
    prob_vals = jnp.exp(scores - log_total)
    prob_b = prob_vals.astype(jnp.bfloat16)
    d_value = jnp.einsum(
        "thqk,tqhd->tkd", prob_b, grad_tiles, preferred_element_type=jnp.float32
    ).reshape(row_count, head_width)
    d_probs = jnp.einsum(
        "tqhd,tkd->thqk", grad_tiles, value_tiles, preferred_element_type=jnp.float32
    )
    row_delta = jnp.sum(prob_vals * d_probs, axis=-1, keepdims=True)
    d_scores = (prob_vals * (d_probs - row_delta) * head_width ** (-0.5)).astype(jnp.bfloat16)
    d_query = jnp.einsum(
        "thqk,tkd->tqhd", d_scores, key_tiles, preferred_element_type=jnp.float32
    ).reshape(row_count, head_count, head_width)
    d_key = jnp.einsum(
        "thqk,tqhd->tkd", d_scores, query_tiles, preferred_element_type=jnp.float32
    ).reshape(row_count, head_width)
    return (d_query, d_key, d_value)


def local(
    inputs,
    segments,
    w_query,
    w_key,
    w_value,
    w_out,
    g_in,
    g_attn,
    g_query,
    g_key,
    w_gate,
    w_up,
    w_down,
    g_pre,
    g_post,
    cotangent,
):
    n = lax.axis_size("dp")
    depth = w_query.shape[0]
    rows = -(-depth // 16) * 16
    width = w_gate.shape[1]
    gains = jnp.stack([g_in, g_attn, g_pre, g_post], axis=1)
    attn_pack = jnp.concatenate(
        [w_query, w_key, w_value, w_out.T, jnp.pad(gains, ((0, 0), (0, 124)))], axis=1
    )
    attn_all, ffn_all = ring_gather(
        n, pack_rows(attn_pack, rows), pack_ffn(w_gate, w_up, w_down.T, rows)
    )
    attn_all = attn_all[:, :depth].reshape(n * depth, -1)
    ffn_all = ffn_all[:, :, :depth].reshape(ffn_all.shape[0], n * depth, -1)
    wq_full, wk_full, wv_full, wo_t = (attn_all[:, k * HD : (k + 1) * HD] for k in range(4))
    wo_full = wo_t.T
    gin_full, gattn_full, gpre_full, gpost_full = (attn_all[:, 4 * HD + k] for k in range(4))
    wg_full, wu_full, wd_t = unpack_ffn(ffn_all, width)
    wd_full = wd_t.T
    gain_in = gin_full.astype(jnp.float32)
    gain_attn = gattn_full.astype(jnp.float32)
    gain_query = g_query.astype(jnp.float32)
    gain_key = g_key.astype(jnp.float32)
    cosine, sine_tab = rotary_tables(segments)
    inputs_f = inputs.astype(jnp.float32)
    normed_shard = rms_scale(inputs_f, gain_in).astype(jnp.bfloat16)
    normed_in = lax.all_gather(normed_shard, "tensor", axis=0, tiled=True)
    row_count = normed_in.shape[0]
    head_count = wq_full.shape[1] // HD
    key_proj = plain_product(normed_in, wk_full)
    value_b = plain_product(normed_in, wv_full).astype(jnp.bfloat16)
    key_ready = prepare(key_proj[:, None, :], gain_key, cosine, sine_tab)[:, 0, :].astype(
        jnp.bfloat16
    )
    query_proj = plain_product(normed_in, wq_full).reshape(row_count, head_count, HD)
    query_ready = prepare(query_proj, gain_query, cosine, sine_tab).astype(jnp.bfloat16)
    attended, log_total = attend(query_ready, key_ready, value_b, segments)
    projected = lax.psum_scatter(
        plain_product(attended, wo_full), "tensor", scatter_dimension=0, tiled=True
    )
    residual_mid = inputs_f + rms_scale(projected, gain_attn)
    gain_pre = gpre_full.astype(jnp.float32)
    gain_post = gpost_full.astype(jnp.float32)
    normed_mid = lax.all_gather(
        rms_scale(residual_mid, gain_pre).astype(jnp.bfloat16), "tensor", axis=0, tiled=True
    )
    gate_proj = plain_product(normed_mid, wg_full)
    up_proj = plain_product(normed_mid, wu_full)
    hidden = gelu_product(gate_proj, up_proj).astype(jnp.bfloat16)
    feed = lax.psum_scatter(
        plain_product(hidden, wd_full), "tensor", scatter_dimension=0, tiled=True
    )
    output = (residual_mid + rms_scale(feed, gain_post)).astype(jnp.bfloat16)
    wg_back, wu_back, wd_back = wg_full, wu_full, wd_full
    grad_output = cotangent.astype(jnp.float32)
    d_feed_f, grad_g_post = jax.vjp(rms_scale, feed, gain_post)[1](grad_output)
    d_feed = lax.all_gather(d_feed_f.astype(jnp.bfloat16), "tensor", axis=0, tiled=True)
    d_hidden = cols_product(d_feed, wd_back)
    d_gate_f, d_up_f = jax.vjp(gelu_product, gate_proj, up_proj)[1](d_hidden)
    d_gate = d_gate_f.astype(jnp.bfloat16)
    d_up = d_up_f.astype(jnp.bfloat16)
    grad_gate = rows_product(normed_mid, d_gate)
    grad_up = rows_product(normed_mid, d_up)
    d_normed_mid = lax.psum_scatter(
        cols_product(d_gate, wg_back) + cols_product(d_up, wu_back),
        "tensor",
        scatter_dimension=0,
        tiled=True,
    )
    d_mid_n, grad_g_pre = jax.vjp(rms_scale, residual_mid, gain_pre)[1](d_normed_mid)
    d_mid = grad_output + d_mid_n
    d_proj_f, grad_g_attn = jax.vjp(rms_scale, projected, gain_attn)[1](d_mid)
    wq_back, wk_back, wv_back, wo_back = wq_full, wk_full, wv_full, wo_full
    d_proj = lax.all_gather(d_proj_f.astype(jnp.bfloat16), "tensor", axis=0, tiled=True)
    d_attended = cols_product(d_proj, wo_back).astype(jnp.bfloat16)
    d_query_ready, d_key_ready, d_value_f = attend_back(
        query_ready, key_ready, value_b, segments, log_total, d_attended
    )
    rotate_fn = partial(prepare, cosine=cosine, sine_tab=sine_tab)
    d_query_f, grad_g_query = jax.vjp(rotate_fn, query_proj, gain_query)[1](d_query_ready)
    d_key_f, grad_g_key = jax.vjp(rotate_fn, key_proj[:, None, :], gain_key)[1](
        d_key_ready[:, None, :]
    )
    d_query = d_query_f.reshape(row_count, head_count * HD).astype(jnp.bfloat16)
    d_key = d_key_f[:, 0, :].astype(jnp.bfloat16)
    d_value = d_value_f.astype(jnp.bfloat16)
    grad_query = rows_product(normed_in, d_query)
    grad_key = rows_product(normed_in, d_key)
    grad_value = rows_product(normed_in, d_value)
    d_normed_terms = (
        cols_product(d_query, wq_back)
        + cols_product(d_key, wk_back)
        + cols_product(d_value, wv_back)
    )
    d_normed_in = lax.psum_scatter(
        d_normed_terms.astype(jnp.bfloat16), "tensor", scatter_dimension=0, tiled=True
    ).astype(jnp.float32)
    d_in_n, grad_g_in = jax.vjp(rms_scale, inputs_f, gain_in)[1](d_normed_in)
    d_inputs = (d_mid + d_in_n).astype(jnp.bfloat16)
    attn_part = jnp.concatenate(
        [grad_query, grad_key, grad_value, rows_product(d_proj, attended)], axis=1
    ).astype(BF)
    attn_part = pack_blocks(attn_part, n, rows)
    ffn_part = pack_ffn(
        grad_gate.astype(BF), grad_up.astype(BF), rows_product(d_feed, hidden).astype(BF), n * depth
    )
    ffn_part = jax.vmap(lambda a: pack_blocks(a, n, rows))(ffn_part)
    attn_sum, ffn_sum = ring_reduce(n, attn_part, ffn_part)
    attn_sum, ffn_sum = attn_sum[:depth], ffn_sum[:, :depth]
    sum_gate, sum_up, sum_down_t = unpack_ffn(ffn_sum, width)
    split_grads = (
        attn_sum[:, :HD],
        attn_sum[:, 3 * HD : 4 * HD].T,
        sum_gate,
        sum_up,
        sum_down_t.T,
    )
    sum_key, sum_value = attn_sum[:, HD : 2 * HD], attn_sum[:, 2 * HD : 3 * HD]
    shared = (
        lax.psum_scatter(sum_key, "tensor", scatter_dimension=0, tiled=True),
        lax.psum_scatter(sum_value, "tensor", scatter_dimension=0, tiled=True),
        lax.psum_scatter(grad_g_in, ("dp", "tensor"), scatter_dimension=0, tiled=True),
        lax.psum_scatter(grad_g_attn, ("dp", "tensor"), scatter_dimension=0, tiled=True),
        lax.psum_scatter(grad_g_pre, ("dp", "tensor"), scatter_dimension=0, tiled=True),
        lax.psum_scatter(grad_g_post, ("dp", "tensor"), scatter_dimension=0, tiled=True),
        lax.psum_scatter(grad_g_query, ("dp", "tensor"), scatter_dimension=0, tiled=True),
        lax.psum_scatter(grad_g_key, ("dp", "tensor"), scatter_dimension=0, tiled=True),
    )
    return (
        output,
        d_inputs,
        split_grads[0],
        shared[0],
        shared[1],
        split_grads[1],
        shared[2],
        shared[3],
        shared[6],
        shared[7],
        split_grads[2],
        split_grads[3],
        split_grads[4],
        shared[4],
        shared[5],
    )


SCALE = HD**-0.5
ROOT = 0.7978845608028654
CUBIC = 0.044715


def dot_nn(a, b):
    return jnp.dot(a, b, preferred_element_type=F32)


def dot_nt(a, b):
    return lax.dot_general(a, b, (((1,), (1,)), ((), ())), preferred_element_type=F32)


def dot_tn(a, b):
    return lax.dot_general(a, b, (((0,), (0,)), ((), ())), preferred_element_type=F32)


def inverse_rms(values):
    return lax.rsqrt(jnp.mean(values * values, axis=-1, keepdims=True) + EPSILON)


def rms_back(values, gain_vec, grad):
    inverse = inverse_rms(values)
    unit = values * inverse
    scaled = grad * gain_vec
    back = inverse * (scaled - unit * jnp.mean(scaled * unit, axis=-1, keepdims=True))
    return back, grad * unit


def gelu_parts(gate):
    bent = jnp.tanh(ROOT * (gate + CUBIC * gate * gate * gate))
    return 0.5 * gate * (1.0 + bent), bent


class Quad:
    def __init__(self, part, near, far, gather_sems, reduce_sems):
        self.me = lax.axis_index("tensor")
        self.twin = self.me + 1 - 2 * (self.me % 2)
        self.across = (self.me + 2) % 4
        self.corner = (self.twin + 2) % 4
        self.part, self.near, self.far = part, near, far
        self.gather_sems, self.reduce_sems = gather_sems, reduce_sems

    def copy(self, src, dst, sems, use, k, peer):
        return pltpu.make_async_remote_copy(
            src,
            dst,
            sems[0].at[use, k],
            sems[1].at[use, k],
            device_id={"tensor": peer},
            device_id_type=MESH,
        )

    def gather(self, use, k, buf):
        place = self.across if k == 2 else self.me
        block = buf(place) if callable(buf) else buf.at[place]
        peer = self.across if k == 1 else self.twin
        return self.copy(block, block, self.gather_sems, use, k, peer)

    def gather_start(self, use, buf):
        self.gather(use, 1, buf).start()
        self.gather(use, 0, buf).start()

    def gather_relay(self, use, buf):
        self.gather(use, 1, buf).wait_recv()
        self.gather(use, 2, buf).start()

    def gather_end(self, use, buf):
        self.gather(use, 0, buf).wait_recv()
        self.gather(use, 2, buf).wait_recv()
        for k in range(3):
            self.gather(use, k, buf).wait_send()

    def reduce(self, use, k):
        block = self.part.at[(self.twin, self.corner, self.across)[k]]
        land = self.far if k == 2 else self.near.at[k]
        peer = self.across if k == 2 else self.twin
        return self.copy(block, land, self.reduce_sems, use, k, peer)

    def reduce_start(self, use):
        self.reduce(use, 1).start()
        self.reduce(use, 0).start()

    def reduce_relay(self, use):
        self.reduce(use, 1).wait_recv()
        for low in range(0, self.part.shape[1], 64):
            rows = pl.ds(low, 64)
            total = self.part[self.across, rows].astype(F32) + self.near[1, rows].astype(F32)
            self.part[self.across, rows] = total.astype(BF)
        self.reduce(use, 2).start()

    def reduce_end(self, use):
        self.reduce(use, 0).wait_recv()
        self.reduce(use, 2).wait_recv()
        for k in range(3):
            self.reduce(use, k).wait_send()


class Octet:
    def __init__(self, part, near, far, bend, gather_sems, reduce_sems):
        tensor, dp = lax.axis_index("tensor"), lax.axis_index("dp")
        z = dp // 2
        self.low, self.x, self.core = z % 2, tensor // 2, tensor % 2
        self.twin = {"tensor": tensor + 1 - 2 * self.core}
        self.across = {"tensor": (tensor + 2) % 4}
        self.pair = {"dp": dp + 2 - 4 * self.low}
        self.part, self.near, self.far, self.bend = part, near, far, bend
        self.gather_sems, self.reduce_sems = gather_sems, reduce_sems

    def block(self, p, other=0):
        core = (self.core + other) % 2
        return (self.low + p // 2) % 2 * 4 + (self.x + p % 2) % 2 * 2 + core

    def copy(self, src, dst, sems, use, k, peer):
        return pltpu.make_async_remote_copy(
            src, dst, sems[0].at[use, k], sems[1].at[use, k], device_id=peer, device_id_type=MESH
        )

    def gather(self, use, k, buf, come=False):
        half = buf.shape[1] // 2
        if k < 2:
            place, peer = (k + 1 if come else 0), (self.across, self.pair)[k]
            ref = buf.at[self.block(place)]
        elif k < 6:
            ref = buf.at[self.block(k - 2, 1 if come else 0)]
            peer = self.twin
        else:
            place = 3 if come else k - 5
            ref = buf.at[self.block(place), pl.ds((k - 6) * half, half)]
            peer = (self.pair, self.across)[k - 6]
        return self.copy(ref, ref, self.gather_sems, use, k, peer)

    def gather_start(self, use, buf):
        for k in range(3):
            self.gather(use, k, buf).start()

    def gather_relay(self, use, buf, k):
        self.gather(use, k, buf, True).wait_recv()
        self.gather(use, 6 + k, buf).start()
        self.gather(use, 3 + k, buf).start()

    def gather_corner(self, use, buf):
        for k in (6, 7):
            self.gather(use, k, buf, True).wait_recv()
        self.gather(use, 5, buf).start()

    def gather_end(self, use, buf):
        for k in range(2, 6):
            self.gather(use, k, buf, True).wait_recv()
        for k in range(8):
            self.gather(use, k, buf).wait_send()

    def reduce(self, use, k):
        half = self.part.shape[1] // 2
        if k < 4:
            return self.copy(
                self.part.at[self.block(k, 1)], self.near.at[k], self.reduce_sems, use, k, self.twin
            )
        peer = (self.across, self.pair)[k % 2]
        if k < 6:
            src, dst = self.part.at[self.block(3), pl.ds((k - 4) * half, half)], self.bend.at[k - 4]
        else:
            src, dst = self.part.at[self.block(k - 5)], self.far.at[k - 6]
        return self.copy(src, dst, self.reduce_sems, use, k, peer)

    def add(self, place, low, count, came):
        step = 32

        def body(i, _):
            at = pl.multiple_of(i * step, step)
            rows = pl.ds(low + at, step)
            total = self.part[self.block(place), rows].astype(F32) + came[pl.ds(at, step)].astype(F32)
            self.part[self.block(place), rows] = total.astype(BF)
            return 0

        lax.fori_loop(0, count // step, body, 0)

    def reduce_near(self, use, place):
        self.reduce(use, place).wait_recv()
        self.add(place, 0, self.part.shape[1], self.near.at[place])

    def reduce_relay(self, use):
        half = self.part.shape[1] // 2
        for k in range(2):
            self.reduce(use, 4 + k).wait_recv()
            self.add(2 - k, k * half, half, self.bend.at[k])
            self.reduce(use, 7 - k).start()

    def reduce_after(self, use, i):
        for k in range(4):
            pl.when(i == 6 - 2 * k)(lambda k=k: self.reduce(use, k).start())
        for k in (1, 2):
            pl.when(i == 7 - 2 * k)(lambda k=k: self.reduce_near(use, k))
        pl.when(i == 6)(lambda: self.reduce_relay(use))

        @pl.when(i == 1)
        def _():
            self.reduce_near(use, 3)
            self.reduce(use, 4).start()
            self.reduce(use, 5).start()

    @staticmethod
    def arrival(j):
        a, b = j // 2, j % 2
        up = (a + 1) // 2
        mid = up * (2 - up)
        return up + mid * b + a // 3, (1 - mid) * b + mid * (a // 2)

    def gather_before(self, use, buf, j):
        for at, k in ((1, 2), (4, 3), (5, 4), (7, 5)):
            pl.when(j == at)(lambda k=k: self.gather(use, k, buf, True).wait_recv())

        @pl.when(j == 2)
        def _():
            self.gather_relay(use, buf, 0)
            self.gather_relay(use, buf, 1)

        pl.when(j == 6)(lambda: self.gather_corner(use, buf))

    def gather_sends_done(self, use, buf):
        for k in range(8):
            self.gather(use, k, buf).wait_send()

    def reduce_end(self, use):
        for k in (0, 6, 7):
            self.reduce(use, k).wait_recv()
        for k in range(8):
            self.reduce(use, k).wait_send()


class Columns:
    def __init__(self, ffn, other, land, gather_sems, reduce_sems):
        dp = lax.axis_index("dp")
        z, y = dp // 2, dp % 2
        self.low = z % 2
        self.inner = z * (3 - z) > 0
        self.outer = z * (3 - z) < 1
        ranks = (z, z + 1 - 2 * (z % 2), (z + 2) % 4, 3 - z)
        self.mine = [rank * 2 + y for rank in ranks]
        self.theirs = [rank * 2 + 1 - y for rank in ranks]
        self.ffn, self.other, self.land = ffn, other, land
        self.gather_sems, self.reduce_sems = gather_sems, reduce_sems

    def copy(self, src, dst, sems, u, send, recv, peer):
        return pltpu.make_async_remote_copy(
            src,
            dst,
            sems[0].at[u, send],
            sems[1].at[u, recv],
            device_id={"dp": peer},
            device_id_type=MESH,
        )

    def gather(self, u, k):
        own = self.ffn.at[u, self.mine[0]]
        sems = self.gather_sems
        if k == 0:
            return self.copy(own, own, sems, u, 0, 0, self.mine[2])
        if k == 1:
            return self.copy(self.other.at[u], own, sems, u, 1, 1, self.mine[1])
        if k == 2:
            return self.copy(self.other.at[u], own, sems, u, 2, 2, self.mine[3])
        if k == 3:
            block = self.ffn.at[u, self.mine[1]]
            return self.copy(block, block, sems, u, 3, 2, self.mine[2])
        block = self.ffn.at[u, self.mine[k - 4]]
        return self.copy(block, block, sems, u, k, k, self.theirs[0])

    def come(self, u, k):
        place = self.theirs[k - 4] if k >= 4 else self.mine[(2, 1, 3)[k]]
        block = self.ffn.at[u, place]
        self.copy(block, block, self.gather_sems, u, k, k, place).wait_recv()

    def gather_step(self, u, step):
        if step == 0:
            self.gather(u, 0).start()
            self.gather(u, 1).start()
            pl.when(self.inner)(lambda: self.gather(u, 2).start())
            self.gather(u, 4).start()
        elif step == 1:
            self.come(u, 1)
            pl.when(self.inner)(lambda: self.gather(u, 3).start())
            self.gather(u, 5).start()
        elif step == 2:
            self.come(u, 0)
            self.gather(u, 6).start()
        elif step == 3:
            self.come(u, 2)
            self.gather(u, 7).start()
        else:
            for k in range(4, 8):
                self.come(u, k)

    def gather_sends_done(self, u):
        for k in (0, 1, 4, 5, 6, 7):
            self.gather(u, k).wait_send()

        @pl.when(self.inner)
        def _():
            self.gather(u, 2).wait_send()
            self.gather(u, 3).wait_send()

    def piece(self, item, place):
        unit, count, lane, lanes = item[1:]
        return self.ffn.at[pl.ds(unit, count), place, :, pl.ds(lane, lanes)]

    def reduce(self, item, k):
        if k < 4:
            place, peer = self.theirs[k], self.theirs[0]
        else:
            place = self.mine[(2, 1, 3, 3)[k - 4]]
            peer = self.mine[(2, 1, 3, 2)[k - 4]]
        unit, count, lane, lanes = item[1:]
        land = self.land.at[pl.ds(unit, count), k, :, pl.ds(lane, lanes)]
        return self.copy(
            self.piece(item, place), land, self.reduce_sems, item[0], min(k, 6), k, peer
        )

    def came(self, item, k):
        unit, count, lane, lanes = item[1:]
        return [
            self.land[u, k, :, lane : lane + lanes].astype(F32) for u in range(unit, unit + count)
        ]

    def own(self, item, place):
        unit, count, lane, lanes = item[1:]
        return [
            self.ffn.at[u, self.mine[place], :, pl.ds(lane, lanes)]
            for u in range(unit, unit + count)
        ]

    def add(self, item, place, k):
        self.reduce(item, k).wait_recv()
        for own, came in zip(self.own(item, place), self.came(item, k), strict=True):
            own[...] = (own[...].astype(F32) + came).astype(BF)

    def reduce_step(self, item, step):
        if step == 0:
            for k in (3, 2, 1, 0):
                self.reduce(item, k).start()
        elif step == 1:
            self.add(item, 3, 3)
            pl.when(self.inner)(lambda: self.reduce(item, 6).start())
            pl.when(self.outer)(lambda: self.reduce(item, 7).start())
        elif step == 2:
            self.add(item, 2, 2)
            self.reduce(item, 4).start()
        else:
            self.add(item, 1, 1)
            pl.when(self.inner)(lambda: self.add(item, 1, 7))
            self.reduce(item, 5).start()

    def sum_own(self, item, out):
        for k in (0, 4):
            self.reduce(item, k).wait_recv()
        lanes = item[4]
        for i, (own, one, two) in enumerate(
            zip(self.own(item, 0), self.came(item, 0), self.came(item, 4), strict=True)
        ):
            out[:, i * lanes : (i + 1) * lanes] = own[...].astype(F32) + one + two

    def sum_other(self, item, out):
        self.reduce(item, 5).wait_recv()
        lanes = item[4]
        for i, came in enumerate(self.came(item, 5)):
            out[:, i * lanes : (i + 1) * lanes] = came

        @pl.when(self.inner)
        def _():
            self.reduce(item, 6).wait_recv()
            for i, came in enumerate(self.came(item, 6)):
                out[:, i * lanes : (i + 1) * lanes] += came

    def reduce_sends_done(self, item):
        for k in range(7):
            self.reduce(item, k).wait_send()


class Queue:
    def __init__(self):
        self.steps = []

    def add(self, tag, fn):
        self.steps.append((tag, fn))

    def run(self, count, ready=None):
        while count > 0 and self.steps:
            tag, fn = self.steps[0]
            if ready is not None and tag not in ready:
                return
            self.steps.pop(0)
            fn()
            count -= 1

    def until(self, tag):
        while any(t == tag for t, _ in self.steps):
            self.run(1)


def layer_kernel(
    n,
    x_ref,
    cot_ref,
    seg_row,
    small_ref,
    wo_in,
    wq_in,
    wk_in,
    wv_in,
    gain_in,
    ffn_in,
    dx_ref,
    sums_ref,
    out_hbm,
    ggate_hbm,
    gup_hbm,
    gdown_hbm,
    attn,
    ffn,
    other,
    attn_land,
    ffn_land,
    gate_buf,
    up_buf,
    hid_buf,
    part,
    near,
    far,
    bend,
    xa,
    nm,
    df,
    dp_buf,
    proj_s,
    res_s,
    gains,
    gsum,
    gqk,
    q_proj,
    k_proj,
    qr,
    kr,
    vb,
    att,
    probs,
    cos_s,
    sin_s,
    stage,
    kvg,
    kvg_land,
    local_sem,
    stage_sem,
    ag_send,
    ag_recv,
    rs_send,
    rs_recv,
    cg_send,
    cg_recv,
    cr_send,
    cr_recv,
    og_send,
    og_recv,
    or_send,
    or_recv,
    qg_send,
    qg_recv,
    qr_send,
    qr_recv,
    kv_send,
    kv_recv,
):
    units, _, depth, cols = ffn.shape
    rows, width = x_ref.shape
    attn_cut = ((0, HD), (HD, 2 * HD), (2 * HD, 4 * HD), (4 * HD, attn.shape[-1]))
    parts = part_views(attn, attn_cut)
    landing = part_views(attn_land, attn_cut)
    first = len(attn_cut)
    spot4 = lax.axis_index("tensor")

    def quarter_of(t):
        return attn.at[:, :, pl.ds(pl.multiple_of(2 * HD + t * 128, 128), 128)]

    gathered = list(parts)
    gathered[2] = lambda b: attn.at[
        b, :, pl.ds(pl.multiple_of(2 * HD + spot4 * 128, 128), 128)
    ]
    ring = Ring(n, gathered, ag_send, ag_recv)
    back = Ring(n, parts, rs_send, rs_recv, lambda p, slot: landing[p](slot))
    quad = Quad(part, near, far.at[0], (qg_send, qg_recv), (qr_send, qr_recv))
    octet = Octet(part, near, far, bend, (og_send, og_recv), (or_send, or_recv))
    columns = Columns(ffn, other, ffn_land, (cg_send, cg_recv), (cr_send, cr_recv))
    me, spot = quad.me, octet.block(0)
    gq_ref, gk_ref = small_ref.at[0:1], small_ref.at[1:2]
    freq_ref = small_ref.at[2:3, pl.ds(0, HD // 2)]

    def attn_cols(low, high):
        return attn[:, :, low:high].reshape(width, high - low)

    def unit_cols(u, k, count=1):
        return ffn[u, :, :, k * UNIT : (k + count) * UNIT].reshape(width, count * UNIT)

    def across_units(k, low=0, high=units):
        return jnp.concatenate([unit_cols(u, k) for u in range(low, high)], axis=1)

    mine = [
        pltpu.make_async_copy(wo_in, attn.at[ring.me, :, pl.ds(0, HD)], local_sem.at[0]),
        pltpu.make_async_copy(wq_in, attn.at[ring.me, :, pl.ds(HD, HD)], local_sem.at[4]),
        pltpu.make_async_copy(gain_in, attn.at[ring.me, :, pl.ds(4 * HD, 128)], local_sem.at[5]),
        pltpu.make_async_copy(
            ffn_in.at[pl.ds(columns.low * units, units)], ffn.at[:, ring.me], local_sem.at[1]
        ),
        pltpu.make_async_copy(x_ref, xa.at[me], local_sem.at[2]),
        pltpu.make_async_copy(
            ffn_in.at[pl.ds((1 - columns.low) * units, units)], other, local_sem.at[3]
        ),
    ]
    for copy in mine:
        copy.start()

    def quarter_copy(source):
        cols = pl.ds(pl.multiple_of(me % 2 * 128, 128), 128)
        return pltpu.make_async_copy(
            source.at[:, cols], quarter_of(me).at[ring.me], local_sem.at[6]
        )

    pl.when(me < 2)(lambda: quarter_copy(wk_in).start())
    pl.when(me > 1)(lambda: quarter_copy(wv_in).start())
    greet = [{"dp": peer} for peer in columns.mine[1:] + columns.theirs[:1]]
    greet += [{"tensor": quad.twin}, {"tensor": quad.across}]
    barrier(greet)
    for copy in mine:
        copy.wait()
    quarter_copy(wk_in).wait()
    quad.gather_start(0, xa)

    queue = Queue()
    def ring_gather_step(parts, hop, tag):
        for p in parts:
            for way in range(2):
                if 0 < hop <= ring.reach(p, way) + 1:
                    queue.add(tag, partial(ring.gather_step, p, way, hop))

    for hop in range(1, n // 2 + 1):
        ring_gather_step((2, 3, 1), hop, -1)
        ring_gather_step((0,), hop - 2, -1)
    ring_gather_step((2, 3), n // 2 + 1, -1)
    queue.add(-1, partial(quad.gather_start, 2, quarter_of))
    queue.add(-1, partial(quad.gather_relay, 0, xa))
    queue.add(-1, partial(columns.gather_step, 0, 0))
    ring_gather_step((1,), n // 2 + 1, -1)
    ring_gather_step((0,), n // 2 - 1, -1)
    queue.add(-1, partial(quad.gather_relay, 2, quarter_of))
    ring_gather_step((0,), n // 2, -3)
    for u in range(1, EARLY):
        queue.add(-3, partial(columns.gather_step, u, 0))
    ring_gather_step((0,), n // 2 + 1, -3)
    for u in range(units + 2):
        if u < units:
            queue.add(-2, partial(columns.gather_step, u, 1))
            queue.add(-2, partial(columns.gather_step, u, 2))
        if u + EARLY < units:
            queue.add(-2, partial(columns.gather_step, u + EARLY, 0))
        if 0 < u <= units:
            queue.add(-2, partial(columns.gather_step, u - 1, 3))
        if u > 1:
            queue.add(u - 2, partial(columns.gather_step, u - 2, 4))

    queue.run(AHEAD[0])
    quarter = SEGMAX // 2

    def seg_column(seg_j, half):
        cut = seg_j[:, half * quarter : (half + 1) * quarter].astype(F32)
        return jnp.transpose(jnp.broadcast_to(cut, (128, quarter)))[:, :1]

    def tables(tile, _):
        seg_j = seg_row[pl.ds(tile, 1), :]
        for half in range(2):
            r = 2 * tile + half
            same = seg_column(seg_j, half) == seg_j.astype(F32)
            j = lax.broadcasted_iota(jnp.int32, (quarter, SEGMAX), 1)
            start = jnp.min(jnp.where(same, j, SEGMAX).astype(F32), axis=1, keepdims=True)
            i = lax.broadcasted_iota(jnp.int32, (quarter, 1), 0).astype(F32) + half * quarter
            angle = (i - start) * freq_ref[...]
            cos_s[r] = jnp.cos(angle)
            sin_s[r] = jnp.sin(angle)
        return 0

    lax.fori_loop(0, N_TILES, tables, 0)
    queue.until(-1)
    flipped = jnp.transpose(attn_cols(4 * HD, 4 * HD + 128).astype(F32))
    gains[...] = flipped[:8]
    quad.gather_end(0, xa)
    queue.run(AHEAD[2])

    sub = 32
    per = rows // sub

    def normalize(i, _):
        b, at = i // per, pl.ds(pl.multiple_of(i % per * sub, sub), sub)
        values = xa[b, at].astype(F32)
        xa[b, at] = (values * inverse_rms(values) * gains[0:1, :]).astype(BF)
        return 0

    lax.fori_loop(0, 4 * per, normalize, 0)

    def rope(values, gain_vec, r):
        normed = values * inverse_rms(values) * gain_vec
        low, high = normed[:, : HD // 2], normed[:, HD // 2 :]
        cosine, sine = cos_s[r], sin_s[r]
        return jnp.concatenate([low * cosine - high * sine, high * cosine + low * sine], axis=1)

    queue.run(AHEAD[3])

    quad.gather_end(2, quarter_of)

    def project(r, _):
        block = xa[r]
        query = dot_nn(block, attn_cols(HD, 2 * HD))
        q_proj[r] = query.astype(BF)
        qr[r] = rope(query, gq_ref[...], r).astype(BF)
        key = dot_nn(block, attn_cols(2 * HD, 3 * HD))
        k_proj[r] = key.astype(BF)
        kr[r] = rope(key, gk_ref[...], r).astype(BF)
        vb[r] = dot_nn(block, attn_cols(3 * HD, 4 * HD)).astype(BF)
        return 0

    lax.fori_loop(0, 4, project, 0)
    queue.run(AHEAD[4])

    def attend_tile(tile, _):
        two = pl.ds(2 * tile, 2)
        keys = kr[two].reshape(SEGMAX, HD)
        values = vb[two].reshape(SEGMAX, HD)
        seg_j = seg_row[pl.ds(tile, 1), :]
        for half in range(2):
            r = 2 * tile + half
            scores = dot_nt(qr[r], keys) * SCALE
            j = lax.broadcasted_iota(jnp.int32, (quarter, SEGMAX), 1)
            i = lax.broadcasted_iota(jnp.int32, (quarter, SEGMAX), 0) + half * quarter
            seen = (seg_column(seg_j, half) == seg_j.astype(F32)) & (i >= j)
            scores = jnp.where(seen, scores, NEG_LARGE)
            powers = jnp.exp(scores - jnp.max(scores, axis=1, keepdims=True))
            weights = (powers / jnp.sum(powers, axis=1, keepdims=True)).astype(BF)
            probs[r] = weights
            att[r] = dot_nn(weights, values).astype(BF)
        return 0

    lax.fori_loop(0, N_TILES, attend_tile, 0)
    queue.run(AHEAD[5])

    queue.until(-3)

    def out_block(r, _):
        part[r] = dot_nt(att[r], attn_cols(0, HD)).astype(BF)
        return 0

    lax.fori_loop(0, 4, out_block, 0)
    quad.reduce_start(0)
    queue.run(AHEAD[6])
    quad.reduce_relay(0)
    queue.run(AHEAD[7])
    quad.reduce_end(0)

    def total(at):
        return part[me, at].astype(F32) + near[0, at].astype(F32) + far[0, at].astype(F32)

    def total_ffn(at):
        return part[spot, at].astype(F32) + near[0, at].astype(F32) + (
            far[0, at].astype(F32) + far[1, at].astype(F32)
        )

    def at_rows(i):
        return pl.ds(pl.multiple_of(i * sub, sub), sub)

    def middle(i, _):
        at = at_rows(i)
        projected = total(at)
        proj_s[at] = projected.astype(BF)
        mid = x_ref[at].astype(F32) + projected * inverse_rms(projected) * gains[1:2, :]
        res_s[at] = mid
        nm[spot, at] = (mid * inverse_rms(mid) * gains[2:3, :]).astype(BF)
        return 0

    lax.fori_loop(0, per, middle, 0)
    octet.gather_start(0, nm)
    queue.run(AHEAD[8])
    octet.gather_relay(0, nm, 0)
    octet.gather_relay(0, nm, 1)
    queue.run(AHEAD[9])
    octet.gather_corner(0, nm)
    queue.run(AHEAD[9])
    octet.gather_end(0, nm)

    for u in range(units):
        queue.until(u)
        lanes = slice(u * UNIT, (u + 1) * UNIT)

        def ffn_block(r, _):
            both = dot_nn(nm[r], unit_cols(u, 0, 2))
            gate, up = both[:, :UNIT], both[:, UNIT:]
            gate_buf[r, :, lanes] = gate.astype(BF)
            up_buf[r, :, lanes] = up.astype(BF)
            hid_buf[r, :, lanes] = (gelu_parts(gate)[0] * up).astype(BF)
            return 0

        lax.fori_loop(0, 8, ffn_block, 0)
        queue.run(AHEAD[10])
    queue.run(10**6)

    def feed_block(i, _):
        b = octet.block(3 - i // 2, 1 - i % 2)
        part[b] = dot_nt(hid_buf[b], across_units(2)).astype(BF)
        octet.reduce_after(0, i)
        return 0

    lax.fori_loop(0, 8, feed_block, 0)
    for p in range(first):
        ring.gather_sends_done(p)
    for u in range(units):
        columns.gather_sends_done(u)
    octet.reduce_end(0)
    eight = (8, width)

    def fold(values):
        return jnp.sum(values.reshape(sub // 8, 8, values.shape[-1]), axis=0)

    def after_feed(i, carry):
        at = at_rows(i)
        feed = total_ffn(at)
        dx_ref[at] = (res_s[at] + feed * inverse_rms(feed) * gains[3:4, :]).astype(BF)
        grad, gain_part = rms_back(feed, gains[3:4, :], cot_ref[at].astype(F32))
        df[spot, at] = grad.astype(BF)
        return carry + fold(gain_part)

    gain_sum = lax.fori_loop(0, per, after_feed, jnp.zeros(eight, F32))
    gsum[3:4, :] = jnp.sum(gain_sum, axis=0, keepdims=True)
    put_out = pltpu.make_async_copy(dx_ref, out_hbm, local_sem.at[0])
    put_out.start()
    octet.gather_start(1, df)

    queue = Queue()
    pending = []

    def finish(item, other):
        k = len(pending)
        if k >= 2:
            for copy in pending[k - 2]:
                copy.wait()
        (columns.sum_other if other else columns.sum_own)(item, stage.at[k % 2])
        half = 1 - columns.low if other else columns.low
        unit, count, lane, lanes = item[1:]
        at = pl.multiple_of(half * (units * UNIT) + unit * UNIT, UNIT)
        outs = ((ggate_hbm, UNIT), (gup_hbm, UNIT)) if lane == 0 else ((gdown_hbm, count * UNIT),)
        copies = [
            pltpu.make_async_copy(
                stage.at[k % 2, :, pl.ds(which * UNIT, wide)],
                hbm.at[:, pl.ds(at, wide)],
                stage_sem.at[k % 2, which],
            )
            for which, (hbm, wide) in enumerate(outs)
        ]
        for copy in copies:
            copy.start()
        pending.append(copies)

    pairs = [(low, min(low + 2, units)) for low in range(0, units, 2)]
    items = [(k, low, high - low, 2 * UNIT, UNIT) for k, (low, high) in enumerate(pairs)]
    items += [(len(pairs) + u, u, 1, 0, 2 * UNIT) for u in range(units)]
    count = len(items)
    queue.add(0, partial(columns.reduce_step, items[0], 0))
    for k in range(count + 2):
        if k + 1 < count:
            queue.add(k + 1, partial(columns.reduce_step, items[k + 1], 0))
        if k < count:
            for step in range(1, 4):
                queue.add(k, partial(columns.reduce_step, items[k], step))
        if k > 1:
            queue.add(k - 2, partial(finish, items[k - 2], False))
            queue.add(k - 2, partial(finish, items[k - 2], True))
    ready = set()
    def tall(ref, lanes):
        return ref[:, :, lanes].reshape(8 * rows, lanes.stop - lanes.start)

    def down_grad(low, high):
        value = dot_tn(df[...].reshape(8 * rows, width), tall(hid_buf, slice(low * UNIT, high * UNIT)))
        value = value.astype(BF)
        for u in range(low, high):
            piece = value[:, (u - low) * UNIT : (u - low + 1) * UNIT]
            ffn[u, :, :, 2 * UNIT :] = piece.reshape(n, depth, UNIT)
        ready.add(low // 2)

    def back_block(j, _):
        octet.gather_before(1, df, j)
        b = octet.block(*octet.arrival(j))
        for low, high in pairs:
            lanes = slice(low * UNIT, high * UNIT)
            grad = dot_nn(df[b], across_units(2, low, high))
            gate, up = gate_buf[b, :, lanes].astype(F32), up_buf[b, :, lanes].astype(F32)
            act, bent = gelu_parts(gate)
            slope = 0.5 * (1.0 + bent) + 0.5 * gate * (1.0 - bent * bent) * ROOT * (
                1.0 + 3.0 * CUBIC * gate * gate
            )
            gate_buf[b, :, lanes] = (grad * up * slope).astype(BF)
            up_buf[b, :, lanes] = (grad * act).astype(BF)
        return 0

    lax.fori_loop(0, 8, back_block, 0)
    octet.gather_sends_done(1, df)

    def down_grads(some):
        for low, high in some:
            down_grad(low, high)
            queue.run(PACE[0], ready)

    down_grads(pairs[: WORK[3]])

    def back_part(i, _):
        b = octet.block(3 - i // 2, 1 - i % 2)
        grown = dot_nt(gate_buf[b], across_units(0)) + dot_nt(up_buf[b], across_units(1))
        part[b] = grown.astype(BF)
        octet.reduce_after(1, i)
        return 0

    def gate_grad(u, _):
        lanes = pl.ds(pl.multiple_of(u * UNIT, UNIT), UNIT)
        both = jnp.concatenate(
            [ref[:, :, lanes].reshape(8 * rows, UNIT) for ref in (gate_buf, up_buf)], axis=1
        )
        value = dot_tn(nm[...].reshape(8 * rows, width), both)
        ffn[u, :, :, : 2 * UNIT] = value.astype(BF).reshape(n, depth, 2 * UNIT)
        return 0

    done = [0]

    def do_work(count):
        low, done[0] = done[0], min(units, done[0] + count)
        if low < done[0]:
            lax.fori_loop(low, done[0], gate_grad, 0)
            ready.update(range(len(pairs) + low, len(pairs) + done[0]))
            queue.run(PACE[1] * (done[0] - low), ready)

    lax.fori_loop(0, 4, back_part, 0)
    queue.run(2 * PACE[0], ready)
    lax.fori_loop(4, 8, back_part, 0)
    down_grads(pairs[WORK[3] :])
    do_work(WORK[0])
    do_work(WORK[1])
    queue.run(PACE[2], ready)
    octet.reduce_end(1)

    def after_ffn(i, carry):
        at = at_rows(i)
        grad, pre_part = rms_back(res_s[at], gains[2:3, :], total_ffn(at))
        grad = cot_ref[at].astype(F32) + grad
        res_s[at] = grad
        grad, attn_part = rms_back(proj_s[at].astype(F32), gains[1:2, :], grad)
        dp_buf[me, at] = grad.astype(BF)
        return carry[0] + fold(pre_part), carry[1] + fold(attn_part)

    zero = jnp.zeros(eight, F32)
    pre_sum, attn_sum = lax.fori_loop(0, per, after_ffn, (zero, zero))
    gsum[2:3, :] = jnp.sum(pre_sum, axis=0, keepdims=True)
    gsum[1:2, :] = jnp.sum(attn_sum, axis=0, keepdims=True)
    quad.gather_start(1, dp_buf)
    do_work(WORK[2])
    queue.run(PACE[3], ready)
    quad.gather_relay(1, dp_buf)
    do_work(units)
    queue.run(PACE[4], ready)
    quad.gather_end(1, dp_buf)

    d_q, d_k, d_v = (gate_buf.at[pl.ds(0, 4), :, pl.ds(k * HD, HD)] for k in range(3))
    datt = up_buf.at[pl.ds(0, 4), :, pl.ds(0, HD)]

    def attn_grad(low, left, right):
        value = dot_tn(left.reshape(4 * rows, width), right.reshape(4 * rows, HD))
        attn[:, :, low : low + HD] = value.astype(BF).reshape(n, width // n, HD)

    def ring_hop(hop, *some):
        for p in some:
            for way in range(2):
                back.reduce_step(p, way, hop)

    ready.add(-1)
    def back_out(r, _):
        datt[r] = dot_nn(dp_buf[r], attn_cols(0, HD)).astype(BF)
        return 0

    lax.fori_loop(0, 4, back_out, 0)
    attn_grad(0, dp_buf[...], att[...])
    ring_hop(1, 0)
    queue.run(PACE[5], ready)
    gqk[...] = jnp.zeros_like(gqk)

    def unrope(grad, projection, gain_vec, r, row):
        low, high = grad[:, : HD // 2], grad[:, HD // 2 :]
        cosine, sine = cos_s[r], sin_s[r]
        grad = jnp.concatenate([low * cosine + high * sine, high * cosine - low * sine], axis=1)
        grad, gain_part = rms_back(projection, gain_vec, grad)
        gqk[row : row + 1, :] += jnp.sum(gain_part, axis=0, keepdims=True)
        return grad.astype(BF)

    def back_tile(tile, _):
        two = pl.ds(2 * tile, 2)
        keys = kr[two].reshape(SEGMAX, HD)
        values = vb[two].reshape(SEGMAX, HD)
        d_key = jnp.zeros((SEGMAX, HD), F32)
        d_value = jnp.zeros((SEGMAX, HD), F32)
        for half in range(2):
            r = 2 * tile + half
            d_att = datt[r]
            weights = probs[r]
            d_value = d_value + dot_tn(weights, d_att)
            d_probs = dot_nt(d_att, values)
            weights = weights.astype(F32)
            delta = jnp.sum(weights * d_probs, axis=1, keepdims=True)
            d_scores = (weights * (d_probs - delta) * SCALE).astype(BF)
            d_key = d_key + dot_tn(d_scores, qr[r])
            d_query = dot_nn(d_scores, keys)
            d_q[r] = unrope(d_query, q_proj[r].astype(F32), gq_ref[...], r, 4)
        for half in range(2):
            r = 2 * tile + half
            cut = slice(half * quarter, (half + 1) * quarter)
            d_k[r] = unrope(d_key[cut], k_proj[r].astype(F32), gk_ref[...], r, 5)
            d_v[r] = d_value[cut].astype(BF)
        return 0

    lax.fori_loop(0, N_TILES, back_tile, 0)
    queue.run(PACE[5], ready)

    def back_in(r, _):
        grown = dot_nt(d_q[r], attn_cols(HD, 2 * HD))
        grown = grown + dot_nt(d_k[r], attn_cols(2 * HD, 3 * HD))
        grown = grown + dot_nt(d_v[r], attn_cols(3 * HD, 4 * HD))
        part[r] = grown.astype(BF)
        return 0

    lax.fori_loop(0, 4, back_in, 0)
    quad.reduce_start(1)
    queue.run(PACE[5], ready)

    def three_grads(k, _):
        grad = gate_buf[0:4, :, pl.ds(pl.multiple_of(k * HD, HD), HD)]
        value = dot_tn(xa[...].reshape(4 * rows, width), grad.reshape(4 * rows, HD))
        low = pl.multiple_of((k + 1) * HD, HD)
        attn[:, :, pl.ds(low, HD)] = value.astype(BF).reshape(n, depth, HD)
        return 0

    lax.fori_loop(0, 3, three_grads, 0)
    def input_gain(i, carry):
        b, at = i // per, pl.ds(pl.multiple_of(i % per * sub, sub), sub)
        return carry + fold(part[b, at].astype(F32) * xa[b, at].astype(F32))

    gain_sum = lax.fori_loop(0, 4 * per, input_gain, zero)
    gsum[0:1, :] = jnp.sum(gain_sum, axis=0, keepdims=True) / gains[0:1, :]
    gsum[4:8, :] = jnp.zeros((4, width), F32)
    long = jnp.concatenate([gsum[...], jnp.zeros((120, width), F32)], axis=0)
    long = jnp.transpose(long).reshape(n, width // n, 128)
    short = jnp.concatenate([gqk[...], jnp.zeros((120, HD), F32)], axis=0)
    short = jnp.transpose(short).reshape(n, HD // n, 128)
    attn[:, :, 4 * HD : 4 * HD + 128] = long.astype(BF)
    attn[:, : HD // n, 4 * HD : 4 * HD + 128] = (long[:, : HD // n] + short).astype(BF)

    ring_hop(1, 2, 3, 1)
    quad.reduce_relay(1)
    ring_hop(2, 0)
    queue.run(PACE[6], ready)
    for hop in range(2, n // 2 + 1):
        ring_hop(hop, 2, 3, 1)
        if hop < n // 2:
            ring_hop(hop + 1, 0)
        queue.run(PACE[7], ready)
    kvg[0, :, : 2 * HD] = back.reduce_end(2).astype(BF)
    kvg[0, :, 2 * HD :] = back.reduce_end(3).astype(BF)

    def swap(k):
        return pltpu.make_async_remote_copy(
            kvg.at[k],
            kvg_land.at[k],
            kv_send.at[k],
            kv_recv.at[k],
            device_id={"tensor": (quad.twin, quad.across)[k]},
            device_id_type=MESH,
        )

    swap(0).start()
    quad.reduce_end(1)
    put_out.wait()

    def after_attn(i, _):
        at = at_rows(i)
        grad, _ = rms_back(x_ref[at].astype(F32), gains[0:1, :], total(at))
        dx_ref[at] = (res_s[at] + grad).astype(BF)
        return 0

    swap(0).wait()
    kvg[1] = (kvg[0].astype(F32) + kvg_land[0].astype(F32)).astype(BF)
    swap(1).start()
    lax.fori_loop(0, per, after_attn, 0)
    queue.run(10**6)
    for p in range(2):
        sums_ref[:, p * HD : (p + 1) * HD] = back.reduce_end(p)
    swap(1).wait()
    sums_ref[:, 2 * HD :] = kvg[1].astype(F32) + kvg_land[1].astype(F32)
    for p in range(len(parts)):
        back.reduce_sends_done(p)
    for item in items:
        columns.reduce_sends_done(item)
    for copies in pending[-2:]:
        for copy in copies:
            copy.wait()


AHEAD = (14, 0, 0, 2, 3, 3, 0, 6, 5, 4, 2)
PACE = (2, 2, 6, 6, 4, 3, 2, 3)
WORK = (2, 3, 2, 2)
EARLY = 3
UNIT = 128
N_TILES = 2


def run_layer(n, x, cot, segments, small, attn_weights, ffn_pack):
    rows, width = x.shape
    both, depth, cols = ffn_pack.shape
    units = both // 2
    tokens = segments.shape[0]
    wide = 4 * HD + 128
    parts = 4
    vmem, dma = pltpu.VMEM, pltpu.SemaphoreType.DMA
    grown = both * UNIT
    return pl.pallas_call(
        partial(layer_kernel, n),
        out_shape=(
            jax.ShapeDtypeStruct((rows, width), BF),
            jax.ShapeDtypeStruct((depth, wide), F32),
            jax.ShapeDtypeStruct((rows, width), BF),
            jax.ShapeDtypeStruct((depth, grown), F32),
            jax.ShapeDtypeStruct((depth, grown), F32),
            jax.ShapeDtypeStruct((depth, grown), F32),
        ),
        in_specs=vmem_specs(4) + any_specs(6),
        out_specs=vmem_specs(2) + any_specs(4),
        scratch_shapes=[
            vmem((n, depth, wide), BF),
            vmem((units, n, depth, cols), BF),
            vmem((units, depth, cols), BF),
            vmem((n - 1, depth, wide), BF),
            vmem((units, 8, depth, cols), BF),
            vmem((8, rows, units * UNIT), BF),
            vmem((8, rows, units * UNIT), BF),
            vmem((8, rows, units * UNIT), BF),
            vmem((8, rows, width), BF),
            vmem((4, rows, width), BF),
            vmem((2, rows, width), BF),
            vmem((2, rows // 2, width), BF),
            vmem((4, rows, width), BF),
            vmem((8, rows, width), BF),
            vmem((8, rows, width), BF),
            vmem((4, rows, width), BF),
            vmem((rows, width), BF),
            vmem((rows, width), F32),
            vmem((8, width), F32),
            vmem((8, width), F32),
            vmem((8, HD), F32),
            vmem((4, rows, HD), BF),
            vmem((4, rows, HD), BF),
            vmem((4, rows, HD), BF),
            vmem((4, rows, HD), BF),
            vmem((4, rows, HD), BF),
            vmem((4, rows, HD), BF),
            vmem((4, rows, SEGMAX), BF),
            vmem((4, rows, HD // 2), F32),
            vmem((4, rows, HD // 2), F32),
            vmem((2, depth, 2 * UNIT), F32),
            vmem((2, depth, wide - 2 * HD), BF),
            vmem((2, depth, wide - 2 * HD), BF),
            dma((7,)),
            dma((2, 3)),
            dma((parts, 2, n // 2)),
            dma((parts, 2, n // 2)),
            dma((parts, 2, n // 2)),
            dma((parts, 2, n // 2)),
            dma((units, 8)),
            dma((units, 8)),
            dma((units + (units + 1) // 2, 8)),
            dma((units + (units + 1) // 2, 8)),
            dma((2, 8)),
            dma((2, 8)),
            dma((2, 8)),
            dma((2, 8)),
            dma((3, 3)),
            dma((3, 3)),
            dma((2, 3)),
            dma((2, 3)),
            dma((2,)),
            dma((2,)),
        ],
        compiler_params=pltpu.CompilerParams(
            collective_id=2, has_side_effects=True, vmem_limit_bytes=67043328
        ),
    )(
        x,
        cot,
        segments.reshape(N_TILES, SEGMAX),
        small,
        *attn_weights,
        ffn_pack,
    )


def fused_local(
    inputs, segments, w_query, w_key, w_value, w_out, g_in, g_attn, g_query, g_key,
    w_gate, w_up, w_down, g_pre, g_post, cotangent,
):
    n = lax.axis_size("dp")
    depth = w_query.shape[0]
    width = w_gate.shape[1]
    lane = lax.broadcasted_iota(jnp.int32, (depth, 128), 1)
    gains = jnp.zeros((depth, 128), BF)
    for k, gain in enumerate((g_in, g_attn, g_pre, g_post)):
        gains = jnp.where(lane == k, gain[:, None], gains)
    exponent = -2.0 * (jnp.arange(HD) % (HD // 2)).astype(F32) / HD
    freq = jnp.power(jnp.float32(THETA), exponent)
    line = lax.broadcasted_iota(jnp.int32, (3, HD), 0)
    small = jnp.where(line == 0, g_query.astype(F32)[None, :], freq[None, :])
    small = jnp.where(line == 1, g_key.astype(F32)[None, :], small)
    ffn_pack = pack_ffn(w_gate, w_up, w_down.T, depth, UNIT)
    d_inputs, sums, output, g_gate, g_up, g_down = run_layer(
        n, inputs, cotangent, segments, small, (w_out.T, w_query, w_key, w_value, gains), ffn_pack
    )
    spot = lax.axis_index("tensor")
    part = depth // 4
    mine = lax.dynamic_slice_in_dim(sums[:, 2 * HD :], spot * part, part, 0)
    small = HD // n // 4
    few = lax.dynamic_slice_in_dim(sums[:, 4 * HD :], spot * small, small, 0)
    return (
        output,
        d_inputs,
        sums[:, HD : 2 * HD],
        mine[:, :HD],
        mine[:, HD : 2 * HD],
        sums[:, :HD].T,
        mine[:, 2 * HD],
        mine[:, 2 * HD + 1],
        few[:, 4],
        few[:, 5],
        g_gate[:, :width],
        g_up[:, :width],
        g_down[:, :width].T,
        mine[:, 2 * HD + 2],
        mine[:, 2 * HD + 3],
    )


def fits(mesh, depth, tokens, rows):
    return mesh.shape["dp"] == 8 and depth % 16 == 0 and mesh.shape["tensor"] == 4 and tokens == 2 * SEGMAX


def layer(mesh):
    def body(*args):
        inputs, segments, w_query = args[0], args[1], args[2]
        if fits(mesh, w_query.shape[0], segments.shape[0], inputs.shape[0]):
            return fused_local(*args)
        return local(*args)

    return body


def solution(mesh):
    return jax.shard_map(
        layer(mesh),
        mesh=mesh,
        in_specs=(
            P(("dp", "tensor"), None),
            P("dp"),
            P("dp", "tensor"),
            P("dp", None),
            P("dp", None),
            P("tensor", "dp"),
            P("dp"),
            P("dp"),
            P(),
            P(),
            P("dp", "tensor"),
            P("dp", "tensor"),
            P("tensor", "dp"),
            P("dp"),
            P("dp"),
            P(("dp", "tensor"), None),
        ),
        out_specs=(
            P(("dp", "tensor"), None),
            P(("dp", "tensor"), None),
            P("dp", "tensor"),
            P(("dp", "tensor"), None),
            P(("dp", "tensor"), None),
            P("tensor", "dp"),
            P(("dp", "tensor")),
            P(("dp", "tensor")),
            P(("dp", "tensor")),
            P(("dp", "tensor")),
            P("dp", "tensor"),
            P("dp", "tensor"),
            P("tensor", "dp"),
            P(("dp", "tensor")),
            P(("dp", "tensor")),
        ),
        check_vma=False,
    )
```

```python
from functools import partial

import jax
import jax.numpy as jnp
from jax import lax
from jax.experimental import pallas as pl
from jax.experimental.pallas import tpu as pltpu
from jax.sharding import PartitionSpec as P

HD = 256
SEGMAX = 512
MESH = pl.DeviceIdType.MESH
BF = jnp.bfloat16
F32 = jnp.float32


def ring_pos(dev, n):
    return (1 - dev % 2) * (dev // 2) + (dev % 2) * (n - 1 - dev // 2)


def ring_dev(pos, n):
    high = pos // (n // 2)
    return (1 - high) * (2 * pos) + high * (2 * (n - 1 - pos) + 1)


def barrier(peers):
    sem = pltpu.get_barrier_semaphore()
    for peer in peers:
        pl.semaphore_signal(sem, inc=1, device_id=peer, device_id_type=MESH)
    pl.semaphore_wait(sem, len(peers))


def reach(bias, way, n):
    return n // 2 if bias == way else n // 2 - 1


class Ring:
    def __init__(self, n, parts, send_sem, recv_sem, land=None):
        self.n, self.parts, self.land = n, parts, land
        self.send_sem, self.recv_sem = send_sem, recv_sem
        self.me = lax.axis_index("dp")
        self.pos = ring_pos(self.me, n)
        self.peer = [{"dp": self.dev(1)}, {"dp": self.dev(-1)}]

    def dev(self, offset):
        return ring_dev((self.pos + (offset + self.n) % self.n) % self.n, self.n)

    def reach(self, part, way):
        return reach(part % 2, way, self.n)

    def gather(self, part, way, hop, ahead):
        away = hop - 1 if ahead else hop
        block = self.parts[part](self.dev(-away if way == 0 else away))
        return pltpu.make_async_remote_copy(
            block,
            block,
            self.send_sem.at[part, way, hop - 1],
            self.recv_sem.at[part, way, hop - 1],
            device_id=self.peer[way],
            device_id_type=MESH,
        )

    def gather_step(self, part, way, hop):
        if hop > 1:
            self.gather(part, way, hop - 1, False).wait_recv()
        if hop <= self.reach(part, way):
            self.gather(part, way, hop, True).start()

    def gather_sends_done(self, part):
        for way in range(2):
            for hop in range(1, self.reach(part, way) + 1):
                self.gather(part, way, hop, True).wait_send()

    def target(self, part, way, hop):
        away = self.reach(part, way) - hop + 1
        return self.dev(away if way == 0 else -away)

    def slot(self, part, way, hop):
        return self.land(part, hop - 1 + (self.reach(part, 0) if way else 0))

    def reduce(self, part, way, hop):
        return pltpu.make_async_remote_copy(
            self.parts[part](self.target(part, way, hop)),
            self.slot(part, way, hop),
            self.send_sem.at[part, way, hop - 1],
            self.recv_sem.at[part, way, hop - 1],
            device_id=self.peer[way],
            device_id_type=MESH,
        )

    def reduce_step(self, part, way, hop):
        if hop > self.reach(part, way):
            return
        if hop > 1:
            self.reduce(part, way, hop - 1).wait_recv()
            own = self.parts[part](self.target(part, way, hop))
            came = self.slot(part, way, hop - 1)
            own[...] = (own[...].astype(F32) + came[...].astype(F32)).astype(BF)
        self.reduce(part, way, hop).start()

    def reduce_end(self, part):
        total = self.parts[part](self.me)[...].astype(F32)
        for way in range(2):
            last = self.reach(part, way)
            self.reduce(part, way, last).wait_recv()
            total = total + self.slot(part, way, last)[...].astype(F32)
        return total

    def reduce_sends_done(self, part):
        for way in range(2):
            for hop in range(1, self.reach(part, way) + 1):
                self.reduce(part, way, hop).wait_send()


def part_views(attn, attn_cut, ffn=None, ffn_cut=()):
    views = []
    for low, high in attn_cut:
        views.append(lambda b, low=low, high=high: attn.at[b, :, pl.ds(low, high - low)])
    for chunk in range(0 if ffn is None else ffn.shape[0]):
        for low, high in ffn_cut:
            views.append(
                lambda b, c=chunk, low=low, high=high: ffn.at[c, b, :, pl.ds(low, high - low)]
            )
    return views


def halves(cols, step=128):
    mid = cols // 2 // step * step
    return ((0, mid), (mid, cols))


def gather_kernel(n, attn_ref, ffn_ref, attn_out, ffn_out, local_sem, send_sem, recv_sem):
    parts = part_views(attn_out, halves(attn_ref.shape[-1]), ffn_out, halves(ffn_ref.shape[-1]))
    ring = Ring(n, parts, send_sem, recv_sem)
    mine = [
        pltpu.make_async_copy(attn_ref, attn_out.at[ring.me], local_sem.at[0]),
        pltpu.make_async_copy(ffn_ref, ffn_out.at[:, ring.me], local_sem.at[1]),
    ]
    for copy in mine:
        copy.start()
    barrier(ring.peer)
    for copy in mine:
        copy.wait()
    width = 4
    for low in range(0, len(parts), width):
        for hop in range(1, n // 2 + 2):
            for part in range(low, min(low + width, len(parts))):
                for way in range(2):
                    if hop <= ring.reach(part, way) + 1:
                        ring.gather_step(part, way, hop)
    for part in range(len(parts)):
        ring.gather_sends_done(part)


def reduce_kernel(n, attn_ref, ffn_ref, attn_out, ffn_out, attn_buf, ffn_buf, attn_land, ffn_land, local_sem, send_sem, recv_sem):
    acut, fcut = halves(attn_ref.shape[-1]), halves(ffn_ref.shape[-1])
    parts = part_views(attn_buf, acut, ffn_buf, fcut)
    landing = part_views(attn_land, acut, ffn_land, fcut)
    ring = Ring(n, parts, send_sem, recv_sem, lambda part, slot: landing[part](slot))
    load = [
        pltpu.make_async_copy(attn_ref, attn_buf, local_sem.at[0]),
        pltpu.make_async_copy(ffn_ref, ffn_buf, local_sem.at[1]),
    ]
    for copy in load:
        copy.start()
    barrier(ring.peer)
    for copy in load:
        copy.wait()
    width = 4
    for low in range(0, len(parts), width):
        for hop in range(1, n // 2 + 1):
            for part in range(low, min(low + width, len(parts))):
                for way in range(2):
                    ring.reduce_step(part, way, hop)
        for part in range(low, min(low + width, len(parts))):
            total = ring.reduce_end(part)
            if part < 2:
                attn_out[:, acut[part][0] : acut[part][1]] = total
            else:
                cut = fcut[part % 2]
                ffn_out[part // 2 - 1, :, cut[0] : cut[1]] = total
    for part in range(len(parts)):
        ring.reduce_sends_done(part)


VMEM_LIMIT = 60 * 2**20


def vmem_specs(count):
    return [pl.BlockSpec(memory_space=pltpu.VMEM)] * count


def any_specs(count):
    return [pl.BlockSpec(memory_space=pl.ANY)] * count


def ring_gather(n, attn, ffn):
    chunks = ffn.shape[0]
    sems = pltpu.SemaphoreType.DMA((2 * (chunks + 1), 2, n // 2))
    return pl.pallas_call(
        partial(gather_kernel, n),
        out_shape=(
            jax.ShapeDtypeStruct((n,) + attn.shape, BF),
            jax.ShapeDtypeStruct((chunks, n) + ffn.shape[1:], BF),
        ),
        in_specs=any_specs(2),
        out_specs=vmem_specs(2),
        scratch_shapes=[pltpu.SemaphoreType.DMA((2,)), sems, sems],
        compiler_params=pltpu.CompilerParams(
            collective_id=0, has_side_effects=True, vmem_limit_bytes=VMEM_LIMIT
        ),
    )(attn, ffn)


def ring_reduce(n, attn, ffn):
    chunks, _, rows, cols = ffn.shape
    sems = pltpu.SemaphoreType.DMA((2 * (chunks + 1), 2, n // 2))
    return pl.pallas_call(
        partial(reduce_kernel, n),
        out_shape=(
            jax.ShapeDtypeStruct(attn.shape[1:], F32),
            jax.ShapeDtypeStruct((chunks, rows, cols), F32),
        ),
        in_specs=any_specs(2),
        out_specs=vmem_specs(2),
        scratch_shapes=[
            pltpu.VMEM(attn.shape, BF),
            pltpu.VMEM(ffn.shape, BF),
            pltpu.VMEM((n - 1,) + attn.shape[1:], BF),
            pltpu.VMEM((chunks, n - 1, rows, cols), BF),
            pltpu.SemaphoreType.DMA((2,)),
            sems,
            sems,
        ],
        compiler_params=pltpu.CompilerParams(
            collective_id=1, has_side_effects=True, vmem_limit_bytes=VMEM_LIMIT
        ),
    )(attn, ffn)


CHUNK = 256


def pack_rows(array, rows):
    return jnp.pad(array, ((0, rows - array.shape[0]), (0, 0)))


def pack_ffn(gate, up, down_t, rows, step=CHUNK):
    width = gate.shape[1]
    chunks = -(-width // step)
    chunks += chunks % 2 if step != CHUNK else 0

    def cut(array):
        array = jnp.pad(array, ((0, rows - array.shape[0]), (0, chunks * step - width)))
        return array.reshape(rows, chunks, step).transpose(1, 0, 2)

    return jnp.concatenate([cut(gate), cut(up), cut(down_t)], axis=2)


def unpack_ffn(packed, width):
    chunks, rows = packed.shape[:2]
    out = []
    for k in range(3):
        piece = packed[:, :, k * CHUNK : (k + 1) * CHUNK]
        out.append(piece.transpose(1, 0, 2).reshape(rows, chunks * CHUNK)[:, :width])
    return out


def pack_blocks(array, n, rows):
    depth = array.shape[0] // n
    return jnp.pad(array.reshape(n, depth, -1), ((0, 0), (0, rows - depth), (0, 0)))


EPSILON = 1e-06
THETA = 1000000.0
NEG_LARGE = -1e30


def rms_scale(values, gain_vec):
    inverse = lax.rsqrt(jnp.mean(values * values, axis=-1, keepdims=True) + EPSILON)
    return values * inverse * gain_vec


def gelu_product(gate_proj, up_proj):
    return jax.nn.gelu(gate_proj, approximate=True) * up_proj


def rows_product(left, right):
    return lax.dot_general(
        left, right, (((0,), (0,)), ((), ())), preferred_element_type=jnp.float32
    )


def cols_product(left, right):
    return lax.dot_general(
        left, right, (((1,), (1,)), ((), ())), preferred_element_type=jnp.float32
    )


def plain_product(left, right):
    return jnp.dot(left, right, preferred_element_type=jnp.float32)


def rotary_tables(segments):
    count = segments.shape[0]
    row_index = jnp.arange(count, dtype=jnp.int32)
    previous = jnp.concatenate([jnp.full((1,), -1, jnp.int32), segments[:-1]])
    starts = jnp.where(segments != previous, row_index, jnp.zeros_like(row_index))
    seq_start = lax.cummax(starts, axis=0)
    position = (row_index - seq_start).astype(jnp.float32)
    half_width = HD // 2
    exponent = -2.0 * jnp.arange(half_width, dtype=jnp.float32) / HD
    inverse = jnp.power(jnp.float32(THETA), exponent)
    angles = position[:, None] * inverse[None, :]
    cosine = jnp.concatenate([jnp.cos(angles), jnp.cos(angles)], axis=1)
    sine_tab = jnp.concatenate([jnp.sin(angles), jnp.sin(angles)], axis=1)
    return (cosine, sine_tab)


def prepare(projection, gain_vec, cosine, sine_tab):
    normed = rms_scale(projection, gain_vec)
    half_width = HD // 2
    turned = jnp.concatenate([-normed[..., half_width:], normed[..., :half_width]], axis=-1)
    return normed * cosine[:, None, :] + turned * sine_tab[:, None, :]


def visible(segments):
    tile_count = segments.shape[0] // SEGMAX
    seg_tiles = segments.reshape(tile_count, SEGMAX)
    offsets = jnp.arange(SEGMAX, dtype=jnp.int32)
    same = seg_tiles[:, :, None] == seg_tiles[:, None, :]
    return same & (offsets[:, None] >= offsets[None, :])


def tile_scores(query_tiles, key_tiles, segments):
    head_width = key_tiles.shape[-1]
    scores = jnp.einsum(
        "tqhd,tkd->thqk", query_tiles, key_tiles, preferred_element_type=jnp.float32
    ) * head_width ** (-0.5)
    return jnp.where(visible(segments)[:, None], scores, NEG_LARGE)


def attend(query_ready, key_ready, value_b, segments):
    row_count, head_count, head_width = query_ready.shape
    tile_count = row_count // SEGMAX
    query_tiles = query_ready.reshape(tile_count, SEGMAX, head_count, head_width)
    key_tiles = key_ready.reshape(tile_count, SEGMAX, head_width)
    value_tiles = value_b.reshape(tile_count, SEGMAX, head_width)
    scores = tile_scores(query_tiles, key_tiles, segments)
    row_max = jnp.max(scores, axis=-1, keepdims=True)
    row_total = jnp.sum(jnp.exp(scores - row_max), axis=-1, keepdims=True)
    log_total = row_max + jnp.log(row_total)
    probs = jnp.exp(scores - log_total).astype(jnp.bfloat16)
    attended = jnp.einsum("thqk,tkd->tqhd", probs, value_tiles, preferred_element_type=jnp.float32)
    return (attended.reshape(row_count, head_count * head_width).astype(jnp.bfloat16), log_total)


def attend_back(query_ready, key_ready, value_b, segments, log_total, d_attended):
    row_count, head_count, head_width = query_ready.shape
    tile_count = row_count // SEGMAX
    query_tiles = query_ready.reshape(tile_count, SEGMAX, head_count, head_width)
    key_tiles = key_ready.reshape(tile_count, SEGMAX, head_width)
    value_tiles = value_b.reshape(tile_count, SEGMAX, head_width)
    grad_tiles = d_attended.reshape(tile_count, SEGMAX, head_count, head_width)
    scores = tile_scores(query_tiles, key_tiles, segments)
    prob_vals = jnp.exp(scores - log_total)
    prob_b = prob_vals.astype(jnp.bfloat16)
    d_value = jnp.einsum(
        "thqk,tqhd->tkd", prob_b, grad_tiles, preferred_element_type=jnp.float32
    ).reshape(row_count, head_width)
    d_probs = jnp.einsum(
        "tqhd,tkd->thqk", grad_tiles, value_tiles, preferred_element_type=jnp.float32
    )
    row_delta = jnp.sum(prob_vals * d_probs, axis=-1, keepdims=True)
    d_scores = (prob_vals * (d_probs - row_delta) * head_width ** (-0.5)).astype(jnp.bfloat16)
    d_query = jnp.einsum(
        "thqk,tkd->tqhd", d_scores, key_tiles, preferred_element_type=jnp.float32
    ).reshape(row_count, head_count, head_width)
    d_key = jnp.einsum(
        "thqk,tqhd->tkd", d_scores, query_tiles, preferred_element_type=jnp.float32
    ).reshape(row_count, head_width)
    return (d_query, d_key, d_value)


def local(
    inputs,
    segments,
    w_query,
    w_key,
    w_value,
    w_out,
    g_in,
    g_attn,
    g_query,
    g_key,
    w_gate,
    w_up,
    w_down,
    g_pre,
    g_post,
    cotangent,
):
    n = lax.axis_size("dp")
    depth = w_query.shape[0]
    rows = -(-depth // 16) * 16
    width = w_gate.shape[1]
    gains = jnp.stack([g_in, g_attn, g_pre, g_post], axis=1)
    attn_pack = jnp.concatenate(
        [w_query, w_key, w_value, w_out.T, jnp.pad(gains, ((0, 0), (0, 124)))], axis=1
    )
    attn_all, ffn_all = ring_gather(
        n, pack_rows(attn_pack, rows), pack_ffn(w_gate, w_up, w_down.T, rows)
    )
    attn_all = attn_all[:, :depth].reshape(n * depth, -1)
    ffn_all = ffn_all[:, :, :depth].reshape(ffn_all.shape[0], n * depth, -1)
    wq_full, wk_full, wv_full, wo_t = (attn_all[:, k * HD : (k + 1) * HD] for k in range(4))
    wo_full = wo_t.T
    gin_full, gattn_full, gpre_full, gpost_full = (attn_all[:, 4 * HD + k] for k in range(4))
    wg_full, wu_full, wd_t = unpack_ffn(ffn_all, width)
    wd_full = wd_t.T
    gain_in = gin_full.astype(jnp.float32)
    gain_attn = gattn_full.astype(jnp.float32)
    gain_query = g_query.astype(jnp.float32)
    gain_key = g_key.astype(jnp.float32)
    cosine, sine_tab = rotary_tables(segments)
    inputs_f = inputs.astype(jnp.float32)
    normed_shard = rms_scale(inputs_f, gain_in).astype(jnp.bfloat16)
    normed_in = lax.all_gather(normed_shard, "tensor", axis=0, tiled=True)
    row_count = normed_in.shape[0]
    head_count = wq_full.shape[1] // HD
    key_proj = plain_product(normed_in, wk_full)
    value_b = plain_product(normed_in, wv_full).astype(jnp.bfloat16)
    key_ready = prepare(key_proj[:, None, :], gain_key, cosine, sine_tab)[:, 0, :].astype(
        jnp.bfloat16
    )
    query_proj = plain_product(normed_in, wq_full).reshape(row_count, head_count, HD)
    query_ready = prepare(query_proj, gain_query, cosine, sine_tab).astype(jnp.bfloat16)
    attended, log_total = attend(query_ready, key_ready, value_b, segments)
    projected = lax.psum_scatter(
        plain_product(attended, wo_full), "tensor", scatter_dimension=0, tiled=True
    )
    residual_mid = inputs_f + rms_scale(projected, gain_attn)
    gain_pre = gpre_full.astype(jnp.float32)
    gain_post = gpost_full.astype(jnp.float32)
    normed_mid = lax.all_gather(
        rms_scale(residual_mid, gain_pre).astype(jnp.bfloat16), "tensor", axis=0, tiled=True
    )
    gate_proj = plain_product(normed_mid, wg_full)
    up_proj = plain_product(normed_mid, wu_full)
    hidden = gelu_product(gate_proj, up_proj).astype(jnp.bfloat16)
    feed = lax.psum_scatter(
        plain_product(hidden, wd_full), "tensor", scatter_dimension=0, tiled=True
    )
    output = (residual_mid + rms_scale(feed, gain_post)).astype(jnp.bfloat16)
    wg_back, wu_back, wd_back = wg_full, wu_full, wd_full
    grad_output = cotangent.astype(jnp.float32)
    d_feed_f, grad_g_post = jax.vjp(rms_scale, feed, gain_post)[1](grad_output)
    d_feed = lax.all_gather(d_feed_f.astype(jnp.bfloat16), "tensor", axis=0, tiled=True)
    d_hidden = cols_product(d_feed, wd_back)
    d_gate_f, d_up_f = jax.vjp(gelu_product, gate_proj, up_proj)[1](d_hidden)
    d_gate = d_gate_f.astype(jnp.bfloat16)
    d_up = d_up_f.astype(jnp.bfloat16)
    grad_gate = rows_product(normed_mid, d_gate)
    grad_up = rows_product(normed_mid, d_up)
    d_normed_mid = lax.psum_scatter(
        cols_product(d_gate, wg_back) + cols_product(d_up, wu_back),
        "tensor",
        scatter_dimension=0,
        tiled=True,
    )
    d_mid_n, grad_g_pre = jax.vjp(rms_scale, residual_mid, gain_pre)[1](d_normed_mid)
    d_mid = grad_output + d_mid_n
    d_proj_f, grad_g_attn = jax.vjp(rms_scale, projected, gain_attn)[1](d_mid)
    wq_back, wk_back, wv_back, wo_back = wq_full, wk_full, wv_full, wo_full
    d_proj = lax.all_gather(d_proj_f.astype(jnp.bfloat16), "tensor", axis=0, tiled=True)
    d_attended = cols_product(d_proj, wo_back).astype(jnp.bfloat16)
    d_query_ready, d_key_ready, d_value_f = attend_back(
        query_ready, key_ready, value_b, segments, log_total, d_attended
    )
    rotate_fn = partial(prepare, cosine=cosine, sine_tab=sine_tab)
    d_query_f, grad_g_query = jax.vjp(rotate_fn, query_proj, gain_query)[1](d_query_ready)
    d_key_f, grad_g_key = jax.vjp(rotate_fn, key_proj[:, None, :], gain_key)[1](
        d_key_ready[:, None, :]
    )
    d_query = d_query_f.reshape(row_count, head_count * HD).astype(jnp.bfloat16)
    d_key = d_key_f[:, 0, :].astype(jnp.bfloat16)
    d_value = d_value_f.astype(jnp.bfloat16)
    grad_query = rows_product(normed_in, d_query)
    grad_key = rows_product(normed_in, d_key)
    grad_value = rows_product(normed_in, d_value)
    d_normed_terms = (
        cols_product(d_query, wq_back)
        + cols_product(d_key, wk_back)
        + cols_product(d_value, wv_back)
    )
    d_normed_in = lax.psum_scatter(
        d_normed_terms.astype(jnp.bfloat16), "tensor", scatter_dimension=0, tiled=True
    ).astype(jnp.float32)
    d_in_n, grad_g_in = jax.vjp(rms_scale, inputs_f, gain_in)[1](d_normed_in)
    d_inputs = (d_mid + d_in_n).astype(jnp.bfloat16)
    attn_part = jnp.concatenate(
        [grad_query, grad_key, grad_value, rows_product(d_proj, attended)], axis=1
    ).astype(BF)
    attn_part = pack_blocks(attn_part, n, rows)
    ffn_part = pack_ffn(
        grad_gate.astype(BF), grad_up.astype(BF), rows_product(d_feed, hidden).astype(BF), n * depth
    )
    ffn_part = jax.vmap(lambda a: pack_blocks(a, n, rows))(ffn_part)
    attn_sum, ffn_sum = ring_reduce(n, attn_part, ffn_part)
    attn_sum, ffn_sum = attn_sum[:depth], ffn_sum[:, :depth]
    sum_gate, sum_up, sum_down_t = unpack_ffn(ffn_sum, width)
    split_grads = (
        attn_sum[:, :HD],
        attn_sum[:, 3 * HD : 4 * HD].T,
        sum_gate,
        sum_up,
        sum_down_t.T,
    )
    sum_key, sum_value = attn_sum[:, HD : 2 * HD], attn_sum[:, 2 * HD : 3 * HD]
    shared = (
        lax.psum_scatter(sum_key, "tensor", scatter_dimension=0, tiled=True),
        lax.psum_scatter(sum_value, "tensor", scatter_dimension=0, tiled=True),
        lax.psum_scatter(grad_g_in, ("dp", "tensor"), scatter_dimension=0, tiled=True),
        lax.psum_scatter(grad_g_attn, ("dp", "tensor"), scatter_dimension=0, tiled=True),
        lax.psum_scatter(grad_g_pre, ("dp", "tensor"), scatter_dimension=0, tiled=True),
        lax.psum_scatter(grad_g_post, ("dp", "tensor"), scatter_dimension=0, tiled=True),
        lax.psum_scatter(grad_g_query, ("dp", "tensor"), scatter_dimension=0, tiled=True),
        lax.psum_scatter(grad_g_key, ("dp", "tensor"), scatter_dimension=0, tiled=True),
    )
    return (
        output,
        d_inputs,
        split_grads[0],
        shared[0],
        shared[1],
        split_grads[1],
        shared[2],
        shared[3],
        shared[6],
        shared[7],
        split_grads[2],
        split_grads[3],
        split_grads[4],
        shared[4],
        shared[5],
    )


SCALE = HD**-0.5
ROOT = 0.7978845608028654
CUBIC = 0.044715


def dot_nn(a, b):
    return jnp.dot(a, b, preferred_element_type=F32)


def dot_nt(a, b):
    return lax.dot_general(a, b, (((1,), (1,)), ((), ())), preferred_element_type=F32)


def dot_tn(a, b):
    return lax.dot_general(a, b, (((0,), (0,)), ((), ())), preferred_element_type=F32)


def inverse_rms(values):
    return lax.rsqrt(jnp.mean(values * values, axis=-1, keepdims=True) + EPSILON)


def rms_back(values, gain_vec, grad):
    inverse = inverse_rms(values)
    unit = values * inverse
    scaled = grad * gain_vec
    back = inverse * (scaled - unit * jnp.mean(scaled * unit, axis=-1, keepdims=True))
    return back, grad * unit


def gelu_parts(gate):
    bent = jnp.tanh(ROOT * (gate + CUBIC * gate * gate * gate))
    return 0.5 * gate * (1.0 + bent), bent


class Quad:
    def __init__(self, part, near, far, gather_sems, reduce_sems):
        self.me = lax.axis_index("tensor")
        self.twin = self.me + 1 - 2 * (self.me % 2)
        self.across = (self.me + 2) % 4
        self.corner = (self.twin + 2) % 4
        self.part, self.near, self.far = part, near, far
        self.gather_sems, self.reduce_sems = gather_sems, reduce_sems

    def copy(self, src, dst, sems, use, k, peer):
        return pltpu.make_async_remote_copy(
            src,
            dst,
            sems[0].at[use, k],
            sems[1].at[use, k],
            device_id={"tensor": peer},
            device_id_type=MESH,
        )

    def gather(self, use, k, buf):
        place = self.across if k == 2 else self.me
        block = buf(place) if callable(buf) else buf.at[place]
        peer = self.across if k == 1 else self.twin
        return self.copy(block, block, self.gather_sems, use, k, peer)

    def gather_start(self, use, buf):
        self.gather(use, 1, buf).start()
        self.gather(use, 0, buf).start()

    def gather_relay(self, use, buf):
        self.gather(use, 1, buf).wait_recv()
        self.gather(use, 2, buf).start()

    def gather_end(self, use, buf):
        self.gather(use, 0, buf).wait_recv()
        self.gather(use, 2, buf).wait_recv()
        for k in range(3):
            self.gather(use, k, buf).wait_send()

    def reduce(self, use, k):
        block = self.part.at[(self.twin, self.corner, self.across)[k]]
        land = self.far if k == 2 else self.near.at[k]
        peer = self.across if k == 2 else self.twin
        return self.copy(block, land, self.reduce_sems, use, k, peer)

    def reduce_start(self, use):
        self.reduce(use, 1).start()
        self.reduce(use, 0).start()

    def reduce_relay(self, use):
        self.reduce(use, 1).wait_recv()
        for low in range(0, self.part.shape[1], 64):
            rows = pl.ds(low, 64)
            total = self.part[self.across, rows].astype(F32) + self.near[1, rows].astype(F32)
            self.part[self.across, rows] = total.astype(BF)
        self.reduce(use, 2).start()

    def reduce_end(self, use):
        self.reduce(use, 0).wait_recv()
        self.reduce(use, 2).wait_recv()
        for k in range(3):
            self.reduce(use, k).wait_send()


class Octet:
    def __init__(self, part, near, far, bend, gather_sems, reduce_sems):
        tensor, dp = lax.axis_index("tensor"), lax.axis_index("dp")
        z = dp // 2
        self.low, self.x, self.core = z % 2, tensor // 2, tensor % 2
        self.twin = {"tensor": tensor + 1 - 2 * self.core}
        self.across = {"tensor": (tensor + 2) % 4}
        self.pair = {"dp": dp + 2 - 4 * self.low}
        self.part, self.near, self.far, self.bend = part, near, far, bend
        self.gather_sems, self.reduce_sems = gather_sems, reduce_sems

    def block(self, p, other=0):
        core = (self.core + other) % 2
        return (self.low + p // 2) % 2 * 4 + (self.x + p % 2) % 2 * 2 + core

    def copy(self, src, dst, sems, use, k, peer):
        return pltpu.make_async_remote_copy(
            src, dst, sems[0].at[use, k], sems[1].at[use, k], device_id=peer, device_id_type=MESH
        )

    def gather(self, use, k, buf, come=False):
        half = buf.shape[1] // 2
        if k < 2:
            place, peer = (k + 1 if come else 0), (self.across, self.pair)[k]
            ref = buf.at[self.block(place)]
        elif k < 6:
            ref = buf.at[self.block(k - 2, 1 if come else 0)]
            peer = self.twin
        else:
            place = 3 if come else k - 5
            ref = buf.at[self.block(place), pl.ds((k - 6) * half, half)]
            peer = (self.pair, self.across)[k - 6]
        return self.copy(ref, ref, self.gather_sems, use, k, peer)

    def gather_start(self, use, buf):
        for k in range(3):
            self.gather(use, k, buf).start()

    def gather_relay(self, use, buf, k):
        self.gather(use, k, buf, True).wait_recv()
        self.gather(use, 6 + k, buf).start()
        self.gather(use, 3 + k, buf).start()

    def gather_corner(self, use, buf):
        for k in (6, 7):
            self.gather(use, k, buf, True).wait_recv()
        self.gather(use, 5, buf).start()

    def gather_end(self, use, buf):
        for k in range(2, 6):
            self.gather(use, k, buf, True).wait_recv()
        for k in range(8):
            self.gather(use, k, buf).wait_send()

    def reduce(self, use, k):
        half = self.part.shape[1] // 2
        if k < 4:
            return self.copy(
                self.part.at[self.block(k, 1)], self.near.at[k], self.reduce_sems, use, k, self.twin
            )
        peer = (self.across, self.pair)[k % 2]
        if k < 6:
            src, dst = self.part.at[self.block(3), pl.ds((k - 4) * half, half)], self.bend.at[k - 4]
        else:
            src, dst = self.part.at[self.block(k - 5)], self.far.at[k - 6]
        return self.copy(src, dst, self.reduce_sems, use, k, peer)

    def add(self, place, low, count, came):
        step = 32

        def body(i, _):
            at = pl.multiple_of(i * step, step)
            rows = pl.ds(low + at, step)
            total = self.part[self.block(place), rows].astype(F32) + came[pl.ds(at, step)].astype(F32)
            self.part[self.block(place), rows] = total.astype(BF)
            return 0

        lax.fori_loop(0, count // step, body, 0)

    def reduce_near(self, use, place):
        self.reduce(use, place).wait_recv()
        self.add(place, 0, self.part.shape[1], self.near.at[place])

    def reduce_relay(self, use):
        half = self.part.shape[1] // 2
        for k in range(2):
            self.reduce(use, 4 + k).wait_recv()
            self.add(2 - k, k * half, half, self.bend.at[k])
            self.reduce(use, 7 - k).start()

    def reduce_after(self, use, i):
        for k in range(4):
            pl.when(i == 6 - 2 * k)(lambda k=k: self.reduce(use, k).start())
        for k in (1, 2):
            pl.when(i == 7 - 2 * k)(lambda k=k: self.reduce_near(use, k))
        pl.when(i == 6)(lambda: self.reduce_relay(use))

        @pl.when(i == 1)
        def _():
            self.reduce_near(use, 3)
            self.reduce(use, 4).start()
            self.reduce(use, 5).start()

    @staticmethod
    def arrival(j):
        a, b = j // 2, j % 2
        up = (a + 1) // 2
        mid = up * (2 - up)
        return up + mid * b + a // 3, (1 - mid) * b + mid * (a // 2)

    def gather_before(self, use, buf, j):
        for at, k in ((1, 2), (4, 3), (5, 4), (7, 5)):
            pl.when(j == at)(lambda k=k: self.gather(use, k, buf, True).wait_recv())

        @pl.when(j == 2)
        def _():
            self.gather_relay(use, buf, 0)
            self.gather_relay(use, buf, 1)

        pl.when(j == 6)(lambda: self.gather_corner(use, buf))

    def gather_sends_done(self, use, buf):
        for k in range(8):
            self.gather(use, k, buf).wait_send()

    def reduce_end(self, use):
        for k in (0, 6, 7):
            self.reduce(use, k).wait_recv()
        for k in range(8):
            self.reduce(use, k).wait_send()


class Columns:
    def __init__(self, ffn, other, land, gather_sems, reduce_sems):
        dp = lax.axis_index("dp")
        z, y = dp // 2, dp % 2
        self.low = z % 2
        self.inner = z * (3 - z) > 0
        self.outer = z * (3 - z) < 1
        ranks = (z, z + 1 - 2 * (z % 2), (z + 2) % 4, 3 - z)
        self.mine = [rank * 2 + y for rank in ranks]
        self.theirs = [rank * 2 + 1 - y for rank in ranks]
        self.ffn, self.other, self.land = ffn, other, land
        self.gather_sems, self.reduce_sems = gather_sems, reduce_sems

    def copy(self, src, dst, sems, u, send, recv, peer):
        return pltpu.make_async_remote_copy(
            src,
            dst,
            sems[0].at[u, send],
            sems[1].at[u, recv],
            device_id={"dp": peer},
            device_id_type=MESH,
        )

    def gather(self, u, k):
        own = self.ffn.at[u, self.mine[0]]
        sems = self.gather_sems
        if k == 0:
            return self.copy(own, own, sems, u, 0, 0, self.mine[2])
        if k == 1:
            return self.copy(self.other.at[u], own, sems, u, 1, 1, self.mine[1])
        if k == 2:
            return self.copy(self.other.at[u], own, sems, u, 2, 2, self.mine[3])
        if k == 3:
            block = self.ffn.at[u, self.mine[1]]
            return self.copy(block, block, sems, u, 3, 2, self.mine[2])
        block = self.ffn.at[u, self.mine[k - 4]]
        return self.copy(block, block, sems, u, k, k, self.theirs[0])

    def come(self, u, k):
        place = self.theirs[k - 4] if k >= 4 else self.mine[(2, 1, 3)[k]]
        block = self.ffn.at[u, place]
        self.copy(block, block, self.gather_sems, u, k, k, place).wait_recv()

    def gather_step(self, u, step):
        if step == 0:
            self.gather(u, 0).start()
            self.gather(u, 1).start()
            pl.when(self.inner)(lambda: self.gather(u, 2).start())
            self.gather(u, 4).start()
        elif step == 1:
            self.come(u, 1)
            pl.when(self.inner)(lambda: self.gather(u, 3).start())
            self.gather(u, 5).start()
        elif step == 2:
            self.come(u, 0)
            self.gather(u, 6).start()
        elif step == 3:
            self.come(u, 2)
            self.gather(u, 7).start()
        else:
            for k in range(4, 8):
                self.come(u, k)

    def gather_sends_done(self, u):
        for k in (0, 1, 4, 5, 6, 7):
            self.gather(u, k).wait_send()

        @pl.when(self.inner)
        def _():
            self.gather(u, 2).wait_send()
            self.gather(u, 3).wait_send()

    def piece(self, item, place):
        unit, count, lane, lanes = item[1:]
        return self.ffn.at[pl.ds(unit, count), place, :, pl.ds(lane, lanes)]

    def reduce(self, item, k):
        if k < 4:
            place, peer = self.theirs[k], self.theirs[0]
        else:
            place = self.mine[(2, 1, 3, 3)[k - 4]]
            peer = self.mine[(2, 1, 3, 2)[k - 4]]
        unit, count, lane, lanes = item[1:]
        land = self.land.at[pl.ds(unit, count), k, :, pl.ds(lane, lanes)]
        return self.copy(
            self.piece(item, place), land, self.reduce_sems, item[0], min(k, 6), k, peer
        )

    def came(self, item, k):
        unit, count, lane, lanes = item[1:]
        return [
            self.land[u, k, :, lane : lane + lanes].astype(F32) for u in range(unit, unit + count)
        ]

    def own(self, item, place):
        unit, count, lane, lanes = item[1:]
        return [
            self.ffn.at[u, self.mine[place], :, pl.ds(lane, lanes)]
            for u in range(unit, unit + count)
        ]

    def add(self, item, place, k):
        self.reduce(item, k).wait_recv()
        for own, came in zip(self.own(item, place), self.came(item, k), strict=True):
            own[...] = (own[...].astype(F32) + came).astype(BF)

    def reduce_step(self, item, step):
        if step == 0:
            for k in (3, 2, 1, 0):
                self.reduce(item, k).start()
        elif step == 1:
            self.add(item, 3, 3)
            pl.when(self.inner)(lambda: self.reduce(item, 6).start())
            pl.when(self.outer)(lambda: self.reduce(item, 7).start())
        elif step == 2:
            self.add(item, 2, 2)
            self.reduce(item, 4).start()
        else:
            self.add(item, 1, 1)
            pl.when(self.inner)(lambda: self.add(item, 1, 7))
            self.reduce(item, 5).start()

    def sum_own(self, item, out):
        for k in (0, 4):
            self.reduce(item, k).wait_recv()
        lanes = item[4]
        for i, (own, one, two) in enumerate(
            zip(self.own(item, 0), self.came(item, 0), self.came(item, 4), strict=True)
        ):
            out[:, i * lanes : (i + 1) * lanes] = own[...].astype(F32) + one + two

    def sum_other(self, item, out):
        self.reduce(item, 5).wait_recv()
        lanes = item[4]
        for i, came in enumerate(self.came(item, 5)):
            out[:, i * lanes : (i + 1) * lanes] = came

        @pl.when(self.inner)
        def _():
            self.reduce(item, 6).wait_recv()
            for i, came in enumerate(self.came(item, 6)):
                out[:, i * lanes : (i + 1) * lanes] += came

    def reduce_sends_done(self, item):
        for k in range(7):
            self.reduce(item, k).wait_send()


class Queue:
    def __init__(self):
        self.steps = []

    def add(self, tag, fn):
        self.steps.append((tag, fn))

    def run(self, count, ready=None):
        while count > 0 and self.steps:
            tag, fn = self.steps[0]
            if ready is not None and tag not in ready:
                return
            self.steps.pop(0)
            fn()
            count -= 1

    def until(self, tag):
        while any(t == tag for t, _ in self.steps):
            self.run(1)


def layer_kernel(
    n,
    x_ref,
    cot_ref,
    seg_row,
    small_ref,
    wo_in,
    wq_in,
    wk_in,
    wv_in,
    gain_in,
    ffn_in,
    dx_ref,
    sums_ref,
    out_hbm,
    ggate_hbm,
    gup_hbm,
    gdown_hbm,
    attn,
    ffn,
    other,
    attn_land,
    ffn_land,
    gate_buf,
    up_buf,
    hid_buf,
    part,
    near,
    far,
    bend,
    xa,
    nm,
    df,
    dp_buf,
    proj_s,
    res_s,
    gains,
    gsum,
    gqk,
    q_proj,
    k_proj,
    qr,
    kr,
    vb,
    att,
    probs,
    cos_s,
    sin_s,
    stage,
    kvg,
    kvg_land,
    local_sem,
    stage_sem,
    ag_send,
    ag_recv,
    rs_send,
    rs_recv,
    cg_send,
    cg_recv,
    cr_send,
    cr_recv,
    og_send,
    og_recv,
    or_send,
    or_recv,
    qg_send,
    qg_recv,
    qr_send,
    qr_recv,
    kv_send,
    kv_recv,
):
    units, _, depth, cols = ffn.shape
    rows, width = x_ref.shape
    attn_cut = ((0, HD), (HD, 2 * HD), (2 * HD, 4 * HD), (4 * HD, attn.shape[-1]))
    parts = part_views(attn, attn_cut)
    landing = part_views(attn_land, attn_cut)
    first = len(attn_cut)
    spot4 = lax.axis_index("tensor")

    def quarter_of(t):
        return attn.at[:, :, pl.ds(pl.multiple_of(2 * HD + t * 128, 128), 128)]

    gathered = list(parts)
    gathered[2] = lambda b: attn.at[
        b, :, pl.ds(pl.multiple_of(2 * HD + spot4 * 128, 128), 128)
    ]
    ring = Ring(n, gathered, ag_send, ag_recv)
    back = Ring(n, parts, rs_send, rs_recv, lambda p, slot: landing[p](slot))
    quad = Quad(part, near, far.at[0], (qg_send, qg_recv), (qr_send, qr_recv))
    octet = Octet(part, near, far, bend, (og_send, og_recv), (or_send, or_recv))
    columns = Columns(ffn, other, ffn_land, (cg_send, cg_recv), (cr_send, cr_recv))
    me, spot = quad.me, octet.block(0)
    gq_ref, gk_ref = small_ref.at[0:1], small_ref.at[1:2]
    freq_ref = small_ref.at[2:3, pl.ds(0, HD // 2)]

    def attn_cols(low, high):
        return attn[:, :, low:high].reshape(width, high - low)

    def unit_cols(u, k, count=1):
        return ffn[u, :, :, k * UNIT : (k + count) * UNIT].reshape(width, count * UNIT)

    def across_units(k, low=0, high=units):
        return jnp.concatenate([unit_cols(u, k) for u in range(low, high)], axis=1)

    mine = [
        pltpu.make_async_copy(wo_in, attn.at[ring.me, :, pl.ds(0, HD)], local_sem.at[0]),
        pltpu.make_async_copy(wq_in, attn.at[ring.me, :, pl.ds(HD, HD)], local_sem.at[4]),
        pltpu.make_async_copy(gain_in, attn.at[ring.me, :, pl.ds(4 * HD, 128)], local_sem.at[5]),
        pltpu.make_async_copy(
            ffn_in.at[pl.ds(columns.low * units, units)], ffn.at[:, ring.me], local_sem.at[1]
        ),
        pltpu.make_async_copy(x_ref, xa.at[me], local_sem.at[2]),
        pltpu.make_async_copy(
            ffn_in.at[pl.ds((1 - columns.low) * units, units)], other, local_sem.at[3]
        ),
    ]
    for copy in mine:
        copy.start()

    def quarter_copy(source):
        cols = pl.ds(pl.multiple_of(me % 2 * 128, 128), 128)
        return pltpu.make_async_copy(
            source.at[:, cols], quarter_of(me).at[ring.me], local_sem.at[6]
        )

    pl.when(me < 2)(lambda: quarter_copy(wk_in).start())
    pl.when(me > 1)(lambda: quarter_copy(wv_in).start())
    greet = [{"dp": peer} for peer in columns.mine[1:] + columns.theirs[:1]]
    greet += [{"tensor": quad.twin}, {"tensor": quad.across}]
    barrier(greet)
    for copy in mine:
        copy.wait()
    quarter_copy(wk_in).wait()
    quad.gather_start(0, xa)

    queue = Queue()
    def ring_gather_step(parts, hop, tag):
        for p in parts:
            for way in range(2):
                if 0 < hop <= ring.reach(p, way) + 1:
                    queue.add(tag, partial(ring.gather_step, p, way, hop))

    for hop in range(1, n // 2 + 1):
        ring_gather_step((2, 3, 1), hop, -1)
        ring_gather_step((0,), hop - 2, -1)
    ring_gather_step((2, 3), n // 2 + 1, -1)
    queue.add(-1, partial(quad.gather_start, 2, quarter_of))
    queue.add(-1, partial(quad.gather_relay, 0, xa))
    queue.add(-1, partial(columns.gather_step, 0, 0))
    ring_gather_step((1,), n // 2 + 1, -1)
    ring_gather_step((0,), n // 2 - 1, -1)
    queue.add(-1, partial(quad.gather_relay, 2, quarter_of))
    ring_gather_step((0,), n // 2, -3)
    for u in range(1, EARLY):
        queue.add(-3, partial(columns.gather_step, u, 0))
    ring_gather_step((0,), n // 2 + 1, -3)
    for u in range(units + 2):
        if u < units:
            queue.add(-2, partial(columns.gather_step, u, 1))
            queue.add(-2, partial(columns.gather_step, u, 2))
        if u + EARLY < units:
            queue.add(-2, partial(columns.gather_step, u + EARLY, 0))
        if 0 < u <= units:
            queue.add(-2, partial(columns.gather_step, u - 1, 3))
        if u > 1:
            queue.add(u - 2, partial(columns.gather_step, u - 2, 4))

    queue.run(AHEAD[0])
    quarter = SEGMAX // 2

    def seg_column(seg_j, half):
        cut = seg_j[:, half * quarter : (half + 1) * quarter].astype(F32)
        return jnp.transpose(jnp.broadcast_to(cut, (128, quarter)))[:, :1]

    def tables(tile, _):
        seg_j = seg_row[pl.ds(tile, 1), :]
        for half in range(2):
            r = 2 * tile + half
            same = seg_column(seg_j, half) == seg_j.astype(F32)
            j = lax.broadcasted_iota(jnp.int32, (quarter, SEGMAX), 1)
            start = jnp.min(jnp.where(same, j, SEGMAX).astype(F32), axis=1, keepdims=True)
            i = lax.broadcasted_iota(jnp.int32, (quarter, 1), 0).astype(F32) + half * quarter
            angle = (i - start) * freq_ref[...]
            cos_s[r] = jnp.cos(angle)
            sin_s[r] = jnp.sin(angle)
        return 0

    lax.fori_loop(0, N_TILES, tables, 0)
    queue.until(-1)
    flipped = jnp.transpose(attn_cols(4 * HD, 4 * HD + 128).astype(F32))
    gains[...] = flipped[:8]
    quad.gather_end(0, xa)
    queue.run(AHEAD[2])

    sub = 64
    per = rows // sub

    def normalize(i, _):
        b, at = i // per, pl.ds(pl.multiple_of(i % per * sub, sub), sub)
        values = xa[b, at].astype(F32)
        xa[b, at] = (values * inverse_rms(values) * gains[0:1, :]).astype(BF)
        return 0

    lax.fori_loop(0, 4 * per, normalize, 0)

    def rope(values, gain_vec, r):
        normed = values * inverse_rms(values) * gain_vec
        low, high = normed[:, : HD // 2], normed[:, HD // 2 :]
        cosine, sine = cos_s[r], sin_s[r]
        return jnp.concatenate([low * cosine - high * sine, high * cosine + low * sine], axis=1)

    queue.run(AHEAD[3])

    quad.gather_end(2, quarter_of)

    def project(r, _):
        block = xa[r]
        query = dot_nn(block, attn_cols(HD, 2 * HD))
        q_proj[r] = query.astype(BF)
        qr[r] = rope(query, gq_ref[...], r).astype(BF)
        key = dot_nn(block, attn_cols(2 * HD, 3 * HD))
        k_proj[r] = key.astype(BF)
        kr[r] = rope(key, gk_ref[...], r).astype(BF)
        vb[r] = dot_nn(block, attn_cols(3 * HD, 4 * HD)).astype(BF)
        return 0

    lax.fori_loop(0, 4, project, 0)
    queue.run(AHEAD[4])

    def attend_tile(tile, _):
        two = pl.ds(2 * tile, 2)
        keys = kr[two].reshape(SEGMAX, HD)
        values = vb[two].reshape(SEGMAX, HD)
        seg_j = seg_row[pl.ds(tile, 1), :]
        for half in range(2):
            r = 2 * tile + half
            scores = dot_nt(qr[r], keys) * SCALE
            j = lax.broadcasted_iota(jnp.int32, (quarter, SEGMAX), 1)
            i = lax.broadcasted_iota(jnp.int32, (quarter, SEGMAX), 0) + half * quarter
            seen = (seg_column(seg_j, half) == seg_j.astype(F32)) & (i >= j)
            scores = jnp.where(seen, scores, NEG_LARGE)
            powers = jnp.exp(scores - jnp.max(scores, axis=1, keepdims=True))
            weights = (powers / jnp.sum(powers, axis=1, keepdims=True)).astype(BF)
            probs[r] = weights
            att[r] = dot_nn(weights, values).astype(BF)
        return 0

    lax.fori_loop(0, N_TILES, attend_tile, 0)
    queue.run(AHEAD[5])

    queue.until(-3)

    def out_block(r, _):
        part[r] = dot_nt(att[r], attn_cols(0, HD)).astype(BF)
        return 0

    lax.fori_loop(0, 4, out_block, 0)
    quad.reduce_start(0)
    queue.run(AHEAD[6])
    quad.reduce_relay(0)
    queue.run(AHEAD[7])
    quad.reduce_end(0)

    def total(at):
        return part[me, at].astype(F32) + near[0, at].astype(F32) + far[0, at].astype(F32)

    def total_ffn(at):
        return part[spot, at].astype(F32) + near[0, at].astype(F32) + (
            far[0, at].astype(F32) + far[1, at].astype(F32)
        )

    def at_rows(i):
        return pl.ds(pl.multiple_of(i * sub, sub), sub)

    def middle(i, _):
        at = at_rows(i)
        projected = total(at)
        proj_s[at] = projected.astype(BF)
        mid = x_ref[at].astype(F32) + projected * inverse_rms(projected) * gains[1:2, :]
        res_s[at] = mid
        nm[spot, at] = (mid * inverse_rms(mid) * gains[2:3, :]).astype(BF)
        return 0

    lax.fori_loop(0, per, middle, 0)
    octet.gather_start(0, nm)
    queue.run(AHEAD[8])
    octet.gather_relay(0, nm, 0)
    octet.gather_relay(0, nm, 1)
    queue.run(AHEAD[9])
    octet.gather_corner(0, nm)
    queue.run(AHEAD[9])
    octet.gather_end(0, nm)

    for u in range(units):
        queue.until(u)
        lanes = slice(u * UNIT, (u + 1) * UNIT)

        def ffn_block(r, _):
            both = dot_nn(nm[r], unit_cols(u, 0, 2))
            gate, up = both[:, :UNIT], both[:, UNIT:]
            gate_buf[r, :, lanes] = gate.astype(BF)
            up_buf[r, :, lanes] = up.astype(BF)
            hid_buf[r, :, lanes] = (gelu_parts(gate)[0] * up).astype(BF)
            return 0

        lax.fori_loop(0, 8, ffn_block, 0)
        queue.run(AHEAD[10])
    queue.run(10**6)

    def feed_block(i, _):
        b = octet.block(3 - i // 2, 1 - i % 2)
        part[b] = dot_nt(hid_buf[b], across_units(2)).astype(BF)
        octet.reduce_after(0, i)
        return 0

    lax.fori_loop(0, 8, feed_block, 0)
    for p in range(first):
        ring.gather_sends_done(p)
    for u in range(units):
        columns.gather_sends_done(u)
    octet.reduce_end(0)
    eight = (8, width)

    def fold(values):
        return jnp.sum(values.reshape(sub // 8, 8, values.shape[-1]), axis=0)

    def after_feed(i, carry):
        at = at_rows(i)
        feed = total_ffn(at)
        dx_ref[at] = (res_s[at] + feed * inverse_rms(feed) * gains[3:4, :]).astype(BF)
        grad, gain_part = rms_back(feed, gains[3:4, :], cot_ref[at].astype(F32))
        df[spot, at] = grad.astype(BF)
        return carry + fold(gain_part)

    gain_sum = lax.fori_loop(0, per, after_feed, jnp.zeros(eight, F32))
    gsum[3:4, :] = jnp.sum(gain_sum, axis=0, keepdims=True)
    put_out = pltpu.make_async_copy(dx_ref, out_hbm, local_sem.at[0])
    put_out.start()
    octet.gather_start(1, df)

    queue = Queue()
    pending = []

    def finish(item, other):
        k = len(pending)
        if k >= 2:
            for copy in pending[k - 2]:
                copy.wait()
        (columns.sum_other if other else columns.sum_own)(item, stage.at[k % 2])
        half = 1 - columns.low if other else columns.low
        unit, count, lane, lanes = item[1:]
        at = pl.multiple_of(half * (units * UNIT) + unit * UNIT, UNIT)
        outs = ((ggate_hbm, UNIT), (gup_hbm, UNIT)) if lane == 0 else ((gdown_hbm, count * UNIT),)
        copies = [
            pltpu.make_async_copy(
                stage.at[k % 2, :, pl.ds(which * UNIT, wide)],
                hbm.at[:, pl.ds(at, wide)],
                stage_sem.at[k % 2, which],
            )
            for which, (hbm, wide) in enumerate(outs)
        ]
        for copy in copies:
            copy.start()
        pending.append(copies)

    pairs = [(low, min(low + 2, units)) for low in range(0, units, 2)]
    items = [(k, low, high - low, 2 * UNIT, UNIT) for k, (low, high) in enumerate(pairs)]
    items += [(len(pairs) + u, u, 1, 0, 2 * UNIT) for u in range(units)]
    count = len(items)
    queue.add(0, partial(columns.reduce_step, items[0], 0))
    for k in range(count + 2):
        if k + 1 < count:
            queue.add(k + 1, partial(columns.reduce_step, items[k + 1], 0))
        if k < count:
            for step in range(1, 4):
                queue.add(k, partial(columns.reduce_step, items[k], step))
        if k > 1:
            queue.add(k - 2, partial(finish, items[k - 2], False))
            queue.add(k - 2, partial(finish, items[k - 2], True))
    ready = set()
    def tall(ref, lanes):
        return ref[:, :, lanes].reshape(8 * rows, lanes.stop - lanes.start)

    def down_grad(low, high):
        value = dot_tn(df[...].reshape(8 * rows, width), tall(hid_buf, slice(low * UNIT, high * UNIT)))
        value = value.astype(BF)
        for u in range(low, high):
            piece = value[:, (u - low) * UNIT : (u - low + 1) * UNIT]
            ffn[u, :, :, 2 * UNIT :] = piece.reshape(n, depth, UNIT)
        ready.add(low // 2)

    def back_block(j, _):
        octet.gather_before(1, df, j)
        b = octet.block(*octet.arrival(j))
        for low, high in pairs:
            lanes = slice(low * UNIT, high * UNIT)
            grad = dot_nn(df[b], across_units(2, low, high))
            gate, up = gate_buf[b, :, lanes].astype(F32), up_buf[b, :, lanes].astype(F32)
            act, bent = gelu_parts(gate)
            slope = 0.5 * (1.0 + bent) + 0.5 * gate * (1.0 - bent * bent) * ROOT * (
                1.0 + 3.0 * CUBIC * gate * gate
            )
            gate_buf[b, :, lanes] = (grad * up * slope).astype(BF)
            up_buf[b, :, lanes] = (grad * act).astype(BF)
        return 0

    lax.fori_loop(0, 8, back_block, 0)
    octet.gather_sends_done(1, df)

    def down_grads(some):
        for low, high in some:
            down_grad(low, high)
            queue.run(PACE[0], ready)

    down_grads(pairs[: WORK[3]])

    def back_part(i, _):
        b = octet.block(3 - i // 2, 1 - i % 2)
        grown = dot_nt(gate_buf[b], across_units(0)) + dot_nt(up_buf[b], across_units(1))
        part[b] = grown.astype(BF)
        octet.reduce_after(1, i)
        return 0

    def gate_grad(u, _):
        lanes = pl.ds(pl.multiple_of(u * UNIT, UNIT), UNIT)
        both = jnp.concatenate(
            [ref[:, :, lanes].reshape(8 * rows, UNIT) for ref in (gate_buf, up_buf)], axis=1
        )
        value = dot_tn(nm[...].reshape(8 * rows, width), both)
        ffn[u, :, :, : 2 * UNIT] = value.astype(BF).reshape(n, depth, 2 * UNIT)
        return 0

    done = [0]

    def do_work(count):
        low, done[0] = done[0], min(units, done[0] + count)
        if low < done[0]:
            lax.fori_loop(low, done[0], gate_grad, 0)
            ready.update(range(len(pairs) + low, len(pairs) + done[0]))
            queue.run(PACE[1] * (done[0] - low), ready)

    lax.fori_loop(0, 4, back_part, 0)
    queue.run(2 * PACE[0], ready)
    lax.fori_loop(4, 8, back_part, 0)
    down_grads(pairs[WORK[3] :])
    do_work(WORK[0])
    do_work(WORK[1])
    queue.run(PACE[2], ready)
    octet.reduce_end(1)

    def after_ffn(i, carry):
        at = at_rows(i)
        grad, pre_part = rms_back(res_s[at], gains[2:3, :], total_ffn(at))
        grad = cot_ref[at].astype(F32) + grad
        res_s[at] = grad
        grad, attn_part = rms_back(proj_s[at].astype(F32), gains[1:2, :], grad)
        dp_buf[me, at] = grad.astype(BF)
        return carry[0] + fold(pre_part), carry[1] + fold(attn_part)

    zero = jnp.zeros(eight, F32)
    pre_sum, attn_sum = lax.fori_loop(0, per, after_ffn, (zero, zero))
    gsum[2:3, :] = jnp.sum(pre_sum, axis=0, keepdims=True)
    gsum[1:2, :] = jnp.sum(attn_sum, axis=0, keepdims=True)
    quad.gather_start(1, dp_buf)
    do_work(WORK[2])
    queue.run(PACE[3], ready)
    quad.gather_relay(1, dp_buf)
    do_work(units)
    queue.run(PACE[4], ready)
    quad.gather_end(1, dp_buf)

    d_q, d_k, d_v = (gate_buf.at[pl.ds(0, 4), :, pl.ds(k * HD, HD)] for k in range(3))
    datt = up_buf.at[pl.ds(0, 4), :, pl.ds(0, HD)]

    def attn_grad(low, left, right):
        value = dot_tn(left.reshape(4 * rows, width), right.reshape(4 * rows, HD))
        attn[:, :, low : low + HD] = value.astype(BF).reshape(n, width // n, HD)

    def ring_hop(hop, *some):
        for p in some:
            for way in range(2):
                back.reduce_step(p, way, hop)

    ready.add(-1)
    def back_out(r, _):
        datt[r] = dot_nn(dp_buf[r], attn_cols(0, HD)).astype(BF)
        return 0

    lax.fori_loop(0, 4, back_out, 0)
    attn_grad(0, dp_buf[...], att[...])
    ring_hop(1, 0)
    queue.run(PACE[5], ready)
    gqk[...] = jnp.zeros_like(gqk)

    def unrope(grad, projection, gain_vec, r, row):
        low, high = grad[:, : HD // 2], grad[:, HD // 2 :]
        cosine, sine = cos_s[r], sin_s[r]
        grad = jnp.concatenate([low * cosine + high * sine, high * cosine - low * sine], axis=1)
        grad, gain_part = rms_back(projection, gain_vec, grad)
        gqk[row : row + 1, :] += jnp.sum(gain_part, axis=0, keepdims=True)
        return grad.astype(BF)

    def back_tile(tile, _):
        two = pl.ds(2 * tile, 2)
        keys = kr[two].reshape(SEGMAX, HD)
        values = vb[two].reshape(SEGMAX, HD)
        d_key = jnp.zeros((SEGMAX, HD), F32)
        d_value = jnp.zeros((SEGMAX, HD), F32)
        for half in range(2):
            r = 2 * tile + half
            d_att = datt[r]
            weights = probs[r]
            d_value = d_value + dot_tn(weights, d_att)
            d_probs = dot_nt(d_att, values)
            weights = weights.astype(F32)
            delta = jnp.sum(weights * d_probs, axis=1, keepdims=True)
            d_scores = (weights * (d_probs - delta) * SCALE).astype(BF)
            d_key = d_key + dot_tn(d_scores, qr[r])
            d_query = dot_nn(d_scores, keys)
            d_q[r] = unrope(d_query, q_proj[r].astype(F32), gq_ref[...], r, 4)
        for half in range(2):
            r = 2 * tile + half
            cut = slice(half * quarter, (half + 1) * quarter)
            d_k[r] = unrope(d_key[cut], k_proj[r].astype(F32), gk_ref[...], r, 5)
            d_v[r] = d_value[cut].astype(BF)
        return 0

    lax.fori_loop(0, N_TILES, back_tile, 0)
    queue.run(PACE[5], ready)

    def back_in(r, _):
        grown = dot_nt(d_q[r], attn_cols(HD, 2 * HD))
        grown = grown + dot_nt(d_k[r], attn_cols(2 * HD, 3 * HD))
        grown = grown + dot_nt(d_v[r], attn_cols(3 * HD, 4 * HD))
        part[r] = grown.astype(BF)
        return 0

    lax.fori_loop(0, 4, back_in, 0)
    quad.reduce_start(1)
    queue.run(PACE[5], ready)

    def three_grads(k, _):
        grad = gate_buf[0:4, :, pl.ds(pl.multiple_of(k * HD, HD), HD)]
        value = dot_tn(xa[...].reshape(4 * rows, width), grad.reshape(4 * rows, HD))
        low = pl.multiple_of((k + 1) * HD, HD)
        attn[:, :, pl.ds(low, HD)] = value.astype(BF).reshape(n, depth, HD)
        return 0

    lax.fori_loop(0, 3, three_grads, 0)
    def input_gain(i, carry):
        b, at = i // per, pl.ds(pl.multiple_of(i % per * sub, sub), sub)
        return carry + fold(part[b, at].astype(F32) * xa[b, at].astype(F32))

    gain_sum = lax.fori_loop(0, 4 * per, input_gain, zero)
    gsum[0:1, :] = jnp.sum(gain_sum, axis=0, keepdims=True) / gains[0:1, :]
    gsum[4:8, :] = jnp.zeros((4, width), F32)
    long = jnp.concatenate([gsum[...], jnp.zeros((120, width), F32)], axis=0)
    long = jnp.transpose(long).reshape(n, width // n, 128)
    short = jnp.concatenate([gqk[...], jnp.zeros((120, HD), F32)], axis=0)
    short = jnp.transpose(short).reshape(n, HD // n, 128)
    attn[:, :, 4 * HD : 4 * HD + 128] = long.astype(BF)
    attn[:, : HD // n, 4 * HD : 4 * HD + 128] = (long[:, : HD // n] + short).astype(BF)

    ring_hop(1, 2, 3, 1)
    quad.reduce_relay(1)
    ring_hop(2, 0)
    queue.run(PACE[6], ready)
    for hop in range(2, n // 2 + 1):
        ring_hop(hop, 2, 3, 1)
        if hop < n // 2:
            ring_hop(hop + 1, 0)
        queue.run(PACE[7], ready)
    kvg[0, :, : 2 * HD] = back.reduce_end(2).astype(BF)
    kvg[0, :, 2 * HD :] = back.reduce_end(3).astype(BF)

    def swap(k):
        return pltpu.make_async_remote_copy(
            kvg.at[k],
            kvg_land.at[k],
            kv_send.at[k],
            kv_recv.at[k],
            device_id={"tensor": (quad.twin, quad.across)[k]},
            device_id_type=MESH,
        )

    swap(0).start()
    quad.reduce_end(1)
    put_out.wait()

    def after_attn(i, _):
        at = at_rows(i)
        grad, _ = rms_back(x_ref[at].astype(F32), gains[0:1, :], total(at))
        dx_ref[at] = (res_s[at] + grad).astype(BF)
        return 0

    swap(0).wait()
    kvg[1] = (kvg[0].astype(F32) + kvg_land[0].astype(F32)).astype(BF)
    swap(1).start()
    lax.fori_loop(0, per, after_attn, 0)
    queue.run(10**6)
    for p in range(2):
        sums_ref[:, p * HD : (p + 1) * HD] = back.reduce_end(p)
    swap(1).wait()
    sums_ref[:, 2 * HD :] = kvg[1].astype(F32) + kvg_land[1].astype(F32)
    for p in range(len(parts)):
        back.reduce_sends_done(p)
    for item in items:
        columns.reduce_sends_done(item)
    for copies in pending[-2:]:
        for copy in copies:
            copy.wait()


AHEAD = (14, 0, 0, 2, 3, 3, 0, 6, 5, 4, 2)
PACE = (2, 2, 6, 6, 4, 3, 2, 3)
WORK = (2, 3, 2, 2)
EARLY = 3
UNIT = 128
N_TILES = 2


def run_layer(n, x, cot, segments, small, attn_weights, ffn_pack):
    rows, width = x.shape
    both, depth, cols = ffn_pack.shape
    units = both // 2
    tokens = segments.shape[0]
    wide = 4 * HD + 128
    parts = 4
    vmem, dma = pltpu.VMEM, pltpu.SemaphoreType.DMA
    grown = both * UNIT
    return pl.pallas_call(
        partial(layer_kernel, n),
        out_shape=(
            jax.ShapeDtypeStruct((rows, width), BF),
            jax.ShapeDtypeStruct((depth, wide), F32),
            jax.ShapeDtypeStruct((rows, width), BF),
            jax.ShapeDtypeStruct((depth, grown), F32),
            jax.ShapeDtypeStruct((depth, grown), F32),
            jax.ShapeDtypeStruct((depth, grown), F32),
        ),
        in_specs=vmem_specs(4) + any_specs(6),
        out_specs=vmem_specs(2) + any_specs(4),
        scratch_shapes=[
            vmem((n, depth, wide), BF),
            vmem((units, n, depth, cols), BF),
            vmem((units, depth, cols), BF),
            vmem((n - 1, depth, wide), BF),
            vmem((units, 8, depth, cols), BF),
            vmem((8, rows, units * UNIT), BF),
            vmem((8, rows, units * UNIT), BF),
            vmem((8, rows, units * UNIT), BF),
            vmem((8, rows, width), BF),
            vmem((4, rows, width), BF),
            vmem((2, rows, width), BF),
            vmem((2, rows // 2, width), BF),
            vmem((4, rows, width), BF),
            vmem((8, rows, width), BF),
            vmem((8, rows, width), BF),
            vmem((4, rows, width), BF),
            vmem((rows, width), BF),
            vmem((rows, width), F32),
            vmem((8, width), F32),
            vmem((8, width), F32),
            vmem((8, HD), F32),
            vmem((4, rows, HD), BF),
            vmem((4, rows, HD), BF),
            vmem((4, rows, HD), BF),
            vmem((4, rows, HD), BF),
            vmem((4, rows, HD), BF),
            vmem((4, rows, HD), BF),
            vmem((4, rows, SEGMAX), BF),
            vmem((4, rows, HD // 2), F32),
            vmem((4, rows, HD // 2), F32),
            vmem((2, depth, 2 * UNIT), F32),
            vmem((2, depth, wide - 2 * HD), BF),
            vmem((2, depth, wide - 2 * HD), BF),
            dma((7,)),
            dma((2, 3)),
            dma((parts, 2, n // 2)),
            dma((parts, 2, n // 2)),
            dma((parts, 2, n // 2)),
            dma((parts, 2, n // 2)),
            dma((units, 8)),
            dma((units, 8)),
            dma((units + (units + 1) // 2, 8)),
            dma((units + (units + 1) // 2, 8)),
            dma((2, 8)),
            dma((2, 8)),
            dma((2, 8)),
            dma((2, 8)),
            dma((3, 3)),
            dma((3, 3)),
            dma((2, 3)),
            dma((2, 3)),
            dma((2,)),
            dma((2,)),
        ],
        compiler_params=pltpu.CompilerParams(
            collective_id=2, has_side_effects=True, vmem_limit_bytes=67043328
        ),
    )(
        x,
        cot,
        segments.reshape(N_TILES, SEGMAX),
        small,
        *attn_weights,
        ffn_pack,
    )


def fused_local(
    inputs, segments, w_query, w_key, w_value, w_out, g_in, g_attn, g_query, g_key,
    w_gate, w_up, w_down, g_pre, g_post, cotangent,
):
    n = lax.axis_size("dp")
    depth = w_query.shape[0]
    width = w_gate.shape[1]
    lane = lax.broadcasted_iota(jnp.int32, (depth, 128), 1)
    gains = jnp.zeros((depth, 128), BF)
    for k, gain in enumerate((g_in, g_attn, g_pre, g_post)):
        gains = jnp.where(lane == k, gain[:, None], gains)
    exponent = -2.0 * (jnp.arange(HD) % (HD // 2)).astype(F32) / HD
    freq = jnp.power(jnp.float32(THETA), exponent)
    line = lax.broadcasted_iota(jnp.int32, (3, HD), 0)
    small = jnp.where(line == 0, g_query.astype(F32)[None, :], freq[None, :])
    small = jnp.where(line == 1, g_key.astype(F32)[None, :], small)
    ffn_pack = pack_ffn(w_gate, w_up, w_down.T, depth, UNIT)
    d_inputs, sums, output, g_gate, g_up, g_down = run_layer(
        n, inputs, cotangent, segments, small, (w_out.T, w_query, w_key, w_value, gains), ffn_pack
    )
    spot = lax.axis_index("tensor")
    part = depth // 4
    mine = lax.dynamic_slice_in_dim(sums[:, 2 * HD :], spot * part, part, 0)
    small = HD // n // 4
    few = lax.dynamic_slice_in_dim(sums[:, 4 * HD :], spot * small, small, 0)
    return (
        output,
        d_inputs,
        sums[:, HD : 2 * HD],
        mine[:, :HD],
        mine[:, HD : 2 * HD],
        sums[:, :HD].T,
        mine[:, 2 * HD],
        mine[:, 2 * HD + 1],
        few[:, 4],
        few[:, 5],
        g_gate[:, :width],
        g_up[:, :width],
        g_down[:, :width].T,
        mine[:, 2 * HD + 2],
        mine[:, 2 * HD + 3],
    )


def fits(mesh, depth, tokens, rows):
    return mesh.shape["dp"] == 8 and depth % 16 == 0 and mesh.shape["tensor"] == 4 and tokens == 2 * SEGMAX


def layer(mesh):
    def body(*args):
        inputs, segments, w_query = args[0], args[1], args[2]
        if fits(mesh, w_query.shape[0], segments.shape[0], inputs.shape[0]):
            return fused_local(*args)
        return local(*args)

    return body


def solution(mesh):
    return jax.shard_map(
        layer(mesh),
        mesh=mesh,
        in_specs=(
            P(("dp", "tensor"), None),
            P("dp"),
            P("dp", "tensor"),
            P("dp", None),
            P("dp", None),
            P("tensor", "dp"),
            P("dp"),
            P("dp"),
            P(),
            P(),
            P("dp", "tensor"),
            P("dp", "tensor"),
            P("tensor", "dp"),
            P("dp"),
            P("dp"),
            P(("dp", "tensor"), None),
        ),
        out_specs=(
            P(("dp", "tensor"), None),
            P(("dp", "tensor"), None),
            P("dp", "tensor"),
            P(("dp", "tensor"), None),
            P(("dp", "tensor"), None),
            P("tensor", "dp"),
            P(("dp", "tensor")),
            P(("dp", "tensor")),
            P(("dp", "tensor")),
            P(("dp", "tensor")),
            P("dp", "tensor"),
            P("dp", "tensor"),
            P("tensor", "dp"),
            P(("dp", "tensor")),
            P(("dp", "tensor")),
        ),
        check_vma=False,
    )
```
